32 devices in a mesh: gx: 2 (over y), gy: 4 (over z), gz: 4 (over x, core).
Axes of the slice: x: 2, y: 2, z: 4, core: 2. Of those that a mesh axis runs over, the one named last changes fastest.
Arguments:
- density: float32 [64, 64, 512], P('gx', 'gy', 'gz'), may hold values from -8 to 8
Outputs:
- potential: float32 [64, 64, 512], P('gx', 'gy', 'gz')
The draws below stay inside these ranges and needn't reach their ends.
All inputs are finite; a program needn't handle non-finite values.
Results may differ from the reference program's by a relative error of at most 0.00002.
Values sent between devices are 32-bit elements; how exact they have to be, the bound alone decides.
No kernel may reach another device: no remote copies, remote signals or barrier semaphores. Data moves between devices by JAX's collectives and lax.ppermute only.
A program may use at most 128 MiB of HBM per device.

```python
import jax
import jax.numpy as jnp
from jax import lax

LEVELS = 7
CSWEEPS = 4
NX = 64
NY = 64
NZ = 512


def rough_field(key, shape):
    return jnp.clip(jax.random.normal(key, shape, jnp.float32), -4.0, 4.0)


def draw_density(key, part):
    first_key = jax.random.fold_in(key, 21)
    second_key = jax.random.fold_in(key, 22)
    shape = (NX, NY, NZ)
    first = rough_field(first_key, shape)
    second = rough_field(second_key, shape)
    beside_all = jnp.zeros(shape, jnp.float32)
    for which in range(3):
        beside_all = beside_all + jnp.roll(first, 1, which) + jnp.roll(first, -1, which)
    sharp = 6.0 * first - beside_all
    total = 0.4 * sharp + 0.4 * second
    return jnp.clip(total, -8.0, 8.0).astype(jnp.float32)


def setup_inputs(seed: int = 0) -> dict:
    key_of = jax.random.split(jax.random.key(seed), 2)
    density = draw_density(jax.random.fold_in(key_of[1], 71), 0)
    return dict(density=density)


rsd_beta = 0.5
centre = 4.0 + 2.0 * (1.0 + rsd_beta)


def stencil_sum(padded):
    plane = padded[2:, 1:-1, 1:-1] + padded[:-2, 1:-1, 1:-1] + padded[1:-1, 2:, 1:-1] + padded[1:-1, :-2, 1:-1]
    sight = padded[1:-1, 1:-1, 2:] + padded[1:-1, 1:-1, :-2]
    return plane + (1.0 + rsd_beta) * sight


def parity_of(shape):
    total = lax.broadcasted_iota(jnp.int32, shape, 0) + lax.broadcasted_iota(jnp.int32, shape, 1)
    total = total + lax.broadcasted_iota(jnp.int32, shape, 2)
    return total % 2


def half_sweep(field, source, scale, chosen):
    update = (source / scale + stencil_sum(jnp.pad(field, 1))) / centre
    return jnp.where(chosen, update, field)


def full_sweep(field, source, scale, parity):
    field = half_sweep(field, source, scale, parity == 0)
    return half_sweep(field, source, scale, parity == 1)


def restrict(residue):
    shape = residue.shape
    blocks = residue.reshape(shape[0] // 2, 2, shape[1] // 2, 2, shape[2] // 2, 2)
    return jnp.mean(blocks, axis=(1, 3, 5))


def prolong(coarse):
    return jnp.repeat(jnp.repeat(jnp.repeat(coarse, 2, 0), 2, 1), 2, 2)


def local_cycle(source, level):
    scale = 0.25 ** level
    parity = parity_of(source.shape)
    field = jnp.zeros_like(source)
    if level == LEVELS - 1:
        for number in range(CSWEEPS):
            field = full_sweep(field, source, scale, parity)
        return field
    for number in range(2):
        field = full_sweep(field, source, scale, parity)
    residue = source - scale * (centre * field - stencil_sum(jnp.pad(field, 1)))
    field = field + prolong(local_cycle(restrict(residue), level + 1))
    for number in range(2):
        field = full_sweep(field, source, scale, parity)
    return field


def reference(density):
    return local_cycle(density, 0)
```

```python
import functools

import jax
import jax.numpy as jnp
from jax import lax
from jax.experimental import pallas as pl
from jax.experimental.pallas import tpu as pltpu
from jax.sharding import PartitionSpec as P

LEVELS = 7
CSWEEPS = 4


rsd_beta = 0.5
centre = 4.0 + 2.0 * (1.0 + rsd_beta)


def extended_2(value, sides, width):
    for axis, dim in sides:
        count, length = (lax.axis_size(axis), value.shape[dim])
        up = [(i, (i + 1) % count) for i in range(count - 1)]
        down = [(j, i) for i, j in up]
        last = lax.slice_in_dim(value, length - width, length, axis=dim)
        leading = lax.slice_in_dim(value, 0, width, axis=dim)
        before = lax.ppermute(last, axis, up)
        after = lax.ppermute(leading, axis, down)
        value = jnp.concatenate([before, value, after], axis=dim)
    return value


def stencil_sum(padded):
    plane = (
        padded[2:, 1:-1, 1:-1]
        + padded[:-2, 1:-1, 1:-1]
        + padded[1:-1, 2:, 1:-1]
        + padded[1:-1, :-2, 1:-1]
    )
    sight = padded[1:-1, 1:-1, 2:] + padded[1:-1, 1:-1, :-2]
    return plane + (1.0 + rsd_beta) * sight


def grid_index(shape, starts):
    return [lax.broadcasted_iota(jnp.int32, shape, which) + starts[which] for which in range(3)]


def parity_of(shape, starts):
    position = grid_index(shape, starts)
    return (position[0] + position[1] + position[2] + 6) % 2


def inside_grid(shape, starts, whole):
    position = grid_index(shape, starts)
    keep = (position[0] >= 0) & (position[0] < whole[0])
    for which in (1, 2):
        keep = keep & (position[which] >= 0) & (position[which] < whole[which])
    return keep


def half_sweep(field, source, scale, chosen):
    update = (source / scale + stencil_sum(jnp.pad(field, 1))) / centre
    return jnp.where(chosen, update, field)


def full_sweep(field, source, scale, parity):
    field = half_sweep(field, source, scale, parity == 0)
    return half_sweep(field, source, scale, parity == 1)


def restrict(residue):
    shape = residue.shape
    blocks = residue.reshape(shape[0] // 2, 2, shape[1] // 2, 2, shape[2] // 2, 2)
    return jnp.mean(blocks, axis=(1, 3, 5))


def prolong(coarse):
    return jnp.repeat(jnp.repeat(jnp.repeat(coarse, 2, 0), 2, 1), 2, 2)


def local_cycle(source, level):
    scale = 0.25**level
    parity = parity_of(source.shape, (0, 0, 0))
    field = jnp.zeros_like(source)
    if level == LEVELS - 1:
        for number in range(CSWEEPS):
            field = full_sweep(field, source, scale, parity)
        return field
    for number in range(2):
        field = full_sweep(field, source, scale, parity)
    residue = source - scale * (centre * field - stencil_sum(jnp.pad(field, 1)))
    field = field + prolong(local_cycle(restrict(residue), level + 1))
    for number in range(2):
        field = full_sweep(field, source, scale, parity)
    return field


def faces(field):
    return extended_2(field, (("gx", 0), ("gy", 1), ("gz", 2)), 1)


def wide(field):
    return extended_2(field, (("gx", 0), ("gy", 1), ("gz", 2)), 2)


def block_starts(shape, margin):
    return (
        lax.axis_index("gx") * shape[0] - margin,
        lax.axis_index("gy") * shape[1] - margin,
        lax.axis_index("gz") * shape[2] - margin,
    )


def padded_half(padded, source, scale, chosen):
    field = padded[1:-1, 1:-1, 1:-1]
    update = (source / scale + stencil_sum(padded)) / centre
    return jnp.where(chosen, update, field)


def wide_sweep(extended, wide_source, scale, red_wide, source, black):
    update = (wide_source / scale + stencil_sum(jnp.pad(extended, 1))) / centre
    extended = jnp.where(red_wide, update, extended)
    return padded_half(extended[1:-1, 1:-1, 1:-1], source, scale, black)


def coarse_level(source, level):
    shape = source.shape
    stack = lax.all_gather(source[None], ("gx", "gy", "gz"), axis=0, tiled=True)
    count_x, count_y, count_z = (lax.axis_size("gx"), lax.axis_size("gy"), lax.axis_size("gz"))
    whole = stack.reshape(count_x, count_y, count_z, shape[0], shape[1], shape[2])
    whole = whole.transpose(0, 3, 1, 4, 2, 5).reshape(
        count_x * shape[0], count_y * shape[1], count_z * shape[2]
    )
    solved = local_cycle(whole, level)
    starts = block_starts(shape, 0)
    return lax.dynamic_slice(solved, starts, shape)


def shared_cycle(source, level, top):
    if level == top:
        return coarse_level(source, level)
    scale = 0.25**level
    shape = source.shape
    whole = (
        shape[0] * lax.axis_size("gx"),
        shape[1] * lax.axis_size("gy"),
        shape[2] * lax.axis_size("gz"),
    )
    parity = parity_of(shape, block_starts(shape, 0))
    black = parity == 1
    wide_shape = (shape[0] + 4, shape[1] + 4, shape[2] + 4)
    wide_starts = block_starts(shape, 2)
    red_wide = (parity_of(wide_shape, wide_starts) == 0) & inside_grid(
        wide_shape, wide_starts, whole
    )
    wide_source = wide(source)
    field = wide_sweep(
        jnp.zeros(wide_shape, jnp.float32), wide_source, scale, red_wide, source, black
    )
    field = wide_sweep(wide(field), wide_source, scale, red_wide, source, black)
    residue = source - scale * (centre * field - stencil_sum(faces(field)))
    field = field + prolong(shared_cycle(restrict(residue), level + 1, top))
    for number in range(2):
        field = wide_sweep(wide(field), wide_source, scale, red_wide, source, black)
    return field


def pairs(count, first):
    swaps = []
    for i in range(first, count - 1, 2):
        swaps += [(i, i + 1), (i + 1, i)]
    return swaps


def flips(count, bit):
    return [(i, i ^ bit) for i in range(count)]


def lanes_of(shape):
    return lax.broadcasted_iota(jnp.int32, shape, len(shape) - 1)


def rows_of(shape):
    return lax.broadcasted_iota(jnp.int32, shape, len(shape) - 2)


def odd_of(shape):
    return ((lanes_of(shape) + rows_of(shape)) & 1) == 1


def beside(value, closed):
    rows, lanes = value.shape
    up = pltpu.roll(value, 1, 0)
    down = pltpu.roll(value, rows - 1, 0)
    left = pltpu.roll(value, 1, 1)
    right = pltpu.roll(value, lanes - 1, 1)
    if closed:
        row, lane = rows_of(value.shape), lanes_of(value.shape)
        up = jnp.where(row == 0, 0.0, up)
        down = jnp.where(row == rows - 1, 0.0, down)
        left = jnp.where(lane == 0, 0.0, left)
        right = jnp.where(lane == lanes - 1, 0.0, right)
    return value + (up + down) + (1.0 + rsd_beta) * (left + right)


def red_sum(black, at, odd, closed, before, after):
    return beside(black[at], closed) + jnp.where(odd, after(black, at), before(black, at))


def black_sum(red, at, odd, closed, before, after):
    return beside(red[at], closed) + jnp.where(odd, before(red, at), after(red, at))


def open_before(ref, at):
    return ref[at - 1] if at > 0 else 0.0


def open_after(ref, at):
    return ref[at + 1] if at + 1 < ref.shape[0] else 0.0


def ring_steps(count, own, at_low, at_high):
    def before(ref, at):
        value = ref[(at - 1) % count]
        return jnp.where(at_low, 0.0, value) if at == 0 else value

    def after(ref, at):
        value = ref[(at + 1) % count]
        return jnp.where(at_high, 0.0, value) if at == own - 1 else value

    return before, after


def exact_dot(a, b):
    return jnp.dot(a, b, precision=lax.Precision.HIGHEST, preferred_element_type=jnp.float32)


def pack_kernel(halo, own_ref, xh_ref, ya_ref, yb_ref, za_ref, zb_ref):
    even_y = lax.axis_index("gy") % 2 == 0
    even_z = lax.axis_index("gz") % 2 == 0
    nx, ny, nz = own_ref.shape
    groups = nz // halo
    shape = (ny + 2 * halo, nz)
    group = lanes_of(shape) // halo
    for j in range(za_ref.shape[0]):
        last = jnp.zeros(shape, jnp.float32)
        first = jnp.zeros(shape, jnp.float32)
        for k in range(groups):
            at = j * groups + k
            if at >= nx + halo:
                break
            plane = block_plane(at, nx, own_ref, xh_ref, ya_ref, yb_ref, even_y)
            last = jnp.where(group == k, pltpu.roll(plane, (halo * k + halo) % nz, 1), last)
            first = jnp.where(group == k, pltpu.roll(plane, halo * k, 1), first)
        za_ref[j] = jnp.where(even_z, last, first)
        zb_ref[j] = jnp.where(even_z, first, last)


def block_plane(at, nx, own_ref, xh_ref, ya_ref, yb_ref, even_y):
    a, b = ya_ref[at], yb_ref[at]
    middle = own_ref[at] if at < nx else xh_ref[at - nx]
    low = jnp.where(even_y, b, a)
    high = jnp.where(even_y, a, b)
    return jnp.concatenate([low, middle, high], axis=0)


def block_mask(own, halo, lanes):
    ny, nz = own
    shape = (ny + 2 * halo, lanes)
    row = rows_of(shape) - halo + lax.axis_index("gy") * ny
    lane = lanes_of(shape)
    lane = jnp.where(lane < lanes - halo, lane, lane - lanes) + lax.axis_index("gz") * nz
    inside = (row >= 0) & (row < ny * lax.axis_size("gy"))
    inside = inside & (lane >= 0) & (lane < nz * lax.axis_size("gz"))
    return jnp.where(inside, 1.0 / centre, 0.0)


def pre_kernel(
    halo, own_ref, xh_ref, ya_ref, yb_ref, za_ref, zb_ref,
    gr_ref, gb_ref, black_ref, send_ref,
    fr_ref, fb_ref, red_ref, rest_ref,
):
    even_y = lax.axis_index("gy") % 2 == 0
    even_z = lax.axis_index("gz") % 2 == 0
    nx, ny, nz = own_ref.shape
    count, rows, lanes = black_ref.shape
    own = nx // 2
    groups = nz // halo
    odd = odd_of((rows, lanes))
    mask = block_mask((ny, nz), halo, lanes)
    lane = lanes_of((rows, nz))
    low, high = lane < halo, lane >= nz - halo

    def plane(at):
        j, k = at // groups, at % groups
        a, b = za_ref[j], zb_ref[j]
        left = jnp.where(even_z, b, a)
        right = jnp.where(even_z, a, b)
        right = pltpu.roll(right, (nz - halo * k) % nz, 1)
        left = pltpu.roll(left, (2 * nz - halo - halo * k) % nz, 1)
        sides = jnp.where(low, right, jnp.where(high, left, 0.0))
        middle = block_plane(at, nx, own_ref, xh_ref, ya_ref, yb_ref, even_y)
        return jnp.concatenate([middle, sides], axis=1)

    for at in range(count):
        p, q = plane(2 * at), plane(2 * at + 1)
        red, black = jnp.where(odd, q, p), jnp.where(odd, p, q)
        fr_ref[at], fb_ref[at] = red, black
        gr_ref[at], gb_ref[at] = mask * red, mask * black
    here = lax.axis_index("gx")
    before, after = ring_steps(count, own, here == 0, here == lax.axis_size("gx") - 1)
    for at in range(count):
        black_ref[at] = gb_ref[at] + mask * black_sum(gr_ref, at, odd, False, before, after)
    for at in range(count):
        red_ref[at] = gr_ref[at] + mask * red_sum(black_ref, at, odd, False, before, after)
    inner = slice(halo, halo + ny)
    for at in range(count):
        total = black_sum(red_ref, at, odd, False, before, after)
        value = gb_ref[at] + mask * total
        black_ref[at] = value
        if at < own:
            left_over = fb_ref[at] + total - centre * value
            rest_ref[at] = left_over[inner, :nz]
    for at in range(own):
        total = red_sum(black_ref, at, odd, False, before, after)
        left_over = fr_ref[at] + total - centre * red_ref[at]
        rest_ref[at] = rest_ref[at] + left_over[inner, :nz]
    half, narrow = ny // 2, nz // 2
    pairs_y = rest_ref[:, pl.ds(0, half, stride=2), :] + rest_ref[:, pl.ds(1, half, stride=2), :]
    weight = jnp.where(
        rows_of((nz, nz)) // 2 == lanes_of((nz, nz)) % narrow, 0.5, 0.0
    )
    coarse = exact_dot(pairs_y.reshape(own * half, nz), weight).reshape(own, half, nz)
    lane = lanes_of((half, nz))
    pick = odd_of((half, nz)) ^ (lane >= narrow)
    for at in range(own // 2):
        packed = jnp.where(pick, coarse[2 * at + 1], coarse[2 * at])
        for member in range(send_ref.shape[0]):
            send_ref[member, at] = packed


def level_shapes(whole):
    shapes = []
    for level in range(1, LEVELS):
        nx, ny, nz = (size >> level for size in whole)
        shapes.append((max(nx // 2, 1), max(ny, 8), max(nz, 128), ny, nz))
    return shapes


LANES = 128


def split_put(ref, at, value):
    for part in range(ref.shape[1]):
        ref[at, part] = value[:, part * LANES : (part + 1) * LANES]


def split_get(ref, at):
    return jnp.concatenate([ref[at, part] for part in range(ref.shape[1])], axis=1)


def twice_put(ref, at, value):
    for part in range(ref.shape[1]):
        column = value[:, part * LANES : (part + 1) * LANES]
        for start in range(2):
            ref[at, part, pl.ds(start, value.shape[0], stride=2), :] = column


def restrict_plane(rest_ref, at, weight):
    half = rest_ref.shape[2] // 2
    columns = [
        rest_ref[at, part, pl.ds(0, half, stride=2), :] + rest_ref[at, part, pl.ds(1, half, stride=2), :]
        for part in range(rest_ref.shape[1])
    ]
    total = jnp.concatenate(columns, axis=1)
    if half < 8:
        total = jnp.concatenate([total, jnp.zeros((8 - half, total.shape[1]), jnp.float32)], axis=0)
    return exact_dot(total, weight)


def solve_kernel(halo, whole, *refs):
    here_ref, flip_ref, next_ref, both_ref, gr_ref, gb_ref, black_ref, out_ref = refs[:8]
    scratch = list(refs[8:])
    shapes = level_shapes(whole)
    fields = [[scratch.pop(0) for _ in range(5)] for _ in shapes]
    full_ref, tall_ref, red_ref, work_ref, wide_ref = scratch
    gx, gy, gz = (lax.axis_index(axis) for axis in ("gx", "gy", "gz"))
    low_bit, high_bit = gz % 2 == 1, gz >= 2

    fr, fb = fields[0][:2]
    members, slots, block_rows, block_lanes = here_ref.shape
    narrow = block_lanes // 2
    count_y = lax.axis_size("gy")
    left = lanes_of((block_rows, block_lanes)) < narrow
    for member in range(members):
        i, j = member // count_y, member % count_y
        rows = slice(j * block_rows, (j + 1) * block_rows)
        for at in range(slots):
            mine = (here_ref[member, at], next_ref[member, at])
            other = (flip_ref[member, at], both_ref[member, at])
            for part in range(2):
                near = high_bit if part else jnp.logical_not(high_bit)
                p = jnp.where(near, mine[0], other[0])
                q = jnp.where(near, mine[1], other[1])
                first = jnp.where(low_bit, q, p)
                second = jnp.where(low_bit, p, q)
                lanes = slice(part * block_lanes, (part + 1) * block_lanes)
                fr[i * slots + at, rows, lanes] = jnp.where(left, first, pltpu.roll(second, narrow, 1))
                fb[i * slots + at, rows, lanes] = jnp.where(left, pltpu.roll(first, narrow, 1), second)

    def mask_of(index):
        _, rows, lanes, ny, nz = shapes[index]
        inside = (rows_of((rows, lanes)) < ny) & (lanes_of((rows, lanes)) < nz)
        return jnp.where(inside, 1.0 / centre, 0.0)

    def sweeps(index, number, start):
        fr, fb, red, black, _ = fields[index]
        count, rows, lanes = red.shape
        odd, mask = odd_of((rows, lanes)), mask_of(index)
        for step in range(number):
            for at in range(count):
                if start and step == 0:
                    red[at] = mask * fr[at]
                else:
                    total = red_sum(black, at, odd, True, open_before, open_after)
                    red[at] = mask * (fr[at] + total)
            for at in range(count):
                total = black_sum(red, at, odd, True, open_before, open_after)
                black[at] = mask * (fb[at] + total)

    def descend(index):
        fr, fb, red, black, rest = fields[index]
        count, rows, lanes = red.shape
        odd = odd_of((rows, lanes))
        for at in range(count):
            first = fb[at] + black_sum(red, at, odd, True, open_before, open_after)
            second = fr[at] + red_sum(black, at, odd, True, open_before, open_after)
            split_put(rest, at, (first - centre * black[at]) + (second - centre * red[at]))
        _, next_rows, next_lanes, _, _ = shapes[index + 1]
        weight = jnp.where(
            rows_of((lanes, next_lanes)) // 2 == lanes_of((lanes, next_lanes)), 0.5, 0.0
        )
        planes = [restrict_plane(rest, at, weight) for at in range(count)]
        next_fr, next_fb = fields[index + 1][:2]
        if count == 1:
            next_fr[0] = planes[0]
            return
        odd = odd_of((next_rows, next_lanes))
        for at in range(count // 2):
            p, q = planes[2 * at], planes[2 * at + 1]
            next_fr[at], next_fb[at] = jnp.where(odd, q, p), jnp.where(odd, p, q)

    def ascend(index):
        _, _, red, black, rest = fields[index]
        count, rows, lanes = red.shape
        _, _, coarse_red, coarse_black, _ = fields[index + 1]
        _, next_rows, next_lanes, _, _ = shapes[index + 1]
        odd = odd_of((next_rows, next_lanes))
        weight = jnp.where(
            rows_of((next_lanes, lanes)) == lanes_of((next_lanes, lanes)) // 2, 1.0, 0.0
        )
        half = rows // 2
        for at in range(count):
            r, b = coarse_red[at // 2], coarse_black[at // 2]
            if count == 1:
                plane = r + b
            else:
                plane = jnp.where(odd, r, b) if at % 2 else jnp.where(odd, b, r)
            twice_put(rest, at, exact_dot(plane, weight)[:half])
            black[at] = black[at] + split_get(rest, at)

    def coarsest(index):
        source, _, red, black, _ = fields[index]
        odd = (lanes_of(source.shape[1:]) & 1) == 1
        mask = mask_of(index)
        mask_red, mask_black = jnp.where(odd, 0.0, mask), jnp.where(odd, mask, 0.0)
        value, dark = source[0], jnp.zeros(source.shape[1:], jnp.float32)

        def along(field):
            return (1.0 + rsd_beta) * (pltpu.roll(field, 1, 1) + pltpu.roll(field, field.shape[1] - 1, 1))

        for step in range(CSWEEPS):
            light = mask_red * (value + along(dark))
            dark = mask_black * (value + along(light))
        red[0], black[0] = light, dark

    last = len(shapes) - 1
    for index in range(last):
        sweeps(index, 2, True)
        descend(index)
    coarsest(last)
    for index in reversed(range(last)):
        ascend(index)
        sweeps(index, 2, False)

    count, rows, lanes = black_ref.shape
    nx, ny, nz = out_ref.shape
    own, reach = nx // 2, halo // 2
    _, _, red1, black1, _ = fields[0]
    _, rows1, lanes1 = red1.shape
    odd1 = odd_of((rows1, lanes1))
    border = jnp.zeros((full_ref.shape[0], 8, lanes1), jnp.float32)
    full_ref[:, :8, :] = border
    full_ref[:, rows1 + 8 :, :] = border
    for at in range(red1.shape[0]):
        r, b = red1[at], black1[at]
        full_ref[2 * at, 8 : rows1 + 8, :] = jnp.where(odd1, b, r)
        full_ref[2 * at + 1, 8 : rows1 + 8, :] = jnp.where(odd1, r, b)
    half, block = rows // 2, ny // 2
    z = lanes_of((lanes1, lanes))
    z = jnp.where(z < lanes - halo, z, z - lanes) + gz * nz
    weight = jnp.where(rows_of((lanes1, lanes)) == lax.shift_right_arithmetic(z, 1), 1.0, 0.0)
    skip = 8 - reach
    for at in range(count):
        if at < own:
            x = gx * own + at
        else:
            x = jnp.where(gx == 0, own, own - (count - own)) + (at - own)
        tall_ref[at] = full_ref[x, pl.ds(pl.multiple_of(gy * block, 8), block + 16), :][skip : skip + half]
    spread = exact_dot(tall_ref[...].reshape(count * half, lanes1), weight).reshape(count, half, lanes)
    for at in range(count):
        twice_put(wide_ref, at, spread[at])
    odd = odd_of((rows, lanes))
    mask = block_mask((ny, nz), halo, lanes)
    for at in range(count):
        work_ref[at] = split_get(wide_ref, at) + black_ref[at]
    before, after = ring_steps(count, own, gx == 0, gx == lax.axis_size("gx") - 1)
    for step in range(2):
        for at in range(count):
            red_ref[at] = gr_ref[at] + mask * red_sum(work_ref, at, odd, False, before, after)
        for at in range(count if step == 0 else own):
            work_ref[at] = gb_ref[at] + mask * black_sum(red_ref, at, odd, False, before, after)
    inner = slice(halo, halo + ny)
    odd = odd_of((ny, nz))
    for at in range(own):
        r, b = red_ref[at, inner, :nz], work_ref[at, inner, :nz]
        out_ref[2 * at] = jnp.where(odd, b, r)
        out_ref[2 * at + 1] = jnp.where(odd, r, b)


def vmem(number):
    return [pl.BlockSpec(memory_space=pltpu.VMEM)] * number


def struct(*shape):
    return jax.ShapeDtypeStruct(shape, jnp.float32)


def scratch(*shape):
    return pltpu.VMEM(shape, jnp.float32)


HALO = 8


def block_cycle(density):
    halo = HALO
    nx, ny, nz = density.shape
    count_x, count_y, count_z = (lax.axis_size(axis) for axis in ("gx", "gy", "gz"))
    whole = (nx * count_x, ny * count_y, nz * count_z)
    gx, gy = lax.axis_index("gx"), lax.axis_index("gy")
    face = lax.dynamic_slice_in_dim(density, jnp.where(gx == 0, nx - halo, 0), halo, 0)
    side = lax.ppermute(face, "gx", flips(count_x, 1))
    tall = jnp.concatenate([density, side], axis=0)
    even = gy % 2 == 0
    ya = lax.dynamic_slice_in_dim(tall, jnp.where(even, ny - halo, 0), halo, 1)
    yb = lax.dynamic_slice_in_dim(tall, jnp.where(even, 0, ny - halo), halo, 1)
    ya = lax.ppermute(ya, "gy", pairs(count_y, 0))
    yb = lax.ppermute(yb, "gy", pairs(count_y, 1))
    rows, lanes = ny + 2 * halo, 2 * nz
    planes = nx + halo
    packs = -(-planes * halo // nz)
    params = pltpu.CompilerParams(vmem_limit_bytes=56 * 1024 * 1024)
    za, zb = pl.pallas_call(
        functools.partial(pack_kernel, halo),
        out_shape=[struct(packs, rows, nz)] * 2,
        in_specs=vmem(4), out_specs=vmem(2), compiler_params=params,
    )(density, side, ya, yb)
    za = lax.ppermute(za, "gz", pairs(count_z, 0))
    zb = lax.ppermute(zb, "gz", pairs(count_z, 1) + [(0, count_z - 1), (count_z - 1, 0)])
    members = count_x * count_y
    slots = (planes // 2, rows, lanes)
    gr, gb, black, send = pl.pallas_call(
        functools.partial(pre_kernel, halo),
        out_shape=[struct(*slots)] * 3 + [struct(members, nx // 4, ny // 2, nz)],
        in_specs=vmem(6), out_specs=vmem(4), compiler_params=params,
        scratch_shapes=[scratch(*slots)] * 3 + [scratch(nx // 2, ny, nz)],
    )(density, side, ya, yb, za, zb)
    here = lax.all_to_all(send, ("gx", "gy"), 0, 0, tiled=True)
    flip = lax.ppermute(here, "gz", flips(count_z, 2))
    beside_here = lax.ppermute(here, "gz", flips(count_z, 1))
    beside_flip = lax.ppermute(flip, "gz", flips(count_z, 1))
    room = []
    for count, high, wide_lanes, _, _ in level_shapes(whole):
        room += [scratch(count, high, wide_lanes)] * 4
        room += [scratch(count, wide_lanes // LANES, high, LANES)]
    room += [
        scratch(whole[0] // 2, whole[1] // 2 + 16, whole[2] // 2),
        scratch(planes // 2, rows // 2, whole[2] // 2),
        scratch(*slots),
        scratch(*slots),
        scratch(planes // 2, lanes // LANES, rows, LANES),
    ]
    return pl.pallas_call(
        functools.partial(solve_kernel, halo, whole),
        out_shape=struct(nx, ny, nz),
        in_specs=vmem(7), out_specs=pl.BlockSpec(memory_space=pltpu.VMEM),
        compiler_params=params, scratch_shapes=room,
    )(here, flip, beside_here, beside_flip, gr, gb, black)


def fits_block_cycle(shape):
    nx, ny, nz = shape
    count_x, count_y, count_z = (lax.axis_size(axis) for axis in ("gx", "gy", "gz"))
    whole = (nx * count_x, ny * count_y, nz * count_z)
    coarsest = [size >> (LEVELS - 1) for size in whole]
    exact = all(c << (LEVELS - 1) == size for c, size in zip(coarsest, whole))
    return (
        exact and coarsest[0] == coarsest[1] == 1 and nz == 128 and ny == 16 and nx >= 16
        and nx % 4 == 0 and count_x == 2 and count_z == 4 and count_y % 2 == 0
    )


def on_device(density):
    if fits_block_cycle(density.shape):
        return block_cycle(density)
    top = 4
    return shared_cycle(density, 0, top)


def solution(mesh):
    return jax.shard_map(
        on_device,
        mesh=mesh,
        in_specs=(P("gx", "gy", "gz"),),
        out_specs=P("gx", "gy", "gz"),
        check_vma=False,
    )
```

```python
import functools

import jax
import jax.numpy as jnp
from jax import lax
from jax.experimental import pallas as pl
from jax.experimental.pallas import tpu as pltpu
from jax.sharding import PartitionSpec as P

LEVELS = 7
CSWEEPS = 4


rsd_beta = 0.5
centre = 4.0 + 2.0 * (1.0 + rsd_beta)


def extended_2(value, sides, width):
    for axis, dim in sides:
        count, length = (lax.axis_size(axis), value.shape[dim])
        up = [(i, (i + 1) % count) for i in range(count - 1)]
        down = [(j, i) for i, j in up]
        last = lax.slice_in_dim(value, length - width, length, axis=dim)
        leading = lax.slice_in_dim(value, 0, width, axis=dim)
        before = lax.ppermute(last, axis, up)
        after = lax.ppermute(leading, axis, down)
        value = jnp.concatenate([before, value, after], axis=dim)
    return value


def stencil_sum(padded):
    plane = (
        padded[2:, 1:-1, 1:-1]
        + padded[:-2, 1:-1, 1:-1]
        + padded[1:-1, 2:, 1:-1]
        + padded[1:-1, :-2, 1:-1]
    )
    sight = padded[1:-1, 1:-1, 2:] + padded[1:-1, 1:-1, :-2]
    return plane + (1.0 + rsd_beta) * sight


def grid_index(shape, starts):
    return [lax.broadcasted_iota(jnp.int32, shape, which) + starts[which] for which in range(3)]


def parity_of(shape, starts):
    position = grid_index(shape, starts)
    return (position[0] + position[1] + position[2] + 6) % 2


def inside_grid(shape, starts, whole):
    position = grid_index(shape, starts)
    keep = (position[0] >= 0) & (position[0] < whole[0])
    for which in (1, 2):
        keep = keep & (position[which] >= 0) & (position[which] < whole[which])
    return keep


def half_sweep(field, source, scale, chosen):
    update = (source / scale + stencil_sum(jnp.pad(field, 1))) / centre
    return jnp.where(chosen, update, field)


def full_sweep(field, source, scale, parity):
    field = half_sweep(field, source, scale, parity == 0)
    return half_sweep(field, source, scale, parity == 1)


def restrict(residue):
    shape = residue.shape
    blocks = residue.reshape(shape[0] // 2, 2, shape[1] // 2, 2, shape[2] // 2, 2)
    return jnp.mean(blocks, axis=(1, 3, 5))


def prolong(coarse):
    return jnp.repeat(jnp.repeat(jnp.repeat(coarse, 2, 0), 2, 1), 2, 2)


def local_cycle(source, level):
    scale = 0.25**level
    parity = parity_of(source.shape, (0, 0, 0))
    field = jnp.zeros_like(source)
    if level == LEVELS - 1:
        for number in range(CSWEEPS):
            field = full_sweep(field, source, scale, parity)
        return field
    for number in range(2):
        field = full_sweep(field, source, scale, parity)
    residue = source - scale * (centre * field - stencil_sum(jnp.pad(field, 1)))
    field = field + prolong(local_cycle(restrict(residue), level + 1))
    for number in range(2):
        field = full_sweep(field, source, scale, parity)
    return field


def faces(field):
    return extended_2(field, (("gx", 0), ("gy", 1), ("gz", 2)), 1)


def wide(field):
    return extended_2(field, (("gx", 0), ("gy", 1), ("gz", 2)), 2)


def block_starts(shape, margin):
    return (
        lax.axis_index("gx") * shape[0] - margin,
        lax.axis_index("gy") * shape[1] - margin,
        lax.axis_index("gz") * shape[2] - margin,
    )


def padded_half(padded, source, scale, chosen):
    field = padded[1:-1, 1:-1, 1:-1]
    update = (source / scale + stencil_sum(padded)) / centre
    return jnp.where(chosen, update, field)


def wide_sweep(extended, wide_source, scale, red_wide, source, black):
    update = (wide_source / scale + stencil_sum(jnp.pad(extended, 1))) / centre
    extended = jnp.where(red_wide, update, extended)
    return padded_half(extended[1:-1, 1:-1, 1:-1], source, scale, black)


def coarse_level(source, level):
    shape = source.shape
    stack = lax.all_gather(source[None], ("gx", "gy", "gz"), axis=0, tiled=True)
    count_x, count_y, count_z = (lax.axis_size("gx"), lax.axis_size("gy"), lax.axis_size("gz"))
    whole = stack.reshape(count_x, count_y, count_z, shape[0], shape[1], shape[2])
    whole = whole.transpose(0, 3, 1, 4, 2, 5).reshape(
        count_x * shape[0], count_y * shape[1], count_z * shape[2]
    )
    solved = local_cycle(whole, level)
    starts = block_starts(shape, 0)
    return lax.dynamic_slice(solved, starts, shape)


def shared_cycle(source, level, top):
    if level == top:
        return coarse_level(source, level)
    scale = 0.25**level
    shape = source.shape
    whole = (
        shape[0] * lax.axis_size("gx"),
        shape[1] * lax.axis_size("gy"),
        shape[2] * lax.axis_size("gz"),
    )
    parity = parity_of(shape, block_starts(shape, 0))
    black = parity == 1
    wide_shape = (shape[0] + 4, shape[1] + 4, shape[2] + 4)
    wide_starts = block_starts(shape, 2)
    red_wide = (parity_of(wide_shape, wide_starts) == 0) & inside_grid(
        wide_shape, wide_starts, whole
    )
    wide_source = wide(source)
    field = wide_sweep(
        jnp.zeros(wide_shape, jnp.float32), wide_source, scale, red_wide, source, black
    )
    field = wide_sweep(wide(field), wide_source, scale, red_wide, source, black)
    residue = source - scale * (centre * field - stencil_sum(faces(field)))
    field = field + prolong(shared_cycle(restrict(residue), level + 1, top))
    for number in range(2):
        field = wide_sweep(wide(field), wide_source, scale, red_wide, source, black)
    return field


def pairs(count, first):
    swaps = []
    for i in range(first, count - 1, 2):
        swaps += [(i, i + 1), (i + 1, i)]
    return swaps


def flips(count, bit):
    return [(i, i ^ bit) for i in range(count)]


def lanes_of(shape):
    return lax.broadcasted_iota(jnp.int32, shape, len(shape) - 1)


def rows_of(shape):
    return lax.broadcasted_iota(jnp.int32, shape, len(shape) - 2)


def odd_of(shape):
    return ((lanes_of(shape) + rows_of(shape)) & 1) == 1


def beside(value, closed):
    rows, lanes = value.shape
    up = pltpu.roll(value, 1, 0)
    down = pltpu.roll(value, rows - 1, 0)
    left = pltpu.roll(value, 1, 1)
    right = pltpu.roll(value, lanes - 1, 1)
    if closed:
        row, lane = rows_of(value.shape), lanes_of(value.shape)
        up = jnp.where(row == 0, 0.0, up)
        down = jnp.where(row == rows - 1, 0.0, down)
        left = jnp.where(lane == 0, 0.0, left)
        right = jnp.where(lane == lanes - 1, 0.0, right)
    return value + (up + down) + (1.0 + rsd_beta) * (left + right)


def red_sum(black, at, odd, closed, before, after):
    return beside(black[at], closed) + jnp.where(odd, after(black, at), before(black, at))


def black_sum(red, at, odd, closed, before, after):
    return beside(red[at], closed) + jnp.where(odd, before(red, at), after(red, at))


def open_before(ref, at):
    return ref[at - 1] if at > 0 else 0.0


def open_after(ref, at):
    return ref[at + 1] if at + 1 < ref.shape[0] else 0.0


def ring_steps(count, own, at_low, at_high):
    def before(ref, at):
        value = ref[(at - 1) % count]
        return jnp.where(at_low, 0.0, value) if at == 0 else value

    def after(ref, at):
        value = ref[(at + 1) % count]
        return jnp.where(at_high, 0.0, value) if at == own - 1 else value

    return before, after


def exact_dot(a, b):
    return jnp.dot(a, b, precision=lax.Precision.HIGHEST, preferred_element_type=jnp.float32)


def pack_kernel(halo, own_ref, xh_ref, ya_ref, yb_ref, za_ref, zb_ref):
    even_y = lax.axis_index("gy") % 2 == 0
    even_z = lax.axis_index("gz") % 2 == 0
    nx, ny, nz = own_ref.shape
    groups = nz // halo
    shape = (ny + 2 * halo, nz)
    group = lanes_of(shape) // halo
    for j in range(za_ref.shape[0]):
        last = jnp.zeros(shape, jnp.float32)
        first = jnp.zeros(shape, jnp.float32)
        for k in range(groups):
            at = j * groups + k
            if at >= nx + halo:
                break
            plane = block_plane(at, nx, own_ref, xh_ref, ya_ref, yb_ref, even_y)
            last = jnp.where(group == k, pltpu.roll(plane, (halo * k + halo) % nz, 1), last)
            first = jnp.where(group == k, pltpu.roll(plane, halo * k, 1), first)
        za_ref[j] = jnp.where(even_z, last, first)
        zb_ref[j] = jnp.where(even_z, first, last)


def block_plane(at, nx, own_ref, xh_ref, ya_ref, yb_ref, even_y):
    a, b = ya_ref[at], yb_ref[at]
    middle = own_ref[at] if at < nx else xh_ref[at - nx]
    low = jnp.where(even_y, b, a)
    high = jnp.where(even_y, a, b)
    return jnp.concatenate([low, middle, high], axis=0)


def block_mask(own, halo, lanes):
    ny, nz = own
    shape = (ny + 2 * halo, lanes)
    row = rows_of(shape) - halo + lax.axis_index("gy") * ny
    lane = lanes_of(shape)
    lane = jnp.where(lane < lanes - halo, lane, lane - lanes) + lax.axis_index("gz") * nz
    inside = (row >= 0) & (row < ny * lax.axis_size("gy"))
    inside = inside & (lane >= 0) & (lane < nz * lax.axis_size("gz"))
    return jnp.where(inside, 1.0 / centre, 0.0)


def pre_kernel(
    halo, own_ref, xh_ref, ya_ref, yb_ref, za_ref, zb_ref,
    gr_ref, gb_ref, black_ref, send_ref,
    fr_ref, fb_ref, red_ref, rest_ref,
):
    even_y = lax.axis_index("gy") % 2 == 0
    even_z = lax.axis_index("gz") % 2 == 0
    nx, ny, nz = own_ref.shape
    count, rows, lanes = black_ref.shape
    own = nx // 2
    groups = nz // halo
    odd = odd_of((rows, lanes))
    mask = block_mask((ny, nz), halo, lanes)
    lane = lanes_of((rows, nz))
    low, high = lane < halo, lane >= nz - halo

    def plane(at):
        j, k = at // groups, at % groups
        a, b = za_ref[j], zb_ref[j]
        left = jnp.where(even_z, b, a)
        right = jnp.where(even_z, a, b)
        right = pltpu.roll(right, (nz - halo * k) % nz, 1)
        left = pltpu.roll(left, (2 * nz - halo - halo * k) % nz, 1)
        sides = jnp.where(low, right, jnp.where(high, left, 0.0))
        middle = block_plane(at, nx, own_ref, xh_ref, ya_ref, yb_ref, even_y)
        return jnp.concatenate([middle, sides], axis=1)

    for at in range(count):
        p, q = plane(2 * at), plane(2 * at + 1)
        red, black = jnp.where(odd, q, p), jnp.where(odd, p, q)
        fr_ref[at], fb_ref[at] = red, black
        gr_ref[at], gb_ref[at] = mask * red, mask * black
    here = lax.axis_index("gx")
    before, after = ring_steps(count, own, here == 0, here == lax.axis_size("gx") - 1)
    for at in range(count):
        black_ref[at] = gb_ref[at] + mask * black_sum(gr_ref, at, odd, False, before, after)
    for at in range(count):
        red_ref[at] = gr_ref[at] + mask * red_sum(black_ref, at, odd, False, before, after)
    inner = slice(halo, halo + ny)
    for at in range(count):
        total = black_sum(red_ref, at, odd, False, before, after)
        value = gb_ref[at] + mask * total
        black_ref[at] = value
        if at < own:
            left_over = fb_ref[at] + total - centre * value
            rest_ref[at] = left_over[inner, :nz]
    for at in range(own):
        total = red_sum(black_ref, at, odd, False, before, after)
        left_over = fr_ref[at] + total - centre * red_ref[at]
        rest_ref[at] = rest_ref[at] + left_over[inner, :nz]
    half, narrow = ny // 2, nz // 2
    pairs_y = rest_ref[:, pl.ds(0, half, stride=2), :] + rest_ref[:, pl.ds(1, half, stride=2), :]
    weight = jnp.where(
        rows_of((nz, nz)) // 2 == lanes_of((nz, nz)) % narrow, 0.5, 0.0
    )
    coarse = exact_dot(pairs_y.reshape(own * half, nz), weight).reshape(own, half, nz)
    lane = lanes_of((half, nz))
    pick = odd_of((half, nz)) ^ (lane >= narrow)
    for at in range(own // 2):
        packed = jnp.where(pick, coarse[2 * at + 1], coarse[2 * at])
        for member in range(send_ref.shape[0]):
            send_ref[member, at] = packed


def level_shapes(whole):
    shapes = []
    for level in range(1, LEVELS):
        nx, ny, nz = (size >> level for size in whole)
        shapes.append((max(nx // 2, 1), max(ny, 8), max(nz, 128), ny, nz))
    return shapes


LANES = 128


def split_put(ref, at, value):
    for part in range(ref.shape[1]):
        ref[at, part] = value[:, part * LANES : (part + 1) * LANES]


def split_get(ref, at):
    return jnp.concatenate([ref[at, part] for part in range(ref.shape[1])], axis=1)


def twice_put(ref, at, value):
    for part in range(ref.shape[1]):
        column = value[:, part * LANES : (part + 1) * LANES]
        for start in range(2):
            ref[at, part, pl.ds(start, value.shape[0], stride=2), :] = column


def restrict_plane(rest_ref, at, weight):
    half = rest_ref.shape[2] // 2
    columns = [
        rest_ref[at, part, pl.ds(0, half, stride=2), :] + rest_ref[at, part, pl.ds(1, half, stride=2), :]
        for part in range(rest_ref.shape[1])
    ]
    total = jnp.concatenate(columns, axis=1)
    if half < 8:
        total = jnp.concatenate([total, jnp.zeros((8 - half, total.shape[1]), jnp.float32)], axis=0)
    return exact_dot(total, weight)


def solve_kernel(halo, whole, *refs):
    here_ref, flip_ref, next_ref, both_ref, gr_ref, gb_ref, black_ref, out_ref = refs[:8]
    scratch = list(refs[8:])
    shapes = level_shapes(whole)
    fields = [[scratch.pop(0) for _ in range(5)] for _ in shapes]
    full_ref, tall_ref, red_ref, work_ref, wide_ref = scratch
    gx, gy, gz = (lax.axis_index(axis) for axis in ("gx", "gy", "gz"))
    low_bit, high_bit = gz % 2 == 1, gz >= 2

    fr, fb = fields[0][:2]
    members, slots, block_rows, block_lanes = here_ref.shape
    narrow = block_lanes // 2
    count_y = lax.axis_size("gy")
    left = lanes_of((block_rows, block_lanes)) < narrow
    for member in range(members):
        i, j = member // count_y, member % count_y
        rows = slice(j * block_rows, (j + 1) * block_rows)
        for at in range(slots):
            mine = (here_ref[member, at], next_ref[member, at])
            other = (flip_ref[member, at], both_ref[member, at])
            for part in range(2):
                near = high_bit if part else jnp.logical_not(high_bit)
                p = jnp.where(near, mine[0], other[0])
                q = jnp.where(near, mine[1], other[1])
                first = jnp.where(low_bit, q, p)
                second = jnp.where(low_bit, p, q)
                lanes = slice(part * block_lanes, (part + 1) * block_lanes)
                fr[i * slots + at, rows, lanes] = jnp.where(left, first, pltpu.roll(second, narrow, 1))
                fb[i * slots + at, rows, lanes] = jnp.where(left, pltpu.roll(first, narrow, 1), second)

    def mask_of(index):
        _, rows, lanes, ny, nz = shapes[index]
        inside = (rows_of((rows, lanes)) < ny) & (lanes_of((rows, lanes)) < nz)
        return jnp.where(inside, 1.0 / centre, 0.0)

    def sweeps(index, number, start):
        fr, fb, red, black, _ = fields[index]
        count, rows, lanes = red.shape
        odd, mask = odd_of((rows, lanes)), mask_of(index)
        for step in range(number):
            for at in range(count):
                if start and step == 0:
                    red[at] = mask * fr[at]
                else:
                    total = red_sum(black, at, odd, True, open_before, open_after)
                    red[at] = mask * (fr[at] + total)
            for at in range(count):
                total = black_sum(red, at, odd, True, open_before, open_after)
                black[at] = mask * (fb[at] + total)

    def descend(index):
        fr, fb, red, black, rest = fields[index]
        count, rows, lanes = red.shape
        odd = odd_of((rows, lanes))
        for at in range(count):
            first = fb[at] + black_sum(red, at, odd, True, open_before, open_after)
            second = fr[at] + red_sum(black, at, odd, True, open_before, open_after)
            split_put(rest, at, (first - centre * black[at]) + (second - centre * red[at]))
        _, next_rows, next_lanes, _, _ = shapes[index + 1]
        weight = jnp.where(
            rows_of((lanes, next_lanes)) // 2 == lanes_of((lanes, next_lanes)), 0.5, 0.0
        )
        planes = [restrict_plane(rest, at, weight) for at in range(count)]
        next_fr, next_fb = fields[index + 1][:2]
        if count == 1:
            next_fr[0] = planes[0]
            return
        odd = odd_of((next_rows, next_lanes))
        for at in range(count // 2):
            p, q = planes[2 * at], planes[2 * at + 1]
            next_fr[at], next_fb[at] = jnp.where(odd, q, p), jnp.where(odd, p, q)

    def ascend(index):
        _, _, red, black, rest = fields[index]
        count, rows, lanes = red.shape
        _, _, coarse_red, coarse_black, _ = fields[index + 1]
        _, next_rows, next_lanes, _, _ = shapes[index + 1]
        odd = odd_of((next_rows, next_lanes))
        weight = jnp.where(
            rows_of((next_lanes, lanes)) == lanes_of((next_lanes, lanes)) // 2, 1.0, 0.0
        )
        half = rows // 2
        for at in range(count):
            r, b = coarse_red[at // 2], coarse_black[at // 2]
            if count == 1:
                plane = r + b
            else:
                plane = jnp.where(odd, r, b) if at % 2 else jnp.where(odd, b, r)
            twice_put(rest, at, exact_dot(plane, weight)[:half])
            black[at] = black[at] + split_get(rest, at)

    def coarsest(index):
        source, _, red, black, _ = fields[index]
        odd = (lanes_of(source.shape[1:]) & 1) == 1
        mask = mask_of(index)
        mask_red, mask_black = jnp.where(odd, 0.0, mask), jnp.where(odd, mask, 0.0)
        value, dark = source[0], jnp.zeros(source.shape[1:], jnp.float32)

        def along(field):
            return (1.0 + rsd_beta) * (pltpu.roll(field, 1, 1) + pltpu.roll(field, field.shape[1] - 1, 1))

        for step in range(CSWEEPS):
            light = mask_red * (value + along(dark))
            dark = mask_black * (value + along(light))
        red[0], black[0] = light, dark

    last = len(shapes) - 1
    for index in range(last):
        sweeps(index, 2, True)
        descend(index)
    coarsest(last)
    for index in reversed(range(last)):
        ascend(index)
        sweeps(index, 2, False)

    count, rows, lanes = black_ref.shape
    nx, ny, nz = out_ref.shape
    own, reach = nx // 2, halo // 2
    _, _, red1, black1, _ = fields[0]
    _, rows1, lanes1 = red1.shape
    odd1 = odd_of((rows1, lanes1))
    border = jnp.zeros((full_ref.shape[0], 8, lanes1), jnp.float32)
    full_ref[:, :8, :] = border
    full_ref[:, rows1 + 8 :, :] = border
    for at in range(red1.shape[0]):
        r, b = red1[at], black1[at]
        full_ref[2 * at, 8 : rows1 + 8, :] = jnp.where(odd1, b, r)
        full_ref[2 * at + 1, 8 : rows1 + 8, :] = jnp.where(odd1, r, b)
    half, block = rows // 2, ny // 2
    z = lanes_of((lanes1, lanes))
    z = jnp.where(z < lanes - halo, z, z - lanes) + gz * nz
    weight = jnp.where(rows_of((lanes1, lanes)) == lax.shift_right_arithmetic(z, 1), 1.0, 0.0)
    skip = 8 - reach
    for at in range(count):
        if at < own:
            x = gx * own + at
        else:
            x = jnp.where(gx == 0, own, own - (count - own)) + (at - own)
        tall_ref[at] = full_ref[x, pl.ds(pl.multiple_of(gy * block, 8), block + 16), :][skip : skip + half]
    spread = exact_dot(tall_ref[...].reshape(count * half, lanes1), weight).reshape(count, half, lanes)
    for at in range(count):
        twice_put(wide_ref, at, spread[at])
    odd = odd_of((rows, lanes))
    mask = block_mask((ny, nz), halo, lanes)
    for at in range(count):
        work_ref[at] = split_get(wide_ref, at) + black_ref[at]
    before, after = ring_steps(count, own, gx == 0, gx == lax.axis_size("gx") - 1)
    for step in range(2):
        for at in range(count):
            red_ref[at] = gr_ref[at] + mask * red_sum(work_ref, at, odd, False, before, after)
        for at in range(count if step == 0 else own):
            work_ref[at] = gb_ref[at] + mask * black_sum(red_ref, at, odd, False, before, after)
    inner = slice(halo, halo + ny)
    odd = odd_of((ny, nz))
    for at in range(own):
        r, b = red_ref[at, inner, :nz], work_ref[at, inner, :nz]
        out_ref[2 * at] = jnp.where(odd, b, r)
        out_ref[2 * at + 1] = jnp.where(odd, r, b)


def vmem(number):
    return [pl.BlockSpec(memory_space=pltpu.VMEM)] * number


def struct(*shape):
    return jax.ShapeDtypeStruct(shape, jnp.float32)


def scratch(*shape):
    return pltpu.VMEM(shape, jnp.float32)


HALO = 8


def block_cycle(density):
    halo = HALO
    nx, ny, nz = density.shape
    count_x, count_y, count_z = (lax.axis_size(axis) for axis in ("gx", "gy", "gz"))
    whole = (nx * count_x, ny * count_y, nz * count_z)
    gx, gy = lax.axis_index("gx"), lax.axis_index("gy")
    face = lax.dynamic_slice_in_dim(density, jnp.where(gx == 0, nx - halo, 0), halo, 0)
    side = lax.ppermute(face, "gx", flips(count_x, 1))
    tall = jnp.concatenate([density, side], axis=0)
    even = gy % 2 == 0
    ya = lax.dynamic_slice_in_dim(tall, jnp.where(even, ny - halo, 0), halo, 1)
    yb = lax.dynamic_slice_in_dim(tall, jnp.where(even, 0, ny - halo), halo, 1)
    ya = lax.ppermute(ya, "gy", pairs(count_y, 0))
    yb = lax.ppermute(yb, "gy", pairs(count_y, 1))
    rows, lanes = ny + 2 * halo, 2 * nz
    planes = nx + halo
    packs = -(-planes * halo // nz)

    def params(mib):
        return pltpu.CompilerParams(vmem_limit_bytes=mib * 1024 * 1024)

    za, zb = pl.pallas_call(
        functools.partial(pack_kernel, halo),
        out_shape=[struct(packs, rows, nz)] * 2,
        in_specs=vmem(4), out_specs=vmem(2), compiler_params=params(4),
    )(density, side, ya, yb)
    za = lax.ppermute(za, "gz", pairs(count_z, 0))
    zb = lax.ppermute(zb, "gz", pairs(count_z, 1) + [(0, count_z - 1), (count_z - 1, 0)])
    members = count_x * count_y
    slots = (planes // 2, rows, lanes)
    gr, gb, black, send = pl.pallas_call(
        functools.partial(pre_kernel, halo),
        out_shape=[struct(*slots)] * 3 + [struct(members, nx // 4, ny // 2, nz)],
        in_specs=vmem(6), out_specs=vmem(4), compiler_params=params(10),
        scratch_shapes=[scratch(*slots)] * 3 + [scratch(nx // 2, ny, nz)],
    )(density, side, ya, yb, za, zb)
    here = lax.all_to_all(send, ("gx", "gy"), 0, 0, tiled=True)
    flip = lax.ppermute(here, "gz", flips(count_z, 2))
    beside_here = lax.ppermute(here, "gz", flips(count_z, 1))
    beside_flip = lax.ppermute(flip, "gz", flips(count_z, 1))
    room = []
    for count, high, wide_lanes, _, _ in level_shapes(whole):
        room += [scratch(count, high, wide_lanes)] * 4
        room += [scratch(count, wide_lanes // LANES, high, LANES)]
    room += [
        scratch(whole[0] // 2, whole[1] // 2 + 16, whole[2] // 2),
        scratch(planes // 2, rows // 2, whole[2] // 2),
        scratch(*slots),
        scratch(*slots),
        scratch(planes // 2, lanes // LANES, rows, LANES),
    ]
    return pl.pallas_call(
        functools.partial(solve_kernel, halo, whole),
        out_shape=struct(nx, ny, nz),
        in_specs=vmem(7), out_specs=pl.BlockSpec(memory_space=pltpu.VMEM),
        compiler_params=params(16), scratch_shapes=room,
    )(here, flip, beside_here, beside_flip, gr, gb, black)


def fits_block_cycle(shape):
    nx, ny, nz = shape
    count_x, count_y, count_z = (lax.axis_size(axis) for axis in ("gx", "gy", "gz"))
    whole = (nx * count_x, ny * count_y, nz * count_z)
    coarsest = [size >> (LEVELS - 1) for size in whole]
    exact = all(c << (LEVELS - 1) == size for c, size in zip(coarsest, whole))
    return (
        exact and coarsest[0] == coarsest[1] == 1 and nz == 128 and ny == 16 and nx >= 16
        and nx % 4 == 0 and count_x == 2 and count_z == 4 and count_y % 2 == 0
    )


def on_device(density):
    if fits_block_cycle(density.shape):
        return block_cycle(density)
    top = 4
    return shared_cycle(density, 0, top)


def solution(mesh):
    return jax.shard_map(
        on_device,
        mesh=mesh,
        in_specs=(P("gx", "gy", "gz"),),
        out_specs=P("gx", "gy", "gz"),
        check_vma=False,
    )
```

```python
import functools

import jax
import jax.numpy as jnp
from jax import lax
from jax.experimental import pallas as pl
from jax.experimental.pallas import tpu as pltpu
from jax.sharding import PartitionSpec as P

LEVELS = 7
CSWEEPS = 4


rsd_beta = 0.5
centre = 4.0 + 2.0 * (1.0 + rsd_beta)


def extended_2(value, sides, width):
    for axis, dim in sides:
        count, length = (lax.axis_size(axis), value.shape[dim])
        up = [(i, (i + 1) % count) for i in range(count - 1)]
        down = [(j, i) for i, j in up]
        last = lax.slice_in_dim(value, length - width, length, axis=dim)
        leading = lax.slice_in_dim(value, 0, width, axis=dim)
        before = lax.ppermute(last, axis, up)
        after = lax.ppermute(leading, axis, down)
        value = jnp.concatenate([before, value, after], axis=dim)
    return value


def stencil_sum(padded):
    plane = (
        padded[2:, 1:-1, 1:-1]
        + padded[:-2, 1:-1, 1:-1]
        + padded[1:-1, 2:, 1:-1]
        + padded[1:-1, :-2, 1:-1]
    )
    sight = padded[1:-1, 1:-1, 2:] + padded[1:-1, 1:-1, :-2]
    return plane + (1.0 + rsd_beta) * sight


def grid_index(shape, starts):
    return [lax.broadcasted_iota(jnp.int32, shape, which) + starts[which] for which in range(3)]


def parity_of(shape, starts):
    position = grid_index(shape, starts)
    return (position[0] + position[1] + position[2] + 6) % 2


def inside_grid(shape, starts, whole):
    position = grid_index(shape, starts)
    keep = (position[0] >= 0) & (position[0] < whole[0])
    for which in (1, 2):
        keep = keep & (position[which] >= 0) & (position[which] < whole[which])
    return keep


def half_sweep(field, source, scale, chosen):
    update = (source / scale + stencil_sum(jnp.pad(field, 1))) / centre
    return jnp.where(chosen, update, field)


def full_sweep(field, source, scale, parity):
    field = half_sweep(field, source, scale, parity == 0)
    return half_sweep(field, source, scale, parity == 1)


def restrict(residue):
    shape = residue.shape
    blocks = residue.reshape(shape[0] // 2, 2, shape[1] // 2, 2, shape[2] // 2, 2)
    return jnp.mean(blocks, axis=(1, 3, 5))


def prolong(coarse):
    return jnp.repeat(jnp.repeat(jnp.repeat(coarse, 2, 0), 2, 1), 2, 2)


def local_cycle(source, level):
    scale = 0.25**level
    parity = parity_of(source.shape, (0, 0, 0))
    field = jnp.zeros_like(source)
    if level == LEVELS - 1:
        for number in range(CSWEEPS):
            field = full_sweep(field, source, scale, parity)
        return field
    for number in range(2):
        field = full_sweep(field, source, scale, parity)
    residue = source - scale * (centre * field - stencil_sum(jnp.pad(field, 1)))
    field = field + prolong(local_cycle(restrict(residue), level + 1))
    for number in range(2):
        field = full_sweep(field, source, scale, parity)
    return field


def faces(field):
    return extended_2(field, (("gx", 0), ("gy", 1), ("gz", 2)), 1)


def wide(field):
    return extended_2(field, (("gx", 0), ("gy", 1), ("gz", 2)), 2)


def block_starts(shape, margin):
    return (
        lax.axis_index("gx") * shape[0] - margin,
        lax.axis_index("gy") * shape[1] - margin,
        lax.axis_index("gz") * shape[2] - margin,
    )


def padded_half(padded, source, scale, chosen):
    field = padded[1:-1, 1:-1, 1:-1]
    update = (source / scale + stencil_sum(padded)) / centre
    return jnp.where(chosen, update, field)


def wide_sweep(extended, wide_source, scale, red_wide, source, black):
    update = (wide_source / scale + stencil_sum(jnp.pad(extended, 1))) / centre
    extended = jnp.where(red_wide, update, extended)
    return padded_half(extended[1:-1, 1:-1, 1:-1], source, scale, black)


def coarse_level(source, level):
    shape = source.shape
    stack = lax.all_gather(source[None], ("gx", "gy", "gz"), axis=0, tiled=True)
    count_x, count_y, count_z = (lax.axis_size("gx"), lax.axis_size("gy"), lax.axis_size("gz"))
    whole = stack.reshape(count_x, count_y, count_z, shape[0], shape[1], shape[2])
    whole = whole.transpose(0, 3, 1, 4, 2, 5).reshape(
        count_x * shape[0], count_y * shape[1], count_z * shape[2]
    )
    solved = local_cycle(whole, level)
    starts = block_starts(shape, 0)
    return lax.dynamic_slice(solved, starts, shape)


def shared_cycle(source, level, top):
    if level == top:
        return coarse_level(source, level)
    scale = 0.25**level
    shape = source.shape
    whole = (
        shape[0] * lax.axis_size("gx"),
        shape[1] * lax.axis_size("gy"),
        shape[2] * lax.axis_size("gz"),
    )
    parity = parity_of(shape, block_starts(shape, 0))
    black = parity == 1
    wide_shape = (shape[0] + 4, shape[1] + 4, shape[2] + 4)
    wide_starts = block_starts(shape, 2)
    red_wide = (parity_of(wide_shape, wide_starts) == 0) & inside_grid(
        wide_shape, wide_starts, whole
    )
    wide_source = wide(source)
    field = wide_sweep(
        jnp.zeros(wide_shape, jnp.float32), wide_source, scale, red_wide, source, black
    )
    field = wide_sweep(wide(field), wide_source, scale, red_wide, source, black)
    residue = source - scale * (centre * field - stencil_sum(faces(field)))
    field = field + prolong(shared_cycle(restrict(residue), level + 1, top))
    for number in range(2):
        field = wide_sweep(wide(field), wide_source, scale, red_wide, source, black)
    return field


def pairs(count, first):
    swaps = []
    for i in range(first, count - 1, 2):
        swaps += [(i, i + 1), (i + 1, i)]
    return swaps


def flips(count, bit):
    return [(i, i ^ bit) for i in range(count)]


def lanes_of(shape):
    return lax.broadcasted_iota(jnp.int32, shape, len(shape) - 1)


def rows_of(shape):
    return lax.broadcasted_iota(jnp.int32, shape, len(shape) - 2)


LANES = 128
PAD = 8


def odd_of(shape):
    return ((lanes_of(shape) + rows_of(shape)) & 1) == 1


def exact_dot(a, b):
    return jnp.dot(a, b, precision=lax.Precision.HIGHEST, preferred_element_type=jnp.float32)


def window(ref, at, column, count, start=0, shift=0):
    if isinstance(start, int):
        return ref[at, column, PAD + start + shift : PAD + start + shift + count, :]
    first = start + (PAD + shift)
    if shift == 0:
        first = pl.multiple_of(first, 8)
    return ref[at, column, pl.ds(first, count), :]


def clear_pads(ref):
    edge = jnp.zeros((PAD, LANES), jnp.float32)
    for at in range(ref.shape[0]):
        for column in range(ref.shape[1]):
            ref[at, column, :PAD, :] = edge
            ref[at, column, ref.shape[2] - PAD :, :] = edge


def block_sums(ref, at, rows):
    lane = lanes_of((rows, LANES))
    values = [window(ref, at, column, rows) for column in range(2)]
    lefts = [pltpu.roll(value, 1, 1) for value in values]
    rights = [pltpu.roll(value, LANES - 1, 1) for value in values]
    sums = []
    for column in range(2):
        left = jnp.where(lane == 0, lefts[1 - column], lefts[column])
        right = jnp.where(lane == LANES - 1, rights[1 - column], rights[column])
        sides = window(ref, at, column, rows, shift=-1) + window(ref, at, column, rows, shift=1)
        sums.append(values[column] + sides + (1.0 + rsd_beta) * (left + right))
    return sums


def block_totals(ref, at, rows, own, odd, to_red, at_low, at_high):
    slots = ref.shape[0]
    totals = []
    for column, total in enumerate(block_sums(ref, at, rows)):
        before = window(ref, (at - 1) % slots, column, rows)
        after = window(ref, (at + 1) % slots, column, rows)
        if at == 0:
            before = jnp.where(at_low, 0.0, before)
        if at == own - 1:
            after = jnp.where(at_high, 0.0, after)
        totals.append(total + (jnp.where(odd, after, before) if to_red else jnp.where(odd, before, after)))
    return totals


def block_mask(own, halo):
    ny, nz = own
    shape = (ny + 2 * halo, LANES)
    row = rows_of(shape) - halo + lax.axis_index("gy") * ny
    inside_y = (row >= 0) & (row < ny * lax.axis_size("gy"))
    masks = []
    for column in range(2):
        lane = lanes_of(shape)
        if column:
            lane = jnp.where(lane < halo, lane + LANES, lane - LANES)
        lane = lane + lax.axis_index("gz") * nz
        inside = inside_y & (lane >= 0) & (lane < nz * lax.axis_size("gz"))
        masks.append(jnp.where(inside, 1.0 / centre, 0.0))
    return masks


def block_plane(at, nx, own_ref, xh_ref, ya_ref, yb_ref, even_y):
    a, b = ya_ref[at], yb_ref[at]
    middle = own_ref[at] if at < nx else xh_ref[at - nx]
    low = jnp.where(even_y, b, a)
    high = jnp.where(even_y, a, b)
    return jnp.concatenate([low, middle, high], axis=0)


def pack_kernel(halo, own_ref, xh_ref, ya_ref, yb_ref, za_ref, zb_ref):
    even_y = lax.axis_index("gy") % 2 == 0
    even_z = lax.axis_index("gz") % 2 == 0
    nx, ny, nz = own_ref.shape
    groups = nz // halo
    shape = (ny + 2 * halo, nz)
    group = lanes_of(shape) // halo
    for j in range(za_ref.shape[0]):
        last = jnp.zeros(shape, jnp.float32)
        first = jnp.zeros(shape, jnp.float32)
        for k in range(groups):
            at = j * groups + k
            if at >= nx + halo:
                break
            plane = block_plane(at, nx, own_ref, xh_ref, ya_ref, yb_ref, even_y)
            last = jnp.where(group == k, pltpu.roll(plane, (halo * k + halo) % nz, 1), last)
            first = jnp.where(group == k, pltpu.roll(plane, halo * k, 1), first)
        za_ref[j] = jnp.where(even_z, last, first)
        zb_ref[j] = jnp.where(even_z, first, last)


def pre_kernel(
    halo, own_ref, xh_ref, ya_ref, yb_ref, za_ref, zb_ref,
    gr_ref, gb_ref, dark_ref, send_ref,
    fr_ref, fb_ref, red_ref, black_ref, rest_ref,
):
    even_y = lax.axis_index("gy") % 2 == 0
    even_z = lax.axis_index("gz") % 2 == 0
    nx, ny, nz = own_ref.shape
    count, _, rows, _ = gr_ref.shape
    own = nx // 2
    groups = nz // halo
    shape = (rows, LANES)
    odd = odd_of(shape)
    masks = block_mask((ny, nz), halo)
    lane = lanes_of(shape)
    low, high = lane < halo, lane >= nz - halo
    inner = slice(halo, halo + ny)
    body = slice(PAD, PAD + rows)
    here = lax.axis_index("gx")
    ends = (here == 0, here == lax.axis_size("gx") - 1)
    clear_pads(red_ref)
    clear_pads(black_ref)

    def columns(at):
        j, k = at // groups, at % groups
        a, b = za_ref[j], zb_ref[j]
        left = jnp.where(even_z, b, a)
        right = jnp.where(even_z, a, b)
        right = pltpu.roll(right, (nz - halo * k) % nz, 1)
        left = pltpu.roll(left, (2 * nz - halo - halo * k) % nz, 1)
        sides = jnp.where(low, right, jnp.where(high, left, 0.0))
        return block_plane(at, nx, own_ref, xh_ref, ya_ref, yb_ref, even_y), sides

    for at in range(count):
        first, second = columns(2 * at), columns(2 * at + 1)
        for c in range(2):
            red = jnp.where(odd, second[c], first[c])
            black = jnp.where(odd, first[c], second[c])
            if c == 0 and at < own:
                fr_ref[at], fb_ref[at] = red[inner], black[inner]
            red = masks[c] * red
            gr_ref[at, c], gb_ref[at, c] = red, masks[c] * black
            red_ref[at, c, body, :] = red
    for at in range(count):
        totals = block_totals(red_ref, at, rows, own, odd, False, *ends)
        for c in range(2):
            black_ref[at, c, body, :] = gb_ref[at, c] + masks[c] * totals[c]
    for at in range(count):
        totals = block_totals(black_ref, at, rows, own, odd, True, *ends)
        for c in range(2):
            red_ref[at, c, body, :] = gr_ref[at, c] + masks[c] * totals[c]
    for at in range(count):
        totals = block_totals(red_ref, at, rows, own, odd, False, *ends)
        for c in range(2):
            value = gb_ref[at, c] + masks[c] * totals[c]
            black_ref[at, c, body, :] = value
            dark_ref[at, c] = value
            if c == 0 and at < own:
                rest_ref[at] = fb_ref[at] + totals[c][inner] - centre * value[inner]
    for at in range(own):
        total = block_totals(black_ref, at, rows, own, odd, True, *ends)[0]
        left_over = fr_ref[at] + total[inner] - centre * red_ref[at, 0, PAD + halo : PAD + halo + ny, :]
        rest_ref[at] = rest_ref[at] + left_over
    half, quarter = ny // 2, nz // 4
    pairs_y = rest_ref[:, pl.ds(0, half, stride=2), :] + rest_ref[:, pl.ds(1, half, stride=2), :]
    column = lanes_of((nz, nz))
    target = 2 * (column % quarter) + (column // quarter) % 2
    weight = jnp.where(rows_of((nz, nz)) // 2 == target, 0.5, 0.0)
    coarse = exact_dot(pairs_y.reshape(own * half, nz), weight).reshape(own, half, nz)
    part = lanes_of((half, nz)) // quarter
    pick = (((rows_of((half, nz)) + part) & 1) == 1) ^ (part >= 2)
    for at in range(own // 2):
        packed = jnp.where(pick, coarse[2 * at + 1], coarse[2 * at])
        for member in range(send_ref.shape[0]):
            send_ref[member, at] = packed


def small_shapes(whole):
    return [max(whole[0] >> (level + 1), 1) for level in range(2, LEVELS)]


def solve_kernel(halo, whole, *refs):
    here_ref, flip_ref, next_ref, both_ref, gr_ref, gb_ref, dark_ref, out_ref = refs[:8]
    fr1, fb1, red1, black1, rest1, tall_ref, red_ref, work_ref = refs[8:16]
    small = [refs[16 + 4 * i : 20 + 4 * i] for i in range(LEVELS - 2)]
    gx, gy, gz = (lax.axis_index(axis) for axis in ("gx", "gy", "gz"))
    weight_z = 1.0 + rsd_beta
    share = 1.0 / centre
    for ref in (red1, black1, red_ref, work_ref):
        clear_pads(ref)
    for level in small:
        for ref in level[2:]:
            clear_pads(ref)

    members, slots, block_rows, _ = here_ref.shape
    count_y = lax.axis_size("gy")
    count1, _, rows1, _ = fr1.shape
    quarter = LANES // 4
    sources = [
        (ref, jnp.bitwise_xor(gz, bits))
        for ref, bits in ((here_ref, 0), (flip_ref, 2), (next_ref, 1), (both_ref, 3))
    ]
    group = lanes_of((block_rows, LANES)) // quarter
    theirs = [group == which for _, which in sources]
    for part, target in enumerate((fr1, fr1, fb1, fb1)):
        turns = [quarter * jnp.bitwise_and(which - part, 3) for _, which in sources]
        for member in range(members):
            i, j = member // count_y, member % count_y
            for at in range(slots):
                value = None
                for (ref, _), mine, turn in zip(sources, theirs, turns):
                    moved = pltpu.roll(ref[member, at], turn, 1)
                    value = moved if value is None else jnp.where(mine, moved, value)
                rows = slice(j * block_rows, (j + 1) * block_rows)
                target[i * slots + at, part % 2, rows, :] = value

    def fold_total(ref, at, e, start, count, low, high, odds, to_red):
        lane = lanes_of((count, LANES))
        value, other = window(ref, at, e, count, start), window(ref, at, 1 - e, count, start)
        sides = window(ref, at, e, count, start, -1) + window(ref, at, e, count, start, 1)
        if e == 0:
            near = jnp.where(lane == 0, 0.0, pltpu.roll(other, 1, 1))
        else:
            near = jnp.where(lane == LANES - 1, 0.0, pltpu.roll(other, LANES - 1, 1))
        before = 0.0 if low is True else window(ref, at - 1, e, count, start)
        after = 0.0 if high is True else window(ref, at + 1, e, count, start)
        if not isinstance(low, bool):
            before = jnp.where(low, 0.0, window(ref, jnp.maximum(at - 1, 0), e, count, start))
        if not isinstance(high, bool):
            after = jnp.where(high, 0.0, window(ref, jnp.minimum(at + 1, count1 - 1), e, count, start))
        beside = jnp.where(odds[e], after, before) if to_red else jnp.where(odds[e], before, after)
        return value + sides + beside + weight_z * (other + near)

    def fold_odds(count):
        row = rows_of((count, LANES))
        return [((row + e) & 1) == 1 for e in range(2)]

    odds = fold_odds(rows1)
    body1 = slice(PAD, PAD + rows1)

    def down_total(ref, at, e, to_red):
        return fold_total(ref, at, e, 0, rows1, at == 0, at == count1 - 1, odds, to_red)

    for at in range(count1):
        for e in range(2):
            red1[at, e, body1, :] = share * fr1[at, e]
    for at in range(count1):
        for e in range(2):
            black1[at, e, body1, :] = share * (fb1[at, e] + down_total(red1, at, e, False))
    for at in range(count1):
        for e in range(2):
            red1[at, e, body1, :] = share * (fr1[at, e] + down_total(black1, at, e, True))
    for at in range(count1):
        left_over = None
        for e in range(2):
            total = fb1[at, e] + down_total(red1, at, e, False)
            value = share * total
            black1[at, e, body1, :] = value
            term = total - centre * value
            left_over = term if left_over is None else left_over + term
        rest1[at] = left_over
    for at in range(count1):
        left_over = rest1[at]
        for e in range(2):
            total = fr1[at, e] + down_total(black1, at, e, True)
            left_over = left_over + (total - centre * window(red1, at, e, rows1))
        rest1[at] = left_over
    rows2 = rows1 // 2
    shape2 = (rows2, LANES)
    row2, lane2 = rows_of(shape2), lanes_of(shape2)
    odd2 = odd_of(shape2)
    planes = [
        0.5 * (rest1[at, pl.ds(0, rows2, stride=2), :] + rest1[at, pl.ds(1, rows2, stride=2), :])
        for at in range(count1)
    ]

    body2 = slice(PAD, PAD + rows2)

    def grid_of(index):
        step = 1 << index
        return ((row2 & (step - 1)) == 0) & ((lane2 & (step - 1)) == 0)

    def odd_at(index):
        return (((row2 >> index) + (lane2 >> index)) & 1) == 1

    def along(value, step):
        left = jnp.where(lane2 < step, 0.0, pltpu.roll(value, step, 1))
        right = jnp.where(lane2 >= LANES - step, 0.0, pltpu.roll(value, LANES - step, 1))
        return weight_z * (left + right)

    def small_total(index, ref, at, odd, to_red):
        step = 1 << index
        value = ref[at, 0, body2, :]
        total = value + along(value, step)
        total = total + (
            ref[at, 0, PAD - step : PAD - step + rows2, :] + ref[at, 0, PAD + step : PAD + step + rows2, :]
        )
        slots = ref.shape[0]
        if slots == 1:
            return total
        before = ref[at - 1, 0, body2, :] if at > 0 else 0.0
        after = ref[at + 1, 0, body2, :] if at < slots - 1 else 0.0
        return total + (jnp.where(odd, after, before) if to_red else jnp.where(odd, before, after))

    def small_sweeps(index, start):
        fr, fb, red, black = small[index]
        mask, odd = jnp.where(grid_of(index), share, 0.0), odd_at(index)
        slots = fr.shape[0]
        for step in range(2):
            for at in range(slots):
                source = fr[at]
                if not (start and step == 0):
                    source = source + small_total(index, black, at, odd, True)
                red[at, 0, body2, :] = mask * source
            for at in range(slots):
                black[at, 0, body2, :] = mask * (fb[at] + small_total(index, red, at, odd, False))

    last = len(small) - 1
    for index in range(last):
        fr, fb, red, black = small[index]
        slots, odd, step = fr.shape[0], odd_at(index), 1 << index
        if len(planes) == 2 * slots:
            for at in range(slots):
                p, q = planes[2 * at], planes[2 * at + 1]
                fr[at], fb[at] = jnp.where(odd, q, p), jnp.where(odd, p, q)
        small_sweeps(index, True)
        planes = []
        for at in range(slots):
            first = fb[at] + small_total(index, red, at, odd, False) - centre * black[at, 0, body2, :]
            second = fr[at] + small_total(index, black, at, odd, True) - centre * red[at, 0, body2, :]
            total = first + second
            total = total + pltpu.roll(total, rows2 - step, 0)
            planes.append(0.5 * (total + pltpu.roll(total, LANES - step, 1)))

    step = 1 << last
    grid = grid_of(last) & (row2 == 0)
    odd = ((lane2 >> last) & 1) == 1
    mask_red = jnp.where(grid & jnp.logical_not(odd), share, 0.0)
    mask_black = jnp.where(grid & odd, share, 0.0)
    source = planes[0]
    light, dark = None, None
    for sweep in range(CSWEEPS):
        light = mask_red * (source if dark is None else source + along(dark, step))
        dark = mask_black * (source + along(light, step))
    fields = [light + dark]

    for index in reversed(range(last)):
        _, _, red, black = small[index]
        slots, odd, step = red.shape[0], odd_at(index), 1 << index
        for at in range(slots):
            spread = fields[at] + pltpu.roll(fields[at], step, 1)
            spread = spread + pltpu.roll(spread, step, 0)
            black[at, 0, body2, :] = black[at, 0, body2, :] + spread
        small_sweeps(index, False)
        fields = []
        for at in range(slots):
            r, b = red[at, 0, body2, :], black[at, 0, body2, :]
            fields += [jnp.where(odd, b, r), jnp.where(odd, r, b)]

    for at in range(count1):
        for start in range(2):
            rest1[at, pl.ds(start, rows2, stride=2), :] = fields[at]
    for at in range(count1):
        for e in range(2):
            black1[at, e, body1, :] = window(black1, at, e, rows1) + rest1[at]
    nx, ny, nz = out_ref.shape
    own = nx // 2
    part_slots = min(own // 2 + 3, count1)
    part_rows = min(ny // 2 + 16, rows1)
    slot0 = jnp.where(gx == 0, 0, count1 - part_slots)
    row0 = pl.multiple_of(jnp.clip(gy * (ny // 2) - 8, 0, rows1 - part_rows), 8)
    odds = fold_odds(part_rows)

    def up_total(ref, at, e, to_red):
        low = gx == 0 if at == 0 else False
        high = gx != 0 if at == part_slots - 1 else False
        return fold_total(ref, slot0 + at, e, row0, part_rows, low, high, odds, to_red)

    def up_half(target, other, sources, to_red):
        for at in range(part_slots):
            for e in range(2):
                source = sources[slot0 + at, e, pl.ds(row0, part_rows), :]
                value = share * (source + up_total(other, at, e, to_red))
                target[slot0 + at, e, pl.ds(pl.multiple_of(row0 + PAD, 8), part_rows), :] = value

    for sweep in range(2):
        up_half(red1, black1, fr1, True)
        up_half(black1, red1, fb1, False)

    count, _, rows, _ = dark_ref.shape
    half = rows // 2
    odds = fold_odds(half)
    row = gy * (ny // 2) + (PAD - halo // 2)
    for at in range(count):
        if at < own:
            slot = gx * (own // 2) + at // 2
        else:
            slot = jnp.where(gx == 0, own // 2, own // 2 - (count - own) // 2) + (at - own) // 2
        for e in range(2):
            r, b = red1[slot, e, pl.ds(row, half), :], black1[slot, e, pl.ds(row, half), :]
            plane = jnp.where(odds[e], r, b) if at % 2 else jnp.where(odds[e], b, r)
            tall_ref[at, :, e * LANES : (e + 1) * LANES] = plane
    shape = (2 * LANES, 2 * LANES)
    z = lanes_of(shape)
    z = jnp.where(z < 2 * LANES - halo, z, z - 2 * LANES) + gz * nz
    line = rows_of(shape)
    line = jnp.where(line < LANES, 2 * line, 2 * (line - LANES) + 1)
    weight = jnp.where(line == lax.shift_right_arithmetic(z, 1), 1.0, 0.0)
    spread = exact_dot(tall_ref[...].reshape(count * half, 2 * LANES), weight)
    spread = spread.reshape(count, half, 2 * LANES)
    for at in range(count):
        for c in range(2):
            value = spread[at, :, c * LANES : (c + 1) * LANES]
            for start in range(2):
                work_ref[at, c, pl.ds(PAD + start, half, stride=2), :] = value
    body = slice(PAD, PAD + rows)
    for at in range(count):
        for c in range(2):
            work_ref[at, c, body, :] = work_ref[at, c, body, :] + dark_ref[at, c]
    odd = odd_of((rows, LANES))
    masks = block_mask((ny, nz), halo)
    ends = (gx == 0, gx == lax.axis_size("gx") - 1)
    for sweep in range(2):
        for at in range(count):
            totals = block_totals(work_ref, at, rows, own, odd, True, *ends)
            for c in range(2):
                red_ref[at, c, body, :] = gr_ref[at, c] + masks[c] * totals[c]
        for at in range(count if sweep == 0 else own):
            totals = block_totals(red_ref, at, rows, own, odd, False, *ends)
            for c in range(2 if sweep == 0 else 1):
                work_ref[at, c, body, :] = gb_ref[at, c] + masks[c] * totals[c]
    inner = slice(PAD + halo, PAD + halo + ny)
    odd = odd_of((ny, nz))
    for at in range(own):
        r, b = red_ref[at, 0, inner, :], work_ref[at, 0, inner, :]
        out_ref[2 * at] = jnp.where(odd, b, r)
        out_ref[2 * at + 1] = jnp.where(odd, r, b)


def vmem(number):
    return [pl.BlockSpec(memory_space=pltpu.VMEM)] * number


def struct(*shape):
    return jax.ShapeDtypeStruct(shape, jnp.float32)


def scratch(*shape):
    return pltpu.VMEM(shape, jnp.float32)


HALO = 8


def block_cycle(density):
    halo = HALO
    nx, ny, nz = density.shape
    count_x, count_y, count_z = (lax.axis_size(axis) for axis in ("gx", "gy", "gz"))
    whole = (nx * count_x, ny * count_y, nz * count_z)
    gx, gy = lax.axis_index("gx"), lax.axis_index("gy")
    face = lax.dynamic_slice_in_dim(density, jnp.where(gx == 0, nx - halo, 0), halo, 0)
    side = lax.ppermute(face, "gx", flips(count_x, 1))
    tall = jnp.concatenate([density, side], axis=0)
    even = gy % 2 == 0
    ya = lax.dynamic_slice_in_dim(tall, jnp.where(even, ny - halo, 0), halo, 1)
    yb = lax.dynamic_slice_in_dim(tall, jnp.where(even, 0, ny - halo), halo, 1)
    ya = lax.ppermute(ya, "gy", pairs(count_y, 0))
    yb = lax.ppermute(yb, "gy", pairs(count_y, 1))
    rows = ny + 2 * halo
    planes = nx + halo
    packs = -(-planes * halo // nz)

    def params(mib):
        return pltpu.CompilerParams(vmem_limit_bytes=mib * 1024 * 1024)

    za, zb = pl.pallas_call(
        functools.partial(pack_kernel, halo),
        out_shape=[struct(packs, rows, nz)] * 2,
        in_specs=vmem(4), out_specs=vmem(2), compiler_params=params(4),
    )(density, side, ya, yb)
    za = lax.ppermute(za, "gz", pairs(count_z, 0))
    zb = lax.ppermute(zb, "gz", pairs(count_z, 1) + [(0, count_z - 1), (count_z - 1, 0)])
    members = count_x * count_y
    slots = (planes // 2, 2, rows, LANES)
    padded = (planes // 2, 2, rows + 2 * PAD, LANES)
    gr, gb, black, send = pl.pallas_call(
        functools.partial(pre_kernel, halo),
        out_shape=[struct(*slots)] * 3 + [struct(members, nx // 4, ny // 2, nz)],
        in_specs=vmem(6), out_specs=vmem(4), compiler_params=params(10),
        scratch_shapes=[scratch(nx // 2, ny, nz)] * 2
        + [scratch(*padded)] * 2
        + [scratch(nx // 2, ny, nz)],
    )(density, side, ya, yb, za, zb)
    here = lax.all_to_all(send, ("gx", "gy"), 0, 0, tiled=True)
    flip = lax.ppermute(here, "gz", flips(count_z, 2))
    beside_here = lax.ppermute(here, "gz", flips(count_z, 1))
    beside_flip = lax.ppermute(flip, "gz", flips(count_z, 1))
    count1, rows1, rows2 = whole[0] // 4, whole[1] // 2, whole[1] // 4
    room = [scratch(count1, 2, rows1, LANES)] * 2
    room += [scratch(count1, 2, rows1 + 2 * PAD, LANES)] * 2
    room += [scratch(count1, rows1, LANES), scratch(planes // 2, rows // 2, 2 * LANES)]
    room += [scratch(*padded)] * 2
    for count in small_shapes(whole):
        room += [scratch(count, rows2, LANES)] * 2
        room += [scratch(count, 1, rows2 + 2 * PAD, LANES)] * 2
    return pl.pallas_call(
        functools.partial(solve_kernel, halo, whole),
        out_shape=struct(nx, ny, nz),
        in_specs=vmem(7), out_specs=pl.BlockSpec(memory_space=pltpu.VMEM),
        compiler_params=params(16), scratch_shapes=room,
    )(here, flip, beside_here, beside_flip, gr, gb, black)


def fits_block_cycle(shape):
    nx, ny, nz = shape
    count_x, count_y, count_z = (lax.axis_size(axis) for axis in ("gx", "gy", "gz"))
    whole = (nx * count_x, ny * count_y, nz * count_z)
    coarsest = [size >> (LEVELS - 1) for size in whole]
    exact = all(c << (LEVELS - 1) == size for c, size in zip(coarsest, whole))
    return (
        exact and coarsest[0] == coarsest[1] == 1 and nz == LANES and ny == 2 * HALO
        and count_x == 2 and count_z == 4 and count_y % 2 == 0
    )


def on_device(density):
    if fits_block_cycle(density.shape):
        return block_cycle(density)
    top = 4
    return shared_cycle(density, 0, top)


def solution(mesh):
    return jax.shard_map(
        on_device,
        mesh=mesh,
        in_specs=(P("gx", "gy", "gz"),),
        out_specs=P("gx", "gy", "gz"),
        check_vma=False,
    )
```

```python
import functools

import jax
import jax.numpy as jnp
import numpy as np
from jax import lax
from jax.experimental import pallas as pl
from jax.experimental.pallas import tpu as pltpu
from jax.sharding import PartitionSpec as P

LEVELS = 7
CSWEEPS = 4


rsd_beta = 0.5
centre = 4.0 + 2.0 * (1.0 + rsd_beta)


def extended_2(value, sides, width):
    for axis, dim in sides:
        count, length = (lax.axis_size(axis), value.shape[dim])
        up = [(i, (i + 1) % count) for i in range(count - 1)]
        down = [(j, i) for i, j in up]
        last = lax.slice_in_dim(value, length - width, length, axis=dim)
        leading = lax.slice_in_dim(value, 0, width, axis=dim)
        before = lax.ppermute(last, axis, up)
        after = lax.ppermute(leading, axis, down)
        value = jnp.concatenate([before, value, after], axis=dim)
    return value


def stencil_sum(padded):
    plane = (
        padded[2:, 1:-1, 1:-1]
        + padded[:-2, 1:-1, 1:-1]
        + padded[1:-1, 2:, 1:-1]
        + padded[1:-1, :-2, 1:-1]
    )
    sight = padded[1:-1, 1:-1, 2:] + padded[1:-1, 1:-1, :-2]
    return plane + (1.0 + rsd_beta) * sight


def grid_index(shape, starts):
    return [lax.broadcasted_iota(jnp.int32, shape, which) + starts[which] for which in range(3)]


def parity_of(shape, starts):
    position = grid_index(shape, starts)
    return (position[0] + position[1] + position[2] + 6) % 2


def inside_grid(shape, starts, whole):
    position = grid_index(shape, starts)
    keep = (position[0] >= 0) & (position[0] < whole[0])
    for which in (1, 2):
        keep = keep & (position[which] >= 0) & (position[which] < whole[which])
    return keep


def half_sweep(field, source, scale, chosen):
    update = (source / scale + stencil_sum(jnp.pad(field, 1))) / centre
    return jnp.where(chosen, update, field)


def full_sweep(field, source, scale, parity):
    field = half_sweep(field, source, scale, parity == 0)
    return half_sweep(field, source, scale, parity == 1)


def restrict(residue):
    shape = residue.shape
    blocks = residue.reshape(shape[0] // 2, 2, shape[1] // 2, 2, shape[2] // 2, 2)
    return jnp.mean(blocks, axis=(1, 3, 5))


def prolong(coarse):
    return jnp.repeat(jnp.repeat(jnp.repeat(coarse, 2, 0), 2, 1), 2, 2)


def local_cycle(source, level):
    scale = 0.25**level
    parity = parity_of(source.shape, (0, 0, 0))
    field = jnp.zeros_like(source)
    if level == LEVELS - 1:
        for number in range(CSWEEPS):
            field = full_sweep(field, source, scale, parity)
        return field
    for number in range(2):
        field = full_sweep(field, source, scale, parity)
    residue = source - scale * (centre * field - stencil_sum(jnp.pad(field, 1)))
    field = field + prolong(local_cycle(restrict(residue), level + 1))
    for number in range(2):
        field = full_sweep(field, source, scale, parity)
    return field


def faces(field):
    return extended_2(field, (("gx", 0), ("gy", 1), ("gz", 2)), 1)


def wide(field):
    return extended_2(field, (("gx", 0), ("gy", 1), ("gz", 2)), 2)


def block_starts(shape, margin):
    return (
        lax.axis_index("gx") * shape[0] - margin,
        lax.axis_index("gy") * shape[1] - margin,
        lax.axis_index("gz") * shape[2] - margin,
    )


def padded_half(padded, source, scale, chosen):
    field = padded[1:-1, 1:-1, 1:-1]
    update = (source / scale + stencil_sum(padded)) / centre
    return jnp.where(chosen, update, field)


def wide_sweep(extended, wide_source, scale, red_wide, source, black):
    update = (wide_source / scale + stencil_sum(jnp.pad(extended, 1))) / centre
    extended = jnp.where(red_wide, update, extended)
    return padded_half(extended[1:-1, 1:-1, 1:-1], source, scale, black)


def coarse_level(source, level):
    shape = source.shape
    stack = lax.all_gather(source[None], ("gx", "gy", "gz"), axis=0, tiled=True)
    count_x, count_y, count_z = (lax.axis_size("gx"), lax.axis_size("gy"), lax.axis_size("gz"))
    whole = stack.reshape(count_x, count_y, count_z, shape[0], shape[1], shape[2])
    whole = whole.transpose(0, 3, 1, 4, 2, 5).reshape(
        count_x * shape[0], count_y * shape[1], count_z * shape[2]
    )
    solved = local_cycle(whole, level)
    starts = block_starts(shape, 0)
    return lax.dynamic_slice(solved, starts, shape)


def shared_cycle(source, level, top):
    if level == top:
        return coarse_level(source, level)
    scale = 0.25**level
    shape = source.shape
    whole = (
        shape[0] * lax.axis_size("gx"),
        shape[1] * lax.axis_size("gy"),
        shape[2] * lax.axis_size("gz"),
    )
    parity = parity_of(shape, block_starts(shape, 0))
    black = parity == 1
    wide_shape = (shape[0] + 4, shape[1] + 4, shape[2] + 4)
    wide_starts = block_starts(shape, 2)
    red_wide = (parity_of(wide_shape, wide_starts) == 0) & inside_grid(
        wide_shape, wide_starts, whole
    )
    wide_source = wide(source)
    field = wide_sweep(
        jnp.zeros(wide_shape, jnp.float32), wide_source, scale, red_wide, source, black
    )
    field = wide_sweep(wide(field), wide_source, scale, red_wide, source, black)
    residue = source - scale * (centre * field - stencil_sum(faces(field)))
    field = field + prolong(shared_cycle(restrict(residue), level + 1, top))
    for number in range(2):
        field = wide_sweep(wide(field), wide_source, scale, red_wide, source, black)
    return field


def pairs(count, first):
    swaps = []
    for i in range(first, count - 1, 2):
        swaps += [(i, i + 1), (i + 1, i)]
    return swaps


def flips(count, bit):
    return [(i, i ^ bit) for i in range(count)]


def lanes_of(shape):
    return lax.broadcasted_iota(jnp.int32, shape, len(shape) - 1)


def rows_of(shape):
    return lax.broadcasted_iota(jnp.int32, shape, len(shape) - 2)


LANES = 128
PAD = 8


def odd_of(shape):
    return ((lanes_of(shape) + rows_of(shape)) & 1) == 1


def exact_dot(a, b):
    return jnp.dot(a, b, precision=lax.Precision.HIGHEST, preferred_element_type=jnp.float32)


def window(ref, at, column, count, start=0, shift=0):
    if isinstance(start, int):
        return ref[at, column, PAD + start + shift : PAD + start + shift + count, :]
    first = start + (PAD + shift)
    if shift == 0:
        first = pl.multiple_of(first, 8)
    return ref[at, column, pl.ds(first, count), :]


def clear_pads(ref):
    edge = jnp.zeros((PAD, LANES), jnp.float32)
    for at in range(ref.shape[0]):
        for column in range(ref.shape[1]):
            ref[at, column, :PAD, :] = edge
            ref[at, column, ref.shape[2] - PAD :, :] = edge


def block_sums(ref, at, rows):
    lane = lanes_of((rows, LANES))
    values = [window(ref, at, column, rows) for column in range(2)]
    lefts = [pltpu.roll(value, 1, 1) for value in values]
    rights = [pltpu.roll(value, LANES - 1, 1) for value in values]
    sums = []
    for column in range(2):
        left = jnp.where(lane == 0, lefts[1 - column], lefts[column])
        right = jnp.where(lane == LANES - 1, rights[1 - column], rights[column])
        sides = window(ref, at, column, rows, shift=-1) + window(ref, at, column, rows, shift=1)
        sums.append(values[column] + sides + (1.0 + rsd_beta) * (left + right))
    return sums


def block_totals(ref, at, rows, own, odd, to_red, at_low, at_high):
    slots = ref.shape[0]
    totals = []
    for column, total in enumerate(block_sums(ref, at, rows)):
        before = window(ref, (at - 1) % slots, column, rows)
        after = window(ref, (at + 1) % slots, column, rows)
        if at == 0:
            before = jnp.where(at_low, 0.0, before)
        if at == own - 1:
            after = jnp.where(at_high, 0.0, after)
        totals.append(total + (jnp.where(odd, after, before) if to_red else jnp.where(odd, before, after)))
    return totals


def block_mask(own, halo):
    ny, nz = own
    shape = (ny + 2 * halo, LANES)
    row = rows_of(shape) - halo + lax.axis_index("gy") * ny
    inside_y = (row >= 0) & (row < ny * lax.axis_size("gy"))
    masks = []
    for column in range(2):
        lane = lanes_of(shape)
        if column:
            lane = jnp.where(lane < halo, lane + LANES, lane - LANES)
        lane = lane + lax.axis_index("gz") * nz
        inside = inside_y & (lane >= 0) & (lane < nz * lax.axis_size("gz"))
        masks.append(jnp.where(inside, 1.0 / centre, 0.0))
    return masks


def block_plane(at, nx, own_ref, xh_ref, ya_ref, yb_ref, even_y):
    a, b = ya_ref[at], yb_ref[at]
    middle = own_ref[at] if at < nx else xh_ref[at - nx]
    low = jnp.where(even_y, b, a)
    high = jnp.where(even_y, a, b)
    return jnp.concatenate([low, middle, high], axis=0)


def pack_kernel(halo, own_ref, xh_ref, ya_ref, yb_ref, za_ref, zb_ref):
    even_y = lax.axis_index("gy") % 2 == 0
    even_z = lax.axis_index("gz") % 2 == 0
    nx, ny, nz = own_ref.shape
    groups = nz // halo
    shape = (ny + 2 * halo, nz)
    group = lanes_of(shape) // halo
    for j in range(za_ref.shape[0]):
        last = jnp.zeros(shape, jnp.float32)
        first = jnp.zeros(shape, jnp.float32)
        for k in range(groups):
            at = j * groups + k
            if at >= nx + halo:
                break
            plane = block_plane(at, nx, own_ref, xh_ref, ya_ref, yb_ref, even_y)
            last = jnp.where(group == k, pltpu.roll(plane, (halo * k + halo) % nz, 1), last)
            first = jnp.where(group == k, pltpu.roll(plane, halo * k, 1), first)
        za_ref[j] = jnp.where(even_z, last, first)
        zb_ref[j] = jnp.where(even_z, first, last)


def pre_kernel(
    halo, own_ref, xh_ref, ya_ref, yb_ref, za_ref, zb_ref,
    gr_ref, gb_ref, dark_ref, send_ref,
    fr_ref, fb_ref, red_ref, black_ref, rest_ref,
):
    even_y = lax.axis_index("gy") % 2 == 0
    even_z = lax.axis_index("gz") % 2 == 0
    nx, ny, nz = own_ref.shape
    count, _, rows, _ = gr_ref.shape
    own = nx // 2
    groups = nz // halo
    shape = (rows, LANES)
    odd = odd_of(shape)
    masks = block_mask((ny, nz), halo)
    lane = lanes_of(shape)
    low, high = lane < halo, lane >= nz - halo
    inner = slice(halo, halo + ny)
    body = slice(PAD, PAD + rows)
    here = lax.axis_index("gx")
    ends = (here == 0, here == lax.axis_size("gx") - 1)
    clear_pads(red_ref)
    clear_pads(black_ref)

    def columns(at):
        j, k = at // groups, at % groups
        a, b = za_ref[j], zb_ref[j]
        left = jnp.where(even_z, b, a)
        right = jnp.where(even_z, a, b)
        right = pltpu.roll(right, (nz - halo * k) % nz, 1)
        left = pltpu.roll(left, (2 * nz - halo - halo * k) % nz, 1)
        sides = jnp.where(low, right, jnp.where(high, left, 0.0))
        return block_plane(at, nx, own_ref, xh_ref, ya_ref, yb_ref, even_y), sides

    for at in range(count):
        first, second = columns(2 * at), columns(2 * at + 1)
        for c in range(2):
            red = jnp.where(odd, second[c], first[c])
            black = jnp.where(odd, first[c], second[c])
            if c == 0 and at < own:
                fr_ref[at], fb_ref[at] = red[inner], black[inner]
            red = masks[c] * red
            gr_ref[at, c], gb_ref[at, c] = red, masks[c] * black
            red_ref[at, c, body, :] = red
    for at in range(count):
        totals = block_totals(red_ref, at, rows, own, odd, False, *ends)
        for c in range(2):
            black_ref[at, c, body, :] = gb_ref[at, c] + masks[c] * totals[c]
    for at in range(count):
        totals = block_totals(black_ref, at, rows, own, odd, True, *ends)
        for c in range(2):
            red_ref[at, c, body, :] = gr_ref[at, c] + masks[c] * totals[c]
    for at in range(count):
        totals = block_totals(red_ref, at, rows, own, odd, False, *ends)
        for c in range(2):
            value = gb_ref[at, c] + masks[c] * totals[c]
            black_ref[at, c, body, :] = value
            dark_ref[at, c] = value
            if c == 0 and at < own:
                rest_ref[at] = fb_ref[at] + totals[c][inner] - centre * value[inner]
    for at in range(own):
        total = block_totals(black_ref, at, rows, own, odd, True, *ends)[0]
        left_over = fr_ref[at] + total[inner] - centre * red_ref[at, 0, PAD + halo : PAD + halo + ny, :]
        rest_ref[at] = rest_ref[at] + left_over
    half, quarter = ny // 2, nz // 4
    pairs_y = rest_ref[:, pl.ds(0, half, stride=2), :] + rest_ref[:, pl.ds(1, half, stride=2), :]
    column = lanes_of((nz, nz))
    target = 2 * (column % quarter) + (column // quarter) % 2
    weight = jnp.where(rows_of((nz, nz)) // 2 == target, 0.5, 0.0)
    coarse = exact_dot(pairs_y.reshape(own * half, nz), weight).reshape(own, half, nz)
    part = lanes_of((half, nz)) // quarter
    pick = (((rows_of((half, nz)) + part) & 1) == 1) ^ (part >= 2)
    turn = quarter * lax.axis_index("gz")
    for at in range(own // 2):
        packed = pltpu.roll(jnp.where(pick, coarse[2 * at + 1], coarse[2 * at]), turn, 1)
        for member in range(send_ref.shape[0]):
            send_ref[member, at] = packed


def small_shapes(whole):
    return [whole[0] >> (level + 1) for level in range(2, LEVELS - 2)]


def plain_sum(field):
    padded = np.pad(field, ((0, 0), (1, 1), (1, 1), (1, 1)))
    inner = slice(1, -1)
    plane = padded[:, 2:, inner, inner] + padded[:, :-2, inner, inner]
    plane = plane + padded[:, inner, 2:, inner] + padded[:, inner, :-2, inner]
    return plane + (1.0 + rsd_beta) * (padded[:, inner, inner, 2:] + padded[:, inner, inner, :-2])


def plain_cycle(source, level):
    parity = np.indices(source.shape[1:]).sum(axis=0) % 2
    field = np.zeros_like(source)

    def sweeps(field, number):
        for step in range(2 * number):
            field = np.where(parity == step % 2, (source + plain_sum(field)) / centre, field)
        return field

    if level == LEVELS - 1:
        return sweeps(field, CSWEEPS)
    field = sweeps(field, 2)
    rest = source - centre * field + plain_sum(field)
    nx, ny, nz = source.shape[1:]
    rest = rest.reshape(-1, nx // 2, 2, ny // 2, 2, nz // 2, 2).sum(axis=(2, 4, 6)) / 2.0
    coarse = plain_cycle(rest, level + 1)
    for axis in (1, 2, 3):
        coarse = np.repeat(coarse, 2, axis)
    return sweeps(field + coarse, 2)


def cycle_matrix(whole):
    level = LEVELS - 2
    nx, ny, nz = (size >> level for size in whole)
    size = nx * ny * 2 * nz
    unit = np.eye(size).reshape(size, 2 * nz, nx, ny).transpose(0, 2, 3, 1)
    source = unit.reshape(size, nx, ny, nz, 2).sum(axis=-1) / 2.0
    result = np.repeat(plain_cycle(source, level), 2, axis=3)
    return jnp.asarray(result.transpose(0, 3, 1, 2).reshape(size, size), jnp.float32)


def solve_kernel(halo, whole, *refs):
    here_ref, flip_ref, next_ref, both_ref, gr_ref, gb_ref, dark_ref, matrix_ref, out_ref = refs[:9]
    fr1, fb1, red1, black1, rest1, tall_ref, red_ref, work_ref, passing = refs[9:18]
    small = [refs[18 + 4 * i : 22 + 4 * i] for i in range(LEVELS - 4)]
    gx, gy, gz = (lax.axis_index(axis) for axis in ("gx", "gy", "gz"))
    weight_z = 1.0 + rsd_beta
    share = 1.0 / centre
    for ref in (red1, black1, red_ref, work_ref, passing):
        clear_pads(ref)
    for level in small:
        for ref in level[2:]:
            clear_pads(ref)

    members, slots, block_rows, _ = here_ref.shape
    count_y = lax.axis_size("gy")
    count1, _, rows1, _ = fr1.shape
    quarter = LANES // 4
    sources = [
        (ref, jnp.bitwise_xor(gz, bits))
        for ref, bits in ((here_ref, 0), (flip_ref, 2), (next_ref, 1), (both_ref, 3))
    ]
    group = lanes_of((block_rows, LANES)) // quarter
    held = [jnp.bitwise_and(group - which, 3) for _, which in sources]
    for part, target in enumerate((fr1, fr1, fb1, fb1)):
        theirs = [kind == part for kind in held]
        for member in range(members):
            i, j = member // count_y, member % count_y
            for at in range(slots):
                value = sources[0][0][member, at]
                for (ref, _), mine in zip(sources[1:], theirs[1:]):
                    value = jnp.where(mine, ref[member, at], value)
                rows = slice(j * block_rows, (j + 1) * block_rows)
                turned = pltpu.roll(value, LANES - quarter * part, 1) if part else value
                target[i * slots + at, part % 2, rows, :] = turned

    def fold_total(ref, at, e, start, count, low, high, odds, to_red):
        lane = lanes_of((count, LANES))
        value, other = window(ref, at, e, count, start), window(ref, at, 1 - e, count, start)
        sides = window(ref, at, e, count, start, -1) + window(ref, at, e, count, start, 1)
        if e == 0:
            near = jnp.where(lane == 0, 0.0, pltpu.roll(other, 1, 1))
        else:
            near = jnp.where(lane == LANES - 1, 0.0, pltpu.roll(other, LANES - 1, 1))
        before = 0.0 if low is True else window(ref, at - 1, e, count, start)
        after = 0.0 if high is True else window(ref, at + 1, e, count, start)
        if not isinstance(low, bool):
            before = jnp.where(low, 0.0, window(ref, jnp.maximum(at - 1, 0), e, count, start))
        if not isinstance(high, bool):
            after = jnp.where(high, 0.0, window(ref, jnp.minimum(at + 1, count1 - 1), e, count, start))
        beside = jnp.where(odds[e], after, before) if to_red else jnp.where(odds[e], before, after)
        return value + sides + beside + weight_z * (other + near)

    def fold_odds(count):
        row = rows_of((count, LANES))
        return [((row + e) & 1) == 1 for e in range(2)]

    odds = fold_odds(rows1)
    body1 = slice(PAD, PAD + rows1)

    def down_total(ref, at, e, to_red):
        return fold_total(ref, at, e, 0, rows1, at == 0, at == count1 - 1, odds, to_red)

    for at in range(count1):
        for e in range(2):
            red1[at, e, body1, :] = share * fr1[at, e]
    for at in range(count1):
        for e in range(2):
            black1[at, e, body1, :] = share * (fb1[at, e] + down_total(red1, at, e, False))
    for at in range(count1):
        for e in range(2):
            red1[at, e, body1, :] = share * (fr1[at, e] + down_total(black1, at, e, True))
    for at in range(count1):
        left_over = None
        for e in range(2):
            total = fb1[at, e] + down_total(red1, at, e, False)
            value = share * total
            black1[at, e, body1, :] = value
            term = total - centre * value
            left_over = term if left_over is None else left_over + term
        rest1[at] = left_over
    for at in range(count1):
        left_over = rest1[at]
        for e in range(2):
            total = fr1[at, e] + down_total(black1, at, e, True)
            left_over = left_over + (total - centre * window(red1, at, e, rows1))
        rest1[at] = left_over
    rows2 = rows1 // 2
    shape2 = (rows2, LANES)
    row2, lane2 = rows_of(shape2), lanes_of(shape2)
    odd2 = odd_of(shape2)
    planes = [
        0.5 * (rest1[at, pl.ds(0, rows2, stride=2), :] + rest1[at, pl.ds(1, rows2, stride=2), :])
        for at in range(count1)
    ]

    body2 = slice(PAD, PAD + rows2)

    def grid_of(index):
        step = 1 << index
        return ((row2 & (step - 1)) == 0) & ((lane2 & (step - 1)) == 0)

    def odd_at(index):
        return (((row2 >> index) + (lane2 >> index)) & 1) == 1

    def along(value, step):
        left = jnp.where(lane2 < step, 0.0, pltpu.roll(value, step, 1))
        right = jnp.where(lane2 >= LANES - step, 0.0, pltpu.roll(value, LANES - step, 1))
        return weight_z * (left + right)

    def small_total(index, ref, at, odd, to_red):
        step = 1 << index
        value = ref[at, 0, body2, :]
        total = value + along(value, step)
        total = total + (
            ref[at, 0, PAD - step : PAD - step + rows2, :] + ref[at, 0, PAD + step : PAD + step + rows2, :]
        )
        slots = ref.shape[0]
        if slots == 1:
            return total
        before = ref[at - 1, 0, body2, :] if at > 0 else 0.0
        after = ref[at + 1, 0, body2, :] if at < slots - 1 else 0.0
        return total + (jnp.where(odd, after, before) if to_red else jnp.where(odd, before, after))

    def small_sweeps(index, start):
        fr, fb, red, black = small[index]
        mask, odd = jnp.where(grid_of(index), share, 0.0), odd_at(index)
        slots = fr.shape[0]
        for step in range(2):
            for at in range(slots):
                source = fr[at]
                if not (start and step == 0):
                    source = source + small_total(index, black, at, odd, True)
                red[at, 0, body2, :] = mask * source
            for at in range(slots):
                black[at, 0, body2, :] = mask * (fb[at] + small_total(index, red, at, odd, False))

    def spread_rows(value, step, ref, at):
        ref[at, 0, body2, :] = value
        return value + ref[at, 0, PAD - step : PAD - step + rows2, :]

    last = len(small) - 1
    for index in range(len(small)):
        fr, fb, red, black = small[index]
        slots, odd, step = fr.shape[0], odd_at(index), 1 << index
        for at in range(slots):
            p, q = planes[2 * at], planes[2 * at + 1]
            fr[at], fb[at] = jnp.where(odd, q, p), jnp.where(odd, p, q)
        small_sweeps(index, True)
        totals = []
        for at in range(slots):
            first = fb[at] + small_total(index, red, at, odd, False) - centre * black[at, 0, body2, :]
            second = fr[at] + small_total(index, black, at, odd, True) - centre * red[at, 0, body2, :]
            totals.append(first + second)
        for at in range(slots):
            passing[at, 0, body2, :] = totals[at]
        lower = [passing[at, 0, PAD + step : PAD + step + rows2, :] for at in range(slots)]
        if index < last:
            totals = [total + below for total, below in zip(totals, lower)]
            planes = [0.5 * (total + pltpu.roll(total, LANES - step, 1)) for total in totals]

    half_rows = rows2 // 2
    upper = [passing[at, 0, PAD - step : PAD - step + rows2, :] for at in range(slots)]
    odd_line = (row2 & step) != 0
    summed = [
        total + jnp.where(odd_line, above, below) for total, above, below in zip(totals, upper, lower)
    ]
    lines = [total[start : start + half_rows] for total in summed for start in (0, half_rows)]
    place = lanes_of((half_rows, LANES)) & (len(lines) - 1)
    joined = lines[0]
    for q in range(1, len(lines)):
        joined = jnp.where(place == q, pltpu.roll(lines[q], q, 1), joined)
    answer = exact_dot(joined, matrix_ref[...])
    grid = (place == 0) & ((rows_of((half_rows, LANES)) & (step - 1)) == 0)
    parts = []
    for q in range(len(lines)):
        part = pltpu.roll(answer, LANES - q, 1) if q else answer
        parts.append(jnp.where(grid, part, 0.0))
    spreads = [jnp.concatenate(parts[2 * at : 2 * at + 2], axis=0) for at in range(slots)]

    for index in reversed(range(len(small))):
        _, _, red, black = small[index]
        slots, odd, step = red.shape[0], odd_at(index), 1 << index
        if index < last:
            spreads = [
                spread_rows(field + pltpu.roll(field, step, 1), step, passing, at)
                for at, field in enumerate(fields)
            ]
        for at in range(slots):
            black[at, 0, body2, :] = black[at, 0, body2, :] + spreads[at]
        small_sweeps(index, False)
        fields = []
        for at in range(slots):
            r, b = red[at, 0, body2, :], black[at, 0, body2, :]
            fields += [jnp.where(odd, b, r), jnp.where(odd, r, b)]

    for at in range(count1):
        for start in range(2):
            rest1[at, pl.ds(start, rows2, stride=2), :] = fields[at]
    for at in range(count1):
        for e in range(2):
            black1[at, e, body1, :] = window(black1, at, e, rows1) + rest1[at]
    nx, ny, nz = out_ref.shape
    own = nx // 2
    part_slots = min(own // 2 + 3, count1)
    part_rows = min(ny // 2 + 16, rows1)
    slot0 = jnp.where(gx == 0, 0, count1 - part_slots)
    row0 = pl.multiple_of(jnp.clip(gy * (ny // 2) - 8, 0, rows1 - part_rows), 8)
    odds = fold_odds(part_rows)

    def up_total(ref, at, e, to_red):
        low = gx == 0 if at == 0 else False
        high = gx != 0 if at == part_slots - 1 else False
        return fold_total(ref, slot0 + at, e, row0, part_rows, low, high, odds, to_red)

    def up_half(target, other, sources, to_red):
        for at in range(part_slots):
            for e in range(2):
                source = sources[slot0 + at, e, pl.ds(row0, part_rows), :]
                value = share * (source + up_total(other, at, e, to_red))
                target[slot0 + at, e, pl.ds(pl.multiple_of(row0 + PAD, 8), part_rows), :] = value

    for sweep in range(2):
        up_half(red1, black1, fr1, True)
        up_half(black1, red1, fb1, False)

    count, _, rows, _ = dark_ref.shape
    half = rows // 2
    odds = fold_odds(half)
    row = gy * (ny // 2) + (PAD - halo // 2)
    for at in range(count):
        if at < own:
            slot = gx * (own // 2) + at // 2
        else:
            slot = jnp.where(gx == 0, own // 2, own // 2 - (count - own) // 2) + (at - own) // 2
        for e in range(2):
            r, b = red1[slot, e, pl.ds(row, half), :], black1[slot, e, pl.ds(row, half), :]
            plane = jnp.where(odds[e], r, b) if at % 2 else jnp.where(odds[e], b, r)
            tall_ref[at, :, e * LANES : (e + 1) * LANES] = plane
    shape = (2 * LANES, 2 * LANES)
    z = lanes_of(shape)
    z = jnp.where(z < 2 * LANES - halo, z, z - 2 * LANES) + gz * nz
    line = rows_of(shape)
    line = jnp.where(line < LANES, 2 * line, 2 * (line - LANES) + 1)
    weight = jnp.where(line == lax.shift_right_arithmetic(z, 1), 1.0, 0.0)
    spread = exact_dot(tall_ref[...].reshape(count * half, 2 * LANES), weight)
    spread = spread.reshape(count, half, 2 * LANES)
    for at in range(count):
        for c in range(2):
            value = spread[at, :, c * LANES : (c + 1) * LANES]
            for start in range(2):
                work_ref[at, c, pl.ds(PAD + start, half, stride=2), :] = value
    body = slice(PAD, PAD + rows)
    for at in range(count):
        for c in range(2):
            work_ref[at, c, body, :] = work_ref[at, c, body, :] + dark_ref[at, c]
    odd = odd_of((rows, LANES))
    masks = block_mask((ny, nz), halo)
    ends = (gx == 0, gx == lax.axis_size("gx") - 1)
    for sweep in range(2):
        for at in range(count):
            totals = block_totals(work_ref, at, rows, own, odd, True, *ends)
            for c in range(2):
                red_ref[at, c, body, :] = gr_ref[at, c] + masks[c] * totals[c]
        for at in range(count if sweep == 0 else own):
            totals = block_totals(red_ref, at, rows, own, odd, False, *ends)
            for c in range(2 if sweep == 0 else 1):
                work_ref[at, c, body, :] = gb_ref[at, c] + masks[c] * totals[c]
    inner = slice(PAD + halo, PAD + halo + ny)
    odd = odd_of((ny, nz))
    for at in range(own):
        r, b = red_ref[at, 0, inner, :], work_ref[at, 0, inner, :]
        out_ref[2 * at] = jnp.where(odd, b, r)
        out_ref[2 * at + 1] = jnp.where(odd, r, b)


def vmem(number):
    return [pl.BlockSpec(memory_space=pltpu.VMEM)] * number


def struct(*shape):
    return jax.ShapeDtypeStruct(shape, jnp.float32)


def scratch(*shape):
    return pltpu.VMEM(shape, jnp.float32)


HALO = 8


def block_cycle(density):
    halo = HALO
    nx, ny, nz = density.shape
    count_x, count_y, count_z = (lax.axis_size(axis) for axis in ("gx", "gy", "gz"))
    whole = (nx * count_x, ny * count_y, nz * count_z)
    gx, gy = lax.axis_index("gx"), lax.axis_index("gy")
    face = lax.dynamic_slice_in_dim(density, jnp.where(gx == 0, nx - halo, 0), halo, 0)
    side = lax.ppermute(face, "gx", flips(count_x, 1))
    tall = jnp.concatenate([density, side], axis=0)
    even = gy % 2 == 0
    ya = lax.dynamic_slice_in_dim(tall, jnp.where(even, ny - halo, 0), halo, 1)
    yb = lax.dynamic_slice_in_dim(tall, jnp.where(even, 0, ny - halo), halo, 1)
    ya = lax.ppermute(ya, "gy", pairs(count_y, 0))
    yb = lax.ppermute(yb, "gy", pairs(count_y, 1))
    rows = ny + 2 * halo
    planes = nx + halo
    packs = -(-planes * halo // nz)

    def params(mib):
        return pltpu.CompilerParams(vmem_limit_bytes=mib * 1024 * 1024)

    za, zb = pl.pallas_call(
        functools.partial(pack_kernel, halo),
        out_shape=[struct(packs, rows, nz)] * 2,
        in_specs=vmem(4), out_specs=vmem(2), compiler_params=params(4),
    )(density, side, ya, yb)
    za = lax.ppermute(za, "gz", pairs(count_z, 0))
    zb = lax.ppermute(zb, "gz", pairs(count_z, 1) + [(0, count_z - 1), (count_z - 1, 0)])
    members = count_x * count_y
    slots = (planes // 2, 2, rows, LANES)
    padded = (planes // 2, 2, rows + 2 * PAD, LANES)
    gr, gb, black, send = pl.pallas_call(
        functools.partial(pre_kernel, halo),
        out_shape=[struct(*slots)] * 3 + [struct(members, nx // 4, ny // 2, nz)],
        in_specs=vmem(6), out_specs=vmem(4), compiler_params=params(10),
        scratch_shapes=[scratch(nx // 2, ny, nz)] * 2
        + [scratch(*padded)] * 2
        + [scratch(nx // 2, ny, nz)],
    )(density, side, ya, yb, za, zb)
    here = lax.all_to_all(send, ("gx", "gy"), 0, 0, tiled=True)
    flip = lax.ppermute(here, "gz", flips(count_z, 2))
    beside_here = lax.ppermute(here, "gz", flips(count_z, 1))
    beside_flip = lax.ppermute(flip, "gz", flips(count_z, 1))
    count1, rows1, rows2 = whole[0] // 4, whole[1] // 2, whole[1] // 4
    room = [scratch(count1, 2, rows1, LANES)] * 2
    room += [scratch(count1, 2, rows1 + 2 * PAD, LANES)] * 2
    room += [scratch(count1, rows1, LANES), scratch(planes // 2, rows // 2, 2 * LANES)]
    room += [scratch(*padded)] * 2 + [scratch(count1 // 2, 1, rows2 + 2 * PAD, LANES)]
    for count in small_shapes(whole):
        room += [scratch(count, rows2, LANES)] * 2
        room += [scratch(count, 1, rows2 + 2 * PAD, LANES)] * 2
    return pl.pallas_call(
        functools.partial(solve_kernel, halo, whole),
        out_shape=struct(nx, ny, nz),
        in_specs=vmem(8), out_specs=pl.BlockSpec(memory_space=pltpu.VMEM),
        compiler_params=params(16), scratch_shapes=room,
    )(here, flip, beside_here, beside_flip, gr, gb, black, cycle_matrix(whole))


def fits_block_cycle(shape):
    nx, ny, nz = shape
    count_x, count_y, count_z = (lax.axis_size(axis) for axis in ("gx", "gy", "gz"))
    whole = (nx * count_x, ny * count_y, nz * count_z)
    coarsest = [size >> (LEVELS - 1) for size in whole]
    exact = all(c << (LEVELS - 1) == size for c, size in zip(coarsest, whole))
    return (
        exact and coarsest[0] == coarsest[1] == 1 and nz == LANES and ny == 2 * HALO
        and count_x == 2 and count_z == 4 and count_y % 2 == 0
    )


def on_device(density):
    if fits_block_cycle(density.shape):
        return block_cycle(density)
    top = 4
    return shared_cycle(density, 0, top)


def solution(mesh):
    return jax.shard_map(
        on_device,
        mesh=mesh,
        in_specs=(P("gx", "gy", "gz"),),
        out_specs=P("gx", "gy", "gz"),
        check_vma=False,
    )
```

```python
import functools

import jax
import jax.numpy as jnp
import numpy as np
from jax import lax
from jax.experimental import pallas as pl
from jax.experimental.pallas import tpu as pltpu
from jax.sharding import PartitionSpec as P

LEVELS = 7
CSWEEPS = 4


rsd_beta = 0.5
centre = 4.0 + 2.0 * (1.0 + rsd_beta)


def extended_2(value, sides, width):
    for axis, dim in sides:
        count, length = (lax.axis_size(axis), value.shape[dim])
        up = [(i, (i + 1) % count) for i in range(count - 1)]
        down = [(j, i) for i, j in up]
        last = lax.slice_in_dim(value, length - width, length, axis=dim)
        leading = lax.slice_in_dim(value, 0, width, axis=dim)
        before = lax.ppermute(last, axis, up)
        after = lax.ppermute(leading, axis, down)
        value = jnp.concatenate([before, value, after], axis=dim)
    return value


def stencil_sum(padded):
    plane = (
        padded[2:, 1:-1, 1:-1]
        + padded[:-2, 1:-1, 1:-1]
        + padded[1:-1, 2:, 1:-1]
        + padded[1:-1, :-2, 1:-1]
    )
    sight = padded[1:-1, 1:-1, 2:] + padded[1:-1, 1:-1, :-2]
    return plane + (1.0 + rsd_beta) * sight


def grid_index(shape, starts):
    return [lax.broadcasted_iota(jnp.int32, shape, which) + starts[which] for which in range(3)]


def parity_of(shape, starts):
    position = grid_index(shape, starts)
    return (position[0] + position[1] + position[2] + 6) % 2


def inside_grid(shape, starts, whole):
    position = grid_index(shape, starts)
    keep = (position[0] >= 0) & (position[0] < whole[0])
    for which in (1, 2):
        keep = keep & (position[which] >= 0) & (position[which] < whole[which])
    return keep


def half_sweep(field, source, scale, chosen):
    update = (source / scale + stencil_sum(jnp.pad(field, 1))) / centre
    return jnp.where(chosen, update, field)


def full_sweep(field, source, scale, parity):
    field = half_sweep(field, source, scale, parity == 0)
    return half_sweep(field, source, scale, parity == 1)


def restrict(residue):
    shape = residue.shape
    blocks = residue.reshape(shape[0] // 2, 2, shape[1] // 2, 2, shape[2] // 2, 2)
    return jnp.mean(blocks, axis=(1, 3, 5))


def prolong(coarse):
    return jnp.repeat(jnp.repeat(jnp.repeat(coarse, 2, 0), 2, 1), 2, 2)


def local_cycle(source, level):
    scale = 0.25**level
    parity = parity_of(source.shape, (0, 0, 0))
    field = jnp.zeros_like(source)
    if level == LEVELS - 1:
        for number in range(CSWEEPS):
            field = full_sweep(field, source, scale, parity)
        return field
    for number in range(2):
        field = full_sweep(field, source, scale, parity)
    residue = source - scale * (centre * field - stencil_sum(jnp.pad(field, 1)))
    field = field + prolong(local_cycle(restrict(residue), level + 1))
    for number in range(2):
        field = full_sweep(field, source, scale, parity)
    return field


def faces(field):
    return extended_2(field, (("gx", 0), ("gy", 1), ("gz", 2)), 1)


def wide(field):
    return extended_2(field, (("gx", 0), ("gy", 1), ("gz", 2)), 2)


def block_starts(shape, margin):
    return (
        lax.axis_index("gx") * shape[0] - margin,
        lax.axis_index("gy") * shape[1] - margin,
        lax.axis_index("gz") * shape[2] - margin,
    )


def padded_half(padded, source, scale, chosen):
    field = padded[1:-1, 1:-1, 1:-1]
    update = (source / scale + stencil_sum(padded)) / centre
    return jnp.where(chosen, update, field)


def wide_sweep(extended, wide_source, scale, red_wide, source, black):
    update = (wide_source / scale + stencil_sum(jnp.pad(extended, 1))) / centre
    extended = jnp.where(red_wide, update, extended)
    return padded_half(extended[1:-1, 1:-1, 1:-1], source, scale, black)


def coarse_level(source, level):
    shape = source.shape
    stack = lax.all_gather(source[None], ("gx", "gy", "gz"), axis=0, tiled=True)
    count_x, count_y, count_z = (lax.axis_size("gx"), lax.axis_size("gy"), lax.axis_size("gz"))
    whole = stack.reshape(count_x, count_y, count_z, shape[0], shape[1], shape[2])
    whole = whole.transpose(0, 3, 1, 4, 2, 5).reshape(
        count_x * shape[0], count_y * shape[1], count_z * shape[2]
    )
    solved = local_cycle(whole, level)
    starts = block_starts(shape, 0)
    return lax.dynamic_slice(solved, starts, shape)


def shared_cycle(source, level, top):
    if level == top:
        return coarse_level(source, level)
    scale = 0.25**level
    shape = source.shape
    whole = (
        shape[0] * lax.axis_size("gx"),
        shape[1] * lax.axis_size("gy"),
        shape[2] * lax.axis_size("gz"),
    )
    parity = parity_of(shape, block_starts(shape, 0))
    black = parity == 1
    wide_shape = (shape[0] + 4, shape[1] + 4, shape[2] + 4)
    wide_starts = block_starts(shape, 2)
    red_wide = (parity_of(wide_shape, wide_starts) == 0) & inside_grid(
        wide_shape, wide_starts, whole
    )
    wide_source = wide(source)
    field = wide_sweep(
        jnp.zeros(wide_shape, jnp.float32), wide_source, scale, red_wide, source, black
    )
    field = wide_sweep(wide(field), wide_source, scale, red_wide, source, black)
    residue = source - scale * (centre * field - stencil_sum(faces(field)))
    field = field + prolong(shared_cycle(restrict(residue), level + 1, top))
    for number in range(2):
        field = wide_sweep(wide(field), wide_source, scale, red_wide, source, black)
    return field


def pairs(count, first):
    swaps = []
    for i in range(first, count - 1, 2):
        swaps += [(i, i + 1), (i + 1, i)]
    return swaps


def inner_pairs(count_x, count):
    swaps = []
    for x in range(count_x):
        swaps += [(x * count + i, x * count + j) for i, j in pairs(count, 1)]
        swaps += [(x * count + i, (x ^ 1) * count + i) for i in (0, count - 1)]
    return swaps


def flips(count, bit):
    return [(i, i ^ bit) for i in range(count)]


def lanes_of(shape):
    return lax.broadcasted_iota(jnp.int32, shape, len(shape) - 1)


def rows_of(shape):
    return lax.broadcasted_iota(jnp.int32, shape, len(shape) - 2)


LANES = 128
PAD = 8


def odd_of(shape):
    return ((lanes_of(shape) + rows_of(shape)) & 1) == 1


def exact_dot(a, b):
    return jnp.dot(a, b, precision=lax.Precision.HIGHEST, preferred_element_type=jnp.float32)


def window(ref, at, column, count, start=0, shift=0):
    if isinstance(start, int):
        return ref[at, column, PAD + start + shift : PAD + start + shift + count, :]
    first = start + (PAD + shift)
    if shift == 0:
        first = pl.multiple_of(first, 8)
    return ref[at, column, pl.ds(first, count), :]


def clear_pads(ref):
    edge = jnp.zeros((PAD, LANES), jnp.float32)
    for at in range(ref.shape[0]):
        for column in range(ref.shape[1]):
            ref[at, column, :PAD, :] = edge
            ref[at, column, ref.shape[2] - PAD :, :] = edge


def block_sums(ref, at, rows):
    lane = lanes_of((rows, LANES))
    values = [window(ref, at, column, rows) for column in range(2)]
    lefts = [pltpu.roll(value, 1, 1) for value in values]
    rights = [pltpu.roll(value, LANES - 1, 1) for value in values]
    sums = []
    for column in range(2):
        left = jnp.where(lane == 0, lefts[1 - column], lefts[column])
        right = jnp.where(lane == LANES - 1, rights[1 - column], rights[column])
        sides = window(ref, at, column, rows, shift=-1) + window(ref, at, column, rows, shift=1)
        sums.append(values[column] + sides + (1.0 + rsd_beta) * (left + right))
    return sums


def block_totals(ref, at, rows, own, odd, to_red, at_low, at_high):
    slots = ref.shape[0]
    totals = []
    for column, total in enumerate(block_sums(ref, at, rows)):
        before = window(ref, (at - 1) % slots, column, rows)
        after = window(ref, (at + 1) % slots, column, rows)
        if at == 0:
            before = jnp.where(at_low, 0.0, before)
        if at == own - 1:
            after = jnp.where(at_high, 0.0, after)
        totals.append(total + (jnp.where(odd, after, before) if to_red else jnp.where(odd, before, after)))
    return totals


def block_mask(own, halo):
    ny, nz = own
    shape = (ny + 2 * halo, LANES)
    row = rows_of(shape) - halo + lax.axis_index("gy") * ny
    inside_y = (row >= 0) & (row < ny * lax.axis_size("gy"))
    masks = []
    for column in range(2):
        lane = lanes_of(shape)
        if column:
            lane = jnp.where(lane < halo, lane + LANES, lane - LANES)
        lane = lane + lax.axis_index("gz") * nz
        inside = inside_y & (lane >= 0) & (lane < nz * lax.axis_size("gz"))
        masks.append(jnp.where(inside, 1.0 / centre, 0.0))
    return masks


def block_plane(at, nx, own_ref, xh_ref, ya_ref, yb_ref, even_y):
    a, b = ya_ref[at], yb_ref[at]
    middle = own_ref[at] if at < nx else xh_ref[at - nx]
    low = jnp.where(even_y, b, a)
    high = jnp.where(even_y, a, b)
    return jnp.concatenate([low, middle, high], axis=0)


def pack_kernel(halo, own_ref, xh_ref, ya_ref, yb_ref, za_ref, zb_ref):
    even_y = lax.axis_index("gy") % 2 == 0
    even_z = lax.axis_index("gz") % 2 == 0
    nx, ny, nz = own_ref.shape
    groups = nz // halo
    shape = (ny + 2 * halo, nz)
    group = lanes_of(shape) // halo
    for j in range(za_ref.shape[0]):
        last = jnp.zeros(shape, jnp.float32)
        first = jnp.zeros(shape, jnp.float32)
        for k in range(groups):
            at = j * groups + k
            if at >= nx + halo:
                break
            plane = block_plane(at, nx, own_ref, xh_ref, ya_ref, yb_ref, even_y)
            last = jnp.where(group == k, pltpu.roll(plane, (halo * k + halo) % nz, 1), last)
            first = jnp.where(group == k, pltpu.roll(plane, halo * k, 1), first)
        za_ref[j] = jnp.where(even_z, last, first)
        zb_ref[j] = jnp.where(even_z, first, last)


def pre_kernel(
    halo, own_ref, xh_ref, ya_ref, yb_ref, za_ref, zb_ref,
    gr_ref, gb_ref, dark_ref, send_ref,
    fr_ref, fb_ref, red_ref, black_ref, rest_ref,
):
    even_y = lax.axis_index("gy") % 2 == 0
    even_z = lax.axis_index("gz") % 2 == 0
    nx, ny, nz = own_ref.shape
    count, _, rows, _ = gr_ref.shape
    own = nx // 2
    groups = nz // halo
    shape = (rows, LANES)
    odd = odd_of(shape)
    masks = block_mask((ny, nz), halo)
    lane = lanes_of(shape)
    low, high = lane < halo, lane >= nz - halo
    inner = slice(halo, halo + ny)
    body = slice(PAD, PAD + rows)
    here = lax.axis_index("gx")
    ends = (here == 0, here == lax.axis_size("gx") - 1)
    clear_pads(red_ref)
    clear_pads(black_ref)

    def columns(at):
        j, k = at // groups, at % groups
        a, b = za_ref[j], zb_ref[j]
        left = jnp.where(even_z, b, a)
        right = jnp.where(even_z, a, b)
        right = pltpu.roll(right, (nz - halo * k) % nz, 1)
        left = pltpu.roll(left, (2 * nz - halo - halo * k) % nz, 1)
        sides = jnp.where(low, right, jnp.where(high, left, 0.0))
        return block_plane(at, nx, own_ref, xh_ref, ya_ref, yb_ref, even_y), sides

    for at in range(count):
        first, second = columns(2 * at), columns(2 * at + 1)
        for c in range(2):
            red = jnp.where(odd, second[c], first[c])
            black = jnp.where(odd, first[c], second[c])
            if c == 0 and at < own:
                fr_ref[at], fb_ref[at] = red[inner], black[inner]
            red = masks[c] * red
            gr_ref[at, c], gb_ref[at, c] = red, masks[c] * black
            red_ref[at, c, body, :] = red
    for at in range(count):
        totals = block_totals(red_ref, at, rows, own, odd, False, *ends)
        for c in range(2):
            black_ref[at, c, body, :] = gb_ref[at, c] + masks[c] * totals[c]
    for at in range(count):
        totals = block_totals(black_ref, at, rows, own, odd, True, *ends)
        for c in range(2):
            red_ref[at, c, body, :] = gr_ref[at, c] + masks[c] * totals[c]
    for at in range(count):
        totals = block_totals(red_ref, at, rows, own, odd, False, *ends)
        for c in range(2):
            value = gb_ref[at, c] + masks[c] * totals[c]
            black_ref[at, c, body, :] = value
            dark_ref[at, c] = value
            if c == 0 and at < own:
                rest_ref[at] = fb_ref[at] + totals[c][inner] - centre * value[inner]
    for at in range(own):
        total = block_totals(black_ref, at, rows, own, odd, True, *ends)[0]
        left_over = fr_ref[at] + total[inner] - centre * red_ref[at, 0, PAD + halo : PAD + halo + ny, :]
        rest_ref[at] = rest_ref[at] + left_over
    half, quarter = ny // 2, nz // 4
    pairs_y = rest_ref[:, pl.ds(0, half, stride=2), :] + rest_ref[:, pl.ds(1, half, stride=2), :]
    column = lanes_of((nz, nz))
    target = 2 * (column % quarter) + (column // quarter) % 2
    weight = jnp.where(rows_of((nz, nz)) // 2 == target, 0.5, 0.0)
    coarse = exact_dot(pairs_y.reshape(own * half, nz), weight).reshape(own, half, nz)
    part = lanes_of((half, nz)) // quarter
    pick = (((rows_of((half, nz)) + part) & 1) == 1) ^ (part >= 2)
    turn = quarter * lax.axis_index("gz")
    for at in range(own // 2):
        packed = pltpu.roll(jnp.where(pick, coarse[2 * at + 1], coarse[2 * at]), turn, 1)
        for member in range(send_ref.shape[0]):
            send_ref[member, at] = packed


def small_shapes(whole):
    return [whole[0] >> (level + 1) for level in range(2, LEVELS - 2)]


def plain_sum(field):
    padded = np.pad(field, ((0, 0), (1, 1), (1, 1), (1, 1)))
    inner = slice(1, -1)
    plane = padded[:, 2:, inner, inner] + padded[:, :-2, inner, inner]
    plane = plane + padded[:, inner, 2:, inner] + padded[:, inner, :-2, inner]
    return plane + (1.0 + rsd_beta) * (padded[:, inner, inner, 2:] + padded[:, inner, inner, :-2])


def plain_cycle(source, level):
    parity = np.indices(source.shape[1:]).sum(axis=0) % 2
    field = np.zeros_like(source)

    def sweeps(field, number):
        for step in range(2 * number):
            field = np.where(parity == step % 2, (source + plain_sum(field)) / centre, field)
        return field

    if level == LEVELS - 1:
        return sweeps(field, CSWEEPS)
    field = sweeps(field, 2)
    rest = source - centre * field + plain_sum(field)
    nx, ny, nz = source.shape[1:]
    rest = rest.reshape(-1, nx // 2, 2, ny // 2, 2, nz // 2, 2).sum(axis=(2, 4, 6)) / 2.0
    coarse = plain_cycle(rest, level + 1)
    for axis in (1, 2, 3):
        coarse = np.repeat(coarse, 2, axis)
    return sweeps(field + coarse, 2)


def cycle_matrix(whole):
    level = LEVELS - 2
    nx, ny, nz = (size >> level for size in whole)
    size = nx * ny * 2 * nz
    unit = np.eye(size).reshape(size, 2 * nz, nx, ny).transpose(0, 2, 3, 1)
    source = unit.reshape(size, nx, ny, nz, 2).sum(axis=-1) / 2.0
    result = np.repeat(plain_cycle(source, level), 2, axis=3)
    return jnp.asarray(result.transpose(0, 3, 1, 2).reshape(size, size), jnp.float32)


def solve_kernel(halo, whole, *refs):
    here_ref, flip_ref, next_ref, both_ref, gr_ref, gb_ref, dark_ref, matrix_ref, out_ref = refs[:9]
    fr1, fb1, red1, black1, rest1, tall_ref, red_ref, work_ref, passing = refs[9:18]
    small = [refs[18 + 4 * i : 22 + 4 * i] for i in range(LEVELS - 4)]
    gx, gy, gz = (lax.axis_index(axis) for axis in ("gx", "gy", "gz"))
    weight_z = 1.0 + rsd_beta
    share = 1.0 / centre
    for ref in (red1, black1, red_ref, work_ref, passing):
        clear_pads(ref)
    for level in small:
        for ref in level[2:]:
            clear_pads(ref)

    members, slots, block_rows, _ = here_ref.shape
    count_y = lax.axis_size("gy")
    count1, _, rows1, _ = fr1.shape
    quarter = LANES // 4
    sources = [
        (ref, jnp.bitwise_xor(gz, bits))
        for ref, bits in ((here_ref, 0), (flip_ref, 2), (next_ref, 1), (both_ref, 3))
    ]
    group = lanes_of((block_rows, LANES)) // quarter
    held = [jnp.bitwise_and(group - which, 3) for _, which in sources]
    for part, target in enumerate((fr1, fr1, fb1, fb1)):
        theirs = [kind == part for kind in held]
        for member in range(members):
            i, j = member // count_y, member % count_y
            for at in range(slots):
                value = sources[0][0][member, at]
                for (ref, _), mine in zip(sources[1:], theirs[1:]):
                    value = jnp.where(mine, ref[member, at], value)
                rows = slice(j * block_rows, (j + 1) * block_rows)
                turned = pltpu.roll(value, LANES - quarter * part, 1) if part else value
                target[i * slots + at, part % 2, rows, :] = turned

    def fold_total(ref, at, e, start, count, low, high, odds, to_red):
        lane = lanes_of((count, LANES))
        value, other = window(ref, at, e, count, start), window(ref, at, 1 - e, count, start)
        sides = window(ref, at, e, count, start, -1) + window(ref, at, e, count, start, 1)
        if e == 0:
            near = jnp.where(lane == 0, 0.0, pltpu.roll(other, 1, 1))
        else:
            near = jnp.where(lane == LANES - 1, 0.0, pltpu.roll(other, LANES - 1, 1))
        before = 0.0 if low is True else window(ref, at - 1, e, count, start)
        after = 0.0 if high is True else window(ref, at + 1, e, count, start)
        if not isinstance(low, bool):
            before = jnp.where(low, 0.0, window(ref, jnp.maximum(at - 1, 0), e, count, start))
        if not isinstance(high, bool):
            after = jnp.where(high, 0.0, window(ref, jnp.minimum(at + 1, count1 - 1), e, count, start))
        beside = jnp.where(odds[e], after, before) if to_red else jnp.where(odds[e], before, after)
        return value + sides + beside + weight_z * (other + near)

    def fold_odds(count):
        row = rows_of((count, LANES))
        return [((row + e) & 1) == 1 for e in range(2)]

    odds = fold_odds(rows1)
    body1 = slice(PAD, PAD + rows1)

    def down_total(ref, at, e, to_red):
        return fold_total(ref, at, e, 0, rows1, at == 0, at == count1 - 1, odds, to_red)

    for at in range(count1):
        for e in range(2):
            red1[at, e, body1, :] = share * fr1[at, e]
    for at in range(count1):
        for e in range(2):
            black1[at, e, body1, :] = share * (fb1[at, e] + down_total(red1, at, e, False))
    for at in range(count1):
        for e in range(2):
            red1[at, e, body1, :] = share * (fr1[at, e] + down_total(black1, at, e, True))
    for at in range(count1):
        left_over = None
        for e in range(2):
            total = fb1[at, e] + down_total(red1, at, e, False)
            value = share * total
            black1[at, e, body1, :] = value
            term = total - centre * value
            left_over = term if left_over is None else left_over + term
        rest1[at] = left_over
    for at in range(count1):
        left_over = rest1[at]
        for e in range(2):
            total = fr1[at, e] + down_total(black1, at, e, True)
            left_over = left_over + (total - centre * window(red1, at, e, rows1))
        rest1[at] = left_over
    rows2 = rows1 // 2
    shape2 = (rows2, LANES)
    row2, lane2 = rows_of(shape2), lanes_of(shape2)
    odd2 = odd_of(shape2)
    planes = [
        0.5 * (rest1[at, pl.ds(0, rows2, stride=2), :] + rest1[at, pl.ds(1, rows2, stride=2), :])
        for at in range(count1)
    ]

    body2 = slice(PAD, PAD + rows2)

    def grid_of(index):
        step = 1 << index
        return ((row2 & (step - 1)) == 0) & ((lane2 & (step - 1)) == 0)

    def odd_at(index):
        return (((row2 >> index) + (lane2 >> index)) & 1) == 1

    def along(value, step):
        left = jnp.where(lane2 < step, 0.0, pltpu.roll(value, step, 1))
        right = jnp.where(lane2 >= LANES - step, 0.0, pltpu.roll(value, LANES - step, 1))
        return weight_z * (left + right)

    def small_total(index, ref, at, odd, to_red):
        step = 1 << index
        value = ref[at, 0, body2, :]
        total = value + along(value, step)
        total = total + (
            ref[at, 0, PAD - step : PAD - step + rows2, :] + ref[at, 0, PAD + step : PAD + step + rows2, :]
        )
        slots = ref.shape[0]
        if slots == 1:
            return total
        before = ref[at - 1, 0, body2, :] if at > 0 else 0.0
        after = ref[at + 1, 0, body2, :] if at < slots - 1 else 0.0
        return total + (jnp.where(odd, after, before) if to_red else jnp.where(odd, before, after))

    def small_sweeps(index, start):
        fr, fb, red, black = small[index]
        mask, odd = jnp.where(grid_of(index), share, 0.0), odd_at(index)
        slots = fr.shape[0]
        for step in range(2):
            for at in range(slots):
                source = fr[at]
                if not (start and step == 0):
                    source = source + small_total(index, black, at, odd, True)
                red[at, 0, body2, :] = mask * source
            for at in range(slots):
                black[at, 0, body2, :] = mask * (fb[at] + small_total(index, red, at, odd, False))

    def spread_rows(value, step, ref, at):
        ref[at, 0, body2, :] = value
        return value + ref[at, 0, PAD - step : PAD - step + rows2, :]

    last = len(small) - 1
    for index in range(len(small)):
        fr, fb, red, black = small[index]
        slots, odd, step = fr.shape[0], odd_at(index), 1 << index
        for at in range(slots):
            p, q = planes[2 * at], planes[2 * at + 1]
            fr[at], fb[at] = jnp.where(odd, q, p), jnp.where(odd, p, q)
        small_sweeps(index, True)
        totals = []
        for at in range(slots):
            first = fb[at] + small_total(index, red, at, odd, False) - centre * black[at, 0, body2, :]
            second = fr[at] + small_total(index, black, at, odd, True) - centre * red[at, 0, body2, :]
            totals.append(first + second)
        for at in range(slots):
            passing[at, 0, body2, :] = totals[at]
        lower = [passing[at, 0, PAD + step : PAD + step + rows2, :] for at in range(slots)]
        if index < last:
            totals = [total + below for total, below in zip(totals, lower)]
            planes = [0.5 * (total + pltpu.roll(total, LANES - step, 1)) for total in totals]

    half_rows = rows2 // 2
    upper = [passing[at, 0, PAD - step : PAD - step + rows2, :] for at in range(slots)]
    odd_line = (row2 & step) != 0
    summed = [
        total + jnp.where(odd_line, above, below) for total, above, below in zip(totals, upper, lower)
    ]
    lines = [total[start : start + half_rows] for total in summed for start in (0, half_rows)]
    place = lanes_of((half_rows, LANES)) & (len(lines) - 1)
    joined = lines[0]
    for q in range(1, len(lines)):
        joined = jnp.where(place == q, pltpu.roll(lines[q], q, 1), joined)
    answer = exact_dot(joined, matrix_ref[...])
    grid = (place == 0) & ((rows_of((half_rows, LANES)) & (step - 1)) == 0)
    parts = []
    for q in range(len(lines)):
        part = pltpu.roll(answer, LANES - q, 1) if q else answer
        parts.append(jnp.where(grid, part, 0.0))
    spreads = [jnp.concatenate(parts[2 * at : 2 * at + 2], axis=0) for at in range(slots)]

    for index in reversed(range(len(small))):
        _, _, red, black = small[index]
        slots, odd, step = red.shape[0], odd_at(index), 1 << index
        if index < last:
            spreads = [
                spread_rows(field + pltpu.roll(field, step, 1), step, passing, at)
                for at, field in enumerate(fields)
            ]
        for at in range(slots):
            black[at, 0, body2, :] = black[at, 0, body2, :] + spreads[at]
        small_sweeps(index, False)
        fields = []
        for at in range(slots):
            r, b = red[at, 0, body2, :], black[at, 0, body2, :]
            fields += [jnp.where(odd, b, r), jnp.where(odd, r, b)]

    for at in range(count1):
        for start in range(2):
            rest1[at, pl.ds(start, rows2, stride=2), :] = fields[at]
    for at in range(count1):
        for e in range(2):
            black1[at, e, body1, :] = window(black1, at, e, rows1) + rest1[at]
    nx, ny, nz = out_ref.shape
    own = nx // 2
    part_slots = min(own // 2 + 3, count1)
    part_rows = min(ny // 2 + 16, rows1)
    slot0 = jnp.where(gx == 0, 0, count1 - part_slots)
    row0 = pl.multiple_of(jnp.clip(gy * (ny // 2) - 8, 0, rows1 - part_rows), 8)
    odds = fold_odds(part_rows)

    def up_total(ref, at, e, to_red):
        low = gx == 0 if at == 0 else False
        high = gx != 0 if at == part_slots - 1 else False
        return fold_total(ref, slot0 + at, e, row0, part_rows, low, high, odds, to_red)

    def up_half(target, other, sources, to_red):
        for at in range(part_slots):
            for e in range(2):
                source = sources[slot0 + at, e, pl.ds(row0, part_rows), :]
                value = share * (source + up_total(other, at, e, to_red))
                target[slot0 + at, e, pl.ds(pl.multiple_of(row0 + PAD, 8), part_rows), :] = value

    for sweep in range(2):
        up_half(red1, black1, fr1, True)
        up_half(black1, red1, fb1, False)

    count, _, rows, _ = dark_ref.shape
    half = rows // 2
    odds = fold_odds(half)
    row = gy * (ny // 2) + (PAD - halo // 2)
    for at in range(count):
        if at < own:
            slot = gx * (own // 2) + at // 2
        else:
            slot = jnp.where(gx == 0, own // 2, own // 2 - (count - own) // 2) + (at - own) // 2
        for e in range(2):
            r, b = red1[slot, e, pl.ds(row, half), :], black1[slot, e, pl.ds(row, half), :]
            plane = jnp.where(odds[e], r, b) if at % 2 else jnp.where(odds[e], b, r)
            tall_ref[at, :, e * LANES : (e + 1) * LANES] = plane
    shape = (2 * LANES, 2 * LANES)
    z = lanes_of(shape)
    z = jnp.where(z < 2 * LANES - halo, z, z - 2 * LANES) + gz * nz
    line = rows_of(shape)
    line = jnp.where(line < LANES, 2 * line, 2 * (line - LANES) + 1)
    weight = jnp.where(line == lax.shift_right_arithmetic(z, 1), 1.0, 0.0)
    spread = exact_dot(tall_ref[...].reshape(count * half, 2 * LANES), weight)
    spread = spread.reshape(count, half, 2 * LANES)
    for at in range(count):
        for c in range(2):
            value = spread[at, :, c * LANES : (c + 1) * LANES]
            for start in range(2):
                work_ref[at, c, pl.ds(PAD + start, half, stride=2), :] = value
    body = slice(PAD, PAD + rows)
    for at in range(count):
        for c in range(2):
            work_ref[at, c, body, :] = work_ref[at, c, body, :] + dark_ref[at, c]
    odd = odd_of((rows, LANES))
    masks = block_mask((ny, nz), halo)
    ends = (gx == 0, gx == lax.axis_size("gx") - 1)
    for sweep in range(2):
        for at in range(count):
            totals = block_totals(work_ref, at, rows, own, odd, True, *ends)
            for c in range(2):
                red_ref[at, c, body, :] = gr_ref[at, c] + masks[c] * totals[c]
        for at in range(count if sweep == 0 else own):
            totals = block_totals(red_ref, at, rows, own, odd, False, *ends)
            for c in range(2 if sweep == 0 else 1):
                work_ref[at, c, body, :] = gb_ref[at, c] + masks[c] * totals[c]
    inner = slice(PAD + halo, PAD + halo + ny)
    odd = odd_of((ny, nz))
    for at in range(own):
        r, b = red_ref[at, 0, inner, :], work_ref[at, 0, inner, :]
        out_ref[2 * at] = jnp.where(odd, b, r)
        out_ref[2 * at + 1] = jnp.where(odd, r, b)


def vmem(number):
    return [pl.BlockSpec(memory_space=pltpu.VMEM)] * number


def struct(*shape):
    return jax.ShapeDtypeStruct(shape, jnp.float32)


def scratch(*shape):
    return pltpu.VMEM(shape, jnp.float32)


HALO = 8


def block_cycle(density):
    halo = HALO
    nx, ny, nz = density.shape
    count_x, count_y, count_z = (lax.axis_size(axis) for axis in ("gx", "gy", "gz"))
    whole = (nx * count_x, ny * count_y, nz * count_z)
    gx, gy = lax.axis_index("gx"), lax.axis_index("gy")
    face = lax.dynamic_slice_in_dim(density, jnp.where(gx == 0, nx - halo, 0), halo, 0)
    side = lax.ppermute(face, "gx", flips(count_x, 1))
    tall = jnp.concatenate([density, side], axis=0)
    even = gy % 2 == 0
    ya = lax.dynamic_slice_in_dim(tall, jnp.where(even, ny - halo, 0), halo, 1)
    yb = lax.dynamic_slice_in_dim(tall, jnp.where(even, 0, ny - halo), halo, 1)
    ya = lax.ppermute(ya, "gy", pairs(count_y, 0))
    yb = lax.ppermute(yb, ("gx", "gy"), inner_pairs(count_x, count_y))
    rows = ny + 2 * halo
    planes = nx + halo
    packs = -(-planes * halo // nz)

    def params(mib):
        return pltpu.CompilerParams(vmem_limit_bytes=mib * 1024 * 1024)

    za, zb = pl.pallas_call(
        functools.partial(pack_kernel, halo),
        out_shape=[struct(packs, rows, nz)] * 2,
        in_specs=vmem(4), out_specs=vmem(2), compiler_params=params(4),
    )(density, side, ya, yb)
    za = lax.ppermute(za, "gz", pairs(count_z, 0))
    zb = lax.ppermute(zb, "gz", pairs(count_z, 1) + [(0, count_z - 1), (count_z - 1, 0)])
    members = count_x * count_y
    slots = (planes // 2, 2, rows, LANES)
    padded = (planes // 2, 2, rows + 2 * PAD, LANES)
    gr, gb, black, send = pl.pallas_call(
        functools.partial(pre_kernel, halo),
        out_shape=[struct(*slots)] * 3 + [struct(members, nx // 4, ny // 2, nz)],
        in_specs=vmem(6), out_specs=vmem(4), compiler_params=params(10),
        scratch_shapes=[scratch(nx // 2, ny, nz)] * 2
        + [scratch(*padded)] * 2
        + [scratch(nx // 2, ny, nz)],
    )(density, side, ya, yb, za, zb)
    here = lax.all_to_all(send, ("gx", "gy"), 0, 0, tiled=True)
    flip = lax.ppermute(here, "gz", flips(count_z, 2))
    beside_here = lax.ppermute(here, "gz", flips(count_z, 1))
    beside_flip = lax.ppermute(flip, "gz", flips(count_z, 1))
    count1, rows1, rows2 = whole[0] // 4, whole[1] // 2, whole[1] // 4
    room = [scratch(count1, 2, rows1, LANES)] * 2
    room += [scratch(count1, 2, rows1 + 2 * PAD, LANES)] * 2
    room += [scratch(count1, rows1, LANES), scratch(planes // 2, rows // 2, 2 * LANES)]
    room += [scratch(*padded)] * 2 + [scratch(count1 // 2, 1, rows2 + 2 * PAD, LANES)]
    for count in small_shapes(whole):
        room += [scratch(count, rows2, LANES)] * 2
        room += [scratch(count, 1, rows2 + 2 * PAD, LANES)] * 2
    return pl.pallas_call(
        functools.partial(solve_kernel, halo, whole),
        out_shape=struct(nx, ny, nz),
        in_specs=vmem(8), out_specs=pl.BlockSpec(memory_space=pltpu.VMEM),
        compiler_params=params(16), scratch_shapes=room,
    )(here, flip, beside_here, beside_flip, gr, gb, black, cycle_matrix(whole))


def fits_block_cycle(shape):
    nx, ny, nz = shape
    count_x, count_y, count_z = (lax.axis_size(axis) for axis in ("gx", "gy", "gz"))
    whole = (nx * count_x, ny * count_y, nz * count_z)
    coarsest = [size >> (LEVELS - 1) for size in whole]
    exact = all(c << (LEVELS - 1) == size for c, size in zip(coarsest, whole))
    return (
        exact and coarsest[0] == coarsest[1] == 1 and nz == LANES and ny == 2 * HALO
        and count_x == 2 and count_z == 4 and count_y % 2 == 0
    )


def on_device(density):
    if fits_block_cycle(density.shape):
        return block_cycle(density)
    top = 4
    return shared_cycle(density, 0, top)


def solution(mesh):
    return jax.shard_map(
        on_device,
        mesh=mesh,
        in_specs=(P("gx", "gy", "gz"),),
        out_specs=P("gx", "gy", "gz"),
        check_vma=False,
    )
```

```python
import functools

import jax
import jax.numpy as jnp
import numpy as np
from jax import lax
from jax.experimental import pallas as pl
from jax.experimental.pallas import tpu as pltpu
from jax.sharding import PartitionSpec as P

LEVELS = 7
CSWEEPS = 4


rsd_beta = 0.5
centre = 4.0 + 2.0 * (1.0 + rsd_beta)


def extended_2(value, sides, width):
    for axis, dim in sides:
        count, length = (lax.axis_size(axis), value.shape[dim])
        up = [(i, (i + 1) % count) for i in range(count - 1)]
        down = [(j, i) for i, j in up]
        last = lax.slice_in_dim(value, length - width, length, axis=dim)
        leading = lax.slice_in_dim(value, 0, width, axis=dim)
        before = lax.ppermute(last, axis, up)
        after = lax.ppermute(leading, axis, down)
        value = jnp.concatenate([before, value, after], axis=dim)
    return value


def stencil_sum(padded):
    plane = (
        padded[2:, 1:-1, 1:-1]
        + padded[:-2, 1:-1, 1:-1]
        + padded[1:-1, 2:, 1:-1]
        + padded[1:-1, :-2, 1:-1]
    )
    sight = padded[1:-1, 1:-1, 2:] + padded[1:-1, 1:-1, :-2]
    return plane + (1.0 + rsd_beta) * sight


def grid_index(shape, starts):
    return [lax.broadcasted_iota(jnp.int32, shape, which) + starts[which] for which in range(3)]


def parity_of(shape, starts):
    position = grid_index(shape, starts)
    return (position[0] + position[1] + position[2] + 6) % 2


def inside_grid(shape, starts, whole):
    position = grid_index(shape, starts)
    keep = (position[0] >= 0) & (position[0] < whole[0])
    for which in (1, 2):
        keep = keep & (position[which] >= 0) & (position[which] < whole[which])
    return keep


def half_sweep(field, source, scale, chosen):
    update = (source / scale + stencil_sum(jnp.pad(field, 1))) / centre
    return jnp.where(chosen, update, field)


def full_sweep(field, source, scale, parity):
    field = half_sweep(field, source, scale, parity == 0)
    return half_sweep(field, source, scale, parity == 1)


def restrict(residue):
    shape = residue.shape
    blocks = residue.reshape(shape[0] // 2, 2, shape[1] // 2, 2, shape[2] // 2, 2)
    return jnp.mean(blocks, axis=(1, 3, 5))


def prolong(coarse):
    return jnp.repeat(jnp.repeat(jnp.repeat(coarse, 2, 0), 2, 1), 2, 2)


def local_cycle(source, level):
    scale = 0.25**level
    parity = parity_of(source.shape, (0, 0, 0))
    field = jnp.zeros_like(source)
    if level == LEVELS - 1:
        for number in range(CSWEEPS):
            field = full_sweep(field, source, scale, parity)
        return field
    for number in range(2):
        field = full_sweep(field, source, scale, parity)
    residue = source - scale * (centre * field - stencil_sum(jnp.pad(field, 1)))
    field = field + prolong(local_cycle(restrict(residue), level + 1))
    for number in range(2):
        field = full_sweep(field, source, scale, parity)
    return field


def faces(field):
    return extended_2(field, (("gx", 0), ("gy", 1), ("gz", 2)), 1)


def wide(field):
    return extended_2(field, (("gx", 0), ("gy", 1), ("gz", 2)), 2)


def block_starts(shape, margin):
    return (
        lax.axis_index("gx") * shape[0] - margin,
        lax.axis_index("gy") * shape[1] - margin,
        lax.axis_index("gz") * shape[2] - margin,
    )


def padded_half(padded, source, scale, chosen):
    field = padded[1:-1, 1:-1, 1:-1]
    update = (source / scale + stencil_sum(padded)) / centre
    return jnp.where(chosen, update, field)


def wide_sweep(extended, wide_source, scale, red_wide, source, black):
    update = (wide_source / scale + stencil_sum(jnp.pad(extended, 1))) / centre
    extended = jnp.where(red_wide, update, extended)
    return padded_half(extended[1:-1, 1:-1, 1:-1], source, scale, black)


def coarse_level(source, level):
    shape = source.shape
    stack = lax.all_gather(source[None], ("gx", "gy", "gz"), axis=0, tiled=True)
    count_x, count_y, count_z = (lax.axis_size("gx"), lax.axis_size("gy"), lax.axis_size("gz"))
    whole = stack.reshape(count_x, count_y, count_z, shape[0], shape[1], shape[2])
    whole = whole.transpose(0, 3, 1, 4, 2, 5).reshape(
        count_x * shape[0], count_y * shape[1], count_z * shape[2]
    )
    solved = local_cycle(whole, level)
    starts = block_starts(shape, 0)
    return lax.dynamic_slice(solved, starts, shape)


def shared_cycle(source, level, top):
    if level == top:
        return coarse_level(source, level)
    scale = 0.25**level
    shape = source.shape
    whole = (
        shape[0] * lax.axis_size("gx"),
        shape[1] * lax.axis_size("gy"),
        shape[2] * lax.axis_size("gz"),
    )
    parity = parity_of(shape, block_starts(shape, 0))
    black = parity == 1
    wide_shape = (shape[0] + 4, shape[1] + 4, shape[2] + 4)
    wide_starts = block_starts(shape, 2)
    red_wide = (parity_of(wide_shape, wide_starts) == 0) & inside_grid(
        wide_shape, wide_starts, whole
    )
    wide_source = wide(source)
    field = wide_sweep(
        jnp.zeros(wide_shape, jnp.float32), wide_source, scale, red_wide, source, black
    )
    field = wide_sweep(wide(field), wide_source, scale, red_wide, source, black)
    residue = source - scale * (centre * field - stencil_sum(faces(field)))
    field = field + prolong(shared_cycle(restrict(residue), level + 1, top))
    for number in range(2):
        field = wide_sweep(wide(field), wide_source, scale, red_wide, source, black)
    return field


def pairs(count, first):
    swaps = []
    for i in range(first, count - 1, 2):
        swaps += [(i, i + 1), (i + 1, i)]
    return swaps


def inner_pairs(count_x, count):
    swaps = []
    for x in range(count_x):
        swaps += [(x * count + i, x * count + j) for i, j in pairs(count, 1)]
        swaps += [(x * count + i, (x ^ 1) * count + i) for i in (0, count - 1)]
    return swaps


def flips(count, bit):
    return [(i, i ^ bit) for i in range(count)]


def lanes_of(shape):
    return lax.broadcasted_iota(jnp.int32, shape, len(shape) - 1)


def rows_of(shape):
    return lax.broadcasted_iota(jnp.int32, shape, len(shape) - 2)


LANES = 128
PAD = 8


def odd_of(shape):
    return ((lanes_of(shape) + rows_of(shape)) & 1) == 1


def exact_dot(a, b):
    return jnp.dot(a, b, precision=lax.Precision.HIGHEST, preferred_element_type=jnp.float32)


def window(ref, at, column, count, start=0, shift=0):
    if isinstance(start, int):
        return ref[at, column, PAD + start + shift : PAD + start + shift + count, :]
    first = start + (PAD + shift)
    if shift == 0:
        first = pl.multiple_of(first, 8)
    return ref[at, column, pl.ds(first, count), :]


def clear_pads(ref):
    edge = jnp.zeros((PAD, LANES), jnp.float32)
    for at in range(ref.shape[0]):
        for column in range(ref.shape[1]):
            ref[at, column, :PAD, :] = edge
            ref[at, column, ref.shape[2] - PAD :, :] = edge


def block_sums(ref, at, rows):
    lane = lanes_of((rows, LANES))
    values = [window(ref, at, column, rows) for column in range(2)]
    lefts = [pltpu.roll(value, 1, 1) for value in values]
    rights = [pltpu.roll(value, LANES - 1, 1) for value in values]
    sums = []
    for column in range(2):
        left = jnp.where(lane == 0, lefts[1 - column], lefts[column])
        right = jnp.where(lane == LANES - 1, rights[1 - column], rights[column])
        sides = window(ref, at, column, rows, shift=-1) + window(ref, at, column, rows, shift=1)
        sums.append(values[column] + sides + (1.0 + rsd_beta) * (left + right))
    return sums


def block_totals(ref, at, rows, own, odd, to_red, at_low, at_high):
    slots = ref.shape[0]
    totals = []
    for column, total in enumerate(block_sums(ref, at, rows)):
        before = window(ref, (at - 1) % slots, column, rows)
        after = window(ref, (at + 1) % slots, column, rows)
        if at == 0:
            before = jnp.where(at_low, 0.0, before)
        if at == own - 1:
            after = jnp.where(at_high, 0.0, after)
        totals.append(total + (jnp.where(odd, after, before) if to_red else jnp.where(odd, before, after)))
    return totals


def block_mask(own, halo):
    ny, nz = own
    shape = (ny + 2 * halo, LANES)
    row = rows_of(shape) - halo + lax.axis_index("gy") * ny
    inside_y = (row >= 0) & (row < ny * lax.axis_size("gy"))
    masks = []
    for column in range(2):
        lane = lanes_of(shape)
        if column:
            lane = jnp.where(lane < halo, lane + LANES, lane - LANES)
        lane = lane + lax.axis_index("gz") * nz
        inside = inside_y & (lane >= 0) & (lane < nz * lax.axis_size("gz"))
        masks.append(jnp.where(inside, 1.0 / centre, 0.0))
    return masks


def block_plane(at, nx, own_ref, xh_ref, ya_ref, yb_ref, even_y):
    a, b = ya_ref[at], yb_ref[at]
    middle = own_ref[at] if at < nx else xh_ref[at - nx]
    low = jnp.where(even_y, b, a)
    high = jnp.where(even_y, a, b)
    return jnp.concatenate([low, middle, high], axis=0)


def pack_kernel(halo, own_ref, xh_ref, ya_ref, yb_ref, za_ref, zb_ref):
    even_y = lax.axis_index("gy") % 2 == 0
    even_z = lax.axis_index("gz") % 2 == 0
    nx, ny, nz = own_ref.shape
    groups = nz // halo
    shape = (ny + 2 * halo, nz)
    group = lanes_of(shape) // halo
    for j in range(za_ref.shape[0]):
        last = jnp.zeros(shape, jnp.float32)
        first = jnp.zeros(shape, jnp.float32)
        for k in range(groups):
            at = j * groups + k
            if at >= nx + halo:
                break
            plane = block_plane(at, nx, own_ref, xh_ref, ya_ref, yb_ref, even_y)
            last = jnp.where(group == k, pltpu.roll(plane, (halo * k + halo) % nz, 1), last)
            first = jnp.where(group == k, pltpu.roll(plane, halo * k, 1), first)
        za_ref[j] = jnp.where(even_z, last, first)
        zb_ref[j] = jnp.where(even_z, first, last)


def pre_kernel(
    halo, own_ref, xh_ref, ya_ref, yb_ref, za_ref, zb_ref,
    gr_ref, gb_ref, dark_ref, send_ref,
    fr_ref, fb_ref, red_ref, black_ref, rest_ref,
):
    even_y = lax.axis_index("gy") % 2 == 0
    even_z = lax.axis_index("gz") % 2 == 0
    nx, ny, nz = own_ref.shape
    count, _, rows, _ = gr_ref.shape
    own = nx // 2
    groups = nz // halo
    shape = (rows, LANES)
    odd = odd_of(shape)
    masks = block_mask((ny, nz), halo)
    lane = lanes_of(shape)
    low, high = lane < halo, lane >= nz - halo
    inner = slice(halo, halo + ny)
    body = slice(PAD, PAD + rows)
    here = lax.axis_index("gx")
    ends = (here == 0, here == lax.axis_size("gx") - 1)
    clear_pads(red_ref)
    clear_pads(black_ref)

    def columns(at):
        j, k = at // groups, at % groups
        a, b = za_ref[j], zb_ref[j]
        left = jnp.where(even_z, b, a)
        right = jnp.where(even_z, a, b)
        right = pltpu.roll(right, (nz - halo * k) % nz, 1)
        left = pltpu.roll(left, (2 * nz - halo - halo * k) % nz, 1)
        sides = jnp.where(low, right, jnp.where(high, left, 0.0))
        return block_plane(at, nx, own_ref, xh_ref, ya_ref, yb_ref, even_y), sides

    for at in range(count):
        first, second = columns(2 * at), columns(2 * at + 1)
        for c in range(2):
            red = jnp.where(odd, second[c], first[c])
            black = jnp.where(odd, first[c], second[c])
            if c == 0 and at < own:
                fr_ref[at], fb_ref[at] = red[inner], black[inner]
            red = masks[c] * red
            gr_ref[at, c], gb_ref[at, c] = red, masks[c] * black
            red_ref[at, c, body, :] = red
    for at in range(count):
        totals = block_totals(red_ref, at, rows, own, odd, False, *ends)
        for c in range(2):
            black_ref[at, c, body, :] = gb_ref[at, c] + masks[c] * totals[c]
    for at in range(count):
        totals = block_totals(black_ref, at, rows, own, odd, True, *ends)
        for c in range(2):
            red_ref[at, c, body, :] = gr_ref[at, c] + masks[c] * totals[c]
    for at in range(count):
        totals = block_totals(red_ref, at, rows, own, odd, False, *ends)
        for c in range(2):
            value = gb_ref[at, c] + masks[c] * totals[c]
            black_ref[at, c, body, :] = value
            dark_ref[at, c] = value
            if c == 0 and at < own:
                rest_ref[at] = fb_ref[at] + totals[c][inner] - centre * value[inner]
    for at in range(own):
        total = block_totals(black_ref, at, rows, own, odd, True, *ends)[0]
        left_over = fr_ref[at] + total[inner] - centre * red_ref[at, 0, PAD + halo : PAD + halo + ny, :]
        rest_ref[at] = rest_ref[at] + left_over
    half, quarter = ny // 2, nz // 4
    pairs_y = rest_ref[:, pl.ds(0, half, stride=2), :] + rest_ref[:, pl.ds(1, half, stride=2), :]
    column = lanes_of((nz, nz))
    target = 2 * (column % quarter) + (column // quarter) % 2
    weight = jnp.where(rows_of((nz, nz)) // 2 == target, 0.5, 0.0)
    coarse = exact_dot(pairs_y.reshape(own * half, nz), weight).reshape(own, half, nz)
    part = lanes_of((half, nz)) // quarter
    pick = (((rows_of((half, nz)) + part) & 1) == 1) ^ (part >= 2)
    turn = quarter * lax.axis_index("gz")
    for at in range(own // 2):
        send_ref[at] = pltpu.roll(jnp.where(pick, coarse[2 * at + 1], coarse[2 * at]), turn, 1)


def stack_kernel(*refs):
    for which, ref in enumerate(refs[:-1]):
        refs[-1][which] = ref[...]


def small_shapes(whole):
    return [whole[0] >> (level + 1) for level in range(2, LEVELS - 2)]


def plain_sum(field):
    padded = np.pad(field, ((0, 0), (1, 1), (1, 1), (1, 1)))
    inner = slice(1, -1)
    plane = padded[:, 2:, inner, inner] + padded[:, :-2, inner, inner]
    plane = plane + padded[:, inner, 2:, inner] + padded[:, inner, :-2, inner]
    return plane + (1.0 + rsd_beta) * (padded[:, inner, inner, 2:] + padded[:, inner, inner, :-2])


def plain_cycle(source, level):
    parity = np.indices(source.shape[1:]).sum(axis=0) % 2
    field = np.zeros_like(source)

    def sweeps(field, number):
        for step in range(2 * number):
            field = np.where(parity == step % 2, (source + plain_sum(field)) / centre, field)
        return field

    if level == LEVELS - 1:
        return sweeps(field, CSWEEPS)
    field = sweeps(field, 2)
    rest = source - centre * field + plain_sum(field)
    nx, ny, nz = source.shape[1:]
    rest = rest.reshape(-1, nx // 2, 2, ny // 2, 2, nz // 2, 2).sum(axis=(2, 4, 6)) / 2.0
    coarse = plain_cycle(rest, level + 1)
    for axis in (1, 2, 3):
        coarse = np.repeat(coarse, 2, axis)
    return sweeps(field + coarse, 2)


def cycle_matrix(whole):
    level = LEVELS - 2
    nx, ny, nz = (size >> level for size in whole)
    size = nx * ny * 2 * nz
    unit = np.eye(size).reshape(size, 2 * nz, nx, ny).transpose(0, 2, 3, 1)
    source = unit.reshape(size, nx, ny, nz, 2).sum(axis=-1) / 2.0
    result = np.repeat(plain_cycle(source, level), 2, axis=3)
    return jnp.asarray(result.transpose(0, 3, 1, 2).reshape(size, size), jnp.float32)


def solve_kernel(halo, whole, *refs):
    gathered, refs = refs[:8], refs[8:]
    gr_ref, gb_ref, dark_ref, matrix_ref, out_ref = refs[:5]
    fr1, fb1, red1, black1, rest1, tall_ref, red_ref, work_ref, passing = refs[5:14]
    small = [refs[14 + 4 * i : 18 + 4 * i] for i in range(LEVELS - 4)]
    gx, gy, gz = (lax.axis_index(axis) for axis in ("gx", "gy", "gz"))
    weight_z = 1.0 + rsd_beta
    share = 1.0 / centre
    for ref in (red1, black1, red_ref, work_ref, passing):
        clear_pads(ref)
    for level in small:
        for ref in level[2:]:
            clear_pads(ref)

    _, slots, block_rows, _ = gathered[0].shape
    count1, _, rows1, _ = fr1.shape
    quarter = LANES // 4
    group = lanes_of((block_rows, LANES)) // quarter
    held = [jnp.bitwise_and(group - jnp.bitwise_xor(gz, bits), 3) for bits in range(4)]
    theirs = [[kind == part for kind in held] for part in range(4)]
    for far in range(2):
        for second in range(4):
            x = jnp.bitwise_xor(gx, second & 1)
            y = jnp.bitwise_xor(gy, 2 * far + (second >> 1))
            rows = pl.ds(pl.multiple_of(y * block_rows, 8), block_rows)
            for at in range(slots):
                blocks = [gathered[4 * (bits & 1) + second][far + (bits & 2), at] for bits in range(4)]
                for part, target in enumerate((fr1, fr1, fb1, fb1)):
                    value = blocks[0]
                    for block, mine in zip(blocks[1:], theirs[part][1:]):
                        value = jnp.where(mine, block, value)
                    turned = pltpu.roll(value, LANES - quarter * part, 1) if part else value
                    target[x * slots + at, part % 2, rows, :] = turned

    def fold_total(ref, at, e, start, count, low, high, odds, to_red):
        lane = lanes_of((count, LANES))
        value, other = window(ref, at, e, count, start), window(ref, at, 1 - e, count, start)
        sides = window(ref, at, e, count, start, -1) + window(ref, at, e, count, start, 1)
        if e == 0:
            near = jnp.where(lane == 0, 0.0, pltpu.roll(other, 1, 1))
        else:
            near = jnp.where(lane == LANES - 1, 0.0, pltpu.roll(other, LANES - 1, 1))
        before = 0.0 if low is True else window(ref, at - 1, e, count, start)
        after = 0.0 if high is True else window(ref, at + 1, e, count, start)
        if not isinstance(low, bool):
            before = jnp.where(low, 0.0, window(ref, jnp.maximum(at - 1, 0), e, count, start))
        if not isinstance(high, bool):
            after = jnp.where(high, 0.0, window(ref, jnp.minimum(at + 1, count1 - 1), e, count, start))
        beside = jnp.where(odds[e], after, before) if to_red else jnp.where(odds[e], before, after)
        return value + sides + beside + weight_z * (other + near)

    def fold_odds(count):
        row = rows_of((count, LANES))
        return [((row + e) & 1) == 1 for e in range(2)]

    odds = fold_odds(rows1)
    body1 = slice(PAD, PAD + rows1)

    def down_total(ref, at, e, to_red):
        return fold_total(ref, at, e, 0, rows1, at == 0, at == count1 - 1, odds, to_red)

    for at in range(count1):
        for e in range(2):
            red1[at, e, body1, :] = share * fr1[at, e]
    for at in range(count1):
        for e in range(2):
            black1[at, e, body1, :] = share * (fb1[at, e] + down_total(red1, at, e, False))
    for at in range(count1):
        for e in range(2):
            red1[at, e, body1, :] = share * (fr1[at, e] + down_total(black1, at, e, True))
    for at in range(count1):
        left_over = None
        for e in range(2):
            total = fb1[at, e] + down_total(red1, at, e, False)
            value = share * total
            black1[at, e, body1, :] = value
            term = total - centre * value
            left_over = term if left_over is None else left_over + term
        rest1[at] = left_over
    for at in range(count1):
        left_over = rest1[at]
        for e in range(2):
            total = fr1[at, e] + down_total(black1, at, e, True)
            left_over = left_over + (total - centre * window(red1, at, e, rows1))
        rest1[at] = left_over
    rows2 = rows1 // 2
    shape2 = (rows2, LANES)
    row2, lane2 = rows_of(shape2), lanes_of(shape2)
    odd2 = odd_of(shape2)
    planes = [
        0.5 * (rest1[at, pl.ds(0, rows2, stride=2), :] + rest1[at, pl.ds(1, rows2, stride=2), :])
        for at in range(count1)
    ]

    body2 = slice(PAD, PAD + rows2)

    def grid_of(index):
        step = 1 << index
        return ((row2 & (step - 1)) == 0) & ((lane2 & (step - 1)) == 0)

    def odd_at(index):
        return (((row2 >> index) + (lane2 >> index)) & 1) == 1

    def along(value, step):
        left = jnp.where(lane2 < step, 0.0, pltpu.roll(value, step, 1))
        right = jnp.where(lane2 >= LANES - step, 0.0, pltpu.roll(value, LANES - step, 1))
        return weight_z * (left + right)

    def small_total(index, ref, at, odd, to_red):
        step = 1 << index
        value = ref[at, 0, body2, :]
        total = value + along(value, step)
        total = total + (
            ref[at, 0, PAD - step : PAD - step + rows2, :] + ref[at, 0, PAD + step : PAD + step + rows2, :]
        )
        slots = ref.shape[0]
        if slots == 1:
            return total
        before = ref[at - 1, 0, body2, :] if at > 0 else 0.0
        after = ref[at + 1, 0, body2, :] if at < slots - 1 else 0.0
        return total + (jnp.where(odd, after, before) if to_red else jnp.where(odd, before, after))

    def small_sweeps(index, start):
        fr, fb, red, black = small[index]
        mask, odd = jnp.where(grid_of(index), share, 0.0), odd_at(index)
        slots = fr.shape[0]
        for step in range(2):
            for at in range(slots):
                source = fr[at]
                if not (start and step == 0):
                    source = source + small_total(index, black, at, odd, True)
                red[at, 0, body2, :] = mask * source
            for at in range(slots):
                black[at, 0, body2, :] = mask * (fb[at] + small_total(index, red, at, odd, False))

    def spread_rows(value, step, ref, at):
        ref[at, 0, body2, :] = value
        return value + ref[at, 0, PAD - step : PAD - step + rows2, :]

    last = len(small) - 1
    for index in range(len(small)):
        fr, fb, red, black = small[index]
        slots, odd, step = fr.shape[0], odd_at(index), 1 << index
        for at in range(slots):
            p, q = planes[2 * at], planes[2 * at + 1]
            fr[at], fb[at] = jnp.where(odd, q, p), jnp.where(odd, p, q)
        small_sweeps(index, True)
        totals = []
        for at in range(slots):
            first = fb[at] + small_total(index, red, at, odd, False) - centre * black[at, 0, body2, :]
            second = fr[at] + small_total(index, black, at, odd, True) - centre * red[at, 0, body2, :]
            totals.append(first + second)
        for at in range(slots):
            passing[at, 0, body2, :] = totals[at]
        lower = [passing[at, 0, PAD + step : PAD + step + rows2, :] for at in range(slots)]
        if index < last:
            totals = [total + below for total, below in zip(totals, lower)]
            planes = [0.5 * (total + pltpu.roll(total, LANES - step, 1)) for total in totals]

    half_rows = rows2 // 2
    upper = [passing[at, 0, PAD - step : PAD - step + rows2, :] for at in range(slots)]
    odd_line = (row2 & step) != 0
    summed = [
        total + jnp.where(odd_line, above, below) for total, above, below in zip(totals, upper, lower)
    ]
    lines = [total[start : start + half_rows] for total in summed for start in (0, half_rows)]
    place = lanes_of((half_rows, LANES)) & (len(lines) - 1)
    joined = lines[0]
    for q in range(1, len(lines)):
        joined = jnp.where(place == q, pltpu.roll(lines[q], q, 1), joined)
    answer = exact_dot(joined, matrix_ref[...])
    grid = (place == 0) & ((rows_of((half_rows, LANES)) & (step - 1)) == 0)
    parts = []
    for q in range(len(lines)):
        part = pltpu.roll(answer, LANES - q, 1) if q else answer
        parts.append(jnp.where(grid, part, 0.0))
    spreads = [jnp.concatenate(parts[2 * at : 2 * at + 2], axis=0) for at in range(slots)]

    for index in reversed(range(len(small))):
        _, _, red, black = small[index]
        slots, odd, step = red.shape[0], odd_at(index), 1 << index
        if index < last:
            spreads = [
                spread_rows(field + pltpu.roll(field, step, 1), step, passing, at)
                for at, field in enumerate(fields)
            ]
        for at in range(slots):
            black[at, 0, body2, :] = black[at, 0, body2, :] + spreads[at]
        small_sweeps(index, False)
        fields = []
        for at in range(slots):
            r, b = red[at, 0, body2, :], black[at, 0, body2, :]
            fields += [jnp.where(odd, b, r), jnp.where(odd, r, b)]

    for at in range(count1):
        for start in range(2):
            rest1[at, pl.ds(start, rows2, stride=2), :] = fields[at]
    for at in range(count1):
        for e in range(2):
            black1[at, e, body1, :] = window(black1, at, e, rows1) + rest1[at]
    nx, ny, nz = out_ref.shape
    own = nx // 2
    part_slots = min(own // 2 + 3, count1)
    part_rows = min(ny // 2 + 16, rows1)
    slot0 = jnp.where(gx == 0, 0, count1 - part_slots)
    row0 = pl.multiple_of(jnp.clip(gy * (ny // 2) - 8, 0, rows1 - part_rows), 8)
    odds = fold_odds(part_rows)

    def up_total(ref, at, e, to_red):
        low = gx == 0 if at == 0 else False
        high = gx != 0 if at == part_slots - 1 else False
        return fold_total(ref, slot0 + at, e, row0, part_rows, low, high, odds, to_red)

    def up_half(target, other, sources, to_red):
        for at in range(part_slots):
            for e in range(2):
                source = sources[slot0 + at, e, pl.ds(row0, part_rows), :]
                value = share * (source + up_total(other, at, e, to_red))
                target[slot0 + at, e, pl.ds(pl.multiple_of(row0 + PAD, 8), part_rows), :] = value

    for sweep in range(2):
        up_half(red1, black1, fr1, True)
        up_half(black1, red1, fb1, False)

    count, _, rows, _ = dark_ref.shape
    half = rows // 2
    odds = fold_odds(half)
    row = gy * (ny // 2) + (PAD - halo // 2)
    for at in range(count):
        if at < own:
            slot = gx * (own // 2) + at // 2
        else:
            slot = jnp.where(gx == 0, own // 2, own // 2 - (count - own) // 2) + (at - own) // 2
        for e in range(2):
            r, b = red1[slot, e, pl.ds(row, half), :], black1[slot, e, pl.ds(row, half), :]
            plane = jnp.where(odds[e], r, b) if at % 2 else jnp.where(odds[e], b, r)
            tall_ref[at, :, e * LANES : (e + 1) * LANES] = plane
    shape = (2 * LANES, 2 * LANES)
    z = lanes_of(shape)
    z = jnp.where(z < 2 * LANES - halo, z, z - 2 * LANES) + gz * nz
    line = rows_of(shape)
    line = jnp.where(line < LANES, 2 * line, 2 * (line - LANES) + 1)
    weight = jnp.where(line == lax.shift_right_arithmetic(z, 1), 1.0, 0.0)
    spread = exact_dot(tall_ref[...].reshape(count * half, 2 * LANES), weight)
    spread = spread.reshape(count, half, 2 * LANES)
    for at in range(count):
        for c in range(2):
            value = spread[at, :, c * LANES : (c + 1) * LANES]
            for start in range(2):
                work_ref[at, c, pl.ds(PAD + start, half, stride=2), :] = value
    body = slice(PAD, PAD + rows)
    for at in range(count):
        for c in range(2):
            work_ref[at, c, body, :] = work_ref[at, c, body, :] + dark_ref[at, c]
    odd = odd_of((rows, LANES))
    masks = block_mask((ny, nz), halo)
    ends = (gx == 0, gx == lax.axis_size("gx") - 1)
    for sweep in range(2):
        for at in range(count):
            totals = block_totals(work_ref, at, rows, own, odd, True, *ends)
            for c in range(2):
                red_ref[at, c, body, :] = gr_ref[at, c] + masks[c] * totals[c]
        for at in range(count if sweep == 0 else own):
            totals = block_totals(red_ref, at, rows, own, odd, False, *ends)
            for c in range(2 if sweep == 0 else 1):
                work_ref[at, c, body, :] = gb_ref[at, c] + masks[c] * totals[c]
    inner = slice(PAD + halo, PAD + halo + ny)
    odd = odd_of((ny, nz))
    for at in range(own):
        r, b = red_ref[at, 0, inner, :], work_ref[at, 0, inner, :]
        out_ref[2 * at] = jnp.where(odd, b, r)
        out_ref[2 * at + 1] = jnp.where(odd, r, b)


def vmem(number):
    return [pl.BlockSpec(memory_space=pltpu.VMEM)] * number


def struct(*shape):
    return jax.ShapeDtypeStruct(shape, jnp.float32)


def scratch(*shape):
    return pltpu.VMEM(shape, jnp.float32)


HALO = 8


def block_cycle(density):
    halo = HALO
    nx, ny, nz = density.shape
    count_x, count_y, count_z = (lax.axis_size(axis) for axis in ("gx", "gy", "gz"))
    whole = (nx * count_x, ny * count_y, nz * count_z)
    gx, gy = lax.axis_index("gx"), lax.axis_index("gy")
    face = lax.dynamic_slice_in_dim(density, jnp.where(gx == 0, nx - halo, 0), halo, 0)
    side = lax.ppermute(face, "gx", flips(count_x, 1))
    tall = jnp.concatenate([density, side], axis=0)
    even = gy % 2 == 0
    ya = lax.dynamic_slice_in_dim(tall, jnp.where(even, ny - halo, 0), halo, 1)
    yb = lax.dynamic_slice_in_dim(tall, jnp.where(even, 0, ny - halo), halo, 1)
    ya = lax.ppermute(ya, "gy", pairs(count_y, 0))
    yb = lax.ppermute(yb, ("gx", "gy"), inner_pairs(count_x, count_y))
    rows = ny + 2 * halo
    planes = nx + halo
    packs = -(-planes * halo // nz)

    def params(mib):
        return pltpu.CompilerParams(vmem_limit_bytes=mib * 1024 * 1024)

    za, zb = pl.pallas_call(
        functools.partial(pack_kernel, halo),
        out_shape=[struct(packs, rows, nz)] * 2,
        in_specs=vmem(4), out_specs=vmem(2), compiler_params=params(4),
    )(density, side, ya, yb)
    za = lax.ppermute(za, "gz", pairs(count_z, 0))
    zb = lax.ppermute(zb, "gz", pairs(count_z, 1) + [(0, count_z - 1), (count_z - 1, 0)])
    slots = (planes // 2, 2, rows, LANES)
    padded = (planes // 2, 2, rows + 2 * PAD, LANES)
    gr, gb, black, send = pl.pallas_call(
        functools.partial(pre_kernel, halo),
        out_shape=[struct(*slots)] * 3 + [struct(nx // 4, ny // 2, nz)],
        in_specs=vmem(6), out_specs=vmem(4), compiler_params=params(10),
        scratch_shapes=[scratch(nx // 2, ny, nz)] * 2
        + [scratch(*padded)] * 2
        + [scratch(nx // 2, ny, nz)],
    )(density, side, ya, yb, za, zb)
    first = [
        send,
        lax.ppermute(send, "gy", flips(count_y, 2)),
        lax.ppermute(send, "gz", flips(count_z, 2)),
        lax.ppermute(send, ("gy", "gz"), flips(count_y * count_z, 2 * count_z + 2)),
    ]
    block = pl.pallas_call(
        stack_kernel, out_shape=struct(4, *send.shape),
        in_specs=vmem(4), out_specs=pl.BlockSpec(memory_space=pltpu.VMEM), compiler_params=params(2),
    )(*first)
    second = [
        block,
        lax.ppermute(block, "gx", flips(count_x, 1)),
        lax.ppermute(block, "gy", flips(count_y, 1)),
        lax.ppermute(block, ("gx", "gy"), flips(count_x * count_y, count_y + 1)),
    ]
    third = [lax.ppermute(blocks, "gz", flips(count_z, 1)) for blocks in second]
    count1, rows1, rows2 = whole[0] // 4, whole[1] // 2, whole[1] // 4
    room = [scratch(count1, 2, rows1, LANES)] * 2
    room += [scratch(count1, 2, rows1 + 2 * PAD, LANES)] * 2
    room += [scratch(count1, rows1, LANES), scratch(planes // 2, rows // 2, 2 * LANES)]
    room += [scratch(*padded)] * 2 + [scratch(count1 // 2, 1, rows2 + 2 * PAD, LANES)]
    for count in small_shapes(whole):
        room += [scratch(count, rows2, LANES)] * 2
        room += [scratch(count, 1, rows2 + 2 * PAD, LANES)] * 2
    return pl.pallas_call(
        functools.partial(solve_kernel, halo, whole),
        out_shape=struct(nx, ny, nz),
        in_specs=vmem(12), out_specs=pl.BlockSpec(memory_space=pltpu.VMEM),
        compiler_params=params(16), scratch_shapes=room,
    )(*second, *third, gr, gb, black, cycle_matrix(whole))


def fits_block_cycle(shape):
    nx, ny, nz = shape
    count_x, count_y, count_z = (lax.axis_size(axis) for axis in ("gx", "gy", "gz"))
    whole = (nx * count_x, ny * count_y, nz * count_z)
    coarsest = [size >> (LEVELS - 1) for size in whole]
    exact = all(c << (LEVELS - 1) == size for c, size in zip(coarsest, whole))
    return (
        exact and coarsest[0] == coarsest[1] == 1 and nz == LANES and ny == 2 * HALO
        and count_x == 2 and count_y == 4 and count_z == 4
    )


def on_device(density):
    if fits_block_cycle(density.shape):
        return block_cycle(density)
    top = 4
    return shared_cycle(density, 0, top)


def solution(mesh):
    return jax.shard_map(
        on_device,
        mesh=mesh,
        in_specs=(P("gx", "gy", "gz"),),
        out_specs=P("gx", "gy", "gz"),
        check_vma=False,
    )
```

```python
import functools

import jax
import jax.numpy as jnp
import numpy as np
from jax import lax
from jax.experimental import pallas as pl
from jax.experimental.pallas import tpu as pltpu
from jax.sharding import PartitionSpec as P

LEVELS = 7
CSWEEPS = 4


rsd_beta = 0.5
centre = 4.0 + 2.0 * (1.0 + rsd_beta)


def extended_2(value, sides, width):
    for axis, dim in sides:
        count, length = (lax.axis_size(axis), value.shape[dim])
        up = [(i, (i + 1) % count) for i in range(count - 1)]
        down = [(j, i) for i, j in up]
        last = lax.slice_in_dim(value, length - width, length, axis=dim)
        leading = lax.slice_in_dim(value, 0, width, axis=dim)
        before = lax.ppermute(last, axis, up)
        after = lax.ppermute(leading, axis, down)
        value = jnp.concatenate([before, value, after], axis=dim)
    return value


def stencil_sum(padded):
    plane = (
        padded[2:, 1:-1, 1:-1]
        + padded[:-2, 1:-1, 1:-1]
        + padded[1:-1, 2:, 1:-1]
        + padded[1:-1, :-2, 1:-1]
    )
    sight = padded[1:-1, 1:-1, 2:] + padded[1:-1, 1:-1, :-2]
    return plane + (1.0 + rsd_beta) * sight


def grid_index(shape, starts):
    return [lax.broadcasted_iota(jnp.int32, shape, which) + starts[which] for which in range(3)]


def parity_of(shape, starts):
    position = grid_index(shape, starts)
    return (position[0] + position[1] + position[2] + 6) % 2


def inside_grid(shape, starts, whole):
    position = grid_index(shape, starts)
    keep = (position[0] >= 0) & (position[0] < whole[0])
    for which in (1, 2):
        keep = keep & (position[which] >= 0) & (position[which] < whole[which])
    return keep


def half_sweep(field, source, scale, chosen):
    update = (source / scale + stencil_sum(jnp.pad(field, 1))) / centre
    return jnp.where(chosen, update, field)


def full_sweep(field, source, scale, parity):
    field = half_sweep(field, source, scale, parity == 0)
    return half_sweep(field, source, scale, parity == 1)


def restrict(residue):
    shape = residue.shape
    blocks = residue.reshape(shape[0] // 2, 2, shape[1] // 2, 2, shape[2] // 2, 2)
    return jnp.mean(blocks, axis=(1, 3, 5))


def prolong(coarse):
    return jnp.repeat(jnp.repeat(jnp.repeat(coarse, 2, 0), 2, 1), 2, 2)


def local_cycle(source, level):
    scale = 0.25**level
    parity = parity_of(source.shape, (0, 0, 0))
    field = jnp.zeros_like(source)
    if level == LEVELS - 1:
        for number in range(CSWEEPS):
            field = full_sweep(field, source, scale, parity)
        return field
    for number in range(2):
        field = full_sweep(field, source, scale, parity)
    residue = source - scale * (centre * field - stencil_sum(jnp.pad(field, 1)))
    field = field + prolong(local_cycle(restrict(residue), level + 1))
    for number in range(2):
        field = full_sweep(field, source, scale, parity)
    return field


def faces(field):
    return extended_2(field, (("gx", 0), ("gy", 1), ("gz", 2)), 1)


def wide(field):
    return extended_2(field, (("gx", 0), ("gy", 1), ("gz", 2)), 2)


def block_starts(shape, margin):
    return (
        lax.axis_index("gx") * shape[0] - margin,
        lax.axis_index("gy") * shape[1] - margin,
        lax.axis_index("gz") * shape[2] - margin,
    )


def padded_half(padded, source, scale, chosen):
    field = padded[1:-1, 1:-1, 1:-1]
    update = (source / scale + stencil_sum(padded)) / centre
    return jnp.where(chosen, update, field)


def wide_sweep(extended, wide_source, scale, red_wide, source, black):
    update = (wide_source / scale + stencil_sum(jnp.pad(extended, 1))) / centre
    extended = jnp.where(red_wide, update, extended)
    return padded_half(extended[1:-1, 1:-1, 1:-1], source, scale, black)


def coarse_level(source, level):
    shape = source.shape
    stack = lax.all_gather(source[None], ("gx", "gy", "gz"), axis=0, tiled=True)
    count_x, count_y, count_z = (lax.axis_size("gx"), lax.axis_size("gy"), lax.axis_size("gz"))
    whole = stack.reshape(count_x, count_y, count_z, shape[0], shape[1], shape[2])
    whole = whole.transpose(0, 3, 1, 4, 2, 5).reshape(
        count_x * shape[0], count_y * shape[1], count_z * shape[2]
    )
    solved = local_cycle(whole, level)
    starts = block_starts(shape, 0)
    return lax.dynamic_slice(solved, starts, shape)


def shared_cycle(source, level, top):
    if level == top:
        return coarse_level(source, level)
    scale = 0.25**level
    shape = source.shape
    whole = (
        shape[0] * lax.axis_size("gx"),
        shape[1] * lax.axis_size("gy"),
        shape[2] * lax.axis_size("gz"),
    )
    parity = parity_of(shape, block_starts(shape, 0))
    black = parity == 1
    wide_shape = (shape[0] + 4, shape[1] + 4, shape[2] + 4)
    wide_starts = block_starts(shape, 2)
    red_wide = (parity_of(wide_shape, wide_starts) == 0) & inside_grid(
        wide_shape, wide_starts, whole
    )
    wide_source = wide(source)
    field = wide_sweep(
        jnp.zeros(wide_shape, jnp.float32), wide_source, scale, red_wide, source, black
    )
    field = wide_sweep(wide(field), wide_source, scale, red_wide, source, black)
    residue = source - scale * (centre * field - stencil_sum(faces(field)))
    field = field + prolong(shared_cycle(restrict(residue), level + 1, top))
    for number in range(2):
        field = wide_sweep(wide(field), wide_source, scale, red_wide, source, black)
    return field


def pairs(count, first):
    swaps = []
    for i in range(first, count - 1, 2):
        swaps += [(i, i + 1), (i + 1, i)]
    return swaps


def inner_pairs(count_x, count):
    swaps = []
    for x in range(count_x):
        swaps += [(x * count + i, x * count + j) for i, j in pairs(count, 1)]
        swaps += [(x * count + i, (x ^ 1) * count + i) for i in (0, count - 1)]
    return swaps


def flips(count, bit):
    return [(i, i ^ bit) for i in range(count)]


def lanes_of(shape):
    return lax.broadcasted_iota(jnp.int32, shape, len(shape) - 1)


def rows_of(shape):
    return lax.broadcasted_iota(jnp.int32, shape, len(shape) - 2)


LANES = 128
PAD = 8


def odd_of(shape):
    return ((lanes_of(shape) + rows_of(shape)) & 1) == 1


def exact_dot(a, b):
    return jnp.dot(a, b, precision=lax.Precision.HIGHEST, preferred_element_type=jnp.float32)


def window(ref, at, column, count, start=0, shift=0):
    if isinstance(start, int):
        return ref[at, column, PAD + start + shift : PAD + start + shift + count, :]
    first = start + (PAD + shift)
    if shift == 0:
        first = pl.multiple_of(first, 8)
    return ref[at, column, pl.ds(first, count), :]


def clear_pads(ref):
    edge = jnp.zeros((PAD, LANES), jnp.float32)
    for at in range(ref.shape[0]):
        for column in range(ref.shape[1]):
            ref[at, column, :PAD, :] = edge
            ref[at, column, ref.shape[2] - PAD :, :] = edge


def block_sums(ref, at, rows):
    lane = lanes_of((rows, LANES))
    values = [window(ref, at, column, rows) for column in range(2)]
    lefts = [pltpu.roll(value, 1, 1) for value in values]
    rights = [pltpu.roll(value, LANES - 1, 1) for value in values]
    sums = []
    for column in range(2):
        left = jnp.where(lane == 0, lefts[1 - column], lefts[column])
        right = jnp.where(lane == LANES - 1, rights[1 - column], rights[column])
        sides = window(ref, at, column, rows, shift=-1) + window(ref, at, column, rows, shift=1)
        sums.append(values[column] + sides + (1.0 + rsd_beta) * (left + right))
    return sums


def block_totals(ref, at, rows, own, odd, to_red, at_low, at_high):
    slots = ref.shape[0]
    totals = []
    for column, total in enumerate(block_sums(ref, at, rows)):
        before = window(ref, (at - 1) % slots, column, rows)
        after = window(ref, (at + 1) % slots, column, rows)
        if at in (0, own):
            before = jnp.where(at_low if at == 0 else at_high, 0.0, before)
        if at in (own - 1, slots - 1):
            after = jnp.where(at_low if at == slots - 1 else at_high, 0.0, after)
        totals.append(total + (jnp.where(odd, after, before) if to_red else jnp.where(odd, before, after)))
    return totals


def block_mask(own, halo):
    ny, nz = own
    shape = (ny + 2 * halo, LANES)
    row = rows_of(shape) - halo + lax.axis_index("gy") * ny
    inside_y = (row >= 0) & (row < ny * lax.axis_size("gy"))
    masks = []
    for column in range(2):
        lane = lanes_of(shape)
        if column:
            lane = jnp.where(lane < halo, lane + LANES, lane - LANES)
        lane = lane + lax.axis_index("gz") * nz
        inside = inside_y & (lane >= 0) & (lane < nz * lax.axis_size("gz"))
        masks.append(jnp.where(inside, 1.0 / centre, 0.0))
    return masks


def block_plane(at, own_ref, ya_ref, yb_ref, even_y):
    a, b = ya_ref[at], yb_ref[at]
    low = jnp.where(even_y, b, a)
    high = jnp.where(even_y, a, b)
    return jnp.concatenate([low, own_ref[at], high], axis=0)


def block_columns(halo, at, own_ref, ya_ref, yb_ref, za_ref, zb_ref, even_y, even_z):
    _, _, nz = own_ref.shape
    j, k = at // (nz // halo), at % (nz // halo)
    a, b = za_ref[j], zb_ref[j]
    left = pltpu.roll(jnp.where(even_z, b, a), (2 * nz - halo - halo * k) % nz, 1)
    right = pltpu.roll(jnp.where(even_z, a, b), (nz - halo * k) % nz, 1)
    lane = lanes_of(left.shape)
    sides = jnp.where(lane < halo, right, jnp.where(lane >= nz - halo, left, 0.0))
    return block_plane(at, own_ref, ya_ref, yb_ref, even_y), sides


def pack_kernel(halo, own_ref, ya_ref, yb_ref, za_ref, zb_ref):
    even_y = lax.axis_index("gy") % 2 == 0
    even_z = lax.axis_index("gz") % 2 == 0
    nx, ny, nz = own_ref.shape
    groups = nz // halo
    shape = (ny + 2 * halo, nz)
    group = lanes_of(shape) // halo
    for j in range(za_ref.shape[0]):
        last = jnp.zeros(shape, jnp.float32)
        first = jnp.zeros(shape, jnp.float32)
        for k in range(min(groups, nx - j * groups)):
            plane = block_plane(j * groups + k, own_ref, ya_ref, yb_ref, even_y)
            last = jnp.where(group == k, pltpu.roll(plane, (halo * k + halo) % nz, 1), last)
            first = jnp.where(group == k, pltpu.roll(plane, halo * k, 1), first)
        za_ref[j] = jnp.where(even_z, last, first)
        zb_ref[j] = jnp.where(even_z, first, last)


def smooth(count, own, masks, odd, ends, gr_ref, gb_ref, red_ref, black_ref, done):
    rows = odd.shape[0]
    body = slice(PAD, PAD + rows)

    def value_of(source, at, c, total):
        value = masks[c] * total
        return source[at, c] + value if at < source.shape[0] else value

    for at in range(count):
        for c in range(2):
            red_ref[at, c, body, :] = gr_ref[at, c] if at < gr_ref.shape[0] else jnp.zeros_like(masks[c])
    for step in range(3):
        source, target, other = (gr_ref, red_ref, black_ref) if step == 1 else (gb_ref, black_ref, red_ref)
        for at in range(count):
            totals = block_totals(other, at, rows, own, odd, step == 1, *ends)
            for c in range(2):
                value = value_of(source, at, c, totals[c])
                target[at, c, body, :] = value
                if step == 2:
                    done(at, c, totals[c], value)


def x_ends():
    here = lax.axis_index("gx")
    return here == 0, here == lax.axis_size("gx") - 1


def pre_kernel(
    halo, own_ref, ya_ref, yb_ref, za_ref, zb_ref,
    send_ref, face_ref,
    fr_ref, fb_ref, gr_ref, gb_ref, red_ref, black_ref, rest_ref,
):
    even_y = lax.axis_index("gy") % 2 == 0
    even_z = lax.axis_index("gz") % 2 == 0
    nx, ny, nz = own_ref.shape
    count, _, rows, _ = red_ref.shape
    rows = rows - 2 * PAD
    own = nx // 2
    shape = (rows, LANES)
    odd = odd_of(shape)
    masks = block_mask((ny, nz), halo)
    inner = slice(halo, halo + ny)
    ends = x_ends()
    clear_pads(red_ref)
    clear_pads(black_ref)
    group = lanes_of(shape) // (2 * halo)
    low_sides = jnp.zeros(shape, jnp.float32)
    high_sides = jnp.zeros(shape, jnp.float32)
    for at in range(own):
        planes = []
        for x in (2 * at, 2 * at + 1):
            columns = block_columns(halo, x, own_ref, ya_ref, yb_ref, za_ref, zb_ref, even_y, even_z)
            planes.append(columns)
            if x < halo:
                turned = pltpu.roll(columns[1], (halo + 2 * halo * x) % LANES, 1)
                low_sides = jnp.where(group == x, turned, low_sides)

                @pl.when(jnp.logical_not(ends[0]))
                def _(x=x, plane=columns[0]):
                    face_ref[x] = plane

            if x >= nx - halo:
                p = x - (nx - halo)
                turned = pltpu.roll(columns[1], (halo + 2 * halo * p) % LANES, 1)
                high_sides = jnp.where(group == p, turned, high_sides)

                @pl.when(ends[0])
                def _(p=p, plane=columns[0]):
                    face_ref[p] = plane

        for c in range(2):
            red = jnp.where(odd, planes[1][c], planes[0][c])
            black = jnp.where(odd, planes[0][c], planes[1][c])
            if c == 0:
                fr_ref[at], fb_ref[at] = red[inner], black[inner]
            gr_ref[at, c], gb_ref[at, c] = masks[c] * red, masks[c] * black
    face_ref[halo] = jnp.where(ends[0], high_sides, low_sides)

    def keep(at, c, total, value):
        if c == 0:
            left_over = total[inner] - centre * value[inner]
            rest_ref[at] = left_over + fb_ref[at] if at < own else left_over

    smooth(count, own, masks, odd, ends, gr_ref, gb_ref, red_ref, black_ref, keep)
    for at in range(count):
        total = block_totals(black_ref, at, rows, own, odd, True, *ends)[0]
        left_over = total[inner] - centre * red_ref[at, 0, PAD + halo : PAD + halo + ny, :]
        if at < own:
            left_over = left_over + fr_ref[at]
        rest_ref[at] = rest_ref[at] + left_over
    half, quarter = ny // 2, nz // 4
    pairs_y = rest_ref[:, pl.ds(0, half, stride=2), :] + rest_ref[:, pl.ds(1, half, stride=2), :]
    column = lanes_of((nz, nz))
    target = 2 * (column % quarter) + (column // quarter) % 2
    weight = jnp.where(rows_of((nz, nz)) // 2 == target, 0.5, 0.0)
    coarse = exact_dot(pairs_y.reshape(count * half, nz), weight).reshape(count, half, nz)
    part = lanes_of((half, nz)) // quarter
    pick = (((rows_of((half, nz)) + part) & 1) == 1) ^ (part >= 2)
    turn = quarter * lax.axis_index("gz")
    for at in range(count // 2):
        send_ref[at] = pltpu.roll(jnp.where(pick, coarse[2 * at + 1], coarse[2 * at]), turn, 1)


def field_kernel(
    halo, own_ref, ya_ref, yb_ref, za_ref, zb_ref, face_ref, after_ref,
    gr_ref, gb_ref, dark_ref,
    red_ref, black_ref,
):
    even_y = lax.axis_index("gy") % 2 == 0
    even_z = lax.axis_index("gz") % 2 == 0
    nx, ny, nz = own_ref.shape
    count, _, rows, _ = gr_ref.shape
    own = nx // 2
    shape = (rows, LANES)
    odd, lane = odd_of(shape), lanes_of(shape)
    masks = block_mask((ny, nz), halo)
    clear_pads(red_ref)
    clear_pads(black_ref)

    def columns(x):
        if x < nx:
            return block_columns(halo, x, own_ref, ya_ref, yb_ref, za_ref, zb_ref, even_y, even_z)
        p = x - nx
        sides = pltpu.roll(face_ref[halo], (2 * LANES - halo - 2 * halo * p) % LANES, 1)
        return face_ref[p], jnp.where((lane < halo) | (lane >= nz - halo), sides, 0.0)

    for at in range(count):
        first, second = columns(2 * at), columns(2 * at + 1)
        for c in range(2):
            gr_ref[at, c] = masks[c] * jnp.where(odd, second[c], first[c])
            gb_ref[at, c] = masks[c] * jnp.where(odd, first[c], second[c])

    def keep(at, c, total, value):
        dark_ref[at, c] = value

    smooth(count, own, masks, odd, x_ends(), gr_ref, gb_ref, red_ref, black_ref, keep)


def stack_kernel(*refs):
    for which, ref in enumerate(refs[:-1]):
        refs[-1][which] = ref[...]


def small_shapes(whole):
    return [whole[0] >> (level + 1) for level in range(2, LEVELS - 2)]


def plain_sum(field):
    padded = np.pad(field, ((0, 0), (1, 1), (1, 1), (1, 1)))
    inner = slice(1, -1)
    plane = padded[:, 2:, inner, inner] + padded[:, :-2, inner, inner]
    plane = plane + padded[:, inner, 2:, inner] + padded[:, inner, :-2, inner]
    return plane + (1.0 + rsd_beta) * (padded[:, inner, inner, 2:] + padded[:, inner, inner, :-2])


def plain_cycle(source, level):
    parity = np.indices(source.shape[1:]).sum(axis=0) % 2
    field = np.zeros_like(source)

    def sweeps(field, number):
        for step in range(2 * number):
            field = np.where(parity == step % 2, (source + plain_sum(field)) / centre, field)
        return field

    if level == LEVELS - 1:
        return sweeps(field, CSWEEPS)
    field = sweeps(field, 2)
    rest = source - centre * field + plain_sum(field)
    nx, ny, nz = source.shape[1:]
    rest = rest.reshape(-1, nx // 2, 2, ny // 2, 2, nz // 2, 2).sum(axis=(2, 4, 6)) / 2.0
    coarse = plain_cycle(rest, level + 1)
    for axis in (1, 2, 3):
        coarse = np.repeat(coarse, 2, axis)
    return sweeps(field + coarse, 2)


def cycle_matrix(whole):
    level = LEVELS - 2
    nx, ny, nz = (size >> level for size in whole)
    size = nx * ny * 2 * nz
    unit = np.eye(size).reshape(size, 2 * nz, nx, ny).transpose(0, 2, 3, 1)
    source = unit.reshape(size, nx, ny, nz, 2).sum(axis=-1) / 2.0
    result = np.repeat(plain_cycle(source, level), 2, axis=3)
    return jnp.asarray(result.transpose(0, 3, 1, 2).reshape(size, size), jnp.float32)


def solve_kernel(halo, whole, *refs):
    gathered, refs = refs[:8], refs[8:]
    gr_ref, gb_ref, dark_ref, matrix_ref, out_ref = refs[:5]
    fr1, fb1, red1, black1, rest1, tall_ref, red_ref, work_ref, passing = refs[5:14]
    small = [refs[14 + 4 * i : 18 + 4 * i] for i in range(LEVELS - 4)]
    gx, gy, gz = (lax.axis_index(axis) for axis in ("gx", "gy", "gz"))
    weight_z = 1.0 + rsd_beta
    share = 1.0 / centre
    for ref in (red1, black1, red_ref, work_ref, passing):
        clear_pads(ref)
    for level in small:
        for ref in level[2:]:
            clear_pads(ref)

    _, slots, block_rows, _ = gathered[0].shape
    slots = slots - 1
    count1, _, rows1, _ = fr1.shape
    quarter = LANES // 4
    group = lanes_of((block_rows, LANES)) // quarter
    held = [jnp.bitwise_and(group - jnp.bitwise_xor(gz, bits), 3) for bits in range(4)]
    theirs = [[kind == part for kind in held] for part in range(4)]
    def unpack(far, second, at):
        y = jnp.bitwise_xor(gy, 2 * far + (second >> 1))
        rows = pl.ds(pl.multiple_of(y * block_rows, 8), block_rows)
        blocks = [gathered[4 * (bits & 1) + second][far + (bits & 2), at] for bits in range(4)]
        parts = []
        for part in range(4):
            value = blocks[0]
            for block, mine in zip(blocks[1:], theirs[part][1:]):
                value = jnp.where(mine, block, value)
            parts.append(pltpu.roll(value, LANES - quarter * part, 1) if part else value)
        return rows, parts

    half1 = count1 // 2
    for far in range(2):
        for second in range(4):
            x = jnp.bitwise_xor(gx, second & 1)
            for at in range(slots):
                rows, parts = unpack(far, second, at)
                for part, target in enumerate((fr1, fr1, fb1, fb1)):
                    target[x * slots + at, part % 2, rows, :] = parts[part]
    for far in range(2):
        for second in range(4):
            x = jnp.bitwise_xor(gx, second & 1)
            next_slot = jnp.where(x == 0, half1, half1 - 1)
            rows, parts = unpack(far, second, slots)
            for part, target in enumerate((fr1, fr1, fb1, fb1)):
                target[next_slot, part % 2, rows, :] = target[next_slot, part % 2, rows, :] + parts[part]

    def fold_total(ref, at, e, start, count, low, high, odds, to_red):
        lane = lanes_of((count, LANES))
        value, other = window(ref, at, e, count, start), window(ref, at, 1 - e, count, start)
        sides = window(ref, at, e, count, start, -1) + window(ref, at, e, count, start, 1)
        if e == 0:
            near = jnp.where(lane == 0, 0.0, pltpu.roll(other, 1, 1))
        else:
            near = jnp.where(lane == LANES - 1, 0.0, pltpu.roll(other, LANES - 1, 1))
        before = 0.0 if low is True else window(ref, at - 1, e, count, start)
        after = 0.0 if high is True else window(ref, at + 1, e, count, start)
        if not isinstance(low, bool):
            before = jnp.where(low, 0.0, window(ref, jnp.maximum(at - 1, 0), e, count, start))
        if not isinstance(high, bool):
            after = jnp.where(high, 0.0, window(ref, jnp.minimum(at + 1, count1 - 1), e, count, start))
        beside = jnp.where(odds[e], after, before) if to_red else jnp.where(odds[e], before, after)
        return value + sides + beside + weight_z * (other + near)

    def fold_odds(count):
        row = rows_of((count, LANES))
        return [((row + e) & 1) == 1 for e in range(2)]

    odds = fold_odds(rows1)
    body1 = slice(PAD, PAD + rows1)

    def down_total(ref, at, e, to_red):
        return fold_total(ref, at, e, 0, rows1, at == 0, at == count1 - 1, odds, to_red)

    for at in range(count1):
        for e in range(2):
            red1[at, e, body1, :] = share * fr1[at, e]
    for at in range(count1):
        for e in range(2):
            black1[at, e, body1, :] = share * (fb1[at, e] + down_total(red1, at, e, False))
    for at in range(count1):
        for e in range(2):
            red1[at, e, body1, :] = share * (fr1[at, e] + down_total(black1, at, e, True))
    for at in range(count1):
        left_over = None
        for e in range(2):
            total = fb1[at, e] + down_total(red1, at, e, False)
            value = share * total
            black1[at, e, body1, :] = value
            term = total - centre * value
            left_over = term if left_over is None else left_over + term
        rest1[at] = left_over
    for at in range(count1):
        left_over = rest1[at]
        for e in range(2):
            total = fr1[at, e] + down_total(black1, at, e, True)
            left_over = left_over + (total - centre * window(red1, at, e, rows1))
        rest1[at] = left_over
    rows2 = rows1 // 2
    shape2 = (rows2, LANES)
    row2, lane2 = rows_of(shape2), lanes_of(shape2)
    odd2 = odd_of(shape2)
    planes = [
        0.5 * (rest1[at, pl.ds(0, rows2, stride=2), :] + rest1[at, pl.ds(1, rows2, stride=2), :])
        for at in range(count1)
    ]

    body2 = slice(PAD, PAD + rows2)

    def grid_of(index):
        step = 1 << index
        return ((row2 & (step - 1)) == 0) & ((lane2 & (step - 1)) == 0)

    def odd_at(index):
        return (((row2 >> index) + (lane2 >> index)) & 1) == 1

    def along(value, step):
        left = jnp.where(lane2 < step, 0.0, pltpu.roll(value, step, 1))
        right = jnp.where(lane2 >= LANES - step, 0.0, pltpu.roll(value, LANES - step, 1))
        return weight_z * (left + right)

    def small_total(index, ref, at, odd, to_red):
        step = 1 << index
        value = ref[at, 0, body2, :]
        total = value + along(value, step)
        total = total + (
            ref[at, 0, PAD - step : PAD - step + rows2, :] + ref[at, 0, PAD + step : PAD + step + rows2, :]
        )
        slots = ref.shape[0]
        if slots == 1:
            return total
        before = ref[at - 1, 0, body2, :] if at > 0 else 0.0
        after = ref[at + 1, 0, body2, :] if at < slots - 1 else 0.0
        return total + (jnp.where(odd, after, before) if to_red else jnp.where(odd, before, after))

    def small_sweeps(index, start):
        fr, fb, red, black = small[index]
        mask, odd = jnp.where(grid_of(index), share, 0.0), odd_at(index)
        slots = fr.shape[0]
        for step in range(2):
            for at in range(slots):
                source = fr[at]
                if not (start and step == 0):
                    source = source + small_total(index, black, at, odd, True)
                red[at, 0, body2, :] = mask * source
            for at in range(slots):
                black[at, 0, body2, :] = mask * (fb[at] + small_total(index, red, at, odd, False))

    def spread_rows(value, step, ref, at):
        ref[at, 0, body2, :] = value
        return value + ref[at, 0, PAD - step : PAD - step + rows2, :]

    last = len(small) - 1
    for index in range(len(small)):
        fr, fb, red, black = small[index]
        slots, odd, step = fr.shape[0], odd_at(index), 1 << index
        for at in range(slots):
            p, q = planes[2 * at], planes[2 * at + 1]
            fr[at], fb[at] = jnp.where(odd, q, p), jnp.where(odd, p, q)
        small_sweeps(index, True)
        totals = []
        for at in range(slots):
            first = fb[at] + small_total(index, red, at, odd, False) - centre * black[at, 0, body2, :]
            second = fr[at] + small_total(index, black, at, odd, True) - centre * red[at, 0, body2, :]
            totals.append(first + second)
        for at in range(slots):
            passing[at, 0, body2, :] = totals[at]
        lower = [passing[at, 0, PAD + step : PAD + step + rows2, :] for at in range(slots)]
        if index < last:
            totals = [total + below for total, below in zip(totals, lower)]
            planes = [0.5 * (total + pltpu.roll(total, LANES - step, 1)) for total in totals]

    half_rows = rows2 // 2
    upper = [passing[at, 0, PAD - step : PAD - step + rows2, :] for at in range(slots)]
    odd_line = (row2 & step) != 0
    summed = [
        total + jnp.where(odd_line, above, below) for total, above, below in zip(totals, upper, lower)
    ]
    lines = [total[start : start + half_rows] for total in summed for start in (0, half_rows)]
    place = lanes_of((half_rows, LANES)) & (len(lines) - 1)
    joined = lines[0]
    for q in range(1, len(lines)):
        joined = jnp.where(place == q, pltpu.roll(lines[q], q, 1), joined)
    answer = exact_dot(joined, matrix_ref[...])
    grid = (place == 0) & ((rows_of((half_rows, LANES)) & (step - 1)) == 0)
    parts = []
    for q in range(len(lines)):
        part = pltpu.roll(answer, LANES - q, 1) if q else answer
        parts.append(jnp.where(grid, part, 0.0))
    spreads = [jnp.concatenate(parts[2 * at : 2 * at + 2], axis=0) for at in range(slots)]

    for index in reversed(range(len(small))):
        _, _, red, black = small[index]
        slots, odd, step = red.shape[0], odd_at(index), 1 << index
        if index < last:
            spreads = [
                spread_rows(field + pltpu.roll(field, step, 1), step, passing, at)
                for at, field in enumerate(fields)
            ]
        for at in range(slots):
            black[at, 0, body2, :] = black[at, 0, body2, :] + spreads[at]
        small_sweeps(index, False)
        fields = []
        for at in range(slots):
            r, b = red[at, 0, body2, :], black[at, 0, body2, :]
            fields += [jnp.where(odd, b, r), jnp.where(odd, r, b)]

    for at in range(count1):
        for start in range(2):
            rest1[at, pl.ds(start, rows2, stride=2), :] = fields[at]
    for at in range(count1):
        for e in range(2):
            black1[at, e, body1, :] = window(black1, at, e, rows1) + rest1[at]
    nx, ny, nz = out_ref.shape
    own = nx // 2
    part_slots = min(own // 2 + 3, count1)
    part_rows = min(ny // 2 + 16, rows1)
    slot0 = jnp.where(gx == 0, 0, count1 - part_slots)
    row0 = pl.multiple_of(jnp.clip(gy * (ny // 2) - 8, 0, rows1 - part_rows), 8)
    odds = fold_odds(part_rows)

    def up_total(ref, at, e, to_red):
        low = gx == 0 if at == 0 else False
        high = gx != 0 if at == part_slots - 1 else False
        return fold_total(ref, slot0 + at, e, row0, part_rows, low, high, odds, to_red)

    def up_half(target, other, sources, to_red):
        for at in range(part_slots):
            for e in range(2):
                source = sources[slot0 + at, e, pl.ds(row0, part_rows), :]
                value = share * (source + up_total(other, at, e, to_red))
                target[slot0 + at, e, pl.ds(pl.multiple_of(row0 + PAD, 8), part_rows), :] = value

    for sweep in range(2):
        up_half(red1, black1, fr1, True)
        up_half(black1, red1, fb1, False)

    count, _, rows, _ = dark_ref.shape
    half = rows // 2
    odds = fold_odds(half)
    row = gy * (ny // 2) + (PAD - halo // 2)
    for at in range(count):
        if at < own:
            slot = gx * (own // 2) + at // 2
        else:
            slot = jnp.where(gx == 0, own // 2, own // 2 - (count - own) // 2) + (at - own) // 2
        for e in range(2):
            r, b = red1[slot, e, pl.ds(row, half), :], black1[slot, e, pl.ds(row, half), :]
            plane = jnp.where(odds[e], r, b) if at % 2 else jnp.where(odds[e], b, r)
            tall_ref[at, :, e * LANES : (e + 1) * LANES] = plane
    shape = (2 * LANES, 2 * LANES)
    z = lanes_of(shape)
    z = jnp.where(z < 2 * LANES - halo, z, z - 2 * LANES) + gz * nz
    line = rows_of(shape)
    line = jnp.where(line < LANES, 2 * line, 2 * (line - LANES) + 1)
    weight = jnp.where(line == lax.shift_right_arithmetic(z, 1), 1.0, 0.0)
    spread = exact_dot(tall_ref[...].reshape(count * half, 2 * LANES), weight)
    spread = spread.reshape(count, half, 2 * LANES)
    for at in range(count):
        for c in range(2):
            value = spread[at, :, c * LANES : (c + 1) * LANES]
            for start in range(2):
                work_ref[at, c, pl.ds(PAD + start, half, stride=2), :] = value
    body = slice(PAD, PAD + rows)
    for at in range(count):
        for c in range(2):
            work_ref[at, c, body, :] = work_ref[at, c, body, :] + dark_ref[at, c]
    odd = odd_of((rows, LANES))
    masks = block_mask((ny, nz), halo)
    ends = (gx == 0, gx == lax.axis_size("gx") - 1)
    for sweep in range(2):
        for at in range(count):
            totals = block_totals(work_ref, at, rows, own, odd, True, *ends)
            for c in range(2):
                red_ref[at, c, body, :] = gr_ref[at, c] + masks[c] * totals[c]
        for at in range(count if sweep == 0 else own):
            totals = block_totals(red_ref, at, rows, own, odd, False, *ends)
            for c in range(2 if sweep == 0 else 1):
                work_ref[at, c, body, :] = gb_ref[at, c] + masks[c] * totals[c]
    inner = slice(PAD + halo, PAD + halo + ny)
    odd = odd_of((ny, nz))
    for at in range(own):
        r, b = red_ref[at, 0, inner, :], work_ref[at, 0, inner, :]
        out_ref[2 * at] = jnp.where(odd, b, r)
        out_ref[2 * at + 1] = jnp.where(odd, r, b)


def vmem(number):
    return [pl.BlockSpec(memory_space=pltpu.VMEM)] * number


def struct(*shape):
    return jax.ShapeDtypeStruct(shape, jnp.float32)


def scratch(*shape):
    return pltpu.VMEM(shape, jnp.float32)


HALO = 8


def block_cycle(density):
    halo = HALO
    nx, ny, nz = density.shape
    count_x, count_y, count_z = (lax.axis_size(axis) for axis in ("gx", "gy", "gz"))
    whole = (nx * count_x, ny * count_y, nz * count_z)
    even = lax.axis_index("gy") % 2 == 0
    ya = lax.dynamic_slice_in_dim(density, jnp.where(even, ny - halo, 0), halo, 1)
    yb = lax.dynamic_slice_in_dim(density, jnp.where(even, 0, ny - halo), halo, 1)
    ya = lax.ppermute(ya, "gy", pairs(count_y, 0))
    yb = lax.ppermute(yb, ("gx", "gy"), inner_pairs(count_x, count_y))
    rows = ny + 2 * halo
    packs = -(-nx * halo // nz)

    def params(mib):
        return pltpu.CompilerParams(vmem_limit_bytes=mib * 1024 * 1024)

    za, zb = pl.pallas_call(
        functools.partial(pack_kernel, halo),
        out_shape=[struct(packs, rows, nz)] * 2,
        in_specs=vmem(3), out_specs=vmem(2), compiler_params=params(4),
    )(density, ya, yb)
    za = lax.ppermute(za, "gz", pairs(count_z, 0))
    zb = lax.ppermute(zb, "gz", pairs(count_z, 1) + [(0, count_z - 1), (count_z - 1, 0)])
    own, near = nx // 2, nx // 2 + 2
    send, face = pl.pallas_call(
        functools.partial(pre_kernel, halo),
        out_shape=[struct(near // 2, ny // 2, nz), struct(halo + 1, rows, LANES)],
        in_specs=vmem(5), out_specs=vmem(2), compiler_params=params(10),
        scratch_shapes=[scratch(own, ny, nz)] * 2
        + [scratch(own, 2, rows, LANES)] * 2
        + [scratch(near, 2, rows + 2 * PAD, LANES)] * 2
        + [scratch(near, ny, nz)],
    )(density, ya, yb, za, zb)
    face = lax.ppermute(face, "gx", flips(count_x, 1))
    planes = nx + halo
    slots = (planes // 2, 2, rows, LANES)
    padded = (planes // 2, 2, rows + 2 * PAD, LANES)
    first = [
        send,
        lax.ppermute(send, "gy", flips(count_y, 2)),
        lax.ppermute(send, "gz", flips(count_z, 2)),
        lax.ppermute(send, ("gy", "gz"), flips(count_y * count_z, 2 * count_z + 2)),
    ]
    first[3], face = lax.optimization_barrier((first[3], face))
    block = pl.pallas_call(
        stack_kernel, out_shape=struct(4, *send.shape),
        in_specs=vmem(4), out_specs=pl.BlockSpec(memory_space=pltpu.VMEM), compiler_params=params(2),
    )(*first)
    second = [
        block,
        lax.ppermute(block, "gx", flips(count_x, 1)),
        lax.ppermute(block, "gy", flips(count_y, 1)),
        lax.ppermute(block, ("gx", "gy"), flips(count_x * count_y, count_y + 1)),
    ]
    gr, gb, black = pl.pallas_call(
        functools.partial(field_kernel, halo),
        out_shape=[struct(*slots)] * 3,
        in_specs=vmem(7), out_specs=vmem(3), compiler_params=params(8),
        scratch_shapes=[scratch(*padded)] * 2,
        cost_estimate=pl.CostEstimate(flops=20_000_000, bytes_accessed=2_000_000, transcendentals=0),
    )(density, ya, yb, za, zb, face, block)
    *second[1:], gr, gb, black = lax.optimization_barrier((*second[1:], gr, gb, black))
    third = [lax.ppermute(blocks, "gz", flips(count_z, 1)) for blocks in second]
    count1, rows1, rows2 = whole[0] // 4, whole[1] // 2, whole[1] // 4
    room = [scratch(count1, 2, rows1, LANES)] * 2
    room += [scratch(count1, 2, rows1 + 2 * PAD, LANES)] * 2
    room += [scratch(count1, rows1, LANES), scratch(planes // 2, rows // 2, 2 * LANES)]
    room += [scratch(*padded)] * 2 + [scratch(count1 // 2, 1, rows2 + 2 * PAD, LANES)]
    for count in small_shapes(whole):
        room += [scratch(count, rows2, LANES)] * 2
        room += [scratch(count, 1, rows2 + 2 * PAD, LANES)] * 2
    return pl.pallas_call(
        functools.partial(solve_kernel, halo, whole),
        out_shape=struct(nx, ny, nz),
        in_specs=vmem(12), out_specs=pl.BlockSpec(memory_space=pltpu.VMEM),
        compiler_params=params(16), scratch_shapes=room,
    )(*second, *third, gr, gb, black, cycle_matrix(whole))


def fits_block_cycle(shape):
    nx, ny, nz = shape
    count_x, count_y, count_z = (lax.axis_size(axis) for axis in ("gx", "gy", "gz"))
    whole = (nx * count_x, ny * count_y, nz * count_z)
    coarsest = [size >> (LEVELS - 1) for size in whole]
    exact = all(c << (LEVELS - 1) == size for c, size in zip(coarsest, whole))
    return (
        exact and coarsest[0] == coarsest[1] == 1 and nz == LANES and ny == 2 * HALO
        and count_x == 2 and count_y == 4 and count_z == 4
    )


def on_device(density):
    if fits_block_cycle(density.shape):
        return block_cycle(density)
    top = 4
    return shared_cycle(density, 0, top)


def solution(mesh):
    return jax.shard_map(
        on_device,
        mesh=mesh,
        in_specs=(P("gx", "gy", "gz"),),
        out_specs=P("gx", "gy", "gz"),
        check_vma=False,
    )
```

```python
import functools

import jax
import jax.numpy as jnp
import numpy as np
from jax import lax
from jax.experimental import pallas as pl
from jax.experimental.pallas import tpu as pltpu
from jax.sharding import PartitionSpec as P

LEVELS = 7
CSWEEPS = 4


rsd_beta = 0.5
centre = 4.0 + 2.0 * (1.0 + rsd_beta)


def extended_2(value, sides, width):
    for axis, dim in sides:
        count, length = (lax.axis_size(axis), value.shape[dim])
        up = [(i, (i + 1) % count) for i in range(count - 1)]
        down = [(j, i) for i, j in up]
        last = lax.slice_in_dim(value, length - width, length, axis=dim)
        leading = lax.slice_in_dim(value, 0, width, axis=dim)
        before = lax.ppermute(last, axis, up)
        after = lax.ppermute(leading, axis, down)
        value = jnp.concatenate([before, value, after], axis=dim)
    return value


def stencil_sum(padded):
    plane = (
        padded[2:, 1:-1, 1:-1]
        + padded[:-2, 1:-1, 1:-1]
        + padded[1:-1, 2:, 1:-1]
        + padded[1:-1, :-2, 1:-1]
    )
    sight = padded[1:-1, 1:-1, 2:] + padded[1:-1, 1:-1, :-2]
    return plane + (1.0 + rsd_beta) * sight


def grid_index(shape, starts):
    return [lax.broadcasted_iota(jnp.int32, shape, which) + starts[which] for which in range(3)]


def parity_of(shape, starts):
    position = grid_index(shape, starts)
    return (position[0] + position[1] + position[2] + 6) % 2


def inside_grid(shape, starts, whole):
    position = grid_index(shape, starts)
    keep = (position[0] >= 0) & (position[0] < whole[0])
    for which in (1, 2):
        keep = keep & (position[which] >= 0) & (position[which] < whole[which])
    return keep


def half_sweep(field, source, scale, chosen):
    update = (source / scale + stencil_sum(jnp.pad(field, 1))) / centre
    return jnp.where(chosen, update, field)


def full_sweep(field, source, scale, parity):
    field = half_sweep(field, source, scale, parity == 0)
    return half_sweep(field, source, scale, parity == 1)


def restrict(residue):
    shape = residue.shape
    blocks = residue.reshape(shape[0] // 2, 2, shape[1] // 2, 2, shape[2] // 2, 2)
    return jnp.mean(blocks, axis=(1, 3, 5))


def prolong(coarse):
    return jnp.repeat(jnp.repeat(jnp.repeat(coarse, 2, 0), 2, 1), 2, 2)


def local_cycle(source, level):
    scale = 0.25**level
    parity = parity_of(source.shape, (0, 0, 0))
    field = jnp.zeros_like(source)
    if level == LEVELS - 1:
        for number in range(CSWEEPS):
            field = full_sweep(field, source, scale, parity)
        return field
    for number in range(2):
        field = full_sweep(field, source, scale, parity)
    residue = source - scale * (centre * field - stencil_sum(jnp.pad(field, 1)))
    field = field + prolong(local_cycle(restrict(residue), level + 1))
    for number in range(2):
        field = full_sweep(field, source, scale, parity)
    return field


def faces(field):
    return extended_2(field, (("gx", 0), ("gy", 1), ("gz", 2)), 1)


def wide(field):
    return extended_2(field, (("gx", 0), ("gy", 1), ("gz", 2)), 2)


def block_starts(shape, margin):
    return (
        lax.axis_index("gx") * shape[0] - margin,
        lax.axis_index("gy") * shape[1] - margin,
        lax.axis_index("gz") * shape[2] - margin,
    )


def padded_half(padded, source, scale, chosen):
    field = padded[1:-1, 1:-1, 1:-1]
    update = (source / scale + stencil_sum(padded)) / centre
    return jnp.where(chosen, update, field)


def wide_sweep(extended, wide_source, scale, red_wide, source, black):
    update = (wide_source / scale + stencil_sum(jnp.pad(extended, 1))) / centre
    extended = jnp.where(red_wide, update, extended)
    return padded_half(extended[1:-1, 1:-1, 1:-1], source, scale, black)


def coarse_level(source, level):
    shape = source.shape
    stack = lax.all_gather(source[None], ("gx", "gy", "gz"), axis=0, tiled=True)
    count_x, count_y, count_z = (lax.axis_size("gx"), lax.axis_size("gy"), lax.axis_size("gz"))
    whole = stack.reshape(count_x, count_y, count_z, shape[0], shape[1], shape[2])
    whole = whole.transpose(0, 3, 1, 4, 2, 5).reshape(
        count_x * shape[0], count_y * shape[1], count_z * shape[2]
    )
    solved = local_cycle(whole, level)
    starts = block_starts(shape, 0)
    return lax.dynamic_slice(solved, starts, shape)


def shared_cycle(source, level, top):
    if level == top:
        return coarse_level(source, level)
    scale = 0.25**level
    shape = source.shape
    whole = (
        shape[0] * lax.axis_size("gx"),
        shape[1] * lax.axis_size("gy"),
        shape[2] * lax.axis_size("gz"),
    )
    parity = parity_of(shape, block_starts(shape, 0))
    black = parity == 1
    wide_shape = (shape[0] + 4, shape[1] + 4, shape[2] + 4)
    wide_starts = block_starts(shape, 2)
    red_wide = (parity_of(wide_shape, wide_starts) == 0) & inside_grid(
        wide_shape, wide_starts, whole
    )
    wide_source = wide(source)
    field = wide_sweep(
        jnp.zeros(wide_shape, jnp.float32), wide_source, scale, red_wide, source, black
    )
    field = wide_sweep(wide(field), wide_source, scale, red_wide, source, black)
    residue = source - scale * (centre * field - stencil_sum(faces(field)))
    field = field + prolong(shared_cycle(restrict(residue), level + 1, top))
    for number in range(2):
        field = wide_sweep(wide(field), wide_source, scale, red_wide, source, black)
    return field


def pairs(count, first):
    swaps = []
    for i in range(first, count - 1, 2):
        swaps += [(i, i + 1), (i + 1, i)]
    return swaps


def inner_pairs(count_x, count):
    swaps = []
    for x in range(count_x):
        swaps += [(x * count + i, x * count + j) for i, j in pairs(count, 1)]
        swaps += [(x * count + i, (x ^ 1) * count + i) for i in (0, count - 1)]
    return swaps


def flips(count, bit):
    return [(i, i ^ bit) for i in range(count)]


def lanes_of(shape):
    return lax.broadcasted_iota(jnp.int32, shape, len(shape) - 1)


def rows_of(shape):
    return lax.broadcasted_iota(jnp.int32, shape, len(shape) - 2)


LANES = 128
PAD = 8


def odd_of(shape):
    return ((lanes_of(shape) + rows_of(shape)) & 1) == 1


def exact_dot(a, b):
    return jnp.dot(a, b, precision=lax.Precision.HIGHEST, preferred_element_type=jnp.float32)


def window(ref, at, column, count, start=0, shift=0):
    if isinstance(start, int):
        return ref[at, column, PAD + start + shift : PAD + start + shift + count, :]
    first = start + (PAD + shift)
    if shift == 0:
        first = pl.multiple_of(first, 8)
    return ref[at, column, pl.ds(first, count), :]


def clear_pads(ref):
    edge = jnp.zeros((PAD, LANES), jnp.float32)
    for at in range(ref.shape[0]):
        for column in range(ref.shape[1]):
            ref[at, column, :PAD, :] = edge
            ref[at, column, ref.shape[2] - PAD :, :] = edge


def block_sums(ref, at, rows):
    lane = lanes_of((rows, LANES))
    values = [window(ref, at, column, rows) for column in range(2)]
    lefts = [pltpu.roll(value, 1, 1) for value in values]
    rights = [pltpu.roll(value, LANES - 1, 1) for value in values]
    sums = []
    for column in range(2):
        left = jnp.where(lane == 0, lefts[1 - column], lefts[column])
        right = jnp.where(lane == LANES - 1, rights[1 - column], rights[column])
        sides = window(ref, at, column, rows, shift=-1) + window(ref, at, column, rows, shift=1)
        sums.append(values[column] + sides + (1.0 + rsd_beta) * (left + right))
    return sums


def block_totals(ref, at, rows, own, odd, to_red, at_low, at_high):
    slots = ref.shape[0]
    totals = []
    for column, total in enumerate(block_sums(ref, at, rows)):
        before = window(ref, (at - 1) % slots, column, rows)
        after = window(ref, (at + 1) % slots, column, rows)
        if at in (0, own):
            before = jnp.where(at_low if at == 0 else at_high, 0.0, before)
        if at in (own - 1, slots - 1):
            after = jnp.where(at_low if at == slots - 1 else at_high, 0.0, after)
        totals.append(total + (jnp.where(odd, after, before) if to_red else jnp.where(odd, before, after)))
    return totals


def block_mask(own, halo):
    ny, nz = own
    shape = (ny + 2 * halo, LANES)
    row = rows_of(shape) - halo + lax.axis_index("gy") * ny
    inside_y = (row >= 0) & (row < ny * lax.axis_size("gy"))
    masks = []
    for column in range(2):
        lane = lanes_of(shape)
        if column:
            lane = jnp.where(lane < halo, lane + LANES, lane - LANES)
        lane = lane + lax.axis_index("gz") * nz
        inside = inside_y & (lane >= 0) & (lane < nz * lax.axis_size("gz"))
        masks.append(jnp.where(inside, 1.0 / centre, 0.0))
    return masks


def block_plane(at, own_ref, ya_ref, yb_ref, even_y):
    a, b = ya_ref[at], yb_ref[at]
    low = jnp.where(even_y, b, a)
    high = jnp.where(even_y, a, b)
    return jnp.concatenate([low, own_ref[at], high], axis=0)


def block_columns(halo, at, own_ref, ya_ref, yb_ref, za_ref, zb_ref, even_y, even_z):
    _, _, nz = own_ref.shape
    j, k = at // (nz // halo), at % (nz // halo)
    a, b = za_ref[j], zb_ref[j]
    left = pltpu.roll(jnp.where(even_z, b, a), (2 * nz - halo - halo * k) % nz, 1)
    right = pltpu.roll(jnp.where(even_z, a, b), (nz - halo * k) % nz, 1)
    lane = lanes_of(left.shape)
    sides = jnp.where(lane < halo, right, jnp.where(lane >= nz - halo, left, 0.0))
    return block_plane(at, own_ref, ya_ref, yb_ref, even_y), sides


def pack_kernel(halo, own_ref, ya_ref, yb_ref, za_ref, zb_ref):
    even_y = lax.axis_index("gy") % 2 == 0
    even_z = lax.axis_index("gz") % 2 == 0
    nx, ny, nz = own_ref.shape
    groups = nz // halo
    shape = (ny + 2 * halo, nz)
    group = lanes_of(shape) // halo
    for j in range(za_ref.shape[0]):
        last = jnp.zeros(shape, jnp.float32)
        first = jnp.zeros(shape, jnp.float32)
        for k in range(min(groups, nx - j * groups)):
            plane = block_plane(j * groups + k, own_ref, ya_ref, yb_ref, even_y)
            last = jnp.where(group == k, pltpu.roll(plane, (halo * k + halo) % nz, 1), last)
            first = jnp.where(group == k, pltpu.roll(plane, halo * k, 1), first)
        za_ref[j] = jnp.where(even_z, last, first)
        zb_ref[j] = jnp.where(even_z, first, last)


def smooth(count, own, masks, odd, ends, gr_ref, gb_ref, red_ref, black_ref, done):
    rows = odd.shape[0]
    body = slice(PAD, PAD + rows)

    def value_of(source, at, c, total):
        value = masks[c] * total
        return source[at, c] + value if at < source.shape[0] else value

    for at in range(count):
        for c in range(2):
            red_ref[at, c, body, :] = gr_ref[at, c] if at < gr_ref.shape[0] else jnp.zeros_like(masks[c])
    for step in range(3):
        source, target, other = (gr_ref, red_ref, black_ref) if step == 1 else (gb_ref, black_ref, red_ref)
        for at in range(count):
            totals = block_totals(other, at, rows, own, odd, step == 1, *ends)
            for c in range(2):
                value = value_of(source, at, c, totals[c])
                target[at, c, body, :] = value
                if step == 2:
                    done(at, c, totals[c], value)


def x_ends():
    here = lax.axis_index("gx")
    return here == 0, here == lax.axis_size("gx") - 1


def pre_kernel(
    halo, own_ref, ya_ref, yb_ref, za_ref, zb_ref,
    send_ref, face_ref,
    fr_ref, fb_ref, gr_ref, gb_ref, red_ref, black_ref, rest_ref,
):
    even_y = lax.axis_index("gy") % 2 == 0
    even_z = lax.axis_index("gz") % 2 == 0
    nx, ny, nz = own_ref.shape
    count, _, rows, _ = red_ref.shape
    rows = rows - 2 * PAD
    own = nx // 2
    shape = (rows, LANES)
    odd = odd_of(shape)
    masks = block_mask((ny, nz), halo)
    inner = slice(halo, halo + ny)
    ends = x_ends()
    clear_pads(red_ref)
    clear_pads(black_ref)
    group = lanes_of(shape) // (2 * halo)
    low_sides = jnp.zeros(shape, jnp.float32)
    high_sides = jnp.zeros(shape, jnp.float32)
    for at in range(own):
        planes = []
        for x in (2 * at, 2 * at + 1):
            columns = block_columns(halo, x, own_ref, ya_ref, yb_ref, za_ref, zb_ref, even_y, even_z)
            planes.append(columns)
            if x < halo:
                turned = pltpu.roll(columns[1], (halo + 2 * halo * x) % LANES, 1)
                low_sides = jnp.where(group == x, turned, low_sides)
            if x >= nx - halo:
                p = x - (nx - halo)
                turned = pltpu.roll(columns[1], (halo + 2 * halo * p) % LANES, 1)
                high_sides = jnp.where(group == p, turned, high_sides)
        for c in range(2):
            red = jnp.where(odd, planes[1][c], planes[0][c])
            black = jnp.where(odd, planes[0][c], planes[1][c])
            if c == 0:
                fr_ref[at], fb_ref[at] = red[inner], black[inner]
            gr_ref[at, c], gb_ref[at, c] = masks[c] * red, masks[c] * black
    for p in range(halo):
        high = block_plane(nx - halo + p, own_ref, ya_ref, yb_ref, even_y)
        face_ref[p] = jnp.where(ends[0], high, block_plane(p, own_ref, ya_ref, yb_ref, even_y))
    face_ref[halo] = jnp.where(ends[0], high_sides, low_sides)

    def keep(at, c, total, value):
        if c == 0:
            left_over = total[inner] - centre * value[inner]
            rest_ref[at] = left_over + fb_ref[at] if at < own else left_over

    smooth(count, own, masks, odd, ends, gr_ref, gb_ref, red_ref, black_ref, keep)
    for at in range(count):
        total = block_totals(black_ref, at, rows, own, odd, True, *ends)[0]
        left_over = total[inner] - centre * red_ref[at, 0, PAD + halo : PAD + halo + ny, :]
        if at < own:
            left_over = left_over + fr_ref[at]
        rest_ref[at] = rest_ref[at] + left_over
    half, quarter = ny // 2, nz // 4
    pairs_y = rest_ref[:, pl.ds(0, half, stride=2), :] + rest_ref[:, pl.ds(1, half, stride=2), :]
    column = lanes_of((nz, nz))
    target = 2 * (column % quarter) + (column // quarter) % 2
    weight = jnp.where(rows_of((nz, nz)) // 2 == target, 0.5, 0.0)
    coarse = exact_dot(pairs_y.reshape(count * half, nz), weight).reshape(count, half, nz)
    part = lanes_of((half, nz)) // quarter
    pick = (((rows_of((half, nz)) + part) & 1) == 1) ^ (part >= 2)
    turn = quarter * lax.axis_index("gz")
    for at in range(count // 2):
        send_ref[at] = pltpu.roll(jnp.where(pick, coarse[2 * at + 1], coarse[2 * at]), turn, 1)


def field_kernel(
    halo, own_ref, ya_ref, yb_ref, za_ref, zb_ref, face_ref, after_ref,
    gr_ref, gb_ref, dark_ref,
    red_ref, black_ref,
):
    even_y = lax.axis_index("gy") % 2 == 0
    even_z = lax.axis_index("gz") % 2 == 0
    nx, ny, nz = own_ref.shape
    count, _, rows, _ = gr_ref.shape
    own = nx // 2
    shape = (rows, LANES)
    odd, lane = odd_of(shape), lanes_of(shape)
    masks = block_mask((ny, nz), halo)
    clear_pads(red_ref)
    clear_pads(black_ref)

    def columns(x):
        if x < nx:
            return block_columns(halo, x, own_ref, ya_ref, yb_ref, za_ref, zb_ref, even_y, even_z)
        p = x - nx
        sides = pltpu.roll(face_ref[halo], (2 * LANES - halo - 2 * halo * p) % LANES, 1)
        return face_ref[p], jnp.where((lane < halo) | (lane >= nz - halo), sides, 0.0)

    for at in range(count):
        first, second = columns(2 * at), columns(2 * at + 1)
        for c in range(2):
            gr_ref[at, c] = masks[c] * jnp.where(odd, second[c], first[c])
            gb_ref[at, c] = masks[c] * jnp.where(odd, first[c], second[c])

    def keep(at, c, total, value):
        dark_ref[at, c] = value

    smooth(count, own, masks, odd, x_ends(), gr_ref, gb_ref, red_ref, black_ref, keep)


def stack_kernel(*refs):
    for which, ref in enumerate(refs[:-1]):
        refs[-1][which] = ref[...]


def small_shapes(whole):
    return [whole[0] >> (level + 1) for level in range(2, LEVELS - 2)]


def plain_sum(field):
    padded = np.pad(field, ((0, 0), (1, 1), (1, 1), (1, 1)))
    inner = slice(1, -1)
    plane = padded[:, 2:, inner, inner] + padded[:, :-2, inner, inner]
    plane = plane + padded[:, inner, 2:, inner] + padded[:, inner, :-2, inner]
    return plane + (1.0 + rsd_beta) * (padded[:, inner, inner, 2:] + padded[:, inner, inner, :-2])


def plain_cycle(source, level):
    parity = np.indices(source.shape[1:]).sum(axis=0) % 2
    field = np.zeros_like(source)

    def sweeps(field, number):
        for step in range(2 * number):
            field = np.where(parity == step % 2, (source + plain_sum(field)) / centre, field)
        return field

    if level == LEVELS - 1:
        return sweeps(field, CSWEEPS)
    field = sweeps(field, 2)
    rest = source - centre * field + plain_sum(field)
    nx, ny, nz = source.shape[1:]
    rest = rest.reshape(-1, nx // 2, 2, ny // 2, 2, nz // 2, 2).sum(axis=(2, 4, 6)) / 2.0
    coarse = plain_cycle(rest, level + 1)
    for axis in (1, 2, 3):
        coarse = np.repeat(coarse, 2, axis)
    return sweeps(field + coarse, 2)


def cycle_matrix(whole):
    level = LEVELS - 2
    nx, ny, nz = (size >> level for size in whole)
    size = nx * ny * 2 * nz
    unit = np.eye(size).reshape(size, 2 * nz, nx, ny).transpose(0, 2, 3, 1)
    source = unit.reshape(size, nx, ny, nz, 2).sum(axis=-1) / 2.0
    result = np.repeat(plain_cycle(source, level), 2, axis=3)
    return jnp.asarray(result.transpose(0, 3, 1, 2).reshape(size, size), jnp.float32)


def solve_kernel(halo, whole, *refs):
    gathered, refs = refs[:8], refs[8:]
    gr_ref, gb_ref, dark_ref, matrix_ref, out_ref = refs[:5]
    fr1, fb1, red1, black1, rest1, tall_ref, red_ref, work_ref, passing = refs[5:14]
    small = [refs[14 + 4 * i : 18 + 4 * i] for i in range(LEVELS - 4)]
    gx, gy, gz = (lax.axis_index(axis) for axis in ("gx", "gy", "gz"))
    weight_z = 1.0 + rsd_beta
    share = 1.0 / centre
    for ref in (red1, black1, red_ref, work_ref, passing):
        clear_pads(ref)
    for level in small:
        for ref in level[2:]:
            clear_pads(ref)

    _, slots, block_rows, _ = gathered[0].shape
    slots = slots - 1
    count1, _, rows1, _ = fr1.shape
    quarter = LANES // 4
    group = lanes_of((block_rows, LANES)) // quarter
    held = [jnp.bitwise_and(group - jnp.bitwise_xor(gz, bits), 3) for bits in range(4)]
    theirs = [[kind == part for kind in held] for part in range(4)]
    def unpack(far, second, at):
        y = jnp.bitwise_xor(gy, 2 * far + (second >> 1))
        rows = pl.ds(pl.multiple_of(y * block_rows, 8), block_rows)
        blocks = [gathered[4 * (bits & 1) + second][far + (bits & 2), at] for bits in range(4)]
        parts = []
        for part in range(4):
            value = blocks[0]
            for block, mine in zip(blocks[1:], theirs[part][1:]):
                value = jnp.where(mine, block, value)
            parts.append(pltpu.roll(value, LANES - quarter * part, 1) if part else value)
        return rows, parts

    half1 = count1 // 2
    for far in range(2):
        for second in range(4):
            x = jnp.bitwise_xor(gx, second & 1)
            for at in range(slots):
                rows, parts = unpack(far, second, at)
                for part, target in enumerate((fr1, fr1, fb1, fb1)):
                    target[x * slots + at, part % 2, rows, :] = parts[part]
    for far in range(2):
        for second in range(4):
            x = jnp.bitwise_xor(gx, second & 1)
            next_slot = jnp.where(x == 0, half1, half1 - 1)
            rows, parts = unpack(far, second, slots)
            for part, target in enumerate((fr1, fr1, fb1, fb1)):
                target[next_slot, part % 2, rows, :] = target[next_slot, part % 2, rows, :] + parts[part]

    def fold_total(ref, at, e, start, count, low, high, odds, to_red):
        lane = lanes_of((count, LANES))
        value, other = window(ref, at, e, count, start), window(ref, at, 1 - e, count, start)
        sides = window(ref, at, e, count, start, -1) + window(ref, at, e, count, start, 1)
        if e == 0:
            near = jnp.where(lane == 0, 0.0, pltpu.roll(other, 1, 1))
        else:
            near = jnp.where(lane == LANES - 1, 0.0, pltpu.roll(other, LANES - 1, 1))
        before = 0.0 if low is True else window(ref, at - 1, e, count, start)
        after = 0.0 if high is True else window(ref, at + 1, e, count, start)
        if not isinstance(low, bool):
            before = jnp.where(low, 0.0, window(ref, jnp.maximum(at - 1, 0), e, count, start))
        if not isinstance(high, bool):
            after = jnp.where(high, 0.0, window(ref, jnp.minimum(at + 1, count1 - 1), e, count, start))
        beside = jnp.where(odds[e], after, before) if to_red else jnp.where(odds[e], before, after)
        return value + sides + beside + weight_z * (other + near)

    def fold_odds(count):
        row = rows_of((count, LANES))
        return [((row + e) & 1) == 1 for e in range(2)]

    odds = fold_odds(rows1)
    body1 = slice(PAD, PAD + rows1)

    def down_total(ref, at, e, to_red):
        return fold_total(ref, at, e, 0, rows1, at == 0, at == count1 - 1, odds, to_red)

    for at in range(count1):
        for e in range(2):
            red1[at, e, body1, :] = share * fr1[at, e]
    for at in range(count1):
        for e in range(2):
            black1[at, e, body1, :] = share * (fb1[at, e] + down_total(red1, at, e, False))
    for at in range(count1):
        for e in range(2):
            red1[at, e, body1, :] = share * (fr1[at, e] + down_total(black1, at, e, True))
    for at in range(count1):
        left_over = None
        for e in range(2):
            total = fb1[at, e] + down_total(red1, at, e, False)
            value = share * total
            black1[at, e, body1, :] = value
            term = total - centre * value
            left_over = term if left_over is None else left_over + term
        rest1[at] = left_over
    for at in range(count1):
        left_over = rest1[at]
        for e in range(2):
            total = fr1[at, e] + down_total(black1, at, e, True)
            left_over = left_over + (total - centre * window(red1, at, e, rows1))
        rest1[at] = left_over
    rows2 = rows1 // 2
    shape2 = (rows2, LANES)
    row2, lane2 = rows_of(shape2), lanes_of(shape2)
    odd2 = odd_of(shape2)
    planes = [
        0.5 * (rest1[at, pl.ds(0, rows2, stride=2), :] + rest1[at, pl.ds(1, rows2, stride=2), :])
        for at in range(count1)
    ]

    body2 = slice(PAD, PAD + rows2)

    def grid_of(index):
        step = 1 << index
        return ((row2 & (step - 1)) == 0) & ((lane2 & (step - 1)) == 0)

    def odd_at(index):
        return (((row2 >> index) + (lane2 >> index)) & 1) == 1

    def along(value, step):
        left = jnp.where(lane2 < step, 0.0, pltpu.roll(value, step, 1))
        right = jnp.where(lane2 >= LANES - step, 0.0, pltpu.roll(value, LANES - step, 1))
        return weight_z * (left + right)

    def small_total(index, ref, at, odd, to_red):
        step = 1 << index
        value = ref[at, 0, body2, :]
        total = value + along(value, step)
        total = total + (
            ref[at, 0, PAD - step : PAD - step + rows2, :] + ref[at, 0, PAD + step : PAD + step + rows2, :]
        )
        slots = ref.shape[0]
        if slots == 1:
            return total
        before = ref[at - 1, 0, body2, :] if at > 0 else 0.0
        after = ref[at + 1, 0, body2, :] if at < slots - 1 else 0.0
        return total + (jnp.where(odd, after, before) if to_red else jnp.where(odd, before, after))

    def small_sweeps(index, start):
        fr, fb, red, black = small[index]
        mask, odd = jnp.where(grid_of(index), share, 0.0), odd_at(index)
        slots = fr.shape[0]
        for step in range(2):
            for at in range(slots):
                source = fr[at]
                if not (start and step == 0):
                    source = source + small_total(index, black, at, odd, True)
                red[at, 0, body2, :] = mask * source
            for at in range(slots):
                black[at, 0, body2, :] = mask * (fb[at] + small_total(index, red, at, odd, False))

    def spread_rows(value, step, ref, at):
        ref[at, 0, body2, :] = value
        return value + ref[at, 0, PAD - step : PAD - step + rows2, :]

    last = len(small) - 1
    for index in range(len(small)):
        fr, fb, red, black = small[index]
        slots, odd, step = fr.shape[0], odd_at(index), 1 << index
        for at in range(slots):
            p, q = planes[2 * at], planes[2 * at + 1]
            fr[at], fb[at] = jnp.where(odd, q, p), jnp.where(odd, p, q)
        small_sweeps(index, True)
        totals = []
        for at in range(slots):
            first = fb[at] + small_total(index, red, at, odd, False) - centre * black[at, 0, body2, :]
            second = fr[at] + small_total(index, black, at, odd, True) - centre * red[at, 0, body2, :]
            totals.append(first + second)
        for at in range(slots):
            passing[at, 0, body2, :] = totals[at]
        lower = [passing[at, 0, PAD + step : PAD + step + rows2, :] for at in range(slots)]
        if index < last:
            totals = [total + below for total, below in zip(totals, lower)]
            planes = [0.5 * (total + pltpu.roll(total, LANES - step, 1)) for total in totals]

    half_rows = rows2 // 2
    upper = [passing[at, 0, PAD - step : PAD - step + rows2, :] for at in range(slots)]
    odd_line = (row2 & step) != 0
    summed = [
        total + jnp.where(odd_line, above, below) for total, above, below in zip(totals, upper, lower)
    ]
    lines = [total[start : start + half_rows] for total in summed for start in (0, half_rows)]
    place = lanes_of((half_rows, LANES)) & (len(lines) - 1)
    joined = lines[0]
    for q in range(1, len(lines)):
        joined = jnp.where(place == q, pltpu.roll(lines[q], q, 1), joined)
    answer = exact_dot(joined, matrix_ref[...])
    grid = (place == 0) & ((rows_of((half_rows, LANES)) & (step - 1)) == 0)
    parts = []
    for q in range(len(lines)):
        part = pltpu.roll(answer, LANES - q, 1) if q else answer
        parts.append(jnp.where(grid, part, 0.0))
    spreads = [jnp.concatenate(parts[2 * at : 2 * at + 2], axis=0) for at in range(slots)]

    for index in reversed(range(len(small))):
        _, _, red, black = small[index]
        slots, odd, step = red.shape[0], odd_at(index), 1 << index
        if index < last:
            spreads = [
                spread_rows(field + pltpu.roll(field, step, 1), step, passing, at)
                for at, field in enumerate(fields)
            ]
        for at in range(slots):
            black[at, 0, body2, :] = black[at, 0, body2, :] + spreads[at]
        small_sweeps(index, False)
        fields = []
        for at in range(slots):
            r, b = red[at, 0, body2, :], black[at, 0, body2, :]
            fields += [jnp.where(odd, b, r), jnp.where(odd, r, b)]

    for at in range(count1):
        for start in range(2):
            rest1[at, pl.ds(start, rows2, stride=2), :] = fields[at]
    for at in range(count1):
        for e in range(2):
            black1[at, e, body1, :] = window(black1, at, e, rows1) + rest1[at]
    nx, ny, nz = out_ref.shape
    own = nx // 2
    part_slots = min(own // 2 + 3, count1)
    part_rows = min(ny // 2 + 16, rows1)
    slot0 = jnp.where(gx == 0, 0, count1 - part_slots)
    row0 = pl.multiple_of(jnp.clip(gy * (ny // 2) - 8, 0, rows1 - part_rows), 8)
    odds = fold_odds(part_rows)

    def up_total(ref, at, e, to_red):
        low = gx == 0 if at == 0 else False
        high = gx != 0 if at == part_slots - 1 else False
        return fold_total(ref, slot0 + at, e, row0, part_rows, low, high, odds, to_red)

    def up_half(target, other, sources, to_red):
        for at in range(part_slots):
            for e in range(2):
                source = sources[slot0 + at, e, pl.ds(row0, part_rows), :]
                value = share * (source + up_total(other, at, e, to_red))
                target[slot0 + at, e, pl.ds(pl.multiple_of(row0 + PAD, 8), part_rows), :] = value

    for sweep in range(2):
        up_half(red1, black1, fr1, True)
        up_half(black1, red1, fb1, False)

    count, _, rows, _ = dark_ref.shape
    half = rows // 2
    odds = fold_odds(half)
    row = gy * (ny // 2) + (PAD - halo // 2)
    for at in range(count):
        if at < own:
            slot = gx * (own // 2) + at // 2
        else:
            slot = jnp.where(gx == 0, own // 2, own // 2 - (count - own) // 2) + (at - own) // 2
        for e in range(2):
            r, b = red1[slot, e, pl.ds(row, half), :], black1[slot, e, pl.ds(row, half), :]
            plane = jnp.where(odds[e], r, b) if at % 2 else jnp.where(odds[e], b, r)
            tall_ref[at, :, e * LANES : (e + 1) * LANES] = plane
    shape = (2 * LANES, 2 * LANES)
    z = lanes_of(shape)
    z = jnp.where(z < 2 * LANES - halo, z, z - 2 * LANES) + gz * nz
    line = rows_of(shape)
    line = jnp.where(line < LANES, 2 * line, 2 * (line - LANES) + 1)
    weight = jnp.where(line == lax.shift_right_arithmetic(z, 1), 1.0, 0.0)
    spread = exact_dot(tall_ref[...].reshape(count * half, 2 * LANES), weight)
    spread = spread.reshape(count, half, 2 * LANES)
    for at in range(count):
        for c in range(2):
            value = spread[at, :, c * LANES : (c + 1) * LANES]
            for start in range(2):
                work_ref[at, c, pl.ds(PAD + start, half, stride=2), :] = value
    body = slice(PAD, PAD + rows)
    for at in range(count):
        for c in range(2):
            work_ref[at, c, body, :] = work_ref[at, c, body, :] + dark_ref[at, c]
    odd = odd_of((rows, LANES))
    masks = block_mask((ny, nz), halo)
    ends = (gx == 0, gx == lax.axis_size("gx") - 1)
    for sweep in range(2):
        for at in range(count):
            totals = block_totals(work_ref, at, rows, own, odd, True, *ends)
            for c in range(2):
                red_ref[at, c, body, :] = gr_ref[at, c] + masks[c] * totals[c]
        for at in range(count if sweep == 0 else own):
            totals = block_totals(red_ref, at, rows, own, odd, False, *ends)
            for c in range(2 if sweep == 0 else 1):
                work_ref[at, c, body, :] = gb_ref[at, c] + masks[c] * totals[c]
    inner = slice(PAD + halo, PAD + halo + ny)
    odd = odd_of((ny, nz))
    for at in range(own):
        r, b = red_ref[at, 0, inner, :], work_ref[at, 0, inner, :]
        out_ref[2 * at] = jnp.where(odd, b, r)
        out_ref[2 * at + 1] = jnp.where(odd, r, b)


def vmem(number):
    return [pl.BlockSpec(memory_space=pltpu.VMEM)] * number


def struct(*shape):
    return jax.ShapeDtypeStruct(shape, jnp.float32)


def scratch(*shape):
    return pltpu.VMEM(shape, jnp.float32)


HALO = 8


def block_cycle(density):
    halo = HALO
    nx, ny, nz = density.shape
    count_x, count_y, count_z = (lax.axis_size(axis) for axis in ("gx", "gy", "gz"))
    whole = (nx * count_x, ny * count_y, nz * count_z)
    even = lax.axis_index("gy") % 2 == 0
    ya = lax.dynamic_slice_in_dim(density, jnp.where(even, ny - halo, 0), halo, 1)
    yb = lax.dynamic_slice_in_dim(density, jnp.where(even, 0, ny - halo), halo, 1)
    ya = lax.ppermute(ya, "gy", pairs(count_y, 0))
    yb = lax.ppermute(yb, ("gx", "gy"), inner_pairs(count_x, count_y))
    rows = ny + 2 * halo
    packs = -(-nx * halo // nz)

    def params(mib):
        return pltpu.CompilerParams(vmem_limit_bytes=mib * 1024 * 1024)

    za, zb = pl.pallas_call(
        functools.partial(pack_kernel, halo),
        out_shape=[struct(packs, rows, nz)] * 2,
        in_specs=vmem(3), out_specs=vmem(2), compiler_params=params(4),
    )(density, ya, yb)
    za = lax.ppermute(za, "gz", pairs(count_z, 0))
    zb = lax.ppermute(zb, "gz", pairs(count_z, 1) + [(0, count_z - 1), (count_z - 1, 0)])
    own, near = nx // 2, nx // 2 + 2
    send, face = pl.pallas_call(
        functools.partial(pre_kernel, halo),
        out_shape=[struct(near // 2, ny // 2, nz), struct(halo + 1, rows, LANES)],
        in_specs=vmem(5), out_specs=vmem(2), compiler_params=params(10),
        scratch_shapes=[scratch(own, ny, nz)] * 2
        + [scratch(own, 2, rows, LANES)] * 2
        + [scratch(near, 2, rows + 2 * PAD, LANES)] * 2
        + [scratch(near, ny, nz)],
    )(density, ya, yb, za, zb)
    face = lax.ppermute(face, "gx", flips(count_x, 1))
    planes = nx + halo
    slots = (planes // 2, 2, rows, LANES)
    padded = (planes // 2, 2, rows + 2 * PAD, LANES)
    first = [
        send,
        lax.ppermute(send, "gy", flips(count_y, 2)),
        lax.ppermute(send, "gz", flips(count_z, 2)),
        lax.ppermute(send, ("gy", "gz"), flips(count_y * count_z, 2 * count_z + 2)),
    ]
    first[3], face = lax.optimization_barrier((first[3], face))
    block = pl.pallas_call(
        stack_kernel, out_shape=struct(4, *send.shape),
        in_specs=vmem(4), out_specs=pl.BlockSpec(memory_space=pltpu.VMEM), compiler_params=params(2),
    )(*first)
    second = [
        block,
        lax.ppermute(block, "gx", flips(count_x, 1)),
        lax.ppermute(block, "gy", flips(count_y, 1)),
        lax.ppermute(block, ("gx", "gy"), flips(count_x * count_y, count_y + 1)),
    ]
    gr, gb, black = pl.pallas_call(
        functools.partial(field_kernel, halo),
        out_shape=[struct(*slots)] * 3,
        in_specs=vmem(7), out_specs=vmem(3), compiler_params=params(8),
        scratch_shapes=[scratch(*padded)] * 2,
        cost_estimate=pl.CostEstimate(flops=20_000_000, bytes_accessed=2_000_000, transcendentals=0),
    )(density, ya, yb, za, zb, face, block)
    *second[1:], gr, gb, black = lax.optimization_barrier((*second[1:], gr, gb, black))
    third = [lax.ppermute(blocks, "gz", flips(count_z, 1)) for blocks in second]
    count1, rows1, rows2 = whole[0] // 4, whole[1] // 2, whole[1] // 4
    room = [scratch(count1, 2, rows1, LANES)] * 2
    room += [scratch(count1, 2, rows1 + 2 * PAD, LANES)] * 2
    room += [scratch(count1, rows1, LANES), scratch(planes // 2, rows // 2, 2 * LANES)]
    room += [scratch(*padded)] * 2 + [scratch(count1 // 2, 1, rows2 + 2 * PAD, LANES)]
    for count in small_shapes(whole):
        room += [scratch(count, rows2, LANES)] * 2
        room += [scratch(count, 1, rows2 + 2 * PAD, LANES)] * 2
    return pl.pallas_call(
        functools.partial(solve_kernel, halo, whole),
        out_shape=struct(nx, ny, nz),
        in_specs=vmem(12), out_specs=pl.BlockSpec(memory_space=pltpu.VMEM),
        compiler_params=params(16), scratch_shapes=room,
    )(*second, *third, gr, gb, black, cycle_matrix(whole))


def fits_block_cycle(shape):
    nx, ny, nz = shape
    count_x, count_y, count_z = (lax.axis_size(axis) for axis in ("gx", "gy", "gz"))
    whole = (nx * count_x, ny * count_y, nz * count_z)
    coarsest = [size >> (LEVELS - 1) for size in whole]
    exact = all(c << (LEVELS - 1) == size for c, size in zip(coarsest, whole))
    return (
        exact and coarsest[0] == coarsest[1] == 1 and nz == LANES and ny == 2 * HALO
        and count_x == 2 and count_y == 4 and count_z == 4
    )


def on_device(density):
    if fits_block_cycle(density.shape):
        return block_cycle(density)
    top = 4
    return shared_cycle(density, 0, top)


def solution(mesh):
    return jax.shard_map(
        on_device,
        mesh=mesh,
        in_specs=(P("gx", "gy", "gz"),),
        out_specs=P("gx", "gy", "gz"),
        check_vma=False,
    )
```

```python
import functools

import jax
import jax.numpy as jnp
import numpy as np
from jax import lax
from jax.experimental import pallas as pl
from jax.experimental.pallas import tpu as pltpu
from jax.sharding import PartitionSpec as P

LEVELS = 7
CSWEEPS = 4


rsd_beta = 0.5
centre = 4.0 + 2.0 * (1.0 + rsd_beta)


def extended_2(value, sides, width):
    for axis, dim in sides:
        count, length = (lax.axis_size(axis), value.shape[dim])
        up = [(i, (i + 1) % count) for i in range(count - 1)]
        down = [(j, i) for i, j in up]
        last = lax.slice_in_dim(value, length - width, length, axis=dim)
        leading = lax.slice_in_dim(value, 0, width, axis=dim)
        before = lax.ppermute(last, axis, up)
        after = lax.ppermute(leading, axis, down)
        value = jnp.concatenate([before, value, after], axis=dim)
    return value


def stencil_sum(padded):
    plane = (
        padded[2:, 1:-1, 1:-1]
        + padded[:-2, 1:-1, 1:-1]
        + padded[1:-1, 2:, 1:-1]
        + padded[1:-1, :-2, 1:-1]
    )
    sight = padded[1:-1, 1:-1, 2:] + padded[1:-1, 1:-1, :-2]
    return plane + (1.0 + rsd_beta) * sight


def grid_index(shape, starts):
    return [lax.broadcasted_iota(jnp.int32, shape, which) + starts[which] for which in range(3)]


def parity_of(shape, starts):
    position = grid_index(shape, starts)
    return (position[0] + position[1] + position[2] + 6) % 2


def inside_grid(shape, starts, whole):
    position = grid_index(shape, starts)
    keep = (position[0] >= 0) & (position[0] < whole[0])
    for which in (1, 2):
        keep = keep & (position[which] >= 0) & (position[which] < whole[which])
    return keep


def half_sweep(field, source, scale, chosen):
    update = (source / scale + stencil_sum(jnp.pad(field, 1))) / centre
    return jnp.where(chosen, update, field)


def full_sweep(field, source, scale, parity):
    field = half_sweep(field, source, scale, parity == 0)
    return half_sweep(field, source, scale, parity == 1)


def restrict(residue):
    shape = residue.shape
    blocks = residue.reshape(shape[0] // 2, 2, shape[1] // 2, 2, shape[2] // 2, 2)
    return jnp.mean(blocks, axis=(1, 3, 5))


def prolong(coarse):
    return jnp.repeat(jnp.repeat(jnp.repeat(coarse, 2, 0), 2, 1), 2, 2)


def local_cycle(source, level):
    scale = 0.25**level
    parity = parity_of(source.shape, (0, 0, 0))
    field = jnp.zeros_like(source)
    if level == LEVELS - 1:
        for number in range(CSWEEPS):
            field = full_sweep(field, source, scale, parity)
        return field
    for number in range(2):
        field = full_sweep(field, source, scale, parity)
    residue = source - scale * (centre * field - stencil_sum(jnp.pad(field, 1)))
    field = field + prolong(local_cycle(restrict(residue), level + 1))
    for number in range(2):
        field = full_sweep(field, source, scale, parity)
    return field


def faces(field):
    return extended_2(field, (("gx", 0), ("gy", 1), ("gz", 2)), 1)


def wide(field):
    return extended_2(field, (("gx", 0), ("gy", 1), ("gz", 2)), 2)


def block_starts(shape, margin):
    return (
        lax.axis_index("gx") * shape[0] - margin,
        lax.axis_index("gy") * shape[1] - margin,
        lax.axis_index("gz") * shape[2] - margin,
    )


def padded_half(padded, source, scale, chosen):
    field = padded[1:-1, 1:-1, 1:-1]
    update = (source / scale + stencil_sum(padded)) / centre
    return jnp.where(chosen, update, field)


def wide_sweep(extended, wide_source, scale, red_wide, source, black):
    update = (wide_source / scale + stencil_sum(jnp.pad(extended, 1))) / centre
    extended = jnp.where(red_wide, update, extended)
    return padded_half(extended[1:-1, 1:-1, 1:-1], source, scale, black)


def coarse_level(source, level):
    shape = source.shape
    stack = lax.all_gather(source[None], ("gx", "gy", "gz"), axis=0, tiled=True)
    count_x, count_y, count_z = (lax.axis_size("gx"), lax.axis_size("gy"), lax.axis_size("gz"))
    whole = stack.reshape(count_x, count_y, count_z, shape[0], shape[1], shape[2])
    whole = whole.transpose(0, 3, 1, 4, 2, 5).reshape(
        count_x * shape[0], count_y * shape[1], count_z * shape[2]
    )
    solved = local_cycle(whole, level)
    starts = block_starts(shape, 0)
    return lax.dynamic_slice(solved, starts, shape)


def shared_cycle(source, level, top):
    if level == top:
        return coarse_level(source, level)
    scale = 0.25**level
    shape = source.shape
    whole = (
        shape[0] * lax.axis_size("gx"),
        shape[1] * lax.axis_size("gy"),
        shape[2] * lax.axis_size("gz"),
    )
    parity = parity_of(shape, block_starts(shape, 0))
    black = parity == 1
    wide_shape = (shape[0] + 4, shape[1] + 4, shape[2] + 4)
    wide_starts = block_starts(shape, 2)
    red_wide = (parity_of(wide_shape, wide_starts) == 0) & inside_grid(
        wide_shape, wide_starts, whole
    )
    wide_source = wide(source)
    field = wide_sweep(
        jnp.zeros(wide_shape, jnp.float32), wide_source, scale, red_wide, source, black
    )
    field = wide_sweep(wide(field), wide_source, scale, red_wide, source, black)
    residue = source - scale * (centre * field - stencil_sum(faces(field)))
    field = field + prolong(shared_cycle(restrict(residue), level + 1, top))
    for number in range(2):
        field = wide_sweep(wide(field), wide_source, scale, red_wide, source, black)
    return field


def pairs(count, first):
    swaps = []
    for i in range(first, count - 1, 2):
        swaps += [(i, i + 1), (i + 1, i)]
    return swaps


def inner_pairs(count_x, count):
    swaps = []
    for x in range(count_x):
        swaps += [(x * count + i, x * count + j) for i, j in pairs(count, 1)]
        swaps += [(x * count + i, (x ^ 1) * count + i) for i in (0, count - 1)]
    return swaps


def flips(count, bit):
    return [(i, i ^ bit) for i in range(count)]


def lanes_of(shape):
    return lax.broadcasted_iota(jnp.int32, shape, len(shape) - 1)


def rows_of(shape):
    return lax.broadcasted_iota(jnp.int32, shape, len(shape) - 2)


LANES = 128
PAD = 8


def odd_of(shape):
    return ((lanes_of(shape) + rows_of(shape)) & 1) == 1


def exact_dot(a, b):
    return jnp.dot(a, b, precision=lax.Precision.HIGHEST, preferred_element_type=jnp.float32)


def window(ref, at, column, count, start=0, shift=0):
    if isinstance(start, int):
        return ref[at, column, PAD + start + shift : PAD + start + shift + count, :]
    first = start + (PAD + shift)
    if shift == 0:
        first = pl.multiple_of(first, 8)
    return ref[at, column, pl.ds(first, count), :]


def clear_pads(ref):
    edge = jnp.zeros((PAD, LANES), jnp.float32)
    for at in range(ref.shape[0]):
        for column in range(ref.shape[1]):
            ref[at, column, :PAD, :] = edge
            ref[at, column, ref.shape[2] - PAD :, :] = edge


def block_sums(ref, at, rows):
    lane = lanes_of((rows, LANES))
    values = [window(ref, at, column, rows) for column in range(2)]
    lefts = [pltpu.roll(value, 1, 1) for value in values]
    rights = [pltpu.roll(value, LANES - 1, 1) for value in values]
    sums = []
    for column in range(2):
        left = jnp.where(lane == 0, lefts[1 - column], lefts[column])
        right = jnp.where(lane == LANES - 1, rights[1 - column], rights[column])
        sides = window(ref, at, column, rows, shift=-1) + window(ref, at, column, rows, shift=1)
        sums.append(values[column] + sides + (1.0 + rsd_beta) * (left + right))
    return sums


def block_totals(ref, at, rows, own, odd, to_red, at_low, at_high):
    slots = ref.shape[0]
    totals = []
    for column, total in enumerate(block_sums(ref, at, rows)):
        before = window(ref, (at - 1) % slots, column, rows)
        after = window(ref, (at + 1) % slots, column, rows)
        if at in (0, own):
            before = jnp.where(at_low if at == 0 else at_high, 0.0, before)
        if at in (own - 1, slots - 1):
            after = jnp.where(at_low if at == slots - 1 else at_high, 0.0, after)
        totals.append(total + (jnp.where(odd, after, before) if to_red else jnp.where(odd, before, after)))
    return totals


def block_mask(own, halo):
    ny, nz = own
    shape = (ny + 2 * halo, LANES)
    row = rows_of(shape) - halo + lax.axis_index("gy") * ny
    inside_y = (row >= 0) & (row < ny * lax.axis_size("gy"))
    masks = []
    for column in range(2):
        lane = lanes_of(shape)
        if column:
            lane = jnp.where(lane < halo, lane + LANES, lane - LANES)
        lane = lane + lax.axis_index("gz") * nz
        inside = inside_y & (lane >= 0) & (lane < nz * lax.axis_size("gz"))
        masks.append(jnp.where(inside, 1.0 / centre, 0.0))
    return masks


def block_plane(at, own_ref, ya_ref, yb_ref, even_y):
    a, b = ya_ref[at], yb_ref[at]
    low = jnp.where(even_y, b, a)
    high = jnp.where(even_y, a, b)
    return jnp.concatenate([low, own_ref[at], high], axis=0)


def block_columns(halo, at, own_ref, ya_ref, yb_ref, za_ref, zb_ref, even_y, even_z):
    _, _, nz = own_ref.shape
    j, k = at // (nz // halo), at % (nz // halo)
    a, b = za_ref[j], zb_ref[j]
    left = pltpu.roll(jnp.where(even_z, b, a), (2 * nz - halo - halo * k) % nz, 1)
    right = pltpu.roll(jnp.where(even_z, a, b), (nz - halo * k) % nz, 1)
    lane = lanes_of(left.shape)
    sides = jnp.where(lane < halo, right, jnp.where(lane >= nz - halo, left, 0.0))
    return block_plane(at, own_ref, ya_ref, yb_ref, even_y), sides


def faces_kernel(halo, own_ref, ya_ref, yb_ref, sems):
    even = lax.axis_index("gy") % 2 == 0
    far = own_ref.shape[1] - halo
    copies = []
    for which, (ref, start) in enumerate(((ya_ref, jnp.where(even, far, 0)), (yb_ref, jnp.where(even, 0, far)))):
        face = own_ref.at[:, pl.ds(pl.multiple_of(start, 8), halo), :]
        copies.append(pltpu.make_async_copy(face, ref, sems.at[which]))
        copies[-1].start()
    for copy in copies:
        copy.wait()


def pack_kernel(halo, own_ref, ya_ref, yb_ref, za_ref, zb_ref):
    even_y = lax.axis_index("gy") % 2 == 0
    even_z = lax.axis_index("gz") % 2 == 0
    nx, ny, nz = own_ref.shape
    groups = nz // halo
    shape = (ny + 2 * halo, nz)
    group = lanes_of(shape) // halo
    for j in range(za_ref.shape[0]):
        last = jnp.zeros(shape, jnp.float32)
        first = jnp.zeros(shape, jnp.float32)
        for k in range(min(groups, nx - j * groups)):
            plane = block_plane(j * groups + k, own_ref, ya_ref, yb_ref, even_y)
            last = jnp.where(group == k, pltpu.roll(plane, (halo * k + halo) % nz, 1), last)
            first = jnp.where(group == k, pltpu.roll(plane, halo * k, 1), first)
        za_ref[j] = jnp.where(even_z, last, first)
        zb_ref[j] = jnp.where(even_z, first, last)


def smooth(count, own, masks, odd, ends, gr_ref, gb_ref, red_ref, black_ref, done):
    rows = odd.shape[0]
    body = slice(PAD, PAD + rows)

    def value_of(source, at, c, total):
        value = masks[c] * total
        return source[at, c] + value if at < source.shape[0] else value

    for at in range(count):
        for c in range(2):
            red_ref[at, c, body, :] = gr_ref[at, c] if at < gr_ref.shape[0] else jnp.zeros_like(masks[c])
    for step in range(3):
        source, target, other = (gr_ref, red_ref, black_ref) if step == 1 else (gb_ref, black_ref, red_ref)
        for at in range(count):
            totals = block_totals(other, at, rows, own, odd, step == 1, *ends)
            for c in range(2):
                value = value_of(source, at, c, totals[c])
                target[at, c, body, :] = value
                if step == 2:
                    done(at, c, totals[c], value)


def x_ends():
    here = lax.axis_index("gx")
    return here == 0, here == lax.axis_size("gx") - 1


def pre_kernel(
    halo, own_ref, ya_ref, yb_ref, za_ref, zb_ref,
    send_ref, face_ref,
    fr_ref, fb_ref, gr_ref, gb_ref, red_ref, black_ref, rest_ref,
):
    even_y = lax.axis_index("gy") % 2 == 0
    even_z = lax.axis_index("gz") % 2 == 0
    nx, ny, nz = own_ref.shape
    count, _, rows, _ = red_ref.shape
    rows = rows - 2 * PAD
    own = nx // 2
    shape = (rows, LANES)
    odd = odd_of(shape)
    masks = block_mask((ny, nz), halo)
    inner = slice(halo, halo + ny)
    ends = x_ends()
    clear_pads(red_ref)
    clear_pads(black_ref)
    for p in range(halo):
        high = block_plane(nx - halo + p, own_ref, ya_ref, yb_ref, even_y)
        face_ref[p] = jnp.where(ends[0], high, block_plane(p, own_ref, ya_ref, yb_ref, even_y))
    middle = halo * halo
    top = za_ref.shape[0] - 1
    left = [jnp.where(even_z, zb_ref[j], za_ref[j]) for j in (0, top)]
    right = [jnp.where(even_z, za_ref[j], zb_ref[j]) for j in (0, top)]
    left = jnp.where(ends[0], pltpu.roll(left[1], middle, 1), left[0])
    right = jnp.where(ends[0], right[1], pltpu.roll(right[0], middle, 1))
    face_ref[halo] = jnp.where(lanes_of(shape) < middle, left, right)
    for at in range(own):
        planes = [
            block_columns(halo, x, own_ref, ya_ref, yb_ref, za_ref, zb_ref, even_y, even_z)
            for x in (2 * at, 2 * at + 1)
        ]
        for c in range(2):
            red = jnp.where(odd, planes[1][c], planes[0][c])
            black = jnp.where(odd, planes[0][c], planes[1][c])
            if c == 0:
                fr_ref[at], fb_ref[at] = red[inner], black[inner]
            gr_ref[at, c], gb_ref[at, c] = masks[c] * red, masks[c] * black

    def keep(at, c, total, value):
        if c == 0:
            left_over = total[inner] - centre * value[inner]
            rest_ref[at] = left_over + fb_ref[at] if at < own else left_over

    smooth(count, own, masks, odd, ends, gr_ref, gb_ref, red_ref, black_ref, keep)
    for at in range(count):
        total = block_totals(black_ref, at, rows, own, odd, True, *ends)[0]
        left_over = total[inner] - centre * red_ref[at, 0, PAD + halo : PAD + halo + ny, :]
        if at < own:
            left_over = left_over + fr_ref[at]
        rest_ref[at] = rest_ref[at] + left_over
    half, quarter = ny // 2, nz // 4
    pairs_y = rest_ref[:, pl.ds(0, half, stride=2), :] + rest_ref[:, pl.ds(1, half, stride=2), :]
    turn = quarter * lax.axis_index("gz")
    column = (lanes_of((nz, nz)) - turn) & (nz - 1)
    target = 2 * (column % quarter) + (column // quarter) % 2
    weight = jnp.where(rows_of((nz, nz)) // 2 == target, 0.5, 0.0)
    coarse = exact_dot(pairs_y.reshape(count * half, nz), weight).reshape(count, half, nz)
    part = ((lanes_of((half, nz)) - turn) & (nz - 1)) // quarter
    pick = (((rows_of((half, nz)) + part) & 1) == 1) ^ (part >= 2)
    for at in range(count // 2):
        send_ref[at] = jnp.where(pick, coarse[2 * at + 1], coarse[2 * at])


def field_kernel(
    halo, own_ref, ya_ref, yb_ref, za_ref, zb_ref, face_ref, after_ref,
    gr_ref, gb_ref, dark_ref,
    red_ref, black_ref,
):
    even_y = lax.axis_index("gy") % 2 == 0
    even_z = lax.axis_index("gz") % 2 == 0
    nx, ny, nz = own_ref.shape
    count, _, rows, _ = gr_ref.shape
    own = nx // 2
    shape = (rows, LANES)
    odd, lane = odd_of(shape), lanes_of(shape)
    masks = block_mask((ny, nz), halo)
    clear_pads(red_ref)
    clear_pads(black_ref)

    def columns(x):
        if x < nx:
            return block_columns(halo, x, own_ref, ya_ref, yb_ref, za_ref, zb_ref, even_y, even_z)
        p = x - nx
        left = pltpu.roll(face_ref[halo], (2 * LANES - halo - halo * p) % LANES, 1)
        right = pltpu.roll(face_ref[halo], (2 * LANES - halo * halo - halo * p) % LANES, 1)
        return face_ref[p], jnp.where(lane < halo, right, jnp.where(lane >= nz - halo, left, 0.0))

    for at in range(count):
        first, second = columns(2 * at), columns(2 * at + 1)
        for c in range(2):
            gr_ref[at, c] = masks[c] * jnp.where(odd, second[c], first[c])
            gb_ref[at, c] = masks[c] * jnp.where(odd, first[c], second[c])

    def keep(at, c, total, value):
        dark_ref[at, c] = value

    smooth(count, own, masks, odd, x_ends(), gr_ref, gb_ref, red_ref, black_ref, keep)


def stack_kernel(*refs):
    for which, ref in enumerate(refs[:-1]):
        refs[-1][which] = ref[...]


def small_shapes(whole):
    return [whole[0] >> (level + 1) for level in range(2, LEVELS - 2)]


def plain_sum(field):
    padded = np.pad(field, ((0, 0), (1, 1), (1, 1), (1, 1)))
    inner = slice(1, -1)
    plane = padded[:, 2:, inner, inner] + padded[:, :-2, inner, inner]
    plane = plane + padded[:, inner, 2:, inner] + padded[:, inner, :-2, inner]
    return plane + (1.0 + rsd_beta) * (padded[:, inner, inner, 2:] + padded[:, inner, inner, :-2])


def plain_cycle(source, level):
    parity = np.indices(source.shape[1:]).sum(axis=0) % 2
    field = np.zeros_like(source)

    def sweeps(field, number):
        for step in range(2 * number):
            field = np.where(parity == step % 2, (source + plain_sum(field)) / centre, field)
        return field

    if level == LEVELS - 1:
        return sweeps(field, CSWEEPS)
    field = sweeps(field, 2)
    rest = source - centre * field + plain_sum(field)
    nx, ny, nz = source.shape[1:]
    rest = rest.reshape(-1, nx // 2, 2, ny // 2, 2, nz // 2, 2).sum(axis=(2, 4, 6)) / 2.0
    coarse = plain_cycle(rest, level + 1)
    for axis in (1, 2, 3):
        coarse = np.repeat(coarse, 2, axis)
    return sweeps(field + coarse, 2)


def cycle_matrix(whole):
    level = LEVELS - 2
    nx, ny, nz = (size >> level for size in whole)
    size = nx * ny * 2 * nz
    unit = np.eye(size).reshape(size, 2 * nz, nx, ny).transpose(0, 2, 3, 1)
    source = unit.reshape(size, nx, ny, nz, 2).sum(axis=-1) / 2.0
    result = np.repeat(plain_cycle(source, level), 2, axis=3)
    return jnp.asarray(result.transpose(0, 3, 1, 2).reshape(size, size), jnp.float32)


def solve_kernel(halo, whole, *refs):
    gathered, refs = refs[:8], refs[8:]
    gr_ref, gb_ref, dark_ref, matrix_ref, out_ref = refs[:5]
    fr1, fb1, red1, black1, rest1, tall_ref, red_ref, work_ref, passing = refs[5:14]
    small = [refs[14 + 4 * i : 18 + 4 * i] for i in range(LEVELS - 4)]
    gx, gy, gz = (lax.axis_index(axis) for axis in ("gx", "gy", "gz"))
    weight_z = 1.0 + rsd_beta
    share = 1.0 / centre
    for ref in (red1, black1, red_ref, work_ref, passing):
        clear_pads(ref)
    for level in small:
        for ref in level[2:]:
            clear_pads(ref)

    _, slots, block_rows, _ = gathered[0].shape
    slots = slots - 1
    count1, _, rows1, _ = fr1.shape
    quarter = LANES // 4
    group = lanes_of((block_rows, LANES)) // quarter
    held = [jnp.bitwise_and(group - jnp.bitwise_xor(gz, bits), 3) for bits in range(4)]
    theirs = [[kind == part for kind in held] for part in range(4)]
    def unpack(far, second, at):
        y = jnp.bitwise_xor(gy, 2 * far + (second >> 1))
        rows = pl.ds(pl.multiple_of(y * block_rows, 8), block_rows)
        blocks = [gathered[4 * (bits & 1) + second][far + (bits & 2), at] for bits in range(4)]
        parts = []
        for part in range(4):
            value = blocks[0]
            for block, mine in zip(blocks[1:], theirs[part][1:]):
                value = jnp.where(mine, block, value)
            parts.append(pltpu.roll(value, LANES - quarter * part, 1) if part else value)
        return rows, parts

    half1 = count1 // 2
    for far in range(2):
        for second in range(4):
            x = jnp.bitwise_xor(gx, second & 1)
            for at in range(slots):
                rows, parts = unpack(far, second, at)
                for part, target in enumerate((fr1, fr1, fb1, fb1)):
                    target[x * slots + at, part % 2, rows, :] = parts[part]
    for far in range(2):
        for second in range(4):
            x = jnp.bitwise_xor(gx, second & 1)
            next_slot = jnp.where(x == 0, half1, half1 - 1)
            rows, parts = unpack(far, second, slots)
            for part, target in enumerate((fr1, fr1, fb1, fb1)):
                target[next_slot, part % 2, rows, :] = target[next_slot, part % 2, rows, :] + parts[part]

    def fold_total(ref, at, e, start, count, low, high, odds, to_red):
        lane = lanes_of((count, LANES))
        value, other = window(ref, at, e, count, start), window(ref, at, 1 - e, count, start)
        sides = window(ref, at, e, count, start, -1) + window(ref, at, e, count, start, 1)
        if e == 0:
            near = jnp.where(lane == 0, 0.0, pltpu.roll(other, 1, 1))
        else:
            near = jnp.where(lane == LANES - 1, 0.0, pltpu.roll(other, LANES - 1, 1))
        before = 0.0 if low is True else window(ref, at - 1, e, count, start)
        after = 0.0 if high is True else window(ref, at + 1, e, count, start)
        if not isinstance(low, bool):
            before = jnp.where(low, 0.0, window(ref, jnp.maximum(at - 1, 0), e, count, start))
        if not isinstance(high, bool):
            after = jnp.where(high, 0.0, window(ref, jnp.minimum(at + 1, count1 - 1), e, count, start))
        beside = jnp.where(odds[e], after, before) if to_red else jnp.where(odds[e], before, after)
        return value + sides + beside + weight_z * (other + near)

    def fold_odds(count):
        row = rows_of((count, LANES))
        return [((row + e) & 1) == 1 for e in range(2)]

    odds = fold_odds(rows1)
    body1 = slice(PAD, PAD + rows1)

    def down_total(ref, at, e, to_red):
        return fold_total(ref, at, e, 0, rows1, at == 0, at == count1 - 1, odds, to_red)

    for at in range(count1):
        for e in range(2):
            red1[at, e, body1, :] = share * fr1[at, e]
    for at in range(count1):
        for e in range(2):
            black1[at, e, body1, :] = share * (fb1[at, e] + down_total(red1, at, e, False))
    for at in range(count1):
        for e in range(2):
            red1[at, e, body1, :] = share * (fr1[at, e] + down_total(black1, at, e, True))
    for at in range(count1):
        left_over = None
        for e in range(2):
            total = fb1[at, e] + down_total(red1, at, e, False)
            value = share * total
            black1[at, e, body1, :] = value
            term = total - centre * value
            left_over = term if left_over is None else left_over + term
        rest1[at] = left_over
    for at in range(count1):
        left_over = rest1[at]
        for e in range(2):
            total = fr1[at, e] + down_total(black1, at, e, True)
            left_over = left_over + (total - centre * window(red1, at, e, rows1))
        rest1[at] = left_over
    rows2 = rows1 // 2
    shape2 = (rows2, LANES)
    row2, lane2 = rows_of(shape2), lanes_of(shape2)
    odd2 = odd_of(shape2)
    planes = [
        0.5 * (rest1[at, pl.ds(0, rows2, stride=2), :] + rest1[at, pl.ds(1, rows2, stride=2), :])
        for at in range(count1)
    ]

    body2 = slice(PAD, PAD + rows2)

    def grid_of(index):
        step = 1 << index
        return ((row2 & (step - 1)) == 0) & ((lane2 & (step - 1)) == 0)

    def odd_at(index):
        return (((row2 >> index) + (lane2 >> index)) & 1) == 1

    def along(value, step):
        left = jnp.where(lane2 < step, 0.0, pltpu.roll(value, step, 1))
        right = jnp.where(lane2 >= LANES - step, 0.0, pltpu.roll(value, LANES - step, 1))
        return weight_z * (left + right)

    def small_total(index, ref, at, odd, to_red):
        step = 1 << index
        value = ref[at, 0, body2, :]
        total = value + along(value, step)
        total = total + (
            ref[at, 0, PAD - step : PAD - step + rows2, :] + ref[at, 0, PAD + step : PAD + step + rows2, :]
        )
        slots = ref.shape[0]
        if slots == 1:
            return total
        before = ref[at - 1, 0, body2, :] if at > 0 else 0.0
        after = ref[at + 1, 0, body2, :] if at < slots - 1 else 0.0
        return total + (jnp.where(odd, after, before) if to_red else jnp.where(odd, before, after))

    def small_sweeps(index, start):
        fr, fb, red, black = small[index]
        mask, odd = jnp.where(grid_of(index), share, 0.0), odd_at(index)
        slots = fr.shape[0]
        for step in range(2):
            for at in range(slots):
                source = fr[at]
                if not (start and step == 0):
                    source = source + small_total(index, black, at, odd, True)
                red[at, 0, body2, :] = mask * source
            for at in range(slots):
                black[at, 0, body2, :] = mask * (fb[at] + small_total(index, red, at, odd, False))

    def spread_rows(value, step, ref, at):
        ref[at, 0, body2, :] = value
        return value + ref[at, 0, PAD - step : PAD - step + rows2, :]

    last = len(small) - 1
    for index in range(len(small)):
        fr, fb, red, black = small[index]
        slots, odd, step = fr.shape[0], odd_at(index), 1 << index
        for at in range(slots):
            p, q = planes[2 * at], planes[2 * at + 1]
            fr[at], fb[at] = jnp.where(odd, q, p), jnp.where(odd, p, q)
        small_sweeps(index, True)
        totals = []
        for at in range(slots):
            first = fb[at] + small_total(index, red, at, odd, False) - centre * black[at, 0, body2, :]
            second = fr[at] + small_total(index, black, at, odd, True) - centre * red[at, 0, body2, :]
            totals.append(first + second)
        for at in range(slots):
            passing[at, 0, body2, :] = totals[at]
        lower = [passing[at, 0, PAD + step : PAD + step + rows2, :] for at in range(slots)]
        if index < last:
            totals = [total + below for total, below in zip(totals, lower)]
            planes = [0.5 * (total + pltpu.roll(total, LANES - step, 1)) for total in totals]

    half_rows = rows2 // 2
    upper = [passing[at, 0, PAD - step : PAD - step + rows2, :] for at in range(slots)]
    odd_line = (row2 & step) != 0
    summed = [
        total + jnp.where(odd_line, above, below) for total, above, below in zip(totals, upper, lower)
    ]
    lines = [total[start : start + half_rows] for total in summed for start in (0, half_rows)]
    place = lanes_of((half_rows, LANES)) & (len(lines) - 1)
    joined = lines[0]
    for q in range(1, len(lines)):
        joined = jnp.where(place == q, pltpu.roll(lines[q], q, 1), joined)
    answer = exact_dot(joined, matrix_ref[...])
    grid = (place == 0) & ((rows_of((half_rows, LANES)) & (step - 1)) == 0)
    parts = []
    for q in range(len(lines)):
        part = pltpu.roll(answer, LANES - q, 1) if q else answer
        parts.append(jnp.where(grid, part, 0.0))
    spreads = [jnp.concatenate(parts[2 * at : 2 * at + 2], axis=0) for at in range(slots)]

    for index in reversed(range(len(small))):
        _, _, red, black = small[index]
        slots, odd, step = red.shape[0], odd_at(index), 1 << index
        if index < last:
            spreads = [
                spread_rows(field + pltpu.roll(field, step, 1), step, passing, at)
                for at, field in enumerate(fields)
            ]
        for at in range(slots):
            black[at, 0, body2, :] = black[at, 0, body2, :] + spreads[at]
        small_sweeps(index, False)
        fields = []
        for at in range(slots):
            r, b = red[at, 0, body2, :], black[at, 0, body2, :]
            fields += [jnp.where(odd, b, r), jnp.where(odd, r, b)]

    for at in range(count1):
        for start in range(2):
            rest1[at, pl.ds(start, rows2, stride=2), :] = fields[at]
    for at in range(count1):
        for e in range(2):
            black1[at, e, body1, :] = window(black1, at, e, rows1) + rest1[at]
    nx, ny, nz = out_ref.shape
    own = nx // 2
    part_slots = min(own // 2 + 3, count1)
    part_rows = min(ny // 2 + 16, rows1)
    slot0 = jnp.where(gx == 0, 0, count1 - part_slots)
    row0 = pl.multiple_of(jnp.clip(gy * (ny // 2) - 8, 0, rows1 - part_rows), 8)
    odds = fold_odds(part_rows)

    def up_total(ref, at, e, to_red):
        low = gx == 0 if at == 0 else False
        high = gx != 0 if at == part_slots - 1 else False
        return fold_total(ref, slot0 + at, e, row0, part_rows, low, high, odds, to_red)

    def up_half(target, other, sources, to_red):
        for at in range(part_slots):
            for e in range(2):
                source = sources[slot0 + at, e, pl.ds(row0, part_rows), :]
                value = share * (source + up_total(other, at, e, to_red))
                target[slot0 + at, e, pl.ds(pl.multiple_of(row0 + PAD, 8), part_rows), :] = value

    for sweep in range(2):
        up_half(red1, black1, fr1, True)
        up_half(black1, red1, fb1, False)

    count, _, rows, _ = dark_ref.shape
    half = rows // 2
    odds = fold_odds(half)
    row = gy * (ny // 2) + (PAD - halo // 2)
    for at in range(count):
        if at < own:
            slot = gx * (own // 2) + at // 2
        else:
            slot = jnp.where(gx == 0, own // 2, own // 2 - (count - own) // 2) + (at - own) // 2
        for e in range(2):
            r, b = red1[slot, e, pl.ds(row, half), :], black1[slot, e, pl.ds(row, half), :]
            plane = jnp.where(odds[e], r, b) if at % 2 else jnp.where(odds[e], b, r)
            tall_ref[at, :, e * LANES : (e + 1) * LANES] = plane
    shape = (2 * LANES, 2 * LANES)
    z = lanes_of(shape)
    z = jnp.where(z < 2 * LANES - halo, z, z - 2 * LANES) + gz * nz
    line = rows_of(shape)
    line = jnp.where(line < LANES, 2 * line, 2 * (line - LANES) + 1)
    weight = jnp.where(line == lax.shift_right_arithmetic(z, 1), 1.0, 0.0)
    spread = exact_dot(tall_ref[...].reshape(count * half, 2 * LANES), weight)
    spread = spread.reshape(count, half, 2 * LANES)
    for at in range(count):
        for c in range(2):
            value = spread[at, :, c * LANES : (c + 1) * LANES]
            for start in range(2):
                work_ref[at, c, pl.ds(PAD + start, half, stride=2), :] = value
    body = slice(PAD, PAD + rows)
    for at in range(count):
        for c in range(2):
            work_ref[at, c, body, :] = work_ref[at, c, body, :] + dark_ref[at, c]
    odd = odd_of((rows, LANES))
    masks = block_mask((ny, nz), halo)
    ends = (gx == 0, gx == lax.axis_size("gx") - 1)
    for sweep in range(2):
        for at in range(count):
            totals = block_totals(work_ref, at, rows, own, odd, True, *ends)
            for c in range(2):
                red_ref[at, c, body, :] = gr_ref[at, c] + masks[c] * totals[c]
        for at in range(count if sweep == 0 else own):
            totals = block_totals(red_ref, at, rows, own, odd, False, *ends)
            for c in range(2 if sweep == 0 else 1):
                work_ref[at, c, body, :] = gb_ref[at, c] + masks[c] * totals[c]
    inner = slice(PAD + halo, PAD + halo + ny)
    odd = odd_of((ny, nz))
    for at in range(own):
        r, b = red_ref[at, 0, inner, :], work_ref[at, 0, inner, :]
        out_ref[2 * at] = jnp.where(odd, b, r)
        out_ref[2 * at + 1] = jnp.where(odd, r, b)


def vmem(number):
    return [pl.BlockSpec(memory_space=pltpu.VMEM)] * number


def struct(*shape):
    return jax.ShapeDtypeStruct(shape, jnp.float32)


def scratch(*shape):
    return pltpu.VMEM(shape, jnp.float32)


HALO = 8


def block_cycle(density):
    halo = HALO
    nx, ny, nz = density.shape
    count_x, count_y, count_z = (lax.axis_size(axis) for axis in ("gx", "gy", "gz"))
    whole = (nx * count_x, ny * count_y, nz * count_z)

    def params(mib):
        return pltpu.CompilerParams(vmem_limit_bytes=mib * 1024 * 1024)

    ya, yb = pl.pallas_call(
        functools.partial(faces_kernel, halo),
        out_shape=[struct(nx, halo, nz)] * 2,
        in_specs=[pl.BlockSpec(memory_space=pltpu.HBM)], out_specs=vmem(2),
        compiler_params=params(2), scratch_shapes=[pltpu.SemaphoreType.DMA((2,))],
    )(density)
    ya = lax.ppermute(ya, "gy", pairs(count_y, 0))
    yb = lax.ppermute(yb, ("gx", "gy"), inner_pairs(count_x, count_y))
    rows = ny + 2 * halo
    packs = -(-nx * halo // nz)
    za, zb = pl.pallas_call(
        functools.partial(pack_kernel, halo),
        out_shape=[struct(packs, rows, nz)] * 2,
        in_specs=vmem(3), out_specs=vmem(2), compiler_params=params(4),
    )(density, ya, yb)
    za = lax.ppermute(za, "gz", pairs(count_z, 0))
    zb = lax.ppermute(zb, "gz", pairs(count_z, 1) + [(0, count_z - 1), (count_z - 1, 0)])
    own, near = nx // 2, nx // 2 + 2
    send, face = pl.pallas_call(
        functools.partial(pre_kernel, halo),
        out_shape=[struct(near // 2, ny // 2, nz), struct(halo + 1, rows, LANES)],
        in_specs=vmem(5), out_specs=vmem(2), compiler_params=params(10),
        scratch_shapes=[scratch(own, ny, nz)] * 2
        + [scratch(own, 2, rows, LANES)] * 2
        + [scratch(near, 2, rows + 2 * PAD, LANES)] * 2
        + [scratch(near, ny, nz)],
    )(density, ya, yb, za, zb)
    planes = nx + halo
    slots = (planes // 2, 2, rows, LANES)
    padded = (planes // 2, 2, rows + 2 * PAD, LANES)
    first = [
        send,
        lax.ppermute(send, "gy", flips(count_y, 2)),
        lax.ppermute(send, "gz", flips(count_z, 2)),
        lax.ppermute(send, ("gy", "gz"), flips(count_y * count_z, 2 * count_z + 2)),
    ]
    face = lax.ppermute(face, "gx", flips(count_x, 1))
    first[3], face = lax.optimization_barrier((first[3], face))
    block = pl.pallas_call(
        stack_kernel, out_shape=struct(4, *send.shape),
        in_specs=vmem(4), out_specs=pl.BlockSpec(memory_space=pltpu.VMEM), compiler_params=params(2),
    )(*first)
    second = [
        block,
        lax.ppermute(block, "gx", flips(count_x, 1)),
        lax.ppermute(block, "gy", flips(count_y, 1)),
        lax.ppermute(block, ("gx", "gy"), flips(count_x * count_y, count_y + 1)),
    ]
    gr, gb, black = pl.pallas_call(
        functools.partial(field_kernel, halo),
        out_shape=[struct(*slots)] * 3,
        in_specs=vmem(7), out_specs=vmem(3), compiler_params=params(8),
        scratch_shapes=[scratch(*padded)] * 2,
        cost_estimate=pl.CostEstimate(flops=20_000_000, bytes_accessed=2_000_000, transcendentals=0),
    )(density, ya, yb, za, zb, face, block)
    *second[1:], gr, gb, black = lax.optimization_barrier((*second[1:], gr, gb, black))
    third = [lax.ppermute(blocks, "gz", flips(count_z, 1)) for blocks in second]
    count1, rows1, rows2 = whole[0] // 4, whole[1] // 2, whole[1] // 4
    room = [scratch(count1, 2, rows1, LANES)] * 2
    room += [scratch(count1, 2, rows1 + 2 * PAD, LANES)] * 2
    room += [scratch(count1, rows1, LANES), scratch(planes // 2, rows // 2, 2 * LANES)]
    room += [scratch(*padded)] * 2 + [scratch(count1 // 2, 1, rows2 + 2 * PAD, LANES)]
    for count in small_shapes(whole):
        room += [scratch(count, rows2, LANES)] * 2
        room += [scratch(count, 1, rows2 + 2 * PAD, LANES)] * 2
    return pl.pallas_call(
        functools.partial(solve_kernel, halo, whole),
        out_shape=struct(nx, ny, nz),
        in_specs=vmem(12), out_specs=pl.BlockSpec(memory_space=pltpu.VMEM),
        compiler_params=params(16), scratch_shapes=room,
    )(*second, *third, gr, gb, black, cycle_matrix(whole))


def fits_block_cycle(shape):
    nx, ny, nz = shape
    count_x, count_y, count_z = (lax.axis_size(axis) for axis in ("gx", "gy", "gz"))
    whole = (nx * count_x, ny * count_y, nz * count_z)
    coarsest = [size >> (LEVELS - 1) for size in whole]
    exact = all(c << (LEVELS - 1) == size for c, size in zip(coarsest, whole))
    return (
        exact and coarsest[0] == coarsest[1] == 1 and nz == LANES and ny == 2 * HALO
        and count_x == 2 and count_y == 4 and count_z == 4
    )


def on_device(density):
    if fits_block_cycle(density.shape):
        return block_cycle(density)
    top = 4
    return shared_cycle(density, 0, top)


def solution(mesh):
    return jax.shard_map(
        on_device,
        mesh=mesh,
        in_specs=(P("gx", "gy", "gz"),),
        out_specs=P("gx", "gy", "gz"),
        check_vma=False,
    )
```

```python
import functools

import jax
import jax.numpy as jnp
import numpy as np
from jax import lax
from jax.experimental import pallas as pl
from jax.experimental.pallas import tpu as pltpu
from jax.sharding import PartitionSpec as P

LEVELS = 7
CSWEEPS = 4


rsd_beta = 0.5
centre = 4.0 + 2.0 * (1.0 + rsd_beta)


def extended_2(value, sides, width):
    for axis, dim in sides:
        count, length = (lax.axis_size(axis), value.shape[dim])
        up = [(i, (i + 1) % count) for i in range(count - 1)]
        down = [(j, i) for i, j in up]
        last = lax.slice_in_dim(value, length - width, length, axis=dim)
        leading = lax.slice_in_dim(value, 0, width, axis=dim)
        before = lax.ppermute(last, axis, up)
        after = lax.ppermute(leading, axis, down)
        value = jnp.concatenate([before, value, after], axis=dim)
    return value


def stencil_sum(padded):
    plane = (
        padded[2:, 1:-1, 1:-1]
        + padded[:-2, 1:-1, 1:-1]
        + padded[1:-1, 2:, 1:-1]
        + padded[1:-1, :-2, 1:-1]
    )
    sight = padded[1:-1, 1:-1, 2:] + padded[1:-1, 1:-1, :-2]
    return plane + (1.0 + rsd_beta) * sight


def grid_index(shape, starts):
    return [lax.broadcasted_iota(jnp.int32, shape, which) + starts[which] for which in range(3)]


def parity_of(shape, starts):
    position = grid_index(shape, starts)
    return (position[0] + position[1] + position[2] + 6) % 2


def inside_grid(shape, starts, whole):
    position = grid_index(shape, starts)
    keep = (position[0] >= 0) & (position[0] < whole[0])
    for which in (1, 2):
        keep = keep & (position[which] >= 0) & (position[which] < whole[which])
    return keep


def half_sweep(field, source, scale, chosen):
    update = (source / scale + stencil_sum(jnp.pad(field, 1))) / centre
    return jnp.where(chosen, update, field)


def full_sweep(field, source, scale, parity):
    field = half_sweep(field, source, scale, parity == 0)
    return half_sweep(field, source, scale, parity == 1)


def restrict(residue):
    shape = residue.shape
    blocks = residue.reshape(shape[0] // 2, 2, shape[1] // 2, 2, shape[2] // 2, 2)
    return jnp.mean(blocks, axis=(1, 3, 5))


def prolong(coarse):
    return jnp.repeat(jnp.repeat(jnp.repeat(coarse, 2, 0), 2, 1), 2, 2)


def local_cycle(source, level):
    scale = 0.25**level
    parity = parity_of(source.shape, (0, 0, 0))
    field = jnp.zeros_like(source)
    if level == LEVELS - 1:
        for number in range(CSWEEPS):
            field = full_sweep(field, source, scale, parity)
        return field
    for number in range(2):
        field = full_sweep(field, source, scale, parity)
    residue = source - scale * (centre * field - stencil_sum(jnp.pad(field, 1)))
    field = field + prolong(local_cycle(restrict(residue), level + 1))
    for number in range(2):
        field = full_sweep(field, source, scale, parity)
    return field


def faces(field):
    return extended_2(field, (("gx", 0), ("gy", 1), ("gz", 2)), 1)


def wide(field):
    return extended_2(field, (("gx", 0), ("gy", 1), ("gz", 2)), 2)


def block_starts(shape, margin):
    return (
        lax.axis_index("gx") * shape[0] - margin,
        lax.axis_index("gy") * shape[1] - margin,
        lax.axis_index("gz") * shape[2] - margin,
    )


def padded_half(padded, source, scale, chosen):
    field = padded[1:-1, 1:-1, 1:-1]
    update = (source / scale + stencil_sum(padded)) / centre
    return jnp.where(chosen, update, field)


def wide_sweep(extended, wide_source, scale, red_wide, source, black):
    update = (wide_source / scale + stencil_sum(jnp.pad(extended, 1))) / centre
    extended = jnp.where(red_wide, update, extended)
    return padded_half(extended[1:-1, 1:-1, 1:-1], source, scale, black)


def coarse_level(source, level):
    shape = source.shape
    stack = lax.all_gather(source[None], ("gx", "gy", "gz"), axis=0, tiled=True)
    count_x, count_y, count_z = (lax.axis_size("gx"), lax.axis_size("gy"), lax.axis_size("gz"))
    whole = stack.reshape(count_x, count_y, count_z, shape[0], shape[1], shape[2])
    whole = whole.transpose(0, 3, 1, 4, 2, 5).reshape(
        count_x * shape[0], count_y * shape[1], count_z * shape[2]
    )
    solved = local_cycle(whole, level)
    starts = block_starts(shape, 0)
    return lax.dynamic_slice(solved, starts, shape)


def shared_cycle(source, level, top):
    if level == top:
        return coarse_level(source, level)
    scale = 0.25**level
    shape = source.shape
    whole = (
        shape[0] * lax.axis_size("gx"),
        shape[1] * lax.axis_size("gy"),
        shape[2] * lax.axis_size("gz"),
    )
    parity = parity_of(shape, block_starts(shape, 0))
    black = parity == 1
    wide_shape = (shape[0] + 4, shape[1] + 4, shape[2] + 4)
    wide_starts = block_starts(shape, 2)
    red_wide = (parity_of(wide_shape, wide_starts) == 0) & inside_grid(
        wide_shape, wide_starts, whole
    )
    wide_source = wide(source)
    field = wide_sweep(
        jnp.zeros(wide_shape, jnp.float32), wide_source, scale, red_wide, source, black
    )
    field = wide_sweep(wide(field), wide_source, scale, red_wide, source, black)
    residue = source - scale * (centre * field - stencil_sum(faces(field)))
    field = field + prolong(shared_cycle(restrict(residue), level + 1, top))
    for number in range(2):
        field = wide_sweep(wide(field), wide_source, scale, red_wide, source, black)
    return field


def pairs(count, first):
    swaps = []
    for i in range(first, count - 1, 2):
        swaps += [(i, i + 1), (i + 1, i)]
    return swaps


def inner_pairs(count_x, count):
    swaps = []
    for x in range(count_x):
        swaps += [(x * count + i, x * count + j) for i, j in pairs(count, 1)]
        swaps += [(x * count + i, (x ^ 1) * count + i) for i in (0, count - 1)]
    return swaps


def flips(count, bit):
    return [(i, i ^ bit) for i in range(count)]


def lanes_of(shape):
    return lax.broadcasted_iota(jnp.int32, shape, len(shape) - 1)


def rows_of(shape):
    return lax.broadcasted_iota(jnp.int32, shape, len(shape) - 2)


LANES = 128
PAD = 8


def odd_of(shape):
    return ((lanes_of(shape) + rows_of(shape)) & 1) == 1


def exact_dot(a, b):
    return jnp.dot(a, b, precision=lax.Precision.HIGHEST, preferred_element_type=jnp.float32)


def window(ref, at, column, count, start=0, shift=0):
    if isinstance(start, int):
        return ref[at, column, PAD + start + shift : PAD + start + shift + count, :]
    first = start + (PAD + shift)
    if shift == 0:
        first = pl.multiple_of(first, 8)
    return ref[at, column, pl.ds(first, count), :]


def clear_pads(ref):
    edge = jnp.zeros((PAD, LANES), jnp.float32)
    for at in range(ref.shape[0]):
        for column in range(ref.shape[1]):
            ref[at, column, :PAD, :] = edge
            ref[at, column, ref.shape[2] - PAD :, :] = edge


def block_sums(ref, at, rows):
    lane = lanes_of((rows, LANES))
    values = [window(ref, at, column, rows) for column in range(2)]
    lefts = [pltpu.roll(value, 1, 1) for value in values]
    rights = [pltpu.roll(value, LANES - 1, 1) for value in values]
    sums = []
    for column in range(2):
        left = jnp.where(lane == 0, lefts[1 - column], lefts[column])
        right = jnp.where(lane == LANES - 1, rights[1 - column], rights[column])
        sides = window(ref, at, column, rows, shift=-1) + window(ref, at, column, rows, shift=1)
        sums.append(values[column] + sides + (1.0 + rsd_beta) * (left + right))
    return sums


def block_totals(ref, at, rows, own, odd, to_red, at_low, at_high):
    slots = ref.shape[0]
    totals = []
    for column, total in enumerate(block_sums(ref, at, rows)):
        before = window(ref, (at - 1) % slots, column, rows)
        after = window(ref, (at + 1) % slots, column, rows)
        if at in (0, own):
            before = jnp.where(at_low if at == 0 else at_high, 0.0, before)
        if at in (own - 1, slots - 1):
            after = jnp.where(at_low if at == slots - 1 else at_high, 0.0, after)
        totals.append(total + (jnp.where(odd, after, before) if to_red else jnp.where(odd, before, after)))
    return totals


def block_mask(own, halo):
    ny, nz = own
    shape = (ny + 2 * halo, LANES)
    row = rows_of(shape) - halo + lax.axis_index("gy") * ny
    inside_y = (row >= 0) & (row < ny * lax.axis_size("gy"))
    masks = []
    for column in range(2):
        lane = lanes_of(shape)
        if column:
            lane = jnp.where(lane < halo, lane + LANES, lane - LANES)
        lane = lane + lax.axis_index("gz") * nz
        inside = inside_y & (lane >= 0) & (lane < nz * lax.axis_size("gz"))
        masks.append(jnp.where(inside, 1.0 / centre, 0.0))
    return masks


def block_plane(at, own_ref, ya_ref, yb_ref, even_y):
    a, b = ya_ref[at], yb_ref[at]
    low = jnp.where(even_y, b, a)
    high = jnp.where(even_y, a, b)
    return jnp.concatenate([low, own_ref[at], high], axis=0)


def block_columns(halo, at, own_ref, ya_ref, yb_ref, za_ref, zb_ref, even_y, even_z):
    _, _, nz = own_ref.shape
    j, k = at // (nz // halo), at % (nz // halo)
    a, b = za_ref[j], zb_ref[j]
    left = pltpu.roll(jnp.where(even_z, b, a), (2 * nz - halo - halo * k) % nz, 1)
    right = pltpu.roll(jnp.where(even_z, a, b), (nz - halo * k) % nz, 1)
    lane = lanes_of(left.shape)
    sides = jnp.where(lane < halo, right, jnp.where(lane >= nz - halo, left, 0.0))
    return block_plane(at, own_ref, ya_ref, yb_ref, even_y), sides


def pack_kernel(halo, own_ref, ya_ref, yb_ref, za_ref, zb_ref):
    even_y = lax.axis_index("gy") % 2 == 0
    even_z = lax.axis_index("gz") % 2 == 0
    nx, ny, nz = own_ref.shape
    groups = nz // halo
    shape = (ny + 2 * halo, nz)
    group = lanes_of(shape) // halo
    for j in range(za_ref.shape[0]):
        last = jnp.zeros(shape, jnp.float32)
        first = jnp.zeros(shape, jnp.float32)
        for k in range(min(groups, nx - j * groups)):
            plane = block_plane(j * groups + k, own_ref, ya_ref, yb_ref, even_y)
            last = jnp.where(group == k, pltpu.roll(plane, (halo * k + halo) % nz, 1), last)
            first = jnp.where(group == k, pltpu.roll(plane, halo * k, 1), first)
        za_ref[j] = jnp.where(even_z, last, first)
        zb_ref[j] = jnp.where(even_z, first, last)


def smooth(count, own, masks, odd, ends, gr_ref, gb_ref, red_ref, black_ref, done):
    rows = odd.shape[0]
    body = slice(PAD, PAD + rows)

    def value_of(source, at, c, total):
        value = masks[c] * total
        return source[at, c] + value if at < source.shape[0] else value

    for at in range(count):
        for c in range(2):
            red_ref[at, c, body, :] = gr_ref[at, c] if at < gr_ref.shape[0] else jnp.zeros_like(masks[c])
    for step in range(3):
        source, target, other = (gr_ref, red_ref, black_ref) if step == 1 else (gb_ref, black_ref, red_ref)
        for at in range(count):
            totals = block_totals(other, at, rows, own, odd, step == 1, *ends)
            for c in range(2):
                value = value_of(source, at, c, totals[c])
                target[at, c, body, :] = value
                if step == 2:
                    done(at, c, totals[c], value)


def x_ends():
    here = lax.axis_index("gx")
    return here == 0, here == lax.axis_size("gx") - 1


def pre_kernel(
    halo, own_ref, ya_ref, yb_ref, za_ref, zb_ref,
    send_ref, face_ref,
    fr_ref, fb_ref, gr_ref, gb_ref, red_ref, black_ref, rest_ref,
):
    even_y = lax.axis_index("gy") % 2 == 0
    even_z = lax.axis_index("gz") % 2 == 0
    nx, ny, nz = own_ref.shape
    count, _, rows, _ = red_ref.shape
    rows = rows - 2 * PAD
    own = nx // 2
    shape = (rows, LANES)
    odd = odd_of(shape)
    masks = block_mask((ny, nz), halo)
    inner = slice(halo, halo + ny)
    ends = x_ends()
    clear_pads(red_ref)
    clear_pads(black_ref)
    for p in range(halo):
        high = block_plane(nx - halo + p, own_ref, ya_ref, yb_ref, even_y)
        face_ref[p] = jnp.where(ends[0], high, block_plane(p, own_ref, ya_ref, yb_ref, even_y))
    middle = halo * halo
    top = za_ref.shape[0] - 1
    left = [jnp.where(even_z, zb_ref[j], za_ref[j]) for j in (0, top)]
    right = [jnp.where(even_z, za_ref[j], zb_ref[j]) for j in (0, top)]
    left = jnp.where(ends[0], pltpu.roll(left[1], middle, 1), left[0])
    right = jnp.where(ends[0], right[1], pltpu.roll(right[0], middle, 1))
    face_ref[halo] = jnp.where(lanes_of(shape) < middle, left, right)
    for at in range(own):
        planes = [
            block_columns(halo, x, own_ref, ya_ref, yb_ref, za_ref, zb_ref, even_y, even_z)
            for x in (2 * at, 2 * at + 1)
        ]
        for c in range(2):
            red = jnp.where(odd, planes[1][c], planes[0][c])
            black = jnp.where(odd, planes[0][c], planes[1][c])
            if c == 0:
                fr_ref[at], fb_ref[at] = red[inner], black[inner]
            gr_ref[at, c], gb_ref[at, c] = masks[c] * red, masks[c] * black

    def keep(at, c, total, value):
        if c == 0:
            left_over = total[inner] - centre * value[inner]
            rest_ref[at] = left_over + fb_ref[at] if at < own else left_over

    smooth(count, own, masks, odd, ends, gr_ref, gb_ref, red_ref, black_ref, keep)
    for at in range(count):
        total = block_totals(black_ref, at, rows, own, odd, True, *ends)[0]
        left_over = total[inner] - centre * red_ref[at, 0, PAD + halo : PAD + halo + ny, :]
        if at < own:
            left_over = left_over + fr_ref[at]
        rest_ref[at] = rest_ref[at] + left_over
    half, quarter = ny // 2, nz // 4
    pairs_y = rest_ref[:, pl.ds(0, half, stride=2), :] + rest_ref[:, pl.ds(1, half, stride=2), :]
    turn = quarter * lax.axis_index("gz")
    column = (lanes_of((nz, nz)) - turn) & (nz - 1)
    target = 2 * (column % quarter) + (column // quarter) % 2
    weight = jnp.where(rows_of((nz, nz)) // 2 == target, 0.5, 0.0)
    coarse = exact_dot(pairs_y.reshape(count * half, nz), weight).reshape(count, half, nz)
    part = ((lanes_of((half, nz)) - turn) & (nz - 1)) // quarter
    pick = (((rows_of((half, nz)) + part) & 1) == 1) ^ (part >= 2)
    for at in range(count // 2):
        send_ref[at] = jnp.where(pick, coarse[2 * at + 1], coarse[2 * at])


def field_kernel(
    halo, own_ref, ya_ref, yb_ref, za_ref, zb_ref, face_ref, after_ref,
    gr_ref, gb_ref, dark_ref,
    red_ref, black_ref,
):
    even_y = lax.axis_index("gy") % 2 == 0
    even_z = lax.axis_index("gz") % 2 == 0
    nx, ny, nz = own_ref.shape
    count, _, rows, _ = gr_ref.shape
    own = nx // 2
    shape = (rows, LANES)
    odd, lane = odd_of(shape), lanes_of(shape)
    masks = block_mask((ny, nz), halo)
    clear_pads(red_ref)
    clear_pads(black_ref)

    def columns(x):
        if x < nx:
            return block_columns(halo, x, own_ref, ya_ref, yb_ref, za_ref, zb_ref, even_y, even_z)
        p = x - nx
        left = pltpu.roll(face_ref[halo], (2 * LANES - halo - halo * p) % LANES, 1)
        right = pltpu.roll(face_ref[halo], (2 * LANES - halo * halo - halo * p) % LANES, 1)
        return face_ref[p], jnp.where(lane < halo, right, jnp.where(lane >= nz - halo, left, 0.0))

    for at in range(count):
        first, second = columns(2 * at), columns(2 * at + 1)
        for c in range(2):
            gr_ref[at, c] = masks[c] * jnp.where(odd, second[c], first[c])
            gb_ref[at, c] = masks[c] * jnp.where(odd, first[c], second[c])

    def keep(at, c, total, value):
        dark_ref[at, c] = value

    smooth(count, own, masks, odd, x_ends(), gr_ref, gb_ref, red_ref, black_ref, keep)


def stack_kernel(*refs):
    for which, ref in enumerate(refs[:-1]):
        refs[-1][which] = ref[...]


def small_shapes(whole):
    return [whole[0] >> (level + 1) for level in range(2, LEVELS - 2)]


def plain_sum(field):
    padded = np.pad(field, ((0, 0), (1, 1), (1, 1), (1, 1)))
    inner = slice(1, -1)
    plane = padded[:, 2:, inner, inner] + padded[:, :-2, inner, inner]
    plane = plane + padded[:, inner, 2:, inner] + padded[:, inner, :-2, inner]
    return plane + (1.0 + rsd_beta) * (padded[:, inner, inner, 2:] + padded[:, inner, inner, :-2])


def plain_cycle(source, level):
    parity = np.indices(source.shape[1:]).sum(axis=0) % 2
    field = np.zeros_like(source)

    def sweeps(field, number):
        for step in range(2 * number):
            field = np.where(parity == step % 2, (source + plain_sum(field)) / centre, field)
        return field

    if level == LEVELS - 1:
        return sweeps(field, CSWEEPS)
    field = sweeps(field, 2)
    rest = source - centre * field + plain_sum(field)
    nx, ny, nz = source.shape[1:]
    rest = rest.reshape(-1, nx // 2, 2, ny // 2, 2, nz // 2, 2).sum(axis=(2, 4, 6)) / 2.0
    coarse = plain_cycle(rest, level + 1)
    for axis in (1, 2, 3):
        coarse = np.repeat(coarse, 2, axis)
    return sweeps(field + coarse, 2)


def cycle_matrix(whole):
    level = LEVELS - 2
    nx, ny, nz = (size >> level for size in whole)
    size = nx * ny * 2 * nz
    unit = np.eye(size).reshape(size, 2 * nz, nx, ny).transpose(0, 2, 3, 1)
    source = unit.reshape(size, nx, ny, nz, 2).sum(axis=-1) / 2.0
    result = np.repeat(plain_cycle(source, level), 2, axis=3)
    return jnp.asarray(result.transpose(0, 3, 1, 2).reshape(size, size), jnp.float32)


def solve_kernel(halo, whole, *refs):
    gathered, refs = refs[:8], refs[8:]
    gr_ref, gb_ref, dark_ref, matrix_ref, out_ref = refs[:5]
    fr1, fb1, red1, black1, rest1, tall_ref, red_ref, work_ref, passing = refs[5:14]
    small = [refs[14 + 6 * i : 20 + 6 * i] for i in range(LEVELS - 4)]
    gx, gy, gz = (lax.axis_index(axis) for axis in ("gx", "gy", "gz"))
    weight_z = 1.0 + rsd_beta
    share = 1.0 / centre
    for ref in (red1, black1, red_ref, work_ref, passing):
        clear_pads(ref)
    for level in small:
        for ref in level[2:4]:
            clear_pads(ref)

    _, slots, block_rows, _ = gathered[0].shape
    slots = slots - 1
    count1, _, rows1, _ = fr1.shape
    quarter = LANES // 4
    group = lanes_of((block_rows, LANES)) // quarter
    held = [jnp.bitwise_and(group - jnp.bitwise_xor(gz, bits), 3) for bits in range(4)]
    theirs = [[kind == part for kind in held] for part in range(4)]
    def unpack(far, second, at):
        y = jnp.bitwise_xor(gy, 2 * far + (second >> 1))
        rows = pl.ds(pl.multiple_of(y * block_rows, 8), block_rows)
        blocks = [gathered[4 * (bits & 1) + second][far + (bits & 2), at] for bits in range(4)]
        parts = []
        for part in range(4):
            value = blocks[0]
            for block, mine in zip(blocks[1:], theirs[part][1:]):
                value = jnp.where(mine, block, value)
            parts.append(pltpu.roll(value, LANES - quarter * part, 1) if part else value)
        return rows, parts

    half1 = count1 // 2
    for far in range(2):
        for second in range(4):
            x = jnp.bitwise_xor(gx, second & 1)
            for at in range(slots):
                rows, parts = unpack(far, second, at)
                for part, target in enumerate((fr1, fr1, fb1, fb1)):
                    target[x * slots + at, part % 2, rows, :] = parts[part]
    for far in range(2):
        for second in range(4):
            x = jnp.bitwise_xor(gx, second & 1)
            next_slot = jnp.where(x == 0, half1, half1 - 1)
            rows, parts = unpack(far, second, slots)
            for part, target in enumerate((fr1, fr1, fb1, fb1)):
                target[next_slot, part % 2, rows, :] = target[next_slot, part % 2, rows, :] + parts[part]

    def fold_total(ref, at, e, start, count, low, high, odds, to_red):
        lane = lanes_of((count, LANES))
        value, other = window(ref, at, e, count, start), window(ref, at, 1 - e, count, start)
        sides = window(ref, at, e, count, start, -1) + window(ref, at, e, count, start, 1)
        if e == 0:
            near = jnp.where(lane == 0, 0.0, pltpu.roll(other, 1, 1))
        else:
            near = jnp.where(lane == LANES - 1, 0.0, pltpu.roll(other, LANES - 1, 1))
        before = 0.0 if low is True else window(ref, at - 1, e, count, start)
        after = 0.0 if high is True else window(ref, at + 1, e, count, start)
        if not isinstance(low, bool):
            before = jnp.where(low, 0.0, window(ref, jnp.maximum(at - 1, 0), e, count, start))
        if not isinstance(high, bool):
            after = jnp.where(high, 0.0, window(ref, jnp.minimum(at + 1, count1 - 1), e, count, start))
        beside = jnp.where(odds[e], after, before) if to_red else jnp.where(odds[e], before, after)
        return value + sides + beside + weight_z * (other + near)

    def fold_odds(count):
        row = rows_of((count, LANES))
        return [((row + e) & 1) == 1 for e in range(2)]

    odds = fold_odds(rows1)
    body1 = slice(PAD, PAD + rows1)

    def down_total(ref, at, e, to_red):
        return fold_total(ref, at, e, 0, rows1, at == 0, at == count1 - 1, odds, to_red)

    for at in range(count1):
        for e in range(2):
            red1[at, e, body1, :] = share * fr1[at, e]
    for at in range(count1):
        for e in range(2):
            black1[at, e, body1, :] = share * (fb1[at, e] + down_total(red1, at, e, False))
    for at in range(count1):
        for e in range(2):
            red1[at, e, body1, :] = share * (fr1[at, e] + down_total(black1, at, e, True))
    for at in range(count1):
        left_over = None
        for e in range(2):
            total = fb1[at, e] + down_total(red1, at, e, False)
            value = share * total
            black1[at, e, body1, :] = value
            term = total - centre * value
            left_over = term if left_over is None else left_over + term
        rest1[at] = left_over
    for at in range(count1):
        left_over = rest1[at]
        for e in range(2):
            total = fr1[at, e] + down_total(black1, at, e, True)
            left_over = left_over + (total - centre * window(red1, at, e, rows1))
        rest1[at] = left_over
    rows2 = rows1 // 2
    shape2 = (rows2, LANES)
    row2, lane2 = rows_of(shape2), lanes_of(shape2)
    odd2 = odd_of(shape2)
    planes = [
        0.5 * (rest1[at, pl.ds(0, rows2, stride=2), :] + rest1[at, pl.ds(1, rows2, stride=2), :])
        for at in range(count1)
    ]

    body2 = slice(PAD, PAD + rows2)

    def grid_of(index):
        step = 1 << index
        return ((row2 & (step - 1)) == 0) & ((lane2 & (step - 1)) == 0)

    def odd_at(index):
        return (((row2 >> index) + (lane2 >> index)) & 1) == 1

    def turned(value, step):
        inside = lane2 >= step if step > 0 else lane2 < LANES + step
        return jnp.where(inside, pltpu.roll(value, step % LANES, 1), 0.0)

    def small_plane(index, ref, at, odd, to_red):
        step = 1 << index
        total = ref[at, 0, body2, :] + (
            ref[at, 0, PAD - step : PAD - step + rows2, :] + ref[at, 0, PAD + step : PAD + step + rows2, :]
        )
        slots = ref.shape[0]
        if slots == 1:
            return total
        before = ref[at - 1, 0, body2, :] if at > 0 else 0.0
        after = ref[at + 1, 0, body2, :] if at < slots - 1 else 0.0
        return total + (jnp.where(odd, after, before) if to_red else jnp.where(odd, before, after))

    def small_sweeps(index, start):
        fr, fb, red, black, fr_low, fr_high = small[index]
        odd, width = odd_at(index), 1 << index
        mask = jnp.where(grid_of(index), share, 0.0)
        mask_low = jnp.where(lane2 < width, 0.0, mask)
        mask_high = jnp.where(lane2 >= LANES - width, 0.0, mask)
        slots = fr.shape[0]
        if start:
            for at in range(slots):
                fr_low[at] = pltpu.roll(fr[at], width, 1)
                fr_high[at] = pltpu.roll(fr[at], LANES - width, 1)
        for step in range(2):
            sides = []
            for at in range(slots):
                here, low, high = fr[at], fr_low[at], fr_high[at]
                if not (start and step == 0):
                    value = black[at, 0, body2, :]
                    plane = small_plane(index, black, at, odd, True)
                    here = here + plane + weight_z * (turned(value, width) + turned(value, -width))
                    low = low + pltpu.roll(plane, width, 1) + weight_z * (turned(value, 2 * width) + value)
                    high = high + pltpu.roll(plane, LANES - width, 1)
                    high = high + weight_z * (value + turned(value, -2 * width))
                red[at, 0, body2, :] = mask * here
                sides.append(weight_z * (mask_low * low + mask_high * high))
            totals = []
            for at in range(slots):
                total = fb[at] + small_plane(index, red, at, odd, False) + sides[at]
                black[at, 0, body2, :] = mask * total
                totals.append(total)
        return totals

    def spread_rows(value, step, ref, at):
        ref[at, 0, body2, :] = value
        return value + ref[at, 0, PAD - step : PAD - step + rows2, :]

    last = len(small) - 1
    for index in range(len(small)):
        fr, fb, red, black, _, fr_high = small[index]
        slots, odd, step = fr.shape[0], odd_at(index), 1 << index
        for at in range(slots):
            p, q = planes[2 * at], planes[2 * at + 1]
            fr[at], fb[at] = jnp.where(odd, q, p), jnp.where(odd, p, q)
        black_totals = small_sweeps(index, True)
        totals = []
        for at in range(slots):
            value, field = black[at, 0, body2, :], red[at, 0, body2, :]
            plane = small_plane(index, black, at, odd, True)
            total = black_totals[at] - centre * value
            next_total = pltpu.roll(total, LANES - step, 1)
            total = total + (
                fr[at] + plane + weight_z * (turned(value, step) + turned(value, -step)) - centre * field
            )
            if index < last:
                next_total = next_total + (
                    fr_high[at] + pltpu.roll(plane, LANES - step, 1)
                    + weight_z * (value + turned(value, -2 * step))
                    - centre * pltpu.roll(field, LANES - step, 1)
                )
                total = total + next_total
            totals.append(total)
            passing[at, 0, body2, :] = total
        lower = [passing[at, 0, PAD + step : PAD + step + rows2, :] for at in range(slots)]
        planes = [0.5 * (total + below) for total, below in zip(totals, lower)]

    half_rows = rows2 // 2
    upper = [passing[at, 0, PAD - step : PAD - step + rows2, :] for at in range(slots)]
    odd_line = (row2 & step) != 0
    summed = [
        total + jnp.where(odd_line, above, below) for total, above, below in zip(totals, upper, lower)
    ]
    lines = [total[start : start + half_rows] for total in summed for start in (0, half_rows)]
    place = lanes_of((half_rows, LANES)) & (len(lines) - 1)
    joined = lines[0]
    for q in range(1, len(lines)):
        joined = jnp.where(place == q, pltpu.roll(lines[q], q, 1), joined)
    answer = exact_dot(joined, matrix_ref[...])
    grid = (place == 0) & ((rows_of((half_rows, LANES)) & (step - 1)) == 0)
    parts = []
    for q in range(len(lines)):
        part = pltpu.roll(answer, LANES - q, 1) if q else answer
        parts.append(jnp.where(grid, part, 0.0))
    spreads = [jnp.concatenate(parts[2 * at : 2 * at + 2], axis=0) for at in range(slots)]

    for index in reversed(range(len(small))):
        _, _, red, black, _, _ = small[index]
        slots, odd, step = red.shape[0], odd_at(index), 1 << index
        if index < last:
            spreads = [
                spread_rows(field + pltpu.roll(field, step, 1), step, passing, at)
                for at, field in enumerate(fields)
            ]
        for at in range(slots):
            black[at, 0, body2, :] = black[at, 0, body2, :] + spreads[at]
        small_sweeps(index, False)
        fields = []
        for at in range(slots):
            r, b = red[at, 0, body2, :], black[at, 0, body2, :]
            fields += [jnp.where(odd, b, r), jnp.where(odd, r, b)]

    for at in range(count1):
        for start in range(2):
            rest1[at, pl.ds(start, rows2, stride=2), :] = fields[at]
    for at in range(count1):
        for e in range(2):
            black1[at, e, body1, :] = window(black1, at, e, rows1) + rest1[at]
    nx, ny, nz = out_ref.shape
    own = nx // 2
    part_slots = min(own // 2 + 3, count1)
    part_rows = min(ny // 2 + 16, rows1)
    slot0 = jnp.where(gx == 0, 0, count1 - part_slots)
    row0 = pl.multiple_of(jnp.clip(gy * (ny // 2) - 8, 0, rows1 - part_rows), 8)
    odds = fold_odds(part_rows)

    def up_total(ref, at, e, to_red):
        low = gx == 0 if at == 0 else False
        high = gx != 0 if at == part_slots - 1 else False
        return fold_total(ref, slot0 + at, e, row0, part_rows, low, high, odds, to_red)

    def up_half(target, other, sources, to_red):
        for at in range(part_slots):
            for e in range(2):
                source = sources[slot0 + at, e, pl.ds(row0, part_rows), :]
                value = share * (source + up_total(other, at, e, to_red))
                target[slot0 + at, e, pl.ds(pl.multiple_of(row0 + PAD, 8), part_rows), :] = value

    for sweep in range(2):
        up_half(red1, black1, fr1, True)
        up_half(black1, red1, fb1, False)

    count, _, rows, _ = dark_ref.shape
    half = rows // 2
    odds = fold_odds(half)
    row = gy * (ny // 2) + (PAD - halo // 2)
    for at in range(count):
        if at < own:
            slot = gx * (own // 2) + at // 2
        else:
            slot = jnp.where(gx == 0, own // 2, own // 2 - (count - own) // 2) + (at - own) // 2
        for e in range(2):
            r, b = red1[slot, e, pl.ds(row, half), :], black1[slot, e, pl.ds(row, half), :]
            plane = jnp.where(odds[e], r, b) if at % 2 else jnp.where(odds[e], b, r)
            tall_ref[at, :, e * LANES : (e + 1) * LANES] = plane
    shape = (2 * LANES, 2 * LANES)
    z = lanes_of(shape)
    z = jnp.where(z < 2 * LANES - halo, z, z - 2 * LANES) + gz * nz
    line = rows_of(shape)
    line = jnp.where(line < LANES, 2 * line, 2 * (line - LANES) + 1)
    weight = jnp.where(line == lax.shift_right_arithmetic(z, 1), 1.0, 0.0)
    spread = exact_dot(tall_ref[...].reshape(count * half, 2 * LANES), weight)
    spread = spread.reshape(count, half, 2 * LANES)
    for at in range(count):
        for c in range(2):
            value = spread[at, :, c * LANES : (c + 1) * LANES]
            for start in range(2):
                work_ref[at, c, pl.ds(PAD + start, half, stride=2), :] = value
    body = slice(PAD, PAD + rows)
    for at in range(count):
        for c in range(2):
            work_ref[at, c, body, :] = work_ref[at, c, body, :] + dark_ref[at, c]
    odd = odd_of((rows, LANES))
    masks = block_mask((ny, nz), halo)
    ends = (gx == 0, gx == lax.axis_size("gx") - 1)
    for sweep in range(2):
        for at in range(count):
            totals = block_totals(work_ref, at, rows, own, odd, True, *ends)
            for c in range(2):
                red_ref[at, c, body, :] = gr_ref[at, c] + masks[c] * totals[c]
        for at in range(count if sweep == 0 else own):
            totals = block_totals(red_ref, at, rows, own, odd, False, *ends)
            for c in range(2 if sweep == 0 else 1):
                work_ref[at, c, body, :] = gb_ref[at, c] + masks[c] * totals[c]
    inner = slice(PAD + halo, PAD + halo + ny)
    odd = odd_of((ny, nz))
    for at in range(own):
        r, b = red_ref[at, 0, inner, :], work_ref[at, 0, inner, :]
        out_ref[2 * at] = jnp.where(odd, b, r)
        out_ref[2 * at + 1] = jnp.where(odd, r, b)


def vmem(number):
    return [pl.BlockSpec(memory_space=pltpu.VMEM)] * number


def struct(*shape):
    return jax.ShapeDtypeStruct(shape, jnp.float32)


def scratch(*shape):
    return pltpu.VMEM(shape, jnp.float32)


HALO = 8


def block_cycle(density):
    halo = HALO
    nx, ny, nz = density.shape
    count_x, count_y, count_z = (lax.axis_size(axis) for axis in ("gx", "gy", "gz"))
    whole = (nx * count_x, ny * count_y, nz * count_z)

    def params(mib):
        return pltpu.CompilerParams(vmem_limit_bytes=mib * 1024 * 1024)

    even = lax.axis_index("gy") % 2 == 0
    ya = lax.dynamic_slice_in_dim(density, jnp.where(even, ny - halo, 0), halo, 1)
    yb = lax.dynamic_slice_in_dim(density, jnp.where(even, 0, ny - halo), halo, 1)
    ya = lax.ppermute(ya, "gy", pairs(count_y, 0))
    yb = lax.ppermute(yb, ("gx", "gy"), inner_pairs(count_x, count_y))
    rows = ny + 2 * halo
    packs = -(-nx * halo // nz)
    za, zb = pl.pallas_call(
        functools.partial(pack_kernel, halo),
        out_shape=[struct(packs, rows, nz)] * 2,
        in_specs=vmem(3), out_specs=vmem(2), compiler_params=params(4),
    )(density, ya, yb)
    za = lax.ppermute(za, "gz", pairs(count_z, 0))
    zb = lax.ppermute(zb, "gz", pairs(count_z, 1) + [(0, count_z - 1), (count_z - 1, 0)])
    own, near = nx // 2, nx // 2 + 2
    send, face = pl.pallas_call(
        functools.partial(pre_kernel, halo),
        out_shape=[struct(near // 2, ny // 2, nz), struct(halo + 1, rows, LANES)],
        in_specs=vmem(5), out_specs=vmem(2), compiler_params=params(10),
        scratch_shapes=[scratch(own, ny, nz)] * 2
        + [scratch(own, 2, rows, LANES)] * 2
        + [scratch(near, 2, rows + 2 * PAD, LANES)] * 2
        + [scratch(near, ny, nz)],
    )(density, ya, yb, za, zb)
    planes = nx + halo
    slots = (planes // 2, 2, rows, LANES)
    padded = (planes // 2, 2, rows + 2 * PAD, LANES)
    first = [
        send,
        lax.ppermute(send, "gy", flips(count_y, 2)),
        lax.ppermute(send, "gz", flips(count_z, 2)),
        lax.ppermute(send, ("gy", "gz"), flips(count_y * count_z, 2 * count_z + 2)),
    ]
    face = lax.ppermute(face, "gx", flips(count_x, 1))
    first[3], face = lax.optimization_barrier((first[3], face))
    block = pl.pallas_call(
        stack_kernel, out_shape=struct(4, *send.shape),
        in_specs=vmem(4), out_specs=pl.BlockSpec(memory_space=pltpu.VMEM), compiler_params=params(2),
    )(*first)
    second = [
        block,
        lax.ppermute(block, "gx", flips(count_x, 1)),
        lax.ppermute(block, "gy", flips(count_y, 1)),
        lax.ppermute(block, ("gx", "gy"), flips(count_x * count_y, count_y + 1)),
    ]
    gr, gb, black = pl.pallas_call(
        functools.partial(field_kernel, halo),
        out_shape=[struct(*slots)] * 3,
        in_specs=vmem(7), out_specs=vmem(3), compiler_params=params(8),
        scratch_shapes=[scratch(*padded)] * 2,
        cost_estimate=pl.CostEstimate(flops=20_000_000, bytes_accessed=2_000_000, transcendentals=0),
    )(density, ya, yb, za, zb, face, block)
    *second[1:], gr, gb, black = lax.optimization_barrier((*second[1:], gr, gb, black))
    third = [lax.ppermute(blocks, "gz", flips(count_z, 1)) for blocks in second]
    count1, rows1, rows2 = whole[0] // 4, whole[1] // 2, whole[1] // 4
    room = [scratch(count1, 2, rows1, LANES)] * 2
    room += [scratch(count1, 2, rows1 + 2 * PAD, LANES)] * 2
    room += [scratch(count1, rows1, LANES), scratch(planes // 2, rows // 2, 2 * LANES)]
    room += [scratch(*padded)] * 2 + [scratch(count1 // 2, 1, rows2 + 2 * PAD, LANES)]
    for count in small_shapes(whole):
        room += [scratch(count, rows2, LANES)] * 2
        room += [scratch(count, 1, rows2 + 2 * PAD, LANES)] * 2
        room += [scratch(count, rows2, LANES)] * 2
    return pl.pallas_call(
        functools.partial(solve_kernel, halo, whole),
        out_shape=struct(nx, ny, nz),
        in_specs=vmem(12), out_specs=pl.BlockSpec(memory_space=pltpu.VMEM),
        compiler_params=params(16), scratch_shapes=room,
    )(*second, *third, gr, gb, black, cycle_matrix(whole))


def fits_block_cycle(shape):
    nx, ny, nz = shape
    count_x, count_y, count_z = (lax.axis_size(axis) for axis in ("gx", "gy", "gz"))
    whole = (nx * count_x, ny * count_y, nz * count_z)
    coarsest = [size >> (LEVELS - 1) for size in whole]
    exact = all(c << (LEVELS - 1) == size for c, size in zip(coarsest, whole))
    return (
        exact and coarsest[0] == coarsest[1] == 1 and nz == LANES and ny == 2 * HALO
        and count_x == 2 and count_y == 4 and count_z == 4
    )


def on_device(density):
    if fits_block_cycle(density.shape):
        return block_cycle(density)
    top = 4
    return shared_cycle(density, 0, top)


def solution(mesh):
    return jax.shard_map(
        on_device,
        mesh=mesh,
        in_specs=(P("gx", "gy", "gz"),),
        out_specs=P("gx", "gy", "gz"),
        check_vma=False,
    )
```

```python
import functools

import jax
import jax.numpy as jnp
import numpy as np
from jax import lax
from jax.experimental import pallas as pl
from jax.experimental.pallas import tpu as pltpu
from jax.sharding import PartitionSpec as P

LEVELS = 7
CSWEEPS = 4


rsd_beta = 0.5
centre = 4.0 + 2.0 * (1.0 + rsd_beta)


def extended_2(value, sides, width):
    for axis, dim in sides:
        count, length = (lax.axis_size(axis), value.shape[dim])
        up = [(i, (i + 1) % count) for i in range(count - 1)]
        down = [(j, i) for i, j in up]
        last = lax.slice_in_dim(value, length - width, length, axis=dim)
        leading = lax.slice_in_dim(value, 0, width, axis=dim)
        before = lax.ppermute(last, axis, up)
        after = lax.ppermute(leading, axis, down)
        value = jnp.concatenate([before, value, after], axis=dim)
    return value


def stencil_sum(padded):
    plane = (
        padded[2:, 1:-1, 1:-1]
        + padded[:-2, 1:-1, 1:-1]
        + padded[1:-1, 2:, 1:-1]
        + padded[1:-1, :-2, 1:-1]
    )
    sight = padded[1:-1, 1:-1, 2:] + padded[1:-1, 1:-1, :-2]
    return plane + (1.0 + rsd_beta) * sight


def grid_index(shape, starts):
    return [lax.broadcasted_iota(jnp.int32, shape, which) + starts[which] for which in range(3)]


def parity_of(shape, starts):
    position = grid_index(shape, starts)
    return (position[0] + position[1] + position[2] + 6) % 2


def inside_grid(shape, starts, whole):
    position = grid_index(shape, starts)
    keep = (position[0] >= 0) & (position[0] < whole[0])
    for which in (1, 2):
        keep = keep & (position[which] >= 0) & (position[which] < whole[which])
    return keep


def half_sweep(field, source, scale, chosen):
    update = (source / scale + stencil_sum(jnp.pad(field, 1))) / centre
    return jnp.where(chosen, update, field)


def full_sweep(field, source, scale, parity):
    field = half_sweep(field, source, scale, parity == 0)
    return half_sweep(field, source, scale, parity == 1)


def restrict(residue):
    shape = residue.shape
    blocks = residue.reshape(shape[0] // 2, 2, shape[1] // 2, 2, shape[2] // 2, 2)
    return jnp.mean(blocks, axis=(1, 3, 5))


def prolong(coarse):
    return jnp.repeat(jnp.repeat(jnp.repeat(coarse, 2, 0), 2, 1), 2, 2)


def local_cycle(source, level):
    scale = 0.25**level
    parity = parity_of(source.shape, (0, 0, 0))
    field = jnp.zeros_like(source)
    if level == LEVELS - 1:
        for _ in range(CSWEEPS):
            field = full_sweep(field, source, scale, parity)
        return field
    for _ in range(2):
        field = full_sweep(field, source, scale, parity)
    residue = source - scale * (centre * field - stencil_sum(jnp.pad(field, 1)))
    field = field + prolong(local_cycle(restrict(residue), level + 1))
    for _ in range(2):
        field = full_sweep(field, source, scale, parity)
    return field


def faces(field):
    return extended_2(field, (("gx", 0), ("gy", 1), ("gz", 2)), 1)


def wide(field):
    return extended_2(field, (("gx", 0), ("gy", 1), ("gz", 2)), 2)


def block_starts(shape, margin):
    return (
        lax.axis_index("gx") * shape[0] - margin,
        lax.axis_index("gy") * shape[1] - margin,
        lax.axis_index("gz") * shape[2] - margin,
    )


def padded_half(padded, source, scale, chosen):
    field = padded[1:-1, 1:-1, 1:-1]
    update = (source / scale + stencil_sum(padded)) / centre
    return jnp.where(chosen, update, field)


def wide_sweep(extended, wide_source, scale, red_wide, source, black):
    update = (wide_source / scale + stencil_sum(jnp.pad(extended, 1))) / centre
    extended = jnp.where(red_wide, update, extended)
    return padded_half(extended[1:-1, 1:-1, 1:-1], source, scale, black)


def coarse_level(source, level):
    shape = source.shape
    stack = lax.all_gather(source[None], ("gx", "gy", "gz"), axis=0, tiled=True)
    count_x, count_y, count_z = (lax.axis_size("gx"), lax.axis_size("gy"), lax.axis_size("gz"))
    whole = stack.reshape(count_x, count_y, count_z, shape[0], shape[1], shape[2])
    whole = whole.transpose(0, 3, 1, 4, 2, 5).reshape(
        count_x * shape[0], count_y * shape[1], count_z * shape[2]
    )
    solved = local_cycle(whole, level)
    starts = block_starts(shape, 0)
    return lax.dynamic_slice(solved, starts, shape)


def shared_cycle(source, level, top):
    if level == top:
        return coarse_level(source, level)
    scale = 0.25**level
    shape = source.shape
    whole = (
        shape[0] * lax.axis_size("gx"),
        shape[1] * lax.axis_size("gy"),
        shape[2] * lax.axis_size("gz"),
    )
    parity = parity_of(shape, block_starts(shape, 0))
    black = parity == 1
    wide_shape = (shape[0] + 4, shape[1] + 4, shape[2] + 4)
    wide_starts = block_starts(shape, 2)
    red_wide = (parity_of(wide_shape, wide_starts) == 0) & inside_grid(
        wide_shape, wide_starts, whole
    )
    wide_source = wide(source)
    field = wide_sweep(
        jnp.zeros(wide_shape, jnp.float32), wide_source, scale, red_wide, source, black
    )
    field = wide_sweep(wide(field), wide_source, scale, red_wide, source, black)
    residue = source - scale * (centre * field - stencil_sum(faces(field)))
    field = field + prolong(shared_cycle(restrict(residue), level + 1, top))
    for _ in range(2):
        field = wide_sweep(wide(field), wide_source, scale, red_wide, source, black)
    return field


def pairs(count, first):
    swaps = []
    for i in range(first, count - 1, 2):
        swaps += [(i, i + 1), (i + 1, i)]
    return swaps


def inner_pairs(count_x, count):
    swaps = []
    for x in range(count_x):
        swaps += [(x * count + i, x * count + j) for i, j in pairs(count, 1)]
        swaps += [(x * count + i, (x ^ 1) * count + i) for i in (0, count - 1)]
    return swaps


def flips(count, bit):
    return [(i, i ^ bit) for i in range(count)]


def lanes_of(shape):
    return lax.broadcasted_iota(jnp.int32, shape, len(shape) - 1)


def rows_of(shape):
    return lax.broadcasted_iota(jnp.int32, shape, len(shape) - 2)


LANES = 128
PAD = 8


def odd_of(shape):
    return ((lanes_of(shape) + rows_of(shape)) & 1) == 1


def exact_dot(a, b):
    return jnp.dot(a, b, precision=lax.Precision.HIGHEST, preferred_element_type=jnp.float32)


def pick_dot(a, b):
    b = b.astype(jnp.bfloat16)
    total = None
    for _ in range(3):
        high = a.astype(jnp.bfloat16)
        term = jnp.dot(high, b, preferred_element_type=jnp.float32)
        total = term if total is None else total + term
        a = a - high.astype(jnp.float32)
    return total


def window(ref, at, column, count, start=0, shift=0):
    if isinstance(start, int):
        return ref[at, column, PAD + start + shift : PAD + start + shift + count, :]
    first = start + (PAD + shift)
    if shift == 0:
        first = pl.multiple_of(first, 8)
    return ref[at, column, pl.ds(first, count), :]


def clear_pads(ref):
    edge = jnp.zeros((PAD, LANES), jnp.float32)
    for at in range(ref.shape[0]):
        for column in range(ref.shape[1]):
            ref[at, column, :PAD, :] = edge
            ref[at, column, ref.shape[2] - PAD :, :] = edge


def block_sums(ref, at, rows):
    lane = lanes_of((rows, LANES))
    values = [window(ref, at, column, rows) for column in range(2)]
    lefts = [pltpu.roll(value, 1, 1) for value in values]
    rights = [pltpu.roll(value, LANES - 1, 1) for value in values]
    sums = []
    for column in range(2):
        left = jnp.where(lane == 0, lefts[1 - column], lefts[column])
        right = jnp.where(lane == LANES - 1, rights[1 - column], rights[column])
        sides = window(ref, at, column, rows, shift=-1) + window(ref, at, column, rows, shift=1)
        sums.append(values[column] + sides + (1.0 + rsd_beta) * (left + right))
    return sums


def block_totals(ref, at, rows, own, odd, to_red, at_low, at_high):
    slots = ref.shape[0]
    totals = []
    for column, total in enumerate(block_sums(ref, at, rows)):
        before = window(ref, (at - 1) % slots, column, rows)
        after = window(ref, (at + 1) % slots, column, rows)
        if at in (0, own):
            before = jnp.where(at_low if at == 0 else at_high, 0.0, before)
        if at in (own - 1, slots - 1):
            after = jnp.where(at_low if at == slots - 1 else at_high, 0.0, after)
        totals.append(total + (jnp.where(odd, after, before) if to_red else jnp.where(odd, before, after)))
    return totals


def block_mask(own, halo):
    ny, nz = own
    shape = (ny + 2 * halo, LANES)
    row = rows_of(shape) - halo + lax.axis_index("gy") * ny
    inside_y = (row >= 0) & (row < ny * lax.axis_size("gy"))
    masks = []
    for column in range(2):
        lane = lanes_of(shape)
        if column:
            lane = jnp.where(lane < halo, lane + LANES, lane - LANES)
        lane = lane + lax.axis_index("gz") * nz
        inside = inside_y & (lane >= 0) & (lane < nz * lax.axis_size("gz"))
        masks.append(jnp.where(inside, 1.0 / centre, 0.0))
    return masks


def block_plane(at, own_ref, ya_ref, yb_ref, even_y):
    a, b = ya_ref[at], yb_ref[at]
    low = jnp.where(even_y, b, a)
    high = jnp.where(even_y, a, b)
    return jnp.concatenate([low, own_ref[at], high], axis=0)


def block_columns(halo, at, own_ref, ya_ref, yb_ref, za_ref, zb_ref, even_y, even_z):
    _, _, nz = own_ref.shape
    j, k = at // (nz // halo), at % (nz // halo)
    a, b = za_ref[j], zb_ref[j]
    left = pltpu.roll(jnp.where(even_z, b, a), (2 * nz - halo - halo * k) % nz, 1)
    right = pltpu.roll(jnp.where(even_z, a, b), (nz - halo * k) % nz, 1)
    lane = lanes_of(left.shape)
    sides = jnp.where(lane < halo, right, jnp.where(lane >= nz - halo, left, 0.0))
    return block_plane(at, own_ref, ya_ref, yb_ref, even_y), sides


def pack_kernel(halo, own_ref, ya_ref, yb_ref, za_ref, zb_ref):
    even_y = lax.axis_index("gy") % 2 == 0
    even_z = lax.axis_index("gz") % 2 == 0
    nx, ny, nz = own_ref.shape
    groups = nz // halo
    shape = (ny + 2 * halo, nz)
    group = lanes_of(shape) // halo
    for j in range(za_ref.shape[0]):
        last = jnp.zeros(shape, jnp.float32)
        first = jnp.zeros(shape, jnp.float32)
        for k in range(min(groups, nx - j * groups)):
            plane = block_plane(j * groups + k, own_ref, ya_ref, yb_ref, even_y)
            last = jnp.where(group == k, pltpu.roll(plane, (halo * k + halo) % nz, 1), last)
            first = jnp.where(group == k, pltpu.roll(plane, halo * k, 1), first)
        za_ref[j] = jnp.where(even_z, last, first)
        zb_ref[j] = jnp.where(even_z, first, last)


def smooth(count, own, masks, odd, ends, gr_ref, gb_ref, red_ref, black_ref, done):
    rows = odd.shape[0]
    body = slice(PAD, PAD + rows)

    def value_of(source, at, c, total):
        value = masks[c] * total
        return source[at, c] + value if at < source.shape[0] else value

    for at in range(count):
        for c in range(2):
            red_ref[at, c, body, :] = gr_ref[at, c] if at < gr_ref.shape[0] else jnp.zeros_like(masks[c])
    for step in range(3):
        source, target, other = (gr_ref, red_ref, black_ref) if step == 1 else (gb_ref, black_ref, red_ref)
        for at in range(count):
            totals = block_totals(other, at, rows, own, odd, step == 1, *ends)
            for c in range(2):
                value = value_of(source, at, c, totals[c])
                target[at, c, body, :] = value
                if step == 2:
                    done(at, c, totals[c], value)


def x_ends():
    here = lax.axis_index("gx")
    return here == 0, here == lax.axis_size("gx") - 1


def pre_kernel(
    halo, own_ref, ya_ref, yb_ref, za_ref, zb_ref,
    send_ref, face_ref,
    fr_ref, fb_ref, gr_ref, gb_ref, red_ref, black_ref, rest_ref,
):
    even_y = lax.axis_index("gy") % 2 == 0
    even_z = lax.axis_index("gz") % 2 == 0
    nx, ny, nz = own_ref.shape
    count, _, rows, _ = red_ref.shape
    rows = rows - 2 * PAD
    own = nx // 2
    shape = (rows, LANES)
    odd = odd_of(shape)
    masks = block_mask((ny, nz), halo)
    inner = slice(halo, halo + ny)
    ends = x_ends()
    clear_pads(red_ref)
    clear_pads(black_ref)
    for p in range(halo):
        high = block_plane(nx - halo + p, own_ref, ya_ref, yb_ref, even_y)
        face_ref[p] = jnp.where(ends[0], high, block_plane(p, own_ref, ya_ref, yb_ref, even_y))
    middle = halo * halo
    top = za_ref.shape[0] - 1
    left = [jnp.where(even_z, zb_ref[j], za_ref[j]) for j in (0, top)]
    right = [jnp.where(even_z, za_ref[j], zb_ref[j]) for j in (0, top)]
    left = jnp.where(ends[0], pltpu.roll(left[1], middle, 1), left[0])
    right = jnp.where(ends[0], right[1], pltpu.roll(right[0], middle, 1))
    face_ref[halo] = jnp.where(lanes_of(shape) < middle, left, right)
    for at in range(own):
        planes = [
            block_columns(halo, x, own_ref, ya_ref, yb_ref, za_ref, zb_ref, even_y, even_z)
            for x in (2 * at, 2 * at + 1)
        ]
        for c in range(2):
            red = jnp.where(odd, planes[1][c], planes[0][c])
            black = jnp.where(odd, planes[0][c], planes[1][c])
            if c == 0:
                fr_ref[at], fb_ref[at] = red[inner], black[inner]
            gr_ref[at, c], gb_ref[at, c] = masks[c] * red, masks[c] * black

    def keep(at, c, total, value):
        if c == 0:
            left_over = total[inner] - centre * value[inner]
            rest_ref[at] = left_over + fb_ref[at] if at < own else left_over

    smooth(count, own, masks, odd, ends, gr_ref, gb_ref, red_ref, black_ref, keep)
    for at in range(count):
        total = block_totals(black_ref, at, rows, own, odd, True, *ends)[0]
        left_over = total[inner] - centre * red_ref[at, 0, PAD + halo : PAD + halo + ny, :]
        if at < own:
            left_over = left_over + fr_ref[at]
        rest_ref[at] = rest_ref[at] + left_over
    half, quarter = ny // 2, nz // 4
    pairs_y = rest_ref[:, pl.ds(0, half, stride=2), :] + rest_ref[:, pl.ds(1, half, stride=2), :]
    turn = quarter * lax.axis_index("gz")
    column = (lanes_of((nz, nz)) - turn) & (nz - 1)
    target = 2 * (column % quarter) + (column // quarter) % 2
    weight = jnp.where(rows_of((nz, nz)) // 2 == target, 0.5, 0.0)
    coarse = pick_dot(pairs_y.reshape(count * half, nz), weight).reshape(count, half, nz)
    part = ((lanes_of((half, nz)) - turn) & (nz - 1)) // quarter
    pick = (((rows_of((half, nz)) + part) & 1) == 1) ^ (part >= 2)
    for at in range(count // 2):
        send_ref[at] = jnp.where(pick, coarse[2 * at + 1], coarse[2 * at])


def field_kernel(
    halo, own_ref, ya_ref, yb_ref, za_ref, zb_ref, face_ref, after_ref,
    gr_ref, gb_ref, dark_ref,
    red_ref, black_ref,
):
    even_y = lax.axis_index("gy") % 2 == 0
    even_z = lax.axis_index("gz") % 2 == 0
    nx, ny, nz = own_ref.shape
    count, _, rows, _ = gr_ref.shape
    own = nx // 2
    shape = (rows, LANES)
    odd, lane = odd_of(shape), lanes_of(shape)
    masks = block_mask((ny, nz), halo)
    clear_pads(red_ref)
    clear_pads(black_ref)

    def columns(x):
        if x < nx:
            return block_columns(halo, x, own_ref, ya_ref, yb_ref, za_ref, zb_ref, even_y, even_z)
        p = x - nx
        left = pltpu.roll(face_ref[halo], (2 * LANES - halo - halo * p) % LANES, 1)
        right = pltpu.roll(face_ref[halo], (2 * LANES - halo * halo - halo * p) % LANES, 1)
        return face_ref[p], jnp.where(lane < halo, right, jnp.where(lane >= nz - halo, left, 0.0))

    for at in range(count):
        first, second = columns(2 * at), columns(2 * at + 1)
        for c in range(2):
            gr_ref[at, c] = masks[c] * jnp.where(odd, second[c], first[c])
            gb_ref[at, c] = masks[c] * jnp.where(odd, first[c], second[c])

    def keep(at, c, total, value):
        dark_ref[at, c] = value

    smooth(count, own, masks, odd, x_ends(), gr_ref, gb_ref, red_ref, black_ref, keep)


def stack_kernel(*refs):
    for which, ref in enumerate(refs[:-1]):
        refs[-1][which] = ref[...]


def small_shapes(whole):
    return [whole[0] >> (level + 1) for level in range(2, LEVELS - 2)]


def plain_sum(field):
    padded = np.pad(field, ((0, 0), (1, 1), (1, 1), (1, 1)))
    inner = slice(1, -1)
    plane = padded[:, 2:, inner, inner] + padded[:, :-2, inner, inner]
    plane = plane + padded[:, inner, 2:, inner] + padded[:, inner, :-2, inner]
    return plane + (1.0 + rsd_beta) * (padded[:, inner, inner, 2:] + padded[:, inner, inner, :-2])


def plain_cycle(source, level):
    parity = np.indices(source.shape[1:]).sum(axis=0) % 2
    field = np.zeros_like(source)

    def sweeps(field, number):
        for step in range(2 * number):
            field = np.where(parity == step % 2, (source + plain_sum(field)) / centre, field)
        return field

    if level == LEVELS - 1:
        return sweeps(field, CSWEEPS)
    field = sweeps(field, 2)
    rest = source - centre * field + plain_sum(field)
    nx, ny, nz = source.shape[1:]
    rest = rest.reshape(-1, nx // 2, 2, ny // 2, 2, nz // 2, 2).sum(axis=(2, 4, 6)) / 2.0
    coarse = plain_cycle(rest, level + 1)
    for axis in (1, 2, 3):
        coarse = np.repeat(coarse, 2, axis)
    return sweeps(field + coarse, 2)


def cycle_matrix(whole):
    level = LEVELS - 2
    nx, ny, nz = (size >> level for size in whole)
    size = nx * ny * 2 * nz
    unit = np.eye(size).reshape(size, 2 * nz, nx, ny).transpose(0, 2, 3, 1)
    source = unit.reshape(size, nx, ny, nz, 2).sum(axis=-1) / 2.0
    result = np.repeat(plain_cycle(source, level), 2, axis=3)
    return jnp.asarray(result.transpose(0, 3, 1, 2).reshape(size, size), jnp.float32)


def solve_kernel(halo, *refs):
    gathered, refs = refs[:8], refs[8:]
    gr_ref, gb_ref, dark_ref, matrix_ref, out_ref = refs[:5]
    fr1, fb1, red1, black1, rest1, tall_ref, red_ref, work_ref, passing = refs[5:14]
    small = [refs[14 + 6 * i : 20 + 6 * i] for i in range(LEVELS - 4)]
    gx, gy, gz = (lax.axis_index(axis) for axis in ("gx", "gy", "gz"))
    weight_z = 1.0 + rsd_beta
    share = 1.0 / centre
    for ref in (red1, black1, red_ref, work_ref, passing):
        clear_pads(ref)
    for level in small:
        for ref in level[2:4]:
            clear_pads(ref)

    _, slots, block_rows, _ = gathered[0].shape
    slots = slots - 1
    count1, _, rows1, _ = fr1.shape
    quarter = LANES // 4
    group = lanes_of((block_rows, LANES)) // quarter
    held = [jnp.bitwise_and(group - jnp.bitwise_xor(gz, bits), 3) for bits in range(4)]
    theirs = [[kind == part for kind in held] for part in range(4)]

    def unpack(far, second, at):
        y = jnp.bitwise_xor(gy, 2 * far + (second >> 1))
        rows = pl.ds(pl.multiple_of(y * block_rows, 8), block_rows)
        blocks = [gathered[4 * (bits & 1) + second][far + (bits & 2), at] for bits in range(4)]
        parts = []
        for part in range(4):
            value = blocks[0]
            for block, mine in zip(blocks[1:], theirs[part][1:]):
                value = jnp.where(mine, block, value)
            parts.append(pltpu.roll(value, LANES - quarter * part, 1) if part else value)
        return rows, parts

    half1 = count1 // 2
    for far in range(2):
        for second in range(4):
            x = jnp.bitwise_xor(gx, second & 1)
            for at in range(slots):
                rows, parts = unpack(far, second, at)
                for part, target in enumerate((fr1, fr1, fb1, fb1)):
                    target[x * slots + at, part % 2, rows, :] = parts[part]
    for far in range(2):
        for second in range(4):
            x = jnp.bitwise_xor(gx, second & 1)
            next_slot = jnp.where(x == 0, half1, half1 - 1)
            rows, parts = unpack(far, second, slots)
            for part, target in enumerate((fr1, fr1, fb1, fb1)):
                target[next_slot, part % 2, rows, :] = target[next_slot, part % 2, rows, :] + parts[part]

    def fold_total(ref, at, e, start, count, low, high, odds, to_red):
        lane = lanes_of((count, LANES))
        value, other = window(ref, at, e, count, start), window(ref, at, 1 - e, count, start)
        sides = window(ref, at, e, count, start, -1) + window(ref, at, e, count, start, 1)
        if e == 0:
            near = jnp.where(lane == 0, 0.0, pltpu.roll(other, 1, 1))
        else:
            near = jnp.where(lane == LANES - 1, 0.0, pltpu.roll(other, LANES - 1, 1))
        before = 0.0 if low is True else window(ref, at - 1, e, count, start)
        after = 0.0 if high is True else window(ref, at + 1, e, count, start)
        if not isinstance(low, bool):
            before = jnp.where(low, 0.0, window(ref, jnp.maximum(at - 1, 0), e, count, start))
        if not isinstance(high, bool):
            after = jnp.where(high, 0.0, window(ref, jnp.minimum(at + 1, count1 - 1), e, count, start))
        beside = jnp.where(odds[e], after, before) if to_red else jnp.where(odds[e], before, after)
        return value + sides + beside + weight_z * (other + near)

    def fold_odds(count):
        row = rows_of((count, LANES))
        return [((row + e) & 1) == 1 for e in range(2)]

    odds = fold_odds(rows1)
    body1 = slice(PAD, PAD + rows1)

    def down_total(ref, at, e, to_red):
        return fold_total(ref, at, e, 0, rows1, at == 0, at == count1 - 1, odds, to_red)

    for at in range(count1):
        for e in range(2):
            red1[at, e, body1, :] = share * fr1[at, e]
    for at in range(count1):
        for e in range(2):
            black1[at, e, body1, :] = share * (fb1[at, e] + down_total(red1, at, e, False))
    for at in range(count1):
        for e in range(2):
            red1[at, e, body1, :] = share * (fr1[at, e] + down_total(black1, at, e, True))
    for at in range(count1):
        left_over = None
        for e in range(2):
            total = fb1[at, e] + down_total(red1, at, e, False)
            value = share * total
            black1[at, e, body1, :] = value
            term = total - centre * value
            left_over = term if left_over is None else left_over + term
        rest1[at] = left_over
    for at in range(count1):
        left_over = rest1[at]
        for e in range(2):
            total = fr1[at, e] + down_total(black1, at, e, True)
            left_over = left_over + (total - centre * window(red1, at, e, rows1))
        rest1[at] = left_over
    rows2 = rows1 // 2
    shape2 = (rows2, LANES)
    row2, lane2 = rows_of(shape2), lanes_of(shape2)
    odd2 = odd_of(shape2)
    planes = [
        0.5 * (rest1[at, pl.ds(0, rows2, stride=2), :] + rest1[at, pl.ds(1, rows2, stride=2), :])
        for at in range(count1)
    ]

    body2 = slice(PAD, PAD + rows2)

    def grid_of(index):
        step = 1 << index
        return ((row2 & (step - 1)) == 0) & ((lane2 & (step - 1)) == 0)

    def odd_at(index):
        return (((row2 >> index) + (lane2 >> index)) & 1) == 1

    def turned(value, step):
        inside = lane2 >= step if step > 0 else lane2 < LANES + step
        return jnp.where(inside, pltpu.roll(value, step % LANES, 1), 0.0)

    def small_plane(index, ref, at, odd, to_red):
        step = 1 << index
        total = ref[at, 0, body2, :] + (
            ref[at, 0, PAD - step : PAD - step + rows2, :] + ref[at, 0, PAD + step : PAD + step + rows2, :]
        )
        slots = ref.shape[0]
        if slots == 1:
            return total
        before = ref[at - 1, 0, body2, :] if at > 0 else 0.0
        after = ref[at + 1, 0, body2, :] if at < slots - 1 else 0.0
        return total + (jnp.where(odd, after, before) if to_red else jnp.where(odd, before, after))

    def small_sweeps(index, start):
        fr, fb, red, black, fr_low, fr_high = small[index]
        odd, width = odd_at(index), 1 << index
        mask = jnp.where(grid_of(index), share, 0.0)
        mask_low = jnp.where(lane2 < width, 0.0, mask)
        mask_high = jnp.where(lane2 >= LANES - width, 0.0, mask)
        slots = fr.shape[0]
        if start:
            for at in range(slots):
                fr_low[at] = pltpu.roll(fr[at], width, 1)
                fr_high[at] = pltpu.roll(fr[at], LANES - width, 1)
        for step in range(2):
            sides = []
            for at in range(slots):
                here, low, high = fr[at], fr_low[at], fr_high[at]
                if not (start and step == 0):
                    value = black[at, 0, body2, :]
                    plane = small_plane(index, black, at, odd, True)
                    here = here + plane + weight_z * (turned(value, width) + turned(value, -width))
                    low = low + pltpu.roll(plane, width, 1) + weight_z * (turned(value, 2 * width) + value)
                    high = high + pltpu.roll(plane, LANES - width, 1)
                    high = high + weight_z * (value + turned(value, -2 * width))
                red[at, 0, body2, :] = mask * here
                sides.append(weight_z * (mask_low * low + mask_high * high))
            totals = []
            for at in range(slots):
                total = fb[at] + small_plane(index, red, at, odd, False) + sides[at]
                black[at, 0, body2, :] = mask * total
                totals.append(total)
        return totals

    def spread_rows(value, step, ref, at):
        ref[at, 0, body2, :] = value
        return value + ref[at, 0, PAD - step : PAD - step + rows2, :]

    last = len(small) - 1
    for index in range(len(small)):
        fr, fb, red, black, _, fr_high = small[index]
        slots, odd, step = fr.shape[0], odd_at(index), 1 << index
        for at in range(slots):
            p, q = planes[2 * at], planes[2 * at + 1]
            fr[at], fb[at] = jnp.where(odd, q, p), jnp.where(odd, p, q)
        black_totals = small_sweeps(index, True)
        totals = []
        for at in range(slots):
            value, field = black[at, 0, body2, :], red[at, 0, body2, :]
            plane = small_plane(index, black, at, odd, True)
            total = black_totals[at] - centre * value
            next_total = pltpu.roll(total, LANES - step, 1)
            total = total + (
                fr[at] + plane + weight_z * (turned(value, step) + turned(value, -step)) - centre * field
            )
            if index < last:
                next_total = next_total + (
                    fr_high[at] + pltpu.roll(plane, LANES - step, 1)
                    + weight_z * (value + turned(value, -2 * step))
                    - centre * pltpu.roll(field, LANES - step, 1)
                )
                total = total + next_total
            totals.append(total)
            passing[at, 0, body2, :] = total
        lower = [passing[at, 0, PAD + step : PAD + step + rows2, :] for at in range(slots)]
        planes = [0.5 * (total + below) for total, below in zip(totals, lower)]

    half_rows = rows2 // 2
    upper = [passing[at, 0, PAD - step : PAD - step + rows2, :] for at in range(slots)]
    odd_line = (row2 & step) != 0
    summed = [
        total + jnp.where(odd_line, above, below) for total, above, below in zip(totals, upper, lower)
    ]
    lines = [total[start : start + half_rows] for total in summed for start in (0, half_rows)]
    place = lanes_of((half_rows, LANES)) & (len(lines) - 1)
    joined = lines[0]
    for q in range(1, len(lines)):
        joined = jnp.where(place == q, pltpu.roll(lines[q], q, 1), joined)
    answer = exact_dot(joined, matrix_ref[...])
    grid = (place == 0) & ((rows_of((half_rows, LANES)) & (step - 1)) == 0)
    parts = []
    for q in range(len(lines)):
        part = pltpu.roll(answer, LANES - q, 1) if q else answer
        parts.append(jnp.where(grid, part, 0.0))
    spreads = [jnp.concatenate(parts[2 * at : 2 * at + 2], axis=0) for at in range(slots)]

    for index in reversed(range(len(small))):
        _, _, red, black, _, _ = small[index]
        slots, odd, step = red.shape[0], odd_at(index), 1 << index
        if index < last:
            spreads = [
                spread_rows(field + pltpu.roll(field, step, 1), step, passing, at)
                for at, field in enumerate(fields)
            ]
        for at in range(slots):
            black[at, 0, body2, :] = black[at, 0, body2, :] + spreads[at]
        small_sweeps(index, False)
        fields = []
        for at in range(slots):
            r, b = red[at, 0, body2, :], black[at, 0, body2, :]
            fields += [jnp.where(odd, b, r), jnp.where(odd, r, b)]

    for at in range(count1):
        for start in range(2):
            rest1[at, pl.ds(start, rows2, stride=2), :] = fields[at]
    for at in range(count1):
        for e in range(2):
            black1[at, e, body1, :] = window(black1, at, e, rows1) + rest1[at]
    nx, ny, nz = out_ref.shape
    own = nx // 2
    part_slots = min(own // 2 + 3, count1)
    part_rows = min(ny // 2 + 16, rows1)
    slot0 = jnp.where(gx == 0, 0, count1 - part_slots)
    row0 = pl.multiple_of(jnp.clip(gy * (ny // 2) - 8, 0, rows1 - part_rows), 8)
    odds = fold_odds(part_rows)

    def up_total(ref, at, e, to_red):
        low = gx == 0 if at == 0 else False
        high = gx != 0 if at == part_slots - 1 else False
        return fold_total(ref, slot0 + at, e, row0, part_rows, low, high, odds, to_red)

    def up_half(target, other, sources, to_red):
        for at in range(part_slots):
            for e in range(2):
                source = sources[slot0 + at, e, pl.ds(row0, part_rows), :]
                value = share * (source + up_total(other, at, e, to_red))
                target[slot0 + at, e, pl.ds(pl.multiple_of(row0 + PAD, 8), part_rows), :] = value

    for _ in range(2):
        up_half(red1, black1, fr1, True)
        up_half(black1, red1, fb1, False)

    count, _, rows, _ = dark_ref.shape
    half = rows // 2
    odds = fold_odds(half)
    row = gy * (ny // 2) + (PAD - halo // 2)
    for at in range(count):
        if at < own:
            slot = gx * (own // 2) + at // 2
        else:
            slot = jnp.where(gx == 0, own // 2, own // 2 - (count - own) // 2) + (at - own) // 2
        for e in range(2):
            r, b = red1[slot, e, pl.ds(row, half), :], black1[slot, e, pl.ds(row, half), :]
            plane = jnp.where(odds[e], r, b) if at % 2 else jnp.where(odds[e], b, r)
            tall_ref[at, :, e * LANES : (e + 1) * LANES] = plane
    shape = (2 * LANES, 2 * LANES)
    z = lanes_of(shape)
    z = jnp.where(z < 2 * LANES - halo, z, z - 2 * LANES) + gz * nz
    line = rows_of(shape)
    line = jnp.where(line < LANES, 2 * line, 2 * (line - LANES) + 1)
    weight = jnp.where(line == lax.shift_right_arithmetic(z, 1), 1.0, 0.0)
    spread = pick_dot(tall_ref[...].reshape(count * half, 2 * LANES), weight)
    spread = spread.reshape(count, half, 2 * LANES)
    for at in range(count):
        for c in range(2):
            value = spread[at, :, c * LANES : (c + 1) * LANES]
            for start in range(2):
                work_ref[at, c, pl.ds(PAD + start, half, stride=2), :] = value
    body = slice(PAD, PAD + rows)
    for at in range(count):
        for c in range(2):
            work_ref[at, c, body, :] = work_ref[at, c, body, :] + dark_ref[at, c]
    odd = odd_of((rows, LANES))
    masks = block_mask((ny, nz), halo)
    ends = (gx == 0, gx == lax.axis_size("gx") - 1)
    beside_own = [*range(own), own, count - 1]
    for sweep in range(2):
        for at in range(count) if sweep == 0 else beside_own:
            totals = block_totals(work_ref, at, rows, own, odd, True, *ends)
            for c in range(2):
                red_ref[at, c, body, :] = gr_ref[at, c] + masks[c] * totals[c]
        for at in beside_own if sweep == 0 else range(own):
            totals = block_totals(red_ref, at, rows, own, odd, False, *ends)
            for c in range(2 if sweep == 0 else 1):
                work_ref[at, c, body, :] = gb_ref[at, c] + masks[c] * totals[c]
    inner = slice(PAD + halo, PAD + halo + ny)
    odd = odd_of((ny, nz))
    for at in range(own):
        r, b = red_ref[at, 0, inner, :], work_ref[at, 0, inner, :]
        out_ref[2 * at] = jnp.where(odd, b, r)
        out_ref[2 * at + 1] = jnp.where(odd, r, b)


def vmem(number):
    return [pl.BlockSpec(memory_space=pltpu.VMEM)] * number


def struct(*shape):
    return jax.ShapeDtypeStruct(shape, jnp.float32)


def scratch(*shape):
    return pltpu.VMEM(shape, jnp.float32)


HALO = 8


def block_cycle(density):
    halo = HALO
    nx, ny, nz = density.shape
    count_x, count_y, count_z = (lax.axis_size(axis) for axis in ("gx", "gy", "gz"))
    whole = (nx * count_x, ny * count_y, nz * count_z)

    def params(mib):
        return pltpu.CompilerParams(vmem_limit_bytes=mib * 1024 * 1024)

    even = lax.axis_index("gy") % 2 == 0
    ya = lax.dynamic_slice_in_dim(density, jnp.where(even, ny - halo, 0), halo, 1)
    yb = lax.dynamic_slice_in_dim(density, jnp.where(even, 0, ny - halo), halo, 1)
    ya = lax.ppermute(ya, "gy", pairs(count_y, 0))
    yb = lax.ppermute(yb, ("gx", "gy"), inner_pairs(count_x, count_y))
    rows = ny + 2 * halo
    packs = -(-nx * halo // nz)
    za, zb = pl.pallas_call(
        functools.partial(pack_kernel, halo),
        out_shape=[struct(packs, rows, nz)] * 2,
        in_specs=vmem(3), out_specs=vmem(2), compiler_params=params(4),
    )(density, ya, yb)
    za = lax.ppermute(za, "gz", pairs(count_z, 0))
    zb = lax.ppermute(zb, "gz", pairs(count_z, 1) + [(0, count_z - 1), (count_z - 1, 0)])
    own, near = nx // 2, nx // 2 + 2
    send, face = pl.pallas_call(
        functools.partial(pre_kernel, halo),
        out_shape=[struct(near // 2, ny // 2, nz), struct(halo + 1, rows, LANES)],
        in_specs=vmem(5), out_specs=vmem(2), compiler_params=params(10),
        scratch_shapes=[scratch(own, ny, nz)] * 2
        + [scratch(own, 2, rows, LANES)] * 2
        + [scratch(near, 2, rows + 2 * PAD, LANES)] * 2
        + [scratch(near, ny, nz)],
    )(density, ya, yb, za, zb)
    planes = nx + halo
    slots = (planes // 2, 2, rows, LANES)
    padded = (planes // 2, 2, rows + 2 * PAD, LANES)
    first = [
        send,
        lax.ppermute(send, "gy", flips(count_y, 2)),
        lax.ppermute(send, "gz", flips(count_z, 2)),
        lax.ppermute(send, ("gy", "gz"), flips(count_y * count_z, 2 * count_z + 2)),
    ]
    face = lax.ppermute(face, "gx", flips(count_x, 1))
    block = pl.pallas_call(
        stack_kernel, out_shape=struct(4, *send.shape),
        in_specs=vmem(4), out_specs=pl.BlockSpec(memory_space=pltpu.VMEM), compiler_params=params(2),
    )(*first)
    second = [
        block,
        lax.ppermute(block, "gx", flips(count_x, 1)),
        lax.ppermute(block, "gy", flips(count_y, 1)),
        lax.ppermute(block, ("gx", "gy"), flips(count_x * count_y, count_y + 1)),
    ]
    gr, gb, black = pl.pallas_call(
        functools.partial(field_kernel, halo),
        out_shape=[struct(*slots)] * 3,
        in_specs=vmem(7), out_specs=vmem(3), compiler_params=params(8),
        scratch_shapes=[scratch(*padded)] * 2,
        cost_estimate=pl.CostEstimate(flops=20_000_000, bytes_accessed=2_000_000, transcendentals=0),
    )(density, ya, yb, za, zb, face, block)
    *second[1:], gr, gb, black = lax.optimization_barrier((*second[1:], gr, gb, black))
    third = [lax.ppermute(blocks, "gz", flips(count_z, 1)) for blocks in second]
    count1, rows1, rows2 = whole[0] // 4, whole[1] // 2, whole[1] // 4
    room = [scratch(count1, 2, rows1, LANES)] * 2
    room += [scratch(count1, 2, rows1 + 2 * PAD, LANES)] * 2
    room += [scratch(count1, rows1, LANES), scratch(planes // 2, rows // 2, 2 * LANES)]
    room += [scratch(*padded)] * 2 + [scratch(count1 // 2, 1, rows2 + 2 * PAD, LANES)]
    for count in small_shapes(whole):
        room += [scratch(count, rows2, LANES)] * 2
        room += [scratch(count, 1, rows2 + 2 * PAD, LANES)] * 2
        room += [scratch(count, rows2, LANES)] * 2
    return pl.pallas_call(
        functools.partial(solve_kernel, halo),
        out_shape=struct(nx, ny, nz),
        in_specs=vmem(12), out_specs=pl.BlockSpec(memory_space=pltpu.VMEM),
        compiler_params=params(16), scratch_shapes=room,
    )(*second, *third, gr, gb, black, cycle_matrix(whole))


def fits_block_cycle(shape):
    nx, ny, nz = shape
    count_x, count_y, count_z = (lax.axis_size(axis) for axis in ("gx", "gy", "gz"))
    whole = (nx * count_x, ny * count_y, nz * count_z)
    coarsest = [size >> (LEVELS - 1) for size in whole]
    exact = all(c << (LEVELS - 1) == size for c, size in zip(coarsest, whole))
    return (
        exact and coarsest[0] == coarsest[1] == 1 and nz == LANES and ny == 2 * HALO
        and count_x == 2 and count_y == 4 and count_z == 4
    )


def on_device(density):
    if fits_block_cycle(density.shape):
        return block_cycle(density)
    top = 4
    return shared_cycle(density, 0, top)


def solution(mesh):
    return jax.shard_map(
        on_device,
        mesh=mesh,
        in_specs=(P("gx", "gy", "gz"),),
        out_specs=P("gx", "gy", "gz"),
        check_vma=False,
    )
```

```python
import functools

import jax
import jax.numpy as jnp
import numpy as np
from jax import lax
from jax.experimental import pallas as pl
from jax.experimental.pallas import tpu as pltpu
from jax.sharding import PartitionSpec as P

LEVELS = 7
CSWEEPS = 4


rsd_beta = 0.5
centre = 4.0 + 2.0 * (1.0 + rsd_beta)


def extended_2(value, sides, width):
    for axis, dim in sides:
        count, length = (lax.axis_size(axis), value.shape[dim])
        up = [(i, (i + 1) % count) for i in range(count - 1)]
        down = [(j, i) for i, j in up]
        last = lax.slice_in_dim(value, length - width, length, axis=dim)
        leading = lax.slice_in_dim(value, 0, width, axis=dim)
        before = lax.ppermute(last, axis, up)
        after = lax.ppermute(leading, axis, down)
        value = jnp.concatenate([before, value, after], axis=dim)
    return value


def stencil_sum(padded):
    plane = (
        padded[2:, 1:-1, 1:-1]
        + padded[:-2, 1:-1, 1:-1]
        + padded[1:-1, 2:, 1:-1]
        + padded[1:-1, :-2, 1:-1]
    )
    sight = padded[1:-1, 1:-1, 2:] + padded[1:-1, 1:-1, :-2]
    return plane + (1.0 + rsd_beta) * sight


def grid_index(shape, starts):
    return [lax.broadcasted_iota(jnp.int32, shape, which) + starts[which] for which in range(3)]


def parity_of(shape, starts):
    position = grid_index(shape, starts)
    return (position[0] + position[1] + position[2] + 6) % 2


def inside_grid(shape, starts, whole):
    position = grid_index(shape, starts)
    keep = (position[0] >= 0) & (position[0] < whole[0])
    for which in (1, 2):
        keep = keep & (position[which] >= 0) & (position[which] < whole[which])
    return keep


def half_sweep(field, source, scale, chosen):
    update = (source / scale + stencil_sum(jnp.pad(field, 1))) / centre
    return jnp.where(chosen, update, field)


def full_sweep(field, source, scale, parity):
    field = half_sweep(field, source, scale, parity == 0)
    return half_sweep(field, source, scale, parity == 1)


def restrict(residue):
    shape = residue.shape
    blocks = residue.reshape(shape[0] // 2, 2, shape[1] // 2, 2, shape[2] // 2, 2)
    return jnp.mean(blocks, axis=(1, 3, 5))


def prolong(coarse):
    return jnp.repeat(jnp.repeat(jnp.repeat(coarse, 2, 0), 2, 1), 2, 2)


def local_cycle(source, level):
    scale = 0.25**level
    parity = parity_of(source.shape, (0, 0, 0))
    field = jnp.zeros_like(source)
    if level == LEVELS - 1:
        for _ in range(CSWEEPS):
            field = full_sweep(field, source, scale, parity)
        return field
    for _ in range(2):
        field = full_sweep(field, source, scale, parity)
    residue = source - scale * (centre * field - stencil_sum(jnp.pad(field, 1)))
    field = field + prolong(local_cycle(restrict(residue), level + 1))
    for _ in range(2):
        field = full_sweep(field, source, scale, parity)
    return field


def faces(field):
    return extended_2(field, (("gx", 0), ("gy", 1), ("gz", 2)), 1)


def wide(field):
    return extended_2(field, (("gx", 0), ("gy", 1), ("gz", 2)), 2)


def block_starts(shape, margin):
    return (
        lax.axis_index("gx") * shape[0] - margin,
        lax.axis_index("gy") * shape[1] - margin,
        lax.axis_index("gz") * shape[2] - margin,
    )


def padded_half(padded, source, scale, chosen):
    field = padded[1:-1, 1:-1, 1:-1]
    update = (source / scale + stencil_sum(padded)) / centre
    return jnp.where(chosen, update, field)


def wide_sweep(extended, wide_source, scale, red_wide, source, black):
    update = (wide_source / scale + stencil_sum(jnp.pad(extended, 1))) / centre
    extended = jnp.where(red_wide, update, extended)
    return padded_half(extended[1:-1, 1:-1, 1:-1], source, scale, black)


def coarse_level(source, level):
    shape = source.shape
    stack = lax.all_gather(source[None], ("gx", "gy", "gz"), axis=0, tiled=True)
    count_x, count_y, count_z = (lax.axis_size("gx"), lax.axis_size("gy"), lax.axis_size("gz"))
    whole = stack.reshape(count_x, count_y, count_z, shape[0], shape[1], shape[2])
    whole = whole.transpose(0, 3, 1, 4, 2, 5).reshape(
        count_x * shape[0], count_y * shape[1], count_z * shape[2]
    )
    solved = local_cycle(whole, level)
    starts = block_starts(shape, 0)
    return lax.dynamic_slice(solved, starts, shape)


def shared_cycle(source, level, top):
    if level == top:
        return coarse_level(source, level)
    scale = 0.25**level
    shape = source.shape
    whole = (
        shape[0] * lax.axis_size("gx"),
        shape[1] * lax.axis_size("gy"),
        shape[2] * lax.axis_size("gz"),
    )
    parity = parity_of(shape, block_starts(shape, 0))
    black = parity == 1
    wide_shape = (shape[0] + 4, shape[1] + 4, shape[2] + 4)
    wide_starts = block_starts(shape, 2)
    red_wide = (parity_of(wide_shape, wide_starts) == 0) & inside_grid(
        wide_shape, wide_starts, whole
    )
    wide_source = wide(source)
    field = wide_sweep(
        jnp.zeros(wide_shape, jnp.float32), wide_source, scale, red_wide, source, black
    )
    field = wide_sweep(wide(field), wide_source, scale, red_wide, source, black)
    residue = source - scale * (centre * field - stencil_sum(faces(field)))
    field = field + prolong(shared_cycle(restrict(residue), level + 1, top))
    for _ in range(2):
        field = wide_sweep(wide(field), wide_source, scale, red_wide, source, black)
    return field


def pairs(count, first):
    swaps = []
    for i in range(first, count - 1, 2):
        swaps += [(i, i + 1), (i + 1, i)]
    return swaps


def inner_pairs(count_x, count):
    swaps = []
    for x in range(count_x):
        swaps += [(x * count + i, x * count + j) for i, j in pairs(count, 1)]
        swaps += [(x * count + i, (x ^ 1) * count + i) for i in (0, count - 1)]
    return swaps


def flips(count, bit):
    return [(i, i ^ bit) for i in range(count)]


def lanes_of(shape):
    return lax.broadcasted_iota(jnp.int32, shape, len(shape) - 1)


def rows_of(shape):
    return lax.broadcasted_iota(jnp.int32, shape, len(shape) - 2)


LANES = 128
PAD = 8


def odd_of(shape):
    return ((lanes_of(shape) + rows_of(shape)) & 1) == 1


def exact_dot(a, b):
    return jnp.dot(a, b, precision=lax.Precision.HIGHEST, preferred_element_type=jnp.float32)


def pick_dot(a, b):
    b = b.astype(jnp.bfloat16)
    total = None
    for _ in range(3):
        high = a.astype(jnp.bfloat16)
        term = jnp.dot(high, b, preferred_element_type=jnp.float32)
        total = term if total is None else total + term
        a = a - high.astype(jnp.float32)
    return total


def window(ref, at, column, count, start=0, shift=0):
    if isinstance(start, int):
        return ref[at, column, PAD + start + shift : PAD + start + shift + count, :]
    first = start + (PAD + shift)
    if shift == 0:
        first = pl.multiple_of(first, 8)
    return ref[at, column, pl.ds(first, count), :]


def clear_pads(ref):
    edge = jnp.zeros((PAD, LANES), jnp.float32)
    for at in range(ref.shape[0]):
        for column in range(ref.shape[1]):
            ref[at, column, :PAD, :] = edge
            ref[at, column, ref.shape[2] - PAD :, :] = edge


def block_sums(ref, at, rows):
    lane = lanes_of((rows, LANES))
    values = [window(ref, at, column, rows) for column in range(2)]
    lefts = [pltpu.roll(value, 1, 1) for value in values]
    rights = [pltpu.roll(value, LANES - 1, 1) for value in values]
    sums = []
    for column in range(2):
        left = jnp.where(lane == 0, lefts[1 - column], lefts[column])
        right = jnp.where(lane == LANES - 1, rights[1 - column], rights[column])
        sides = window(ref, at, column, rows, shift=-1) + window(ref, at, column, rows, shift=1)
        sums.append(values[column] + sides + (1.0 + rsd_beta) * (left + right))
    return sums


def block_totals(ref, at, rows, own, odd, to_red, at_low, at_high):
    slots = ref.shape[0]
    totals = []
    for column, total in enumerate(block_sums(ref, at, rows)):
        before = window(ref, (at - 1) % slots, column, rows)
        after = window(ref, (at + 1) % slots, column, rows)
        if at in (0, own):
            before = jnp.where(at_low if at == 0 else at_high, 0.0, before)
        if at in (own - 1, slots - 1):
            after = jnp.where(at_low if at == slots - 1 else at_high, 0.0, after)
        totals.append(total + (jnp.where(odd, after, before) if to_red else jnp.where(odd, before, after)))
    return totals


def block_mask(own, halo):
    ny, nz = own
    shape = (ny + 2 * halo, LANES)
    row = rows_of(shape) - halo + lax.axis_index("gy") * ny
    inside_y = (row >= 0) & (row < ny * lax.axis_size("gy"))
    masks = []
    for column in range(2):
        lane = lanes_of(shape)
        if column:
            lane = jnp.where(lane < halo, lane + LANES, lane - LANES)
        lane = lane + lax.axis_index("gz") * nz
        inside = inside_y & (lane >= 0) & (lane < nz * lax.axis_size("gz"))
        masks.append(jnp.where(inside, 1.0 / centre, 0.0))
    return masks


def block_plane(at, own_ref, ya_ref, yb_ref, even_y):
    a, b = ya_ref[at], yb_ref[at]
    low = jnp.where(even_y, b, a)
    high = jnp.where(even_y, a, b)
    return jnp.concatenate([low, own_ref[at], high], axis=0)


def block_columns(halo, at, own_ref, ya_ref, yb_ref, za_ref, zb_ref, even_y, even_z):
    _, _, nz = own_ref.shape
    j, k = at // (nz // halo), at % (nz // halo)
    a, b = za_ref[j], zb_ref[j]
    left = pltpu.roll(jnp.where(even_z, b, a), (2 * nz - halo - halo * k) % nz, 1)
    right = pltpu.roll(jnp.where(even_z, a, b), (nz - halo * k) % nz, 1)
    lane = lanes_of(left.shape)
    sides = jnp.where(lane < halo, right, jnp.where(lane >= nz - halo, left, 0.0))
    return block_plane(at, own_ref, ya_ref, yb_ref, even_y), sides


def pack_kernel(halo, own_ref, ya_ref, yb_ref, za_ref, zb_ref):
    even_y = lax.axis_index("gy") % 2 == 0
    even_z = lax.axis_index("gz") % 2 == 0
    nx, ny, nz = own_ref.shape
    groups = nz // halo
    shape = (ny + 2 * halo, nz)
    group = lanes_of(shape) // halo
    for j in range(za_ref.shape[0]):
        last = jnp.zeros(shape, jnp.float32)
        first = jnp.zeros(shape, jnp.float32)
        for k in range(min(groups, nx - j * groups)):
            plane = block_plane(j * groups + k, own_ref, ya_ref, yb_ref, even_y)
            last = jnp.where(group == k, pltpu.roll(plane, (halo * k + halo) % nz, 1), last)
            first = jnp.where(group == k, pltpu.roll(plane, halo * k, 1), first)
        za_ref[j] = jnp.where(even_z, last, first)
        zb_ref[j] = jnp.where(even_z, first, last)


def smooth(count, own, masks, odd, ends, gr_ref, gb_ref, red_ref, black_ref, done):
    rows = odd.shape[0]
    body = slice(PAD, PAD + rows)

    def value_of(source, at, c, total):
        value = masks[c] * total
        return source[at, c] + value if at < source.shape[0] else value

    for at in range(count):
        for c in range(2):
            red_ref[at, c, body, :] = gr_ref[at, c] if at < gr_ref.shape[0] else jnp.zeros_like(masks[c])
    for step in range(3):
        source, target, other = (gr_ref, red_ref, black_ref) if step == 1 else (gb_ref, black_ref, red_ref)
        for at in range(count):
            totals = block_totals(other, at, rows, own, odd, step == 1, *ends)
            for c in range(2):
                value = value_of(source, at, c, totals[c])
                target[at, c, body, :] = value
                if step == 2:
                    done(at, c, totals[c], value)


def x_ends():
    here = lax.axis_index("gx")
    return here == 0, here == lax.axis_size("gx") - 1


def pre_kernel(
    halo, own_ref, ya_ref, yb_ref, za_ref, zb_ref,
    send_ref, face_ref,
    fr_ref, fb_ref, gr_ref, gb_ref, red_ref, black_ref, rest_ref,
):
    even_y = lax.axis_index("gy") % 2 == 0
    even_z = lax.axis_index("gz") % 2 == 0
    nx, ny, nz = own_ref.shape
    count, _, rows, _ = red_ref.shape
    rows = rows - 2 * PAD
    own = nx // 2
    shape = (rows, LANES)
    odd = odd_of(shape)
    masks = block_mask((ny, nz), halo)
    inner = slice(halo, halo + ny)
    ends = x_ends()
    clear_pads(red_ref)
    clear_pads(black_ref)
    for p in range(halo):
        high = block_plane(nx - halo + p, own_ref, ya_ref, yb_ref, even_y)
        face_ref[p] = jnp.where(ends[0], high, block_plane(p, own_ref, ya_ref, yb_ref, even_y))
    middle = halo * halo
    top = za_ref.shape[0] - 1
    left = [jnp.where(even_z, zb_ref[j], za_ref[j]) for j in (0, top)]
    right = [jnp.where(even_z, za_ref[j], zb_ref[j]) for j in (0, top)]
    left = jnp.where(ends[0], pltpu.roll(left[1], middle, 1), left[0])
    right = jnp.where(ends[0], right[1], pltpu.roll(right[0], middle, 1))
    face_ref[halo] = jnp.where(lanes_of(shape) < middle, left, right)
    for at in range(own):
        planes = [
            block_columns(halo, x, own_ref, ya_ref, yb_ref, za_ref, zb_ref, even_y, even_z)
            for x in (2 * at, 2 * at + 1)
        ]
        for c in range(2):
            red = jnp.where(odd, planes[1][c], planes[0][c])
            black = jnp.where(odd, planes[0][c], planes[1][c])
            if c == 0:
                fr_ref[at], fb_ref[at] = red[inner], black[inner]
            gr_ref[at, c], gb_ref[at, c] = masks[c] * red, masks[c] * black

    def keep(at, c, total, value):
        if c == 0:
            left_over = total[inner] - centre * value[inner]
            rest_ref[at] = left_over + fb_ref[at] if at < own else left_over

    smooth(count, own, masks, odd, ends, gr_ref, gb_ref, red_ref, black_ref, keep)
    for at in range(count):
        total = block_totals(black_ref, at, rows, own, odd, True, *ends)[0]
        left_over = total[inner] - centre * red_ref[at, 0, PAD + halo : PAD + halo + ny, :]
        if at < own:
            left_over = left_over + fr_ref[at]
        rest_ref[at] = rest_ref[at] + left_over
    half, quarter = ny // 2, nz // 4
    pairs_y = rest_ref[:, pl.ds(0, half, stride=2), :] + rest_ref[:, pl.ds(1, half, stride=2), :]
    turn = quarter * lax.axis_index("gz")
    column = (lanes_of((nz, nz)) - turn) & (nz - 1)
    target = 2 * (column % quarter) + (column // quarter) % 2
    weight = jnp.where(rows_of((nz, nz)) // 2 == target, 0.5, 0.0)
    coarse = pick_dot(pairs_y.reshape(count * half, nz), weight).reshape(count, half, nz)
    part = ((lanes_of((half, nz)) - turn) & (nz - 1)) // quarter
    pick = (((rows_of((half, nz)) + part) & 1) == 1) ^ (part >= 2)
    for at in range(count // 2):
        send_ref[at] = jnp.where(pick, coarse[2 * at + 1], coarse[2 * at])


def field_kernel(
    halo, own_ref, ya_ref, yb_ref, za_ref, zb_ref, face_ref, after_ref,
    gr_ref, gb_ref, dark_ref,
    red_ref, black_ref,
):
    even_y = lax.axis_index("gy") % 2 == 0
    even_z = lax.axis_index("gz") % 2 == 0
    nx, ny, nz = own_ref.shape
    count, _, rows, _ = gr_ref.shape
    own = nx // 2
    shape = (rows, LANES)
    odd, lane = odd_of(shape), lanes_of(shape)
    masks = block_mask((ny, nz), halo)
    clear_pads(red_ref)
    clear_pads(black_ref)

    def columns(x):
        if x < nx:
            return block_columns(halo, x, own_ref, ya_ref, yb_ref, za_ref, zb_ref, even_y, even_z)
        p = x - nx
        left = pltpu.roll(face_ref[halo], (2 * LANES - halo - halo * p) % LANES, 1)
        right = pltpu.roll(face_ref[halo], (2 * LANES - halo * halo - halo * p) % LANES, 1)
        return face_ref[p], jnp.where(lane < halo, right, jnp.where(lane >= nz - halo, left, 0.0))

    for at in range(count):
        first, second = columns(2 * at), columns(2 * at + 1)
        for c in range(2):
            gr_ref[at, c] = masks[c] * jnp.where(odd, second[c], first[c])
            gb_ref[at, c] = masks[c] * jnp.where(odd, first[c], second[c])

    def keep(at, c, total, value):
        dark_ref[at, c] = value

    smooth(count, own, masks, odd, x_ends(), gr_ref, gb_ref, red_ref, black_ref, keep)


def stack_kernel(*refs):
    for which, ref in enumerate(refs[:-1]):
        refs[-1][which] = ref[...]


def small_shapes(whole):
    return [whole[0] >> (level + 1) for level in range(2, LEVELS - 2)]


def plain_sum(field):
    padded = np.pad(field, ((0, 0), (1, 1), (1, 1), (1, 1)))
    inner = slice(1, -1)
    plane = padded[:, 2:, inner, inner] + padded[:, :-2, inner, inner]
    plane = plane + padded[:, inner, 2:, inner] + padded[:, inner, :-2, inner]
    return plane + (1.0 + rsd_beta) * (padded[:, inner, inner, 2:] + padded[:, inner, inner, :-2])


def plain_cycle(source, level):
    parity = np.indices(source.shape[1:]).sum(axis=0) % 2
    field = np.zeros_like(source)

    def sweeps(field, number):
        for step in range(2 * number):
            field = np.where(parity == step % 2, (source + plain_sum(field)) / centre, field)
        return field

    if level == LEVELS - 1:
        return sweeps(field, CSWEEPS)
    field = sweeps(field, 2)
    rest = source - centre * field + plain_sum(field)
    nx, ny, nz = source.shape[1:]
    rest = rest.reshape(-1, nx // 2, 2, ny // 2, 2, nz // 2, 2).sum(axis=(2, 4, 6)) / 2.0
    coarse = plain_cycle(rest, level + 1)
    for axis in (1, 2, 3):
        coarse = np.repeat(coarse, 2, axis)
    return sweeps(field + coarse, 2)


def cycle_matrix(whole):
    level = LEVELS - 2
    nx, ny, nz = (size >> level for size in whole)
    size = nx * ny * 2 * nz
    unit = np.eye(size).reshape(size, 2 * nz, nx, ny).transpose(0, 2, 3, 1)
    source = unit.reshape(size, nx, ny, nz, 2).sum(axis=-1) / 2.0
    result = np.repeat(plain_cycle(source, level), 2, axis=3)
    return jnp.asarray(result.transpose(0, 3, 1, 2).reshape(size, size), jnp.float32)


def solve_kernel(halo, *refs):
    gathered, refs = refs[:8], refs[8:]
    gr_ref, gb_ref, dark_ref, matrix_ref, out_ref = refs[:5]
    fr1, fb1, red1, black1, rest1, tall_ref, red_ref, work_ref, passing = refs[5:14]
    small = [refs[14 + 6 * i : 20 + 6 * i] for i in range(LEVELS - 4)]
    gx, gy, gz = (lax.axis_index(axis) for axis in ("gx", "gy", "gz"))
    weight_z = 1.0 + rsd_beta
    share = 1.0 / centre
    for ref in (red1, black1, red_ref, work_ref, passing):
        clear_pads(ref)
    for level in small:
        for ref in level[2:4]:
            clear_pads(ref)

    _, slots, block_rows, _ = gathered[0].shape
    slots = slots - 1
    count1, _, rows1, _ = fr1.shape
    quarter = LANES // 4
    group = lanes_of((block_rows, LANES)) // quarter
    held = [jnp.bitwise_and(group - jnp.bitwise_xor(gz, bits), 3) for bits in range(4)]
    theirs = [[kind == part for kind in held] for part in range(4)]

    def unpack(far, second, at):
        y = jnp.bitwise_xor(gy, 2 * far + (second >> 1))
        rows = pl.ds(pl.multiple_of(y * block_rows, 8), block_rows)
        blocks = [gathered[4 * (bits & 1) + second][far + (bits & 2), at] for bits in range(4)]
        parts = []
        for part in range(4):
            value = blocks[0]
            for block, mine in zip(blocks[1:], theirs[part][1:]):
                value = jnp.where(mine, block, value)
            parts.append(pltpu.roll(value, LANES - quarter * part, 1) if part else value)
        return rows, parts

    half1 = count1 // 2
    for far in range(2):
        for second in range(4):
            x = jnp.bitwise_xor(gx, second & 1)
            for at in range(slots):
                rows, parts = unpack(far, second, at)
                for part, target in enumerate((fr1, fr1, fb1, fb1)):
                    target[x * slots + at, part % 2, rows, :] = parts[part]
    for far in range(2):
        for second in range(4):
            x = jnp.bitwise_xor(gx, second & 1)
            next_slot = jnp.where(x == 0, half1, half1 - 1)
            rows, parts = unpack(far, second, slots)
            for part, target in enumerate((fr1, fr1, fb1, fb1)):
                target[next_slot, part % 2, rows, :] = target[next_slot, part % 2, rows, :] + parts[part]

    def fold_total(ref, at, e, start, count, low, high, odds, to_red):
        lane = lanes_of((count, LANES))
        value, other = window(ref, at, e, count, start), window(ref, at, 1 - e, count, start)
        sides = window(ref, at, e, count, start, -1) + window(ref, at, e, count, start, 1)
        if e == 0:
            near = jnp.where(lane == 0, 0.0, pltpu.roll(other, 1, 1))
        else:
            near = jnp.where(lane == LANES - 1, 0.0, pltpu.roll(other, LANES - 1, 1))
        before = 0.0 if low is True else window(ref, at - 1, e, count, start)
        after = 0.0 if high is True else window(ref, at + 1, e, count, start)
        if not isinstance(low, bool):
            before = jnp.where(low, 0.0, window(ref, jnp.maximum(at - 1, 0), e, count, start))
        if not isinstance(high, bool):
            after = jnp.where(high, 0.0, window(ref, jnp.minimum(at + 1, count1 - 1), e, count, start))
        beside = jnp.where(odds[e], after, before) if to_red else jnp.where(odds[e], before, after)
        return value + sides + beside + weight_z * (other + near)

    def fold_odds(count):
        row = rows_of((count, LANES))
        return [((row + e) & 1) == 1 for e in range(2)]

    odds = fold_odds(rows1)
    body1 = slice(PAD, PAD + rows1)

    def down_total(ref, at, e, to_red):
        return fold_total(ref, at, e, 0, rows1, at == 0, at == count1 - 1, odds, to_red)

    for at in range(count1):
        for e in range(2):
            red1[at, e, body1, :] = share * fr1[at, e]
    for at in range(count1):
        for e in range(2):
            black1[at, e, body1, :] = share * (fb1[at, e] + down_total(red1, at, e, False))
    for at in range(count1):
        for e in range(2):
            red1[at, e, body1, :] = share * (fr1[at, e] + down_total(black1, at, e, True))
    for at in range(count1):
        left_over = None
        for e in range(2):
            total = fb1[at, e] + down_total(red1, at, e, False)
            value = share * total
            black1[at, e, body1, :] = value
            term = total - centre * value
            left_over = term if left_over is None else left_over + term
        rest1[at] = left_over
    for at in range(count1):
        left_over = rest1[at]
        for e in range(2):
            total = fr1[at, e] + down_total(black1, at, e, True)
            left_over = left_over + (total - centre * window(red1, at, e, rows1))
        rest1[at] = left_over
    rows2 = rows1 // 2
    shape2 = (rows2, LANES)
    row2, lane2 = rows_of(shape2), lanes_of(shape2)
    odd2 = odd_of(shape2)
    planes = [
        0.5 * (rest1[at, pl.ds(0, rows2, stride=2), :] + rest1[at, pl.ds(1, rows2, stride=2), :])
        for at in range(count1)
    ]

    body2 = slice(PAD, PAD + rows2)

    def grid_of(index):
        step = 1 << index
        return ((row2 & (step - 1)) == 0) & ((lane2 & (step - 1)) == 0)

    def odd_at(index):
        return (((row2 >> index) + (lane2 >> index)) & 1) == 1

    def turned(value, step):
        inside = lane2 >= step if step > 0 else lane2 < LANES + step
        return jnp.where(inside, pltpu.roll(value, step % LANES, 1), 0.0)

    def small_plane(index, ref, at, odd, to_red):
        step = 1 << index
        total = ref[at, 0, body2, :] + (
            ref[at, 0, PAD - step : PAD - step + rows2, :] + ref[at, 0, PAD + step : PAD + step + rows2, :]
        )
        slots = ref.shape[0]
        if slots == 1:
            return total
        before = ref[at - 1, 0, body2, :] if at > 0 else 0.0
        after = ref[at + 1, 0, body2, :] if at < slots - 1 else 0.0
        return total + (jnp.where(odd, after, before) if to_red else jnp.where(odd, before, after))

    def small_sweeps(index, start):
        fr, fb, red, black, fr_low, fr_high = small[index]
        odd, width = odd_at(index), 1 << index
        mask = jnp.where(grid_of(index), share, 0.0)
        mask_low = jnp.where(lane2 < width, 0.0, mask)
        mask_high = jnp.where(lane2 >= LANES - width, 0.0, mask)
        slots = fr.shape[0]
        if start:
            for at in range(slots):
                fr_low[at] = pltpu.roll(fr[at], width, 1)
                fr_high[at] = pltpu.roll(fr[at], LANES - width, 1)
        for step in range(2):
            sides = []
            for at in range(slots):
                here, low, high = fr[at], fr_low[at], fr_high[at]
                if not (start and step == 0):
                    value = black[at, 0, body2, :]
                    plane = small_plane(index, black, at, odd, True)
                    here = here + plane + weight_z * (turned(value, width) + turned(value, -width))
                    low = low + pltpu.roll(plane, width, 1) + weight_z * (turned(value, 2 * width) + value)
                    high = high + pltpu.roll(plane, LANES - width, 1)
                    high = high + weight_z * (value + turned(value, -2 * width))
                red[at, 0, body2, :] = mask * here
                sides.append(weight_z * (mask_low * low + mask_high * high))
            totals = []
            for at in range(slots):
                total = fb[at] + small_plane(index, red, at, odd, False) + sides[at]
                black[at, 0, body2, :] = mask * total
                totals.append(total)
        return totals

    def spread_rows(value, step, ref, at):
        ref[at, 0, body2, :] = value
        return value + ref[at, 0, PAD - step : PAD - step + rows2, :]

    last = len(small) - 1
    for index in range(len(small)):
        fr, fb, red, black, _, fr_high = small[index]
        slots, odd, step = fr.shape[0], odd_at(index), 1 << index
        for at in range(slots):
            p, q = planes[2 * at], planes[2 * at + 1]
            fr[at], fb[at] = jnp.where(odd, q, p), jnp.where(odd, p, q)
        black_totals = small_sweeps(index, True)
        totals = []
        for at in range(slots):
            value, field = black[at, 0, body2, :], red[at, 0, body2, :]
            plane = small_plane(index, black, at, odd, True)
            total = black_totals[at] - centre * value
            next_total = pltpu.roll(total, LANES - step, 1)
            total = total + (
                fr[at] + plane + weight_z * (turned(value, step) + turned(value, -step)) - centre * field
            )
            if index < last:
                next_total = next_total + (
                    fr_high[at] + pltpu.roll(plane, LANES - step, 1)
                    + weight_z * (value + turned(value, -2 * step))
                    - centre * pltpu.roll(field, LANES - step, 1)
                )
                total = total + next_total
            totals.append(total)
            passing[at, 0, body2, :] = total
        lower = [passing[at, 0, PAD + step : PAD + step + rows2, :] for at in range(slots)]
        planes = [0.5 * (total + below) for total, below in zip(totals, lower)]

    half_rows = rows2 // 2
    upper = [passing[at, 0, PAD - step : PAD - step + rows2, :] for at in range(slots)]
    odd_line = (row2 & step) != 0
    summed = [
        total + jnp.where(odd_line, above, below) for total, above, below in zip(totals, upper, lower)
    ]
    lines = [total[start : start + half_rows] for total in summed for start in (0, half_rows)]
    place = lanes_of((half_rows, LANES)) & (len(lines) - 1)
    joined = lines[0]
    for q in range(1, len(lines)):
        joined = jnp.where(place == q, pltpu.roll(lines[q], q, 1), joined)
    answer = exact_dot(joined, matrix_ref[...])
    grid = (place == 0) & ((rows_of((half_rows, LANES)) & (step - 1)) == 0)
    parts = []
    for q in range(len(lines)):
        part = pltpu.roll(answer, LANES - q, 1) if q else answer
        parts.append(jnp.where(grid, part, 0.0))
    spreads = [jnp.concatenate(parts[2 * at : 2 * at + 2], axis=0) for at in range(slots)]

    for index in reversed(range(len(small))):
        _, _, red, black, _, _ = small[index]
        slots, odd, step = red.shape[0], odd_at(index), 1 << index
        if index < last:
            spreads = [
                spread_rows(field + pltpu.roll(field, step, 1), step, passing, at)
                for at, field in enumerate(fields)
            ]
        for at in range(slots):
            black[at, 0, body2, :] = black[at, 0, body2, :] + spreads[at]
        small_sweeps(index, False)
        fields = []
        for at in range(slots):
            r, b = red[at, 0, body2, :], black[at, 0, body2, :]
            fields += [jnp.where(odd, b, r), jnp.where(odd, r, b)]

    for at in range(count1):
        for start in range(2):
            rest1[at, pl.ds(start, rows2, stride=2), :] = fields[at]
    for at in range(count1):
        for e in range(2):
            black1[at, e, body1, :] = window(black1, at, e, rows1) + rest1[at]
    nx, ny, nz = out_ref.shape
    own = nx // 2
    part_slots = min(own // 2 + 3, count1)
    part_rows = min(ny // 2 + 16, rows1)
    slot0 = jnp.where(gx == 0, 0, count1 - part_slots)
    row0 = pl.multiple_of(jnp.clip(gy * (ny // 2) - 8, 0, rows1 - part_rows), 8)
    odds = fold_odds(part_rows)

    def up_total(ref, at, e, to_red):
        low = gx == 0 if at == 0 else False
        high = gx != 0 if at == part_slots - 1 else False
        return fold_total(ref, slot0 + at, e, row0, part_rows, low, high, odds, to_red)

    def up_half(target, other, sources, to_red):
        for at in range(part_slots):
            for e in range(2):
                source = sources[slot0 + at, e, pl.ds(row0, part_rows), :]
                value = share * (source + up_total(other, at, e, to_red))
                target[slot0 + at, e, pl.ds(pl.multiple_of(row0 + PAD, 8), part_rows), :] = value

    for _ in range(2):
        up_half(red1, black1, fr1, True)
        up_half(black1, red1, fb1, False)

    count, _, rows, _ = dark_ref.shape
    half = rows // 2
    odds = fold_odds(half)
    row = gy * (ny // 2) + (PAD - halo // 2)
    for at in range(count):
        if at < own:
            slot = gx * (own // 2) + at // 2
        else:
            slot = jnp.where(gx == 0, own // 2, own // 2 - (count - own) // 2) + (at - own) // 2
        for e in range(2):
            r, b = red1[slot, e, pl.ds(row, half), :], black1[slot, e, pl.ds(row, half), :]
            plane = jnp.where(odds[e], r, b) if at % 2 else jnp.where(odds[e], b, r)
            tall_ref[at, :, e * LANES : (e + 1) * LANES] = plane
    shape = (2 * LANES, 2 * LANES)
    z = lanes_of(shape)
    z = jnp.where(z < 2 * LANES - halo, z, z - 2 * LANES) + gz * nz
    line = rows_of(shape)
    line = jnp.where(line < LANES, 2 * line, 2 * (line - LANES) + 1)
    weight = jnp.where(line == lax.shift_right_arithmetic(z, 1), 1.0, 0.0)
    spread = pick_dot(tall_ref[...].reshape(count * half, 2 * LANES), weight)
    spread = spread.reshape(count, half, 2 * LANES)
    for at in range(count):
        for c in range(2):
            value = spread[at, :, c * LANES : (c + 1) * LANES]
            for start in range(2):
                work_ref[at, c, pl.ds(PAD + start, half, stride=2), :] = value
    body = slice(PAD, PAD + rows)
    for at in range(count):
        for c in range(2):
            work_ref[at, c, body, :] = work_ref[at, c, body, :] + dark_ref[at, c]
    odd = odd_of((rows, LANES))
    masks = block_mask((ny, nz), halo)
    ends = (gx == 0, gx == lax.axis_size("gx") - 1)
    beside_own = [*range(own), own, count - 1]
    for sweep in range(2):
        for at in range(count) if sweep == 0 else beside_own:
            totals = block_totals(work_ref, at, rows, own, odd, True, *ends)
            for c in range(2):
                red_ref[at, c, body, :] = gr_ref[at, c] + masks[c] * totals[c]
        for at in beside_own if sweep == 0 else range(own):
            totals = block_totals(red_ref, at, rows, own, odd, False, *ends)
            for c in range(2 if sweep == 0 else 1):
                work_ref[at, c, body, :] = gb_ref[at, c] + masks[c] * totals[c]
    inner = slice(PAD + halo, PAD + halo + ny)
    odd = odd_of((ny, nz))
    for at in range(own):
        r, b = red_ref[at, 0, inner, :], work_ref[at, 0, inner, :]
        out_ref[2 * at] = jnp.where(odd, b, r)
        out_ref[2 * at + 1] = jnp.where(odd, r, b)


def vmem(number):
    return [pl.BlockSpec(memory_space=pltpu.VMEM)] * number


def struct(*shape):
    return jax.ShapeDtypeStruct(shape, jnp.float32)


def scratch(*shape):
    return pltpu.VMEM(shape, jnp.float32)


HALO = 8


def block_cycle(density):
    halo = HALO
    nx, ny, nz = density.shape
    count_x, count_y, count_z = (lax.axis_size(axis) for axis in ("gx", "gy", "gz"))
    whole = (nx * count_x, ny * count_y, nz * count_z)

    def params(mib):
        return pltpu.CompilerParams(vmem_limit_bytes=mib * 1024 * 1024)

    even = lax.axis_index("gy") % 2 == 0
    ya = lax.dynamic_slice_in_dim(density, jnp.where(even, ny - halo, 0), halo, 1)
    yb = lax.dynamic_slice_in_dim(density, jnp.where(even, 0, ny - halo), halo, 1)
    ya = lax.ppermute(ya, "gy", pairs(count_y, 0))
    yb = lax.ppermute(yb, ("gx", "gy"), inner_pairs(count_x, count_y))
    rows = ny + 2 * halo
    packs = -(-nx * halo // nz)
    za, zb = pl.pallas_call(
        functools.partial(pack_kernel, halo),
        out_shape=[struct(packs, rows, nz)] * 2,
        in_specs=vmem(3), out_specs=vmem(2), compiler_params=params(4),
    )(density, ya, yb)
    za = lax.ppermute(za, "gz", pairs(count_z, 0))
    zb = lax.ppermute(zb, "gz", pairs(count_z, 1) + [(0, count_z - 1), (count_z - 1, 0)])
    own, near = nx // 2, nx // 2 + 2
    send, face = pl.pallas_call(
        functools.partial(pre_kernel, halo),
        out_shape=[struct(near // 2, ny // 2, nz), struct(halo + 1, rows, LANES)],
        in_specs=vmem(5), out_specs=vmem(2), compiler_params=params(10),
        scratch_shapes=[scratch(own, ny, nz)] * 2
        + [scratch(own, 2, rows, LANES)] * 2
        + [scratch(near, 2, rows + 2 * PAD, LANES)] * 2
        + [scratch(near, ny, nz)],
    )(density, ya, yb, za, zb)
    planes = nx + halo
    slots = (planes // 2, 2, rows, LANES)
    padded = (planes // 2, 2, rows + 2 * PAD, LANES)
    first = [send]
    first.append(lax.ppermute(send, "gy", flips(count_y, 2)))
    first.append(lax.ppermute(send, "gz", flips(count_z, 2)))
    swaps = flips(count_y * count_z, 2 * count_z + 2)
    first.append(lax.ppermute(send, ("gy", "gz"), swaps))
    face = lax.ppermute(face, "gx", flips(count_x, 1))
    block = pl.pallas_call(
        stack_kernel, out_shape=struct(4, *send.shape),
        in_specs=vmem(4), out_specs=pl.BlockSpec(memory_space=pltpu.VMEM), compiler_params=params(2),
    )(*first)
    second = [
        block,
        lax.ppermute(block, "gx", flips(count_x, 1)),
        lax.ppermute(block, "gy", flips(count_y, 1)),
        lax.ppermute(block, ("gx", "gy"), flips(count_x * count_y, count_y + 1)),
    ]
    gr, gb, black = pl.pallas_call(
        functools.partial(field_kernel, halo),
        out_shape=[struct(*slots)] * 3,
        in_specs=vmem(7), out_specs=vmem(3), compiler_params=params(8),
        scratch_shapes=[scratch(*padded)] * 2,
        cost_estimate=pl.CostEstimate(flops=20_000_000, bytes_accessed=2_000_000, transcendentals=0),
    )(density, ya, yb, za, zb, face, block)
    second[3], gr, gb, black = lax.optimization_barrier((second[3], gr, gb, black))
    third = [lax.ppermute(blocks, "gz", flips(count_z, 1)) for blocks in second]
    count1, rows1, rows2 = whole[0] // 4, whole[1] // 2, whole[1] // 4
    room = [scratch(count1, 2, rows1, LANES)] * 2
    room += [scratch(count1, 2, rows1 + 2 * PAD, LANES)] * 2
    room += [scratch(count1, rows1, LANES), scratch(planes // 2, rows // 2, 2 * LANES)]
    room += [scratch(*padded)] * 2 + [scratch(count1 // 2, 1, rows2 + 2 * PAD, LANES)]
    for count in small_shapes(whole):
        room += [scratch(count, rows2, LANES)] * 2
        room += [scratch(count, 1, rows2 + 2 * PAD, LANES)] * 2
        room += [scratch(count, rows2, LANES)] * 2
    return pl.pallas_call(
        functools.partial(solve_kernel, halo),
        out_shape=struct(nx, ny, nz),
        in_specs=vmem(12), out_specs=pl.BlockSpec(memory_space=pltpu.VMEM),
        compiler_params=params(16), scratch_shapes=room,
    )(*second, *third, gr, gb, black, cycle_matrix(whole))


def fits_block_cycle(shape):
    nx, ny, nz = shape
    count_x, count_y, count_z = (lax.axis_size(axis) for axis in ("gx", "gy", "gz"))
    whole = (nx * count_x, ny * count_y, nz * count_z)
    coarsest = [size >> (LEVELS - 1) for size in whole]
    exact = all(c << (LEVELS - 1) == size for c, size in zip(coarsest, whole))
    return (
        exact and coarsest[0] == coarsest[1] == 1 and nz == LANES and ny == 2 * HALO
        and count_x == 2 and count_y == 4 and count_z == 4
    )


def on_device(density):
    if fits_block_cycle(density.shape):
        return block_cycle(density)
    top = 4
    return shared_cycle(density, 0, top)


def solution(mesh):
    return jax.shard_map(
        on_device,
        mesh=mesh,
        in_specs=(P("gx", "gy", "gz"),),
        out_specs=P("gx", "gy", "gz"),
        check_vma=False,
    )
```

```python
import functools

import jax
import jax.numpy as jnp
import numpy as np
from jax import lax
from jax.experimental import pallas as pl
from jax.experimental.pallas import tpu as pltpu
from jax.sharding import PartitionSpec as P

LEVELS = 7
CSWEEPS = 4


rsd_beta = 0.5
centre = 4.0 + 2.0 * (1.0 + rsd_beta)


def extended_2(value, sides, width):
    for axis, dim in sides:
        count, length = (lax.axis_size(axis), value.shape[dim])
        up = [(i, (i + 1) % count) for i in range(count - 1)]
        down = [(j, i) for i, j in up]
        last = lax.slice_in_dim(value, length - width, length, axis=dim)
        leading = lax.slice_in_dim(value, 0, width, axis=dim)
        before = lax.ppermute(last, axis, up)
        after = lax.ppermute(leading, axis, down)
        value = jnp.concatenate([before, value, after], axis=dim)
    return value


def stencil_sum(padded):
    plane = (
        padded[2:, 1:-1, 1:-1]
        + padded[:-2, 1:-1, 1:-1]
        + padded[1:-1, 2:, 1:-1]
        + padded[1:-1, :-2, 1:-1]
    )
    sight = padded[1:-1, 1:-1, 2:] + padded[1:-1, 1:-1, :-2]
    return plane + (1.0 + rsd_beta) * sight


def grid_index(shape, starts):
    return [lax.broadcasted_iota(jnp.int32, shape, which) + starts[which] for which in range(3)]


def parity_of(shape, starts):
    position = grid_index(shape, starts)
    return (position[0] + position[1] + position[2] + 6) % 2


def inside_grid(shape, starts, whole):
    position = grid_index(shape, starts)
    keep = (position[0] >= 0) & (position[0] < whole[0])
    for which in (1, 2):
        keep = keep & (position[which] >= 0) & (position[which] < whole[which])
    return keep


def half_sweep(field, source, scale, chosen):
    update = (source / scale + stencil_sum(jnp.pad(field, 1))) / centre
    return jnp.where(chosen, update, field)


def full_sweep(field, source, scale, parity):
    field = half_sweep(field, source, scale, parity == 0)
    return half_sweep(field, source, scale, parity == 1)


def restrict(residue):
    shape = residue.shape
    blocks = residue.reshape(shape[0] // 2, 2, shape[1] // 2, 2, shape[2] // 2, 2)
    return jnp.mean(blocks, axis=(1, 3, 5))


def prolong(coarse):
    return jnp.repeat(jnp.repeat(jnp.repeat(coarse, 2, 0), 2, 1), 2, 2)


def local_cycle(source, level):
    scale = 0.25**level
    parity = parity_of(source.shape, (0, 0, 0))
    field = jnp.zeros_like(source)
    if level == LEVELS - 1:
        for _ in range(CSWEEPS):
            field = full_sweep(field, source, scale, parity)
        return field
    for _ in range(2):
        field = full_sweep(field, source, scale, parity)
    residue = source - scale * (centre * field - stencil_sum(jnp.pad(field, 1)))
    field = field + prolong(local_cycle(restrict(residue), level + 1))
    for _ in range(2):
        field = full_sweep(field, source, scale, parity)
    return field


def faces(field):
    return extended_2(field, (("gx", 0), ("gy", 1), ("gz", 2)), 1)


def wide(field):
    return extended_2(field, (("gx", 0), ("gy", 1), ("gz", 2)), 2)


def block_starts(shape, margin):
    return (
        lax.axis_index("gx") * shape[0] - margin,
        lax.axis_index("gy") * shape[1] - margin,
        lax.axis_index("gz") * shape[2] - margin,
    )


def padded_half(padded, source, scale, chosen):
    field = padded[1:-1, 1:-1, 1:-1]
    update = (source / scale + stencil_sum(padded)) / centre
    return jnp.where(chosen, update, field)


def wide_sweep(extended, wide_source, scale, red_wide, source, black):
    update = (wide_source / scale + stencil_sum(jnp.pad(extended, 1))) / centre
    extended = jnp.where(red_wide, update, extended)
    return padded_half(extended[1:-1, 1:-1, 1:-1], source, scale, black)


def coarse_level(source, level):
    shape = source.shape
    stack = lax.all_gather(source[None], ("gx", "gy", "gz"), axis=0, tiled=True)
    count_x, count_y, count_z = (lax.axis_size("gx"), lax.axis_size("gy"), lax.axis_size("gz"))
    whole = stack.reshape(count_x, count_y, count_z, shape[0], shape[1], shape[2])
    whole = whole.transpose(0, 3, 1, 4, 2, 5).reshape(
        count_x * shape[0], count_y * shape[1], count_z * shape[2]
    )
    solved = local_cycle(whole, level)
    starts = block_starts(shape, 0)
    return lax.dynamic_slice(solved, starts, shape)


def shared_cycle(source, level, top):
    if level == top:
        return coarse_level(source, level)
    scale = 0.25**level
    shape = source.shape
    whole = (
        shape[0] * lax.axis_size("gx"),
        shape[1] * lax.axis_size("gy"),
        shape[2] * lax.axis_size("gz"),
    )
    parity = parity_of(shape, block_starts(shape, 0))
    black = parity == 1
    wide_shape = (shape[0] + 4, shape[1] + 4, shape[2] + 4)
    wide_starts = block_starts(shape, 2)
    red_wide = (parity_of(wide_shape, wide_starts) == 0) & inside_grid(
        wide_shape, wide_starts, whole
    )
    wide_source = wide(source)
    field = wide_sweep(
        jnp.zeros(wide_shape, jnp.float32), wide_source, scale, red_wide, source, black
    )
    field = wide_sweep(wide(field), wide_source, scale, red_wide, source, black)
    residue = source - scale * (centre * field - stencil_sum(faces(field)))
    field = field + prolong(shared_cycle(restrict(residue), level + 1, top))
    for _ in range(2):
        field = wide_sweep(wide(field), wide_source, scale, red_wide, source, black)
    return field


def pairs(count, first):
    swaps = []
    for i in range(first, count - 1, 2):
        swaps += [(i, i + 1), (i + 1, i)]
    return swaps


def inner_pairs(count_x, count):
    swaps = []
    for x in range(count_x):
        swaps += [(x * count + i, x * count + j) for i, j in pairs(count, 1)]
        swaps += [(x * count + i, (x ^ 1) * count + i) for i in (0, count - 1)]
    return swaps


def flips(count, bit):
    return [(i, i ^ bit) for i in range(count)]


def lanes_of(shape):
    return lax.broadcasted_iota(jnp.int32, shape, len(shape) - 1)


def rows_of(shape):
    return lax.broadcasted_iota(jnp.int32, shape, len(shape) - 2)


LANES = 128
PAD = 8


def odd_of(shape):
    return ((lanes_of(shape) + rows_of(shape)) & 1) == 1


def exact_dot(a, b):
    return jnp.dot(a, b, precision=lax.Precision.HIGHEST, preferred_element_type=jnp.float32)


def pick_dot(a, b):
    b = b.astype(jnp.bfloat16)
    total = None
    for _ in range(3):
        high = a.astype(jnp.bfloat16)
        term = jnp.dot(high, b, preferred_element_type=jnp.float32)
        total = term if total is None else total + term
        a = a - high.astype(jnp.float32)
    return total


def window(ref, at, column, count, start=0, shift=0):
    if isinstance(start, int):
        return ref[at, column, PAD + start + shift : PAD + start + shift + count, :]
    first = start + (PAD + shift)
    if shift == 0:
        first = pl.multiple_of(first, 8)
    return ref[at, column, pl.ds(first, count), :]


def clear_pads(ref):
    edge = jnp.zeros((PAD, LANES), jnp.float32)
    for at in range(ref.shape[0]):
        for column in range(ref.shape[1]):
            ref[at, column, :PAD, :] = edge
            ref[at, column, ref.shape[2] - PAD :, :] = edge


def block_sums(ref, at, rows):
    lane = lanes_of((rows, LANES))
    values = [window(ref, at, column, rows) for column in range(2)]
    lefts = [pltpu.roll(value, 1, 1) for value in values]
    rights = [pltpu.roll(value, LANES - 1, 1) for value in values]
    sums = []
    for column in range(2):
        left = jnp.where(lane == 0, lefts[1 - column], lefts[column])
        right = jnp.where(lane == LANES - 1, rights[1 - column], rights[column])
        sides = window(ref, at, column, rows, shift=-1) + window(ref, at, column, rows, shift=1)
        sums.append(values[column] + sides + (1.0 + rsd_beta) * (left + right))
    return sums


def block_totals(ref, at, rows, own, odd, to_red, at_low, at_high):
    slots = ref.shape[0]
    totals = []
    for column, total in enumerate(block_sums(ref, at, rows)):
        before = window(ref, (at - 1) % slots, column, rows)
        after = window(ref, (at + 1) % slots, column, rows)
        if at in (0, own):
            before = jnp.where(at_low if at == 0 else at_high, 0.0, before)
        if at in (own - 1, slots - 1):
            after = jnp.where(at_low if at == slots - 1 else at_high, 0.0, after)
        totals.append(total + (jnp.where(odd, after, before) if to_red else jnp.where(odd, before, after)))
    return totals


def block_mask(own, halo):
    ny, nz = own
    shape = (ny + 2 * halo, LANES)
    row = rows_of(shape) - halo + lax.axis_index("gy") * ny
    inside_y = (row >= 0) & (row < ny * lax.axis_size("gy"))
    masks = []
    for column in range(2):
        lane = lanes_of(shape)
        if column:
            lane = jnp.where(lane < halo, lane + LANES, lane - LANES)
        lane = lane + lax.axis_index("gz") * nz
        inside = inside_y & (lane >= 0) & (lane < nz * lax.axis_size("gz"))
        masks.append(jnp.where(inside, 1.0 / centre, 0.0))
    return masks


def block_plane(at, own_ref, ya_ref, yb_ref, even_y):
    a, b = ya_ref[at], yb_ref[at]
    low = jnp.where(even_y, b, a)
    high = jnp.where(even_y, a, b)
    return jnp.concatenate([low, own_ref[at], high], axis=0)


def block_columns(halo, at, own_ref, ya_ref, yb_ref, za_ref, zb_ref, even_y, even_z):
    _, _, nz = own_ref.shape
    j, k = at // (nz // halo), at % (nz // halo)
    a, b = za_ref[j], zb_ref[j]
    left = pltpu.roll(jnp.where(even_z, b, a), (2 * nz - halo - halo * k) % nz, 1)
    right = pltpu.roll(jnp.where(even_z, a, b), (nz - halo * k) % nz, 1)
    lane = lanes_of(left.shape)
    sides = jnp.where(lane < halo, right, jnp.where(lane >= nz - halo, left, 0.0))
    return block_plane(at, own_ref, ya_ref, yb_ref, even_y), sides


def pack_kernel(halo, own_ref, ya_ref, yb_ref, za_ref, zb_ref):
    even_y = lax.axis_index("gy") % 2 == 0
    even_z = lax.axis_index("gz") % 2 == 0
    nx, ny, nz = own_ref.shape
    groups = nz // halo
    shape = (ny + 2 * halo, nz)
    group = lanes_of(shape) // halo
    for j in range(za_ref.shape[0]):
        last = jnp.zeros(shape, jnp.float32)
        first = jnp.zeros(shape, jnp.float32)
        for k in range(min(groups, nx - j * groups)):
            plane = block_plane(j * groups + k, own_ref, ya_ref, yb_ref, even_y)
            last = jnp.where(group == k, pltpu.roll(plane, (halo * k + halo) % nz, 1), last)
            first = jnp.where(group == k, pltpu.roll(plane, halo * k, 1), first)
        za_ref[j] = jnp.where(even_z, last, first)
        zb_ref[j] = jnp.where(even_z, first, last)


def smooth(count, own, masks, odd, ends, gr_ref, gb_ref, red_ref, black_ref, done):
    rows = odd.shape[0]
    body = slice(PAD, PAD + rows)

    def value_of(source, at, c, total):
        value = masks[c] * total
        return source[at, c] + value if at < source.shape[0] else value

    for at in range(count):
        for c in range(2):
            red_ref[at, c, body, :] = gr_ref[at, c] if at < gr_ref.shape[0] else jnp.zeros_like(masks[c])
    for step in range(3):
        source, target, other = (gr_ref, red_ref, black_ref) if step == 1 else (gb_ref, black_ref, red_ref)
        for at in range(count):
            totals = block_totals(other, at, rows, own, odd, step == 1, *ends)
            for c in range(2):
                value = value_of(source, at, c, totals[c])
                target[at, c, body, :] = value
                if step == 2:
                    done(at, c, totals[c], value)


def x_ends():
    here = lax.axis_index("gx")
    return here == 0, here == lax.axis_size("gx") - 1


def pre_kernel(
    halo, own_ref, ya_ref, yb_ref, za_ref, zb_ref,
    send_ref, face_ref,
    fr_ref, fb_ref, gr_ref, gb_ref, red_ref, black_ref, rest_ref,
):
    even_y = lax.axis_index("gy") % 2 == 0
    even_z = lax.axis_index("gz") % 2 == 0
    nx, ny, nz = own_ref.shape
    count, _, rows, _ = red_ref.shape
    rows = rows - 2 * PAD
    own = nx // 2
    shape = (rows, LANES)
    odd = odd_of(shape)
    masks = block_mask((ny, nz), halo)
    inner = slice(halo, halo + ny)
    ends = x_ends()
    clear_pads(red_ref)
    clear_pads(black_ref)
    for p in range(halo):
        high = block_plane(nx - halo + p, own_ref, ya_ref, yb_ref, even_y)
        face_ref[p] = jnp.where(ends[0], high, block_plane(p, own_ref, ya_ref, yb_ref, even_y))
    middle = halo * halo
    top = za_ref.shape[0] - 1
    left = [jnp.where(even_z, zb_ref[j], za_ref[j]) for j in (0, top)]
    right = [jnp.where(even_z, za_ref[j], zb_ref[j]) for j in (0, top)]
    left = jnp.where(ends[0], pltpu.roll(left[1], middle, 1), left[0])
    right = jnp.where(ends[0], right[1], pltpu.roll(right[0], middle, 1))
    face_ref[halo] = jnp.where(lanes_of(shape) < middle, left, right)
    for at in range(own):
        planes = [
            block_columns(halo, x, own_ref, ya_ref, yb_ref, za_ref, zb_ref, even_y, even_z)
            for x in (2 * at, 2 * at + 1)
        ]
        for c in range(2):
            red = jnp.where(odd, planes[1][c], planes[0][c])
            black = jnp.where(odd, planes[0][c], planes[1][c])
            if c == 0:
                fr_ref[at], fb_ref[at] = red[inner], black[inner]
            gr_ref[at, c], gb_ref[at, c] = masks[c] * red, masks[c] * black

    def keep(at, c, total, value):
        if c == 0:
            left_over = total[inner] - centre * value[inner]
            rest_ref[at] = left_over + fb_ref[at] if at < own else left_over

    smooth(count, own, masks, odd, ends, gr_ref, gb_ref, red_ref, black_ref, keep)
    for at in range(count):
        total = block_totals(black_ref, at, rows, own, odd, True, *ends)[0]
        left_over = total[inner] - centre * red_ref[at, 0, PAD + halo : PAD + halo + ny, :]
        if at < own:
            left_over = left_over + fr_ref[at]
        rest_ref[at] = rest_ref[at] + left_over
    half, quarter = ny // 2, nz // 4
    pairs_y = rest_ref[:, pl.ds(0, half, stride=2), :] + rest_ref[:, pl.ds(1, half, stride=2), :]
    turn = quarter * lax.axis_index("gz")
    column = (lanes_of((nz, nz)) - turn) & (nz - 1)
    target = 2 * (column % quarter) + (column // quarter) % 2
    weight = jnp.where(rows_of((nz, nz)) // 2 == target, 0.5, 0.0)
    coarse = pick_dot(pairs_y.reshape(count * half, nz), weight).reshape(count, half, nz)
    part = ((lanes_of((half, nz)) - turn) & (nz - 1)) // quarter
    pick = (((rows_of((half, nz)) + part) & 1) == 1) ^ (part >= 2)
    for at in range(count // 2):
        send_ref[at] = jnp.where(pick, coarse[2 * at + 1], coarse[2 * at])


def field_kernel(
    halo, own_ref, ya_ref, yb_ref, za_ref, zb_ref, face_ref, after_ref,
    gr_ref, gb_ref, dark_ref,
    red_ref, black_ref,
):
    even_y = lax.axis_index("gy") % 2 == 0
    even_z = lax.axis_index("gz") % 2 == 0
    nx, ny, nz = own_ref.shape
    count, _, rows, _ = gr_ref.shape
    own = nx // 2
    shape = (rows, LANES)
    odd, lane = odd_of(shape), lanes_of(shape)
    masks = block_mask((ny, nz), halo)
    clear_pads(red_ref)
    clear_pads(black_ref)

    def columns(x):
        if x < nx:
            return block_columns(halo, x, own_ref, ya_ref, yb_ref, za_ref, zb_ref, even_y, even_z)
        p = x - nx
        left = pltpu.roll(face_ref[halo], (2 * LANES - halo - halo * p) % LANES, 1)
        right = pltpu.roll(face_ref[halo], (2 * LANES - halo * halo - halo * p) % LANES, 1)
        return face_ref[p], jnp.where(lane < halo, right, jnp.where(lane >= nz - halo, left, 0.0))

    for at in range(count):
        first, second = columns(2 * at), columns(2 * at + 1)
        for c in range(2):
            gr_ref[at, c] = masks[c] * jnp.where(odd, second[c], first[c])
            gb_ref[at, c] = masks[c] * jnp.where(odd, first[c], second[c])

    def keep(at, c, total, value):
        dark_ref[at, c] = value

    smooth(count, own, masks, odd, x_ends(), gr_ref, gb_ref, red_ref, black_ref, keep)


def stack_kernel(*refs):
    for which, ref in enumerate(refs[:-1]):
        refs[-1][which] = ref[...]


def small_shapes(whole):
    return [whole[0] >> (level + 1) for level in range(2, LEVELS - 2)]


def plain_sum(field):
    padded = np.pad(field, ((0, 0), (1, 1), (1, 1), (1, 1)))
    inner = slice(1, -1)
    plane = padded[:, 2:, inner, inner] + padded[:, :-2, inner, inner]
    plane = plane + padded[:, inner, 2:, inner] + padded[:, inner, :-2, inner]
    return plane + (1.0 + rsd_beta) * (padded[:, inner, inner, 2:] + padded[:, inner, inner, :-2])


def plain_cycle(source, level):
    parity = np.indices(source.shape[1:]).sum(axis=0) % 2
    field = np.zeros_like(source)

    def sweeps(field, number):
        for step in range(2 * number):
            field = np.where(parity == step % 2, (source + plain_sum(field)) / centre, field)
        return field

    if level == LEVELS - 1:
        return sweeps(field, CSWEEPS)
    field = sweeps(field, 2)
    rest = source - centre * field + plain_sum(field)
    nx, ny, nz = source.shape[1:]
    rest = rest.reshape(-1, nx // 2, 2, ny // 2, 2, nz // 2, 2).sum(axis=(2, 4, 6)) / 2.0
    coarse = plain_cycle(rest, level + 1)
    for axis in (1, 2, 3):
        coarse = np.repeat(coarse, 2, axis)
    return sweeps(field + coarse, 2)


def cycle_matrix(whole):
    level = LEVELS - 2
    nx, ny, nz = (size >> level for size in whole)
    size = nx * ny * 2 * nz
    unit = np.eye(size).reshape(size, 2 * nz, nx, ny).transpose(0, 2, 3, 1)
    source = unit.reshape(size, nx, ny, nz, 2).sum(axis=-1) / 2.0
    result = np.repeat(plain_cycle(source, level), 2, axis=3)
    return jnp.asarray(result.transpose(0, 3, 1, 2).reshape(size, size), jnp.float32)


def solve_kernel(halo, *refs):
    gathered, refs = refs[:8], refs[8:]
    gr_ref, gb_ref, dark_ref, matrix_ref, out_ref = refs[:5]
    fr1, fb1, red1, black1, rest1, tall_ref, red_ref, work_ref, passing, result_ref, sems = refs[5:16]
    small = [refs[16 + 6 * i : 22 + 6 * i] for i in range(LEVELS - 4)]
    gx, gy, gz = (lax.axis_index(axis) for axis in ("gx", "gy", "gz"))
    weight_z = 1.0 + rsd_beta
    share = 1.0 / centre
    for ref in (red1, black1, red_ref, work_ref, passing):
        clear_pads(ref)
    for level in small:
        for ref in level[2:4]:
            clear_pads(ref)

    _, slots, block_rows, _ = gathered[0].shape
    slots = slots - 1
    count1, _, rows1, _ = fr1.shape
    quarter = LANES // 4
    group = lanes_of((block_rows, LANES)) // quarter
    held = [jnp.bitwise_and(group - jnp.bitwise_xor(gz, bits), 3) for bits in range(4)]
    theirs = [[kind == part for kind in held] for part in range(4)]

    def unpack(far, second, at):
        y = jnp.bitwise_xor(gy, 2 * far + (second >> 1))
        rows = pl.ds(pl.multiple_of(y * block_rows, 8), block_rows)
        blocks = [gathered[4 * (bits & 1) + second][far + (bits & 2), at] for bits in range(4)]
        parts = []
        for part in range(4):
            value = blocks[0]
            for block, mine in zip(blocks[1:], theirs[part][1:]):
                value = jnp.where(mine, block, value)
            parts.append(pltpu.roll(value, LANES - quarter * part, 1) if part else value)
        return rows, parts

    half1 = count1 // 2
    for far in range(2):
        for second in range(4):
            x = jnp.bitwise_xor(gx, second & 1)
            for at in range(slots):
                rows, parts = unpack(far, second, at)
                for part, target in enumerate((fr1, fr1, fb1, fb1)):
                    target[x * slots + at, part % 2, rows, :] = parts[part]
    for far in range(2):
        for second in range(4):
            x = jnp.bitwise_xor(gx, second & 1)
            next_slot = jnp.where(x == 0, half1, half1 - 1)
            rows, parts = unpack(far, second, slots)
            for part, target in enumerate((fr1, fr1, fb1, fb1)):
                target[next_slot, part % 2, rows, :] = target[next_slot, part % 2, rows, :] + parts[part]

    def fold_total(ref, at, e, start, count, low, high, odds, to_red):
        lane = lanes_of((count, LANES))
        value, other = window(ref, at, e, count, start), window(ref, at, 1 - e, count, start)
        sides = window(ref, at, e, count, start, -1) + window(ref, at, e, count, start, 1)
        if e == 0:
            near = jnp.where(lane == 0, 0.0, pltpu.roll(other, 1, 1))
        else:
            near = jnp.where(lane == LANES - 1, 0.0, pltpu.roll(other, LANES - 1, 1))
        before = 0.0 if low is True else window(ref, at - 1, e, count, start)
        after = 0.0 if high is True else window(ref, at + 1, e, count, start)
        if not isinstance(low, bool):
            before = jnp.where(low, 0.0, window(ref, jnp.maximum(at - 1, 0), e, count, start))
        if not isinstance(high, bool):
            after = jnp.where(high, 0.0, window(ref, jnp.minimum(at + 1, count1 - 1), e, count, start))
        beside = jnp.where(odds[e], after, before) if to_red else jnp.where(odds[e], before, after)
        return value + sides + beside + weight_z * (other + near)

    def fold_odds(count):
        row = rows_of((count, LANES))
        return [((row + e) & 1) == 1 for e in range(2)]

    odds = fold_odds(rows1)
    body1 = slice(PAD, PAD + rows1)

    def down_total(ref, at, e, to_red):
        return fold_total(ref, at, e, 0, rows1, at == 0, at == count1 - 1, odds, to_red)

    for at in range(count1):
        for e in range(2):
            red1[at, e, body1, :] = share * fr1[at, e]
    for at in range(count1):
        for e in range(2):
            black1[at, e, body1, :] = share * (fb1[at, e] + down_total(red1, at, e, False))
    for at in range(count1):
        for e in range(2):
            red1[at, e, body1, :] = share * (fr1[at, e] + down_total(black1, at, e, True))
    for at in range(count1):
        left_over = None
        for e in range(2):
            total = fb1[at, e] + down_total(red1, at, e, False)
            value = share * total
            black1[at, e, body1, :] = value
            term = total - centre * value
            left_over = term if left_over is None else left_over + term
        rest1[at] = left_over
    for at in range(count1):
        left_over = rest1[at]
        for e in range(2):
            total = fr1[at, e] + down_total(black1, at, e, True)
            left_over = left_over + (total - centre * window(red1, at, e, rows1))
        rest1[at] = left_over
    rows2 = rows1 // 2
    shape2 = (rows2, LANES)
    row2, lane2 = rows_of(shape2), lanes_of(shape2)
    odd2 = odd_of(shape2)
    planes = [
        0.5 * (rest1[at, pl.ds(0, rows2, stride=2), :] + rest1[at, pl.ds(1, rows2, stride=2), :])
        for at in range(count1)
    ]

    body2 = slice(PAD, PAD + rows2)

    def grid_of(index):
        step = 1 << index
        return ((row2 & (step - 1)) == 0) & ((lane2 & (step - 1)) == 0)

    def odd_at(index):
        return (((row2 >> index) + (lane2 >> index)) & 1) == 1

    def turned(value, step):
        inside = lane2 >= step if step > 0 else lane2 < LANES + step
        return jnp.where(inside, pltpu.roll(value, step % LANES, 1), 0.0)

    def small_plane(index, ref, at, odd, to_red):
        step = 1 << index
        total = ref[at, 0, body2, :] + (
            ref[at, 0, PAD - step : PAD - step + rows2, :] + ref[at, 0, PAD + step : PAD + step + rows2, :]
        )
        slots = ref.shape[0]
        if slots == 1:
            return total
        before = ref[at - 1, 0, body2, :] if at > 0 else 0.0
        after = ref[at + 1, 0, body2, :] if at < slots - 1 else 0.0
        return total + (jnp.where(odd, after, before) if to_red else jnp.where(odd, before, after))

    def small_sweeps(index, start):
        fr, fb, red, black, fr_low, fr_high = small[index]
        odd, width = odd_at(index), 1 << index
        mask = jnp.where(grid_of(index), share, 0.0)
        mask_low = jnp.where(lane2 < width, 0.0, mask)
        mask_high = jnp.where(lane2 >= LANES - width, 0.0, mask)
        slots = fr.shape[0]
        if start:
            for at in range(slots):
                fr_low[at] = pltpu.roll(fr[at], width, 1)
                fr_high[at] = pltpu.roll(fr[at], LANES - width, 1)
        for step in range(2):
            sides = []
            for at in range(slots):
                here, low, high = fr[at], fr_low[at], fr_high[at]
                if not (start and step == 0):
                    value = black[at, 0, body2, :]
                    plane = small_plane(index, black, at, odd, True)
                    here = here + plane + weight_z * (turned(value, width) + turned(value, -width))
                    low = low + pltpu.roll(plane, width, 1) + weight_z * (turned(value, 2 * width) + value)
                    high = high + pltpu.roll(plane, LANES - width, 1)
                    high = high + weight_z * (value + turned(value, -2 * width))
                red[at, 0, body2, :] = mask * here
                sides.append(weight_z * (mask_low * low + mask_high * high))
            totals = []
            for at in range(slots):
                total = fb[at] + small_plane(index, red, at, odd, False) + sides[at]
                black[at, 0, body2, :] = mask * total
                totals.append(total)
        return totals

    def spread_rows(value, step, ref, at):
        ref[at, 0, body2, :] = value
        return value + ref[at, 0, PAD - step : PAD - step + rows2, :]

    last = len(small) - 1
    for index in range(len(small)):
        fr, fb, red, black, _, fr_high = small[index]
        slots, odd, step = fr.shape[0], odd_at(index), 1 << index
        for at in range(slots):
            p, q = planes[2 * at], planes[2 * at + 1]
            fr[at], fb[at] = jnp.where(odd, q, p), jnp.where(odd, p, q)
        black_totals = small_sweeps(index, True)
        totals = []
        for at in range(slots):
            value, field = black[at, 0, body2, :], red[at, 0, body2, :]
            plane = small_plane(index, black, at, odd, True)
            total = black_totals[at] - centre * value
            next_total = pltpu.roll(total, LANES - step, 1)
            total = total + (
                fr[at] + plane + weight_z * (turned(value, step) + turned(value, -step)) - centre * field
            )
            if index < last:
                next_total = next_total + (
                    fr_high[at] + pltpu.roll(plane, LANES - step, 1)
                    + weight_z * (value + turned(value, -2 * step))
                    - centre * pltpu.roll(field, LANES - step, 1)
                )
                total = total + next_total
            totals.append(total)
            passing[at, 0, body2, :] = total
        lower = [passing[at, 0, PAD + step : PAD + step + rows2, :] for at in range(slots)]
        planes = [0.5 * (total + below) for total, below in zip(totals, lower)]

    half_rows = rows2 // 2
    upper = [passing[at, 0, PAD - step : PAD - step + rows2, :] for at in range(slots)]
    odd_line = (row2 & step) != 0
    summed = [
        total + jnp.where(odd_line, above, below) for total, above, below in zip(totals, upper, lower)
    ]
    lines = [total[start : start + half_rows] for total in summed for start in (0, half_rows)]
    place = lanes_of((half_rows, LANES)) & (len(lines) - 1)
    joined = lines[0]
    for q in range(1, len(lines)):
        joined = jnp.where(place == q, pltpu.roll(lines[q], q, 1), joined)
    answer = exact_dot(joined, matrix_ref[...])
    grid = (place == 0) & ((rows_of((half_rows, LANES)) & (step - 1)) == 0)
    parts = []
    for q in range(len(lines)):
        part = pltpu.roll(answer, LANES - q, 1) if q else answer
        parts.append(jnp.where(grid, part, 0.0))
    spreads = [jnp.concatenate(parts[2 * at : 2 * at + 2], axis=0) for at in range(slots)]

    for index in reversed(range(len(small))):
        _, _, red, black, _, _ = small[index]
        slots, odd, step = red.shape[0], odd_at(index), 1 << index
        if index < last:
            spreads = [
                spread_rows(field + pltpu.roll(field, step, 1), step, passing, at)
                for at, field in enumerate(fields)
            ]
        for at in range(slots):
            black[at, 0, body2, :] = black[at, 0, body2, :] + spreads[at]
        small_sweeps(index, False)
        fields = []
        for at in range(slots):
            r, b = red[at, 0, body2, :], black[at, 0, body2, :]
            fields += [jnp.where(odd, b, r), jnp.where(odd, r, b)]

    for at in range(count1):
        for start in range(2):
            rest1[at, pl.ds(start, rows2, stride=2), :] = fields[at]
    for at in range(count1):
        for e in range(2):
            black1[at, e, body1, :] = window(black1, at, e, rows1) + rest1[at]
    nx, ny, nz = out_ref.shape
    own = nx // 2
    part_slots = min(own // 2 + 3, count1)
    part_rows = min(ny // 2 + 16, rows1)
    slot0 = jnp.where(gx == 0, 0, count1 - part_slots)
    row0 = pl.multiple_of(jnp.clip(gy * (ny // 2) - 8, 0, rows1 - part_rows), 8)
    odds = fold_odds(part_rows)

    def up_total(ref, at, e, to_red):
        low = gx == 0 if at == 0 else False
        high = gx != 0 if at == part_slots - 1 else False
        return fold_total(ref, slot0 + at, e, row0, part_rows, low, high, odds, to_red)

    def up_half(target, other, sources, to_red):
        for at in range(part_slots):
            for e in range(2):
                source = sources[slot0 + at, e, pl.ds(row0, part_rows), :]
                value = share * (source + up_total(other, at, e, to_red))
                target[slot0 + at, e, pl.ds(pl.multiple_of(row0 + PAD, 8), part_rows), :] = value

    for _ in range(2):
        up_half(red1, black1, fr1, True)
        up_half(black1, red1, fb1, False)

    count, _, rows, _ = dark_ref.shape
    half = rows // 2
    odds = fold_odds(half)
    row = gy * (ny // 2) + (PAD - halo // 2)
    for at in range(count):
        if at < own:
            slot = gx * (own // 2) + at // 2
        else:
            slot = jnp.where(gx == 0, own // 2, own // 2 - (count - own) // 2) + (at - own) // 2
        for e in range(2):
            r, b = red1[slot, e, pl.ds(row, half), :], black1[slot, e, pl.ds(row, half), :]
            plane = jnp.where(odds[e], r, b) if at % 2 else jnp.where(odds[e], b, r)
            tall_ref[at, :, e * LANES : (e + 1) * LANES] = plane
    shape = (2 * LANES, 2 * LANES)
    z = lanes_of(shape)
    z = jnp.where(z < 2 * LANES - halo, z, z - 2 * LANES) + gz * nz
    line = rows_of(shape)
    line = jnp.where(line < LANES, 2 * line, 2 * (line - LANES) + 1)
    weight = jnp.where(line == lax.shift_right_arithmetic(z, 1), 1.0, 0.0)
    spread = pick_dot(tall_ref[...].reshape(count * half, 2 * LANES), weight)
    spread = spread.reshape(count, half, 2 * LANES)
    for at in range(count):
        for c in range(2):
            value = spread[at, :, c * LANES : (c + 1) * LANES]
            for start in range(2):
                work_ref[at, c, pl.ds(PAD + start, half, stride=2), :] = value
    body = slice(PAD, PAD + rows)
    for at in range(count):
        for c in range(2):
            work_ref[at, c, body, :] = work_ref[at, c, body, :] + dark_ref[at, c]
    odd = odd_of((rows, LANES))
    masks = block_mask((ny, nz), halo)
    ends = (gx == 0, gx == lax.axis_size("gx") - 1)
    beside_own = [*range(own), own, count - 1]

    def red_half(slots):
        for at in slots:
            totals = block_totals(work_ref, at, rows, own, odd, True, *ends)
            for c in range(2):
                red_ref[at, c, body, :] = gr_ref[at, c] + masks[c] * totals[c]

    red_half(range(count))
    for at in beside_own:
        totals = block_totals(red_ref, at, rows, own, odd, False, *ends)
        for c in range(2):
            work_ref[at, c, body, :] = gb_ref[at, c] + masks[c] * totals[c]
    red_half(beside_own)
    inner = slice(halo, halo + ny)
    odd_inner = odd_of((ny, nz))
    groups = sems.shape[0]
    size = nx // groups
    copies = [
        pltpu.make_async_copy(
            result_ref.at[pl.ds(q * size, size)], out_ref.at[pl.ds(q * size, size)], sems.at[q]
        )
        for q in range(groups)
    ]
    for at in range(own):
        total = block_totals(red_ref, at, rows, own, odd, False, *ends)[0]
        b = (gb_ref[at, 0] + masks[0] * total)[inner]
        r = red_ref[at, 0, PAD + halo : PAD + halo + ny, :]
        result_ref[2 * at] = jnp.where(odd_inner, b, r)
        result_ref[2 * at + 1] = jnp.where(odd_inner, r, b)
        done = (2 * at + 2) // size
        if (2 * at + 2) % size == 0 and done > 1:
            copies[done - 2].start()
    copies[-1].start()
    for copy in copies:
        copy.wait()


def vmem(number):
    return [pl.BlockSpec(memory_space=pltpu.VMEM)] * number


def struct(*shape):
    return jax.ShapeDtypeStruct(shape, jnp.float32)


def scratch(*shape):
    return pltpu.VMEM(shape, jnp.float32)


HALO = 8


def block_cycle(density):
    halo = HALO
    nx, ny, nz = density.shape
    count_x, count_y, count_z = (lax.axis_size(axis) for axis in ("gx", "gy", "gz"))
    whole = (nx * count_x, ny * count_y, nz * count_z)

    def params(mib):
        return pltpu.CompilerParams(vmem_limit_bytes=mib * 1024 * 1024)

    even = lax.axis_index("gy") % 2 == 0
    ya = lax.dynamic_slice_in_dim(density, jnp.where(even, ny - halo, 0), halo, 1)
    yb = lax.dynamic_slice_in_dim(density, jnp.where(even, 0, ny - halo), halo, 1)
    ya = lax.ppermute(ya, "gy", pairs(count_y, 0))
    yb = lax.ppermute(yb, ("gx", "gy"), inner_pairs(count_x, count_y))
    rows = ny + 2 * halo
    packs = -(-nx * halo // nz)
    za, zb = pl.pallas_call(
        functools.partial(pack_kernel, halo),
        out_shape=[struct(packs, rows, nz)] * 2,
        in_specs=vmem(3), out_specs=vmem(2), compiler_params=params(4),
    )(density, ya, yb)
    za = lax.ppermute(za, "gz", pairs(count_z, 0))
    zb = lax.ppermute(zb, "gz", pairs(count_z, 1) + [(0, count_z - 1), (count_z - 1, 0)])
    own, near = nx // 2, nx // 2 + 2
    send, face = pl.pallas_call(
        functools.partial(pre_kernel, halo),
        out_shape=[struct(near // 2, ny // 2, nz), struct(halo + 1, rows, LANES)],
        in_specs=vmem(5), out_specs=vmem(2), compiler_params=params(10),
        scratch_shapes=[scratch(own, ny, nz)] * 2
        + [scratch(own, 2, rows, LANES)] * 2
        + [scratch(near, 2, rows + 2 * PAD, LANES)] * 2
        + [scratch(near, ny, nz)],
    )(density, ya, yb, za, zb)
    planes = nx + halo
    slots = (planes // 2, 2, rows, LANES)
    padded = (planes // 2, 2, rows + 2 * PAD, LANES)
    first = [send]
    first.append(lax.ppermute(send, "gy", flips(count_y, 2)))
    first.append(lax.ppermute(send, "gz", flips(count_z, 2)))
    swaps = flips(count_y * count_z, 2 * count_z + 2)
    first.append(lax.ppermute(send, ("gy", "gz"), swaps))
    face = lax.ppermute(face, "gx", flips(count_x, 1))
    block = pl.pallas_call(
        stack_kernel, out_shape=struct(4, *send.shape),
        in_specs=vmem(4), out_specs=pl.BlockSpec(memory_space=pltpu.VMEM), compiler_params=params(2),
    )(*first)
    second = [
        block,
        lax.ppermute(block, "gx", flips(count_x, 1)),
        lax.ppermute(block, "gy", flips(count_y, 1)),
        lax.ppermute(block, ("gx", "gy"), flips(count_x * count_y, count_y + 1)),
    ]
    gr, gb, black = pl.pallas_call(
        functools.partial(field_kernel, halo),
        out_shape=[struct(*slots)] * 3,
        in_specs=vmem(7), out_specs=vmem(3), compiler_params=params(8),
        scratch_shapes=[scratch(*padded)] * 2,
        cost_estimate=pl.CostEstimate(flops=20_000_000, bytes_accessed=2_000_000, transcendentals=0),
    )(density, ya, yb, za, zb, face, block)
    second[3], gr, gb, black = lax.optimization_barrier((second[3], gr, gb, black))
    third = [lax.ppermute(blocks, "gz", flips(count_z, 1)) for blocks in second]
    count1, rows1, rows2 = whole[0] // 4, whole[1] // 2, whole[1] // 4
    room = [scratch(count1, 2, rows1, LANES)] * 2
    room += [scratch(count1, 2, rows1 + 2 * PAD, LANES)] * 2
    room += [scratch(count1, rows1, LANES), scratch(planes // 2, rows // 2, 2 * LANES)]
    room += [scratch(*padded)] * 2 + [scratch(count1 // 2, 1, rows2 + 2 * PAD, LANES)]
    room += [scratch(nx, ny, nz), pltpu.SemaphoreType.DMA((4,))]
    for count in small_shapes(whole):
        room += [scratch(count, rows2, LANES)] * 2
        room += [scratch(count, 1, rows2 + 2 * PAD, LANES)] * 2
        room += [scratch(count, rows2, LANES)] * 2
    return pl.pallas_call(
        functools.partial(solve_kernel, halo),
        out_shape=struct(nx, ny, nz),
        in_specs=vmem(12), out_specs=pl.BlockSpec(memory_space=pl.ANY),
        compiler_params=params(16), scratch_shapes=room,
    )(*second, *third, gr, gb, black, cycle_matrix(whole))


def fits_block_cycle(shape):
    nx, ny, nz = shape
    count_x, count_y, count_z = (lax.axis_size(axis) for axis in ("gx", "gy", "gz"))
    whole = (nx * count_x, ny * count_y, nz * count_z)
    coarsest = [size >> (LEVELS - 1) for size in whole]
    exact = all(c << (LEVELS - 1) == size for c, size in zip(coarsest, whole))
    return (
        exact and coarsest[0] == coarsest[1] == 1 and nz == LANES and ny == 2 * HALO
        and count_x == 2 and count_y == 4 and count_z == 4
    )


def on_device(density):
    if fits_block_cycle(density.shape):
        return block_cycle(density)
    top = 4
    return shared_cycle(density, 0, top)


def solution(mesh):
    return jax.shard_map(
        on_device,
        mesh=mesh,
        in_specs=(P("gx", "gy", "gz"),),
        out_specs=P("gx", "gy", "gz"),
        check_vma=False,
    )
```

```python
import functools

import jax
import jax.numpy as jnp
import numpy as np
from jax import lax
from jax.experimental import pallas as pl
from jax.experimental.pallas import tpu as pltpu
from jax.sharding import PartitionSpec as P

LEVELS = 7
CSWEEPS = 4


rsd_beta = 0.5
centre = 4.0 + 2.0 * (1.0 + rsd_beta)


def extended_2(value, sides, width):
    for axis, dim in sides:
        count, length = (lax.axis_size(axis), value.shape[dim])
        up = [(i, (i + 1) % count) for i in range(count - 1)]
        down = [(j, i) for i, j in up]
        last = lax.slice_in_dim(value, length - width, length, axis=dim)
        leading = lax.slice_in_dim(value, 0, width, axis=dim)
        before = lax.ppermute(last, axis, up)
        after = lax.ppermute(leading, axis, down)
        value = jnp.concatenate([before, value, after], axis=dim)
    return value


def stencil_sum(padded):
    plane = (
        padded[2:, 1:-1, 1:-1]
        + padded[:-2, 1:-1, 1:-1]
        + padded[1:-1, 2:, 1:-1]
        + padded[1:-1, :-2, 1:-1]
    )
    sight = padded[1:-1, 1:-1, 2:] + padded[1:-1, 1:-1, :-2]
    return plane + (1.0 + rsd_beta) * sight


def grid_index(shape, starts):
    return [lax.broadcasted_iota(jnp.int32, shape, which) + starts[which] for which in range(3)]


def parity_of(shape, starts):
    position = grid_index(shape, starts)
    return (position[0] + position[1] + position[2] + 6) % 2


def inside_grid(shape, starts, whole):
    position = grid_index(shape, starts)
    keep = (position[0] >= 0) & (position[0] < whole[0])
    for which in (1, 2):
        keep = keep & (position[which] >= 0) & (position[which] < whole[which])
    return keep


def half_sweep(field, source, scale, chosen):
    update = (source / scale + stencil_sum(jnp.pad(field, 1))) / centre
    return jnp.where(chosen, update, field)


def full_sweep(field, source, scale, parity):
    field = half_sweep(field, source, scale, parity == 0)
    return half_sweep(field, source, scale, parity == 1)


def restrict(residue):
    shape = residue.shape
    blocks = residue.reshape(shape[0] // 2, 2, shape[1] // 2, 2, shape[2] // 2, 2)
    return jnp.mean(blocks, axis=(1, 3, 5))


def prolong(coarse):
    return jnp.repeat(jnp.repeat(jnp.repeat(coarse, 2, 0), 2, 1), 2, 2)


def local_cycle(source, level):
    scale = 0.25**level
    parity = parity_of(source.shape, (0, 0, 0))
    field = jnp.zeros_like(source)
    if level == LEVELS - 1:
        for _ in range(CSWEEPS):
            field = full_sweep(field, source, scale, parity)
        return field
    for _ in range(2):
        field = full_sweep(field, source, scale, parity)
    residue = source - scale * (centre * field - stencil_sum(jnp.pad(field, 1)))
    field = field + prolong(local_cycle(restrict(residue), level + 1))
    for _ in range(2):
        field = full_sweep(field, source, scale, parity)
    return field


def faces(field):
    return extended_2(field, (("gx", 0), ("gy", 1), ("gz", 2)), 1)


def wide(field):
    return extended_2(field, (("gx", 0), ("gy", 1), ("gz", 2)), 2)


def block_starts(shape, margin):
    return (
        lax.axis_index("gx") * shape[0] - margin,
        lax.axis_index("gy") * shape[1] - margin,
        lax.axis_index("gz") * shape[2] - margin,
    )


def padded_half(padded, source, scale, chosen):
    field = padded[1:-1, 1:-1, 1:-1]
    update = (source / scale + stencil_sum(padded)) / centre
    return jnp.where(chosen, update, field)


def wide_sweep(extended, wide_source, scale, red_wide, source, black):
    update = (wide_source / scale + stencil_sum(jnp.pad(extended, 1))) / centre
    extended = jnp.where(red_wide, update, extended)
    return padded_half(extended[1:-1, 1:-1, 1:-1], source, scale, black)


def coarse_level(source, level):
    shape = source.shape
    stack = lax.all_gather(source[None], ("gx", "gy", "gz"), axis=0, tiled=True)
    count_x, count_y, count_z = (lax.axis_size("gx"), lax.axis_size("gy"), lax.axis_size("gz"))
    whole = stack.reshape(count_x, count_y, count_z, shape[0], shape[1], shape[2])
    whole = whole.transpose(0, 3, 1, 4, 2, 5).reshape(
        count_x * shape[0], count_y * shape[1], count_z * shape[2]
    )
    solved = local_cycle(whole, level)
    starts = block_starts(shape, 0)
    return lax.dynamic_slice(solved, starts, shape)


def shared_cycle(source, level, top):
    if level == top:
        return coarse_level(source, level)
    scale = 0.25**level
    shape = source.shape
    whole = (
        shape[0] * lax.axis_size("gx"),
        shape[1] * lax.axis_size("gy"),
        shape[2] * lax.axis_size("gz"),
    )
    parity = parity_of(shape, block_starts(shape, 0))
    black = parity == 1
    wide_shape = (shape[0] + 4, shape[1] + 4, shape[2] + 4)
    wide_starts = block_starts(shape, 2)
    red_wide = (parity_of(wide_shape, wide_starts) == 0) & inside_grid(
        wide_shape, wide_starts, whole
    )
    wide_source = wide(source)
    field = wide_sweep(
        jnp.zeros(wide_shape, jnp.float32), wide_source, scale, red_wide, source, black
    )
    field = wide_sweep(wide(field), wide_source, scale, red_wide, source, black)
    residue = source - scale * (centre * field - stencil_sum(faces(field)))
    field = field + prolong(shared_cycle(restrict(residue), level + 1, top))
    for _ in range(2):
        field = wide_sweep(wide(field), wide_source, scale, red_wide, source, black)
    return field


def pairs(count, first):
    swaps = []
    for i in range(first, count - 1, 2):
        swaps += [(i, i + 1), (i + 1, i)]
    return swaps


def inner_pairs(count_x, count):
    swaps = []
    for x in range(count_x):
        swaps += [(x * count + i, x * count + j) for i, j in pairs(count, 1)]
        swaps += [(x * count + i, (x ^ 1) * count + i) for i in (0, count - 1)]
    return swaps


def flips(count, bit):
    return [(i, i ^ bit) for i in range(count)]


def lanes_of(shape):
    return lax.broadcasted_iota(jnp.int32, shape, len(shape) - 1)


def rows_of(shape):
    return lax.broadcasted_iota(jnp.int32, shape, len(shape) - 2)


LANES = 128
PAD = 8


def odd_of(shape):
    return ((lanes_of(shape) + rows_of(shape)) & 1) == 1


def exact_dot(a, b):
    return jnp.dot(a, b, precision=lax.Precision.HIGHEST, preferred_element_type=jnp.float32)


def pick_dot(a, b):
    b = b.astype(jnp.bfloat16)
    total = None
    for _ in range(3):
        high = a.astype(jnp.bfloat16)
        term = jnp.dot(high, b, preferred_element_type=jnp.float32)
        total = term if total is None else total + term
        a = a - high.astype(jnp.float32)
    return total


def window(ref, at, column, count, start=0, shift=0):
    if isinstance(start, int):
        return ref[at, column, PAD + start + shift : PAD + start + shift + count, :]
    first = start + (PAD + shift)
    if shift == 0:
        first = pl.multiple_of(first, 8)
    return ref[at, column, pl.ds(first, count), :]


def clear_pads(ref):
    edge = jnp.zeros((PAD, LANES), jnp.float32)
    for at in range(ref.shape[0]):
        for column in range(ref.shape[1]):
            ref[at, column, :PAD, :] = edge
            ref[at, column, ref.shape[2] - PAD :, :] = edge


def block_sums(ref, at, rows):
    lane = lanes_of((rows, LANES))
    values = [window(ref, at, column, rows) for column in range(2)]
    lefts = [pltpu.roll(value, 1, 1) for value in values]
    rights = [pltpu.roll(value, LANES - 1, 1) for value in values]
    sums = []
    for column in range(2):
        left = jnp.where(lane == 0, lefts[1 - column], lefts[column])
        right = jnp.where(lane == LANES - 1, rights[1 - column], rights[column])
        sides = window(ref, at, column, rows, shift=-1) + window(ref, at, column, rows, shift=1)
        sums.append(values[column] + sides + (1.0 + rsd_beta) * (left + right))
    return sums


def block_totals(ref, at, rows, own, odd, to_red, at_low, at_high):
    slots = ref.shape[0]
    totals = []
    for column, total in enumerate(block_sums(ref, at, rows)):
        before = window(ref, (at - 1) % slots, column, rows)
        after = window(ref, (at + 1) % slots, column, rows)
        if at in (0, own):
            before = jnp.where(at_low if at == 0 else at_high, 0.0, before)
        if at in (own - 1, slots - 1):
            after = jnp.where(at_low if at == slots - 1 else at_high, 0.0, after)
        totals.append(total + (jnp.where(odd, after, before) if to_red else jnp.where(odd, before, after)))
    return totals


def block_mask(own, halo):
    ny, nz = own
    shape = (ny + 2 * halo, LANES)
    row = rows_of(shape) - halo + lax.axis_index("gy") * ny
    inside_y = (row >= 0) & (row < ny * lax.axis_size("gy"))
    masks = []
    for column in range(2):
        lane = lanes_of(shape)
        if column:
            lane = jnp.where(lane < halo, lane + LANES, lane - LANES)
        lane = lane + lax.axis_index("gz") * nz
        inside = inside_y & (lane >= 0) & (lane < nz * lax.axis_size("gz"))
        masks.append(jnp.where(inside, 1.0 / centre, 0.0))
    return masks


def block_plane(at, own_ref, ya_ref, yb_ref, even_y):
    a, b = ya_ref[at], yb_ref[at]
    low = jnp.where(even_y, b, a)
    high = jnp.where(even_y, a, b)
    return jnp.concatenate([low, own_ref[at], high], axis=0)


def block_columns(halo, at, own_ref, ya_ref, yb_ref, za_ref, zb_ref, even_y, even_z):
    _, _, nz = own_ref.shape
    j, k = at // (nz // halo), at % (nz // halo)
    a, b = za_ref[j], zb_ref[j]
    left = pltpu.roll(jnp.where(even_z, b, a), (2 * nz - halo - halo * k) % nz, 1)
    right = pltpu.roll(jnp.where(even_z, a, b), (nz - halo * k) % nz, 1)
    lane = lanes_of(left.shape)
    sides = jnp.where(lane < halo, right, jnp.where(lane >= nz - halo, left, 0.0))
    return block_plane(at, own_ref, ya_ref, yb_ref, even_y), sides


def pack_kernel(halo, own_ref, ya_ref, yb_ref, za_ref, zb_ref):
    even_y = lax.axis_index("gy") % 2 == 0
    even_z = lax.axis_index("gz") % 2 == 0
    nx, ny, nz = own_ref.shape
    groups = nz // halo
    shape = (ny + 2 * halo, nz)
    group = lanes_of(shape) // halo
    for j in range(za_ref.shape[0]):
        last = jnp.zeros(shape, jnp.float32)
        first = jnp.zeros(shape, jnp.float32)
        for k in range(min(groups, nx - j * groups)):
            plane = block_plane(j * groups + k, own_ref, ya_ref, yb_ref, even_y)
            last = jnp.where(group == k, pltpu.roll(plane, (halo * k + halo) % nz, 1), last)
            first = jnp.where(group == k, pltpu.roll(plane, halo * k, 1), first)
        za_ref[j] = jnp.where(even_z, last, first)
        zb_ref[j] = jnp.where(even_z, first, last)


def smooth(count, own, masks, odd, ends, gr_ref, gb_ref, red_ref, black_ref, done):
    rows = odd.shape[0]
    body = slice(PAD, PAD + rows)

    def value_of(source, at, c, total):
        value = masks[c] * total
        return source[at, c] + value if at < source.shape[0] else value

    for at in range(count):
        for c in range(2):
            red_ref[at, c, body, :] = gr_ref[at, c] if at < gr_ref.shape[0] else jnp.zeros_like(masks[c])
    for step in range(3):
        source, target, other = (gr_ref, red_ref, black_ref) if step == 1 else (gb_ref, black_ref, red_ref)
        for at in range(count):
            totals = block_totals(other, at, rows, own, odd, step == 1, *ends)
            for c in range(2):
                value = value_of(source, at, c, totals[c])
                target[at, c, body, :] = value
                if step == 2:
                    done(at, c, totals[c], value)


def x_ends():
    here = lax.axis_index("gx")
    return here == 0, here == lax.axis_size("gx") - 1


def pre_kernel(
    halo, own_ref, ya_ref, yb_ref, za_ref, zb_ref,
    send_ref, face_ref,
    fr_ref, fb_ref, gr_ref, gb_ref, red_ref, black_ref, rest_ref,
):
    even_y = lax.axis_index("gy") % 2 == 0
    even_z = lax.axis_index("gz") % 2 == 0
    nx, ny, nz = own_ref.shape
    count, _, rows, _ = red_ref.shape
    rows = rows - 2 * PAD
    own = nx // 2
    shape = (rows, LANES)
    odd = odd_of(shape)
    masks = block_mask((ny, nz), halo)
    inner = slice(halo, halo + ny)
    ends = x_ends()
    clear_pads(red_ref)
    clear_pads(black_ref)
    for p in range(halo):
        high = block_plane(nx - halo + p, own_ref, ya_ref, yb_ref, even_y)
        face_ref[p] = jnp.where(ends[0], high, block_plane(p, own_ref, ya_ref, yb_ref, even_y))
    middle = halo * halo
    top = za_ref.shape[0] - 1
    left = [jnp.where(even_z, zb_ref[j], za_ref[j]) for j in (0, top)]
    right = [jnp.where(even_z, za_ref[j], zb_ref[j]) for j in (0, top)]
    left = jnp.where(ends[0], pltpu.roll(left[1], middle, 1), left[0])
    right = jnp.where(ends[0], right[1], pltpu.roll(right[0], middle, 1))
    face_ref[halo] = jnp.where(lanes_of(shape) < middle, left, right)
    for at in range(own):
        planes = [
            block_columns(halo, x, own_ref, ya_ref, yb_ref, za_ref, zb_ref, even_y, even_z)
            for x in (2 * at, 2 * at + 1)
        ]
        for c in range(2):
            red = jnp.where(odd, planes[1][c], planes[0][c])
            black = jnp.where(odd, planes[0][c], planes[1][c])
            if c == 0:
                fr_ref[at], fb_ref[at] = red[inner], black[inner]
            gr_ref[at, c], gb_ref[at, c] = masks[c] * red, masks[c] * black

    def keep(at, c, total, value):
        if c == 0:
            left_over = total[inner] - centre * value[inner]
            rest_ref[at] = left_over + fb_ref[at] if at < own else left_over

    smooth(count, own, masks, odd, ends, gr_ref, gb_ref, red_ref, black_ref, keep)
    for at in range(count):
        total = block_totals(black_ref, at, rows, own, odd, True, *ends)[0]
        left_over = total[inner] - centre * red_ref[at, 0, PAD + halo : PAD + halo + ny, :]
        if at < own:
            left_over = left_over + fr_ref[at]
        rest_ref[at] = rest_ref[at] + left_over
    half, quarter = ny // 2, nz // 4
    pairs_y = rest_ref[:, pl.ds(0, half, stride=2), :] + rest_ref[:, pl.ds(1, half, stride=2), :]
    turn = quarter * lax.axis_index("gz")
    column = (lanes_of((nz, nz)) - turn) & (nz - 1)
    target = 2 * (column % quarter) + (column // quarter) % 2
    weight = jnp.where(rows_of((nz, nz)) // 2 == target, 0.5, 0.0)
    coarse = pick_dot(pairs_y.reshape(count * half, nz), weight).reshape(count, half, nz)
    part = ((lanes_of((half, nz)) - turn) & (nz - 1)) // quarter
    pick = (((rows_of((half, nz)) + part) & 1) == 1) ^ (part >= 2)
    for at in range(count // 2):
        send_ref[at] = jnp.where(pick, coarse[2 * at + 1], coarse[2 * at])


def field_kernel(
    halo, own_ref, ya_ref, yb_ref, za_ref, zb_ref, face_ref, after_ref,
    gr_ref, gb_ref, dark_ref,
    red_ref, black_ref,
):
    even_y = lax.axis_index("gy") % 2 == 0
    even_z = lax.axis_index("gz") % 2 == 0
    nx, ny, nz = own_ref.shape
    count, _, rows, _ = gr_ref.shape
    own = nx // 2
    shape = (rows, LANES)
    odd, lane = odd_of(shape), lanes_of(shape)
    masks = block_mask((ny, nz), halo)
    clear_pads(red_ref)
    clear_pads(black_ref)

    def columns(x):
        if x < nx:
            return block_columns(halo, x, own_ref, ya_ref, yb_ref, za_ref, zb_ref, even_y, even_z)
        p = x - nx
        left = pltpu.roll(face_ref[halo], (2 * LANES - halo - halo * p) % LANES, 1)
        right = pltpu.roll(face_ref[halo], (2 * LANES - halo * halo - halo * p) % LANES, 1)
        return face_ref[p], jnp.where(lane < halo, right, jnp.where(lane >= nz - halo, left, 0.0))

    for at in range(count):
        first, second = columns(2 * at), columns(2 * at + 1)
        for c in range(2):
            gr_ref[at, c] = masks[c] * jnp.where(odd, second[c], first[c])
            gb_ref[at, c] = masks[c] * jnp.where(odd, first[c], second[c])

    def keep(at, c, total, value):
        dark_ref[at, c] = value

    smooth(count, own, masks, odd, x_ends(), gr_ref, gb_ref, red_ref, black_ref, keep)


def stack_kernel(*refs):
    for which, ref in enumerate(refs[:-1]):
        refs[-1][which] = ref[...]


def small_shapes(whole):
    return [whole[0] >> (level + 1) for level in range(2, LEVELS - 2)]


def plain_sum(field):
    padded = np.pad(field, ((0, 0), (1, 1), (1, 1), (1, 1)))
    inner = slice(1, -1)
    plane = padded[:, 2:, inner, inner] + padded[:, :-2, inner, inner]
    plane = plane + padded[:, inner, 2:, inner] + padded[:, inner, :-2, inner]
    return plane + (1.0 + rsd_beta) * (padded[:, inner, inner, 2:] + padded[:, inner, inner, :-2])


def plain_cycle(source, level):
    parity = np.indices(source.shape[1:]).sum(axis=0) % 2
    field = np.zeros_like(source)

    def sweeps(field, number):
        for step in range(2 * number):
            field = np.where(parity == step % 2, (source + plain_sum(field)) / centre, field)
        return field

    if level == LEVELS - 1:
        return sweeps(field, CSWEEPS)
    field = sweeps(field, 2)
    rest = source - centre * field + plain_sum(field)
    nx, ny, nz = source.shape[1:]
    rest = rest.reshape(-1, nx // 2, 2, ny // 2, 2, nz // 2, 2).sum(axis=(2, 4, 6)) / 2.0
    coarse = plain_cycle(rest, level + 1)
    for axis in (1, 2, 3):
        coarse = np.repeat(coarse, 2, axis)
    return sweeps(field + coarse, 2)


def cycle_matrix(whole):
    level = LEVELS - 2
    nx, ny, nz = (size >> level for size in whole)
    size = nx * ny * 2 * nz
    unit = np.eye(size).reshape(size, 2 * nz, nx, ny).transpose(0, 2, 3, 1)
    source = unit.reshape(size, nx, ny, nz, 2).sum(axis=-1) / 2.0
    result = np.repeat(plain_cycle(source, level), 2, axis=3)
    return jnp.asarray(result.transpose(0, 3, 1, 2).reshape(size, size), jnp.float32)


def solve_kernel(halo, *refs):
    gathered, refs = refs[:8], refs[8:]
    gr_ref, gb_ref, dark_ref, matrix_ref, out_ref = refs[:5]
    fr1, fb1, red1, black1, rest1, tall_ref, red_ref, work_ref, passing = refs[5:14]
    small = [refs[14 + 6 * i : 20 + 6 * i] for i in range(LEVELS - 4)]
    gx, gy, gz = (lax.axis_index(axis) for axis in ("gx", "gy", "gz"))
    weight_z = 1.0 + rsd_beta
    share = 1.0 / centre
    for ref in (red1, black1, red_ref, work_ref, passing):
        clear_pads(ref)
    for level in small:
        for ref in level[2:4]:
            clear_pads(ref)

    _, slots, block_rows, _ = gathered[0].shape
    slots = slots - 1
    count1, _, rows1, _ = fr1.shape
    quarter = LANES // 4
    group = lanes_of((block_rows, LANES)) // quarter
    held = [jnp.bitwise_and(group - jnp.bitwise_xor(gz, bits), 3) for bits in range(4)]
    theirs = [[kind == part for kind in held] for part in range(4)]

    def unpack(far, second, at):
        y = jnp.bitwise_xor(gy, 2 * far + (second >> 1))
        rows = pl.ds(pl.multiple_of(y * block_rows, 8), block_rows)
        blocks = [gathered[4 * (bits & 1) + second][far + (bits & 2), at] for bits in range(4)]
        parts = []
        for part in range(4):
            value = blocks[0]
            for block, mine in zip(blocks[1:], theirs[part][1:]):
                value = jnp.where(mine, block, value)
            parts.append(pltpu.roll(value, LANES - quarter * part, 1) if part else value)
        return rows, parts

    half1 = count1 // 2
    for far in range(2):
        for second in range(4):
            x = jnp.bitwise_xor(gx, second & 1)
            for at in range(slots):
                rows, parts = unpack(far, second, at)
                for part, target in enumerate((fr1, fr1, fb1, fb1)):
                    target[x * slots + at, part % 2, rows, :] = parts[part]
    for far in range(2):
        for second in range(4):
            x = jnp.bitwise_xor(gx, second & 1)
            next_slot = jnp.where(x == 0, half1, half1 - 1)
            rows, parts = unpack(far, second, slots)
            for part, target in enumerate((fr1, fr1, fb1, fb1)):
                target[next_slot, part % 2, rows, :] = target[next_slot, part % 2, rows, :] + parts[part]

    def fold_total(ref, at, e, start, count, low, high, odds, to_red):
        lane = lanes_of((count, LANES))
        value, other = window(ref, at, e, count, start), window(ref, at, 1 - e, count, start)
        sides = window(ref, at, e, count, start, -1) + window(ref, at, e, count, start, 1)
        if e == 0:
            near = jnp.where(lane == 0, 0.0, pltpu.roll(other, 1, 1))
        else:
            near = jnp.where(lane == LANES - 1, 0.0, pltpu.roll(other, LANES - 1, 1))
        before = 0.0 if low is True else window(ref, at - 1, e, count, start)
        after = 0.0 if high is True else window(ref, at + 1, e, count, start)
        if not isinstance(low, bool):
            before = jnp.where(low, 0.0, window(ref, jnp.maximum(at - 1, 0), e, count, start))
        if not isinstance(high, bool):
            after = jnp.where(high, 0.0, window(ref, jnp.minimum(at + 1, count1 - 1), e, count, start))
        beside = jnp.where(odds[e], after, before) if to_red else jnp.where(odds[e], before, after)
        return value + sides + beside + weight_z * (other + near)

    def fold_odds(count):
        row = rows_of((count, LANES))
        return [((row + e) & 1) == 1 for e in range(2)]

    odds = fold_odds(rows1)
    body1 = slice(PAD, PAD + rows1)

    def down_total(ref, at, e, to_red):
        return fold_total(ref, at, e, 0, rows1, at == 0, at == count1 - 1, odds, to_red)

    for at in range(count1):
        for e in range(2):
            red1[at, e, body1, :] = share * fr1[at, e]
    for at in range(count1):
        for e in range(2):
            black1[at, e, body1, :] = share * (fb1[at, e] + down_total(red1, at, e, False))
    for at in range(count1):
        for e in range(2):
            red1[at, e, body1, :] = share * (fr1[at, e] + down_total(black1, at, e, True))
    for at in range(count1):
        left_over = None
        for e in range(2):
            total = fb1[at, e] + down_total(red1, at, e, False)
            value = share * total
            black1[at, e, body1, :] = value
            term = total - centre * value
            left_over = term if left_over is None else left_over + term
        rest1[at] = left_over
    for at in range(count1):
        left_over = rest1[at]
        for e in range(2):
            total = fr1[at, e] + down_total(black1, at, e, True)
            left_over = left_over + (total - centre * window(red1, at, e, rows1))
        rest1[at] = left_over
    rows2 = rows1 // 2
    shape2 = (rows2, LANES)
    row2, lane2 = rows_of(shape2), lanes_of(shape2)
    odd2 = odd_of(shape2)
    planes = [
        0.5 * (rest1[at, pl.ds(0, rows2, stride=2), :] + rest1[at, pl.ds(1, rows2, stride=2), :])
        for at in range(count1)
    ]

    body2 = slice(PAD, PAD + rows2)

    def grid_of(index):
        step = 1 << index
        return ((row2 & (step - 1)) == 0) & ((lane2 & (step - 1)) == 0)

    def odd_at(index):
        return (((row2 >> index) + (lane2 >> index)) & 1) == 1

    def turned(value, step):
        inside = lane2 >= step if step > 0 else lane2 < LANES + step
        return jnp.where(inside, pltpu.roll(value, step % LANES, 1), 0.0)

    def small_plane(index, ref, at, odd, to_red):
        step = 1 << index
        total = ref[at, 0, body2, :] + (
            ref[at, 0, PAD - step : PAD - step + rows2, :] + ref[at, 0, PAD + step : PAD + step + rows2, :]
        )
        slots = ref.shape[0]
        if slots == 1:
            return total
        before = ref[at - 1, 0, body2, :] if at > 0 else 0.0
        after = ref[at + 1, 0, body2, :] if at < slots - 1 else 0.0
        return total + (jnp.where(odd, after, before) if to_red else jnp.where(odd, before, after))

    def small_sweeps(index, start):
        fr, fb, red, black, fr_low, fr_high = small[index]
        odd, width = odd_at(index), 1 << index
        mask = jnp.where(grid_of(index), share, 0.0)
        mask_low = jnp.where(lane2 < width, 0.0, mask)
        mask_high = jnp.where(lane2 >= LANES - width, 0.0, mask)
        slots = fr.shape[0]
        if start:
            for at in range(slots):
                fr_low[at] = pltpu.roll(fr[at], width, 1)
                fr_high[at] = pltpu.roll(fr[at], LANES - width, 1)
        for step in range(2):
            sides = []
            for at in range(slots):
                here, low, high = fr[at], fr_low[at], fr_high[at]
                if not (start and step == 0):
                    value = black[at, 0, body2, :]
                    plane = small_plane(index, black, at, odd, True)
                    here = here + plane + weight_z * (turned(value, width) + turned(value, -width))
                    low = low + pltpu.roll(plane, width, 1) + weight_z * (turned(value, 2 * width) + value)
                    high = high + pltpu.roll(plane, LANES - width, 1)
                    high = high + weight_z * (value + turned(value, -2 * width))
                red[at, 0, body2, :] = mask * here
                sides.append(weight_z * (mask_low * low + mask_high * high))
            totals = []
            for at in range(slots):
                total = fb[at] + small_plane(index, red, at, odd, False) + sides[at]
                black[at, 0, body2, :] = mask * total
                totals.append(total)
        return totals

    def spread_rows(value, step, ref, at):
        ref[at, 0, body2, :] = value
        return value + ref[at, 0, PAD - step : PAD - step + rows2, :]

    last = len(small) - 1
    for index in range(len(small)):
        fr, fb, red, black, _, fr_high = small[index]
        slots, odd, step = fr.shape[0], odd_at(index), 1 << index
        for at in range(slots):
            p, q = planes[2 * at], planes[2 * at + 1]
            fr[at], fb[at] = jnp.where(odd, q, p), jnp.where(odd, p, q)
        black_totals = small_sweeps(index, True)
        totals = []
        for at in range(slots):
            value, field = black[at, 0, body2, :], red[at, 0, body2, :]
            plane = small_plane(index, black, at, odd, True)
            total = black_totals[at] - centre * value
            next_total = pltpu.roll(total, LANES - step, 1)
            total = total + (
                fr[at] + plane + weight_z * (turned(value, step) + turned(value, -step)) - centre * field
            )
            if index < last:
                next_total = next_total + (
                    fr_high[at] + pltpu.roll(plane, LANES - step, 1)
                    + weight_z * (value + turned(value, -2 * step))
                    - centre * pltpu.roll(field, LANES - step, 1)
                )
                total = total + next_total
            totals.append(total)
            passing[at, 0, body2, :] = total
        lower = [passing[at, 0, PAD + step : PAD + step + rows2, :] for at in range(slots)]
        planes = [0.5 * (total + below) for total, below in zip(totals, lower)]

    half_rows = rows2 // 2
    upper = [passing[at, 0, PAD - step : PAD - step + rows2, :] for at in range(slots)]
    odd_line = (row2 & step) != 0
    summed = [
        total + jnp.where(odd_line, above, below) for total, above, below in zip(totals, upper, lower)
    ]
    lines = [total[start : start + half_rows] for total in summed for start in (0, half_rows)]
    place = lanes_of((half_rows, LANES)) & (len(lines) - 1)
    joined = lines[0]
    for q in range(1, len(lines)):
        joined = jnp.where(place == q, pltpu.roll(lines[q], q, 1), joined)
    answer = exact_dot(joined, matrix_ref[...])
    grid = (place == 0) & ((rows_of((half_rows, LANES)) & (step - 1)) == 0)
    parts = []
    for q in range(len(lines)):
        part = pltpu.roll(answer, LANES - q, 1) if q else answer
        parts.append(jnp.where(grid, part, 0.0))
    spreads = [jnp.concatenate(parts[2 * at : 2 * at + 2], axis=0) for at in range(slots)]

    for index in reversed(range(len(small))):
        _, _, red, black, _, _ = small[index]
        slots, odd, step = red.shape[0], odd_at(index), 1 << index
        if index < last:
            spreads = [
                spread_rows(field + pltpu.roll(field, step, 1), step, passing, at)
                for at, field in enumerate(fields)
            ]
        for at in range(slots):
            black[at, 0, body2, :] = black[at, 0, body2, :] + spreads[at]
        small_sweeps(index, False)
        fields = []
        for at in range(slots):
            r, b = red[at, 0, body2, :], black[at, 0, body2, :]
            fields += [jnp.where(odd, b, r), jnp.where(odd, r, b)]

    for at in range(count1):
        for start in range(2):
            rest1[at, pl.ds(start, rows2, stride=2), :] = fields[at]
    for at in range(count1):
        for e in range(2):
            black1[at, e, body1, :] = window(black1, at, e, rows1) + rest1[at]
    nx, ny, nz = out_ref.shape
    own = nx // 2
    part_slots = min(own // 2 + 3, count1)
    part_rows = min(ny // 2 + 16, rows1)
    slot0 = jnp.where(gx == 0, 0, count1 - part_slots)
    row0 = pl.multiple_of(jnp.clip(gy * (ny // 2) - 8, 0, rows1 - part_rows), 8)
    odds = fold_odds(part_rows)

    def up_total(ref, at, e, to_red):
        low = gx == 0 if at == 0 else False
        high = gx != 0 if at == part_slots - 1 else False
        return fold_total(ref, slot0 + at, e, row0, part_rows, low, high, odds, to_red)

    def up_half(target, other, sources, to_red):
        for at in range(part_slots):
            for e in range(2):
                source = sources[slot0 + at, e, pl.ds(row0, part_rows), :]
                value = share * (source + up_total(other, at, e, to_red))
                target[slot0 + at, e, pl.ds(pl.multiple_of(row0 + PAD, 8), part_rows), :] = value

    for _ in range(2):
        up_half(red1, black1, fr1, True)
        up_half(black1, red1, fb1, False)

    count, _, rows, _ = dark_ref.shape
    half = rows // 2
    odds = fold_odds(half)
    row = gy * (ny // 2) + (PAD - halo // 2)
    for at in range(count):
        if at < own:
            slot = gx * (own // 2) + at // 2
        else:
            slot = jnp.where(gx == 0, own // 2, own // 2 - (count - own) // 2) + (at - own) // 2
        for e in range(2):
            r, b = red1[slot, e, pl.ds(row, half), :], black1[slot, e, pl.ds(row, half), :]
            plane = jnp.where(odds[e], r, b) if at % 2 else jnp.where(odds[e], b, r)
            tall_ref[at, :, e * LANES : (e + 1) * LANES] = plane
    shape = (2 * LANES, 2 * LANES)
    z = lanes_of(shape)
    z = jnp.where(z < 2 * LANES - halo, z, z - 2 * LANES) + gz * nz
    line = rows_of(shape)
    line = jnp.where(line < LANES, 2 * line, 2 * (line - LANES) + 1)
    weight = jnp.where(line == lax.shift_right_arithmetic(z, 1), 1.0, 0.0)
    spread = pick_dot(tall_ref[...].reshape(count * half, 2 * LANES), weight)
    spread = spread.reshape(count, half, 2 * LANES)
    for at in range(count):
        for c in range(2):
            value = spread[at, :, c * LANES : (c + 1) * LANES]
            for start in range(2):
                work_ref[at, c, pl.ds(PAD + start, half, stride=2), :] = value
    body = slice(PAD, PAD + rows)
    for at in range(count):
        for c in range(2):
            work_ref[at, c, body, :] = work_ref[at, c, body, :] + dark_ref[at, c]
    odd = odd_of((rows, LANES))
    masks = block_mask((ny, nz), halo)
    ends = (gx == 0, gx == lax.axis_size("gx") - 1)
    beside_own = [*range(own), own, count - 1]

    def red_half(slots):
        for at in slots:
            totals = block_totals(work_ref, at, rows, own, odd, True, *ends)
            for c in range(2):
                red_ref[at, c, body, :] = gr_ref[at, c] + masks[c] * totals[c]

    red_half(range(count))
    for at in beside_own:
        totals = block_totals(red_ref, at, rows, own, odd, False, *ends)
        for c in range(2):
            work_ref[at, c, body, :] = gb_ref[at, c] + masks[c] * totals[c]
    red_half(beside_own)
    inner = slice(halo, halo + ny)
    odd_inner = odd_of((ny, nz))
    for at in range(own):
        total = block_totals(red_ref, at, rows, own, odd, False, *ends)[0]
        b = (gb_ref[at, 0] + masks[0] * total)[inner]
        r = red_ref[at, 0, PAD + halo : PAD + halo + ny, :]
        out_ref[2 * at] = jnp.where(odd_inner, b, r)
        out_ref[2 * at + 1] = jnp.where(odd_inner, r, b)


def vmem(number):
    return [pl.BlockSpec(memory_space=pltpu.VMEM)] * number


def struct(*shape):
    return jax.ShapeDtypeStruct(shape, jnp.float32)


def scratch(*shape):
    return pltpu.VMEM(shape, jnp.float32)


HALO = 8


def block_cycle(density):
    halo = HALO
    nx, ny, nz = density.shape
    count_x, count_y, count_z = (lax.axis_size(axis) for axis in ("gx", "gy", "gz"))
    whole = (nx * count_x, ny * count_y, nz * count_z)

    def params(mib):
        return pltpu.CompilerParams(vmem_limit_bytes=mib * 1024 * 1024)

    even = lax.axis_index("gy") % 2 == 0
    ya = lax.dynamic_slice_in_dim(density, jnp.where(even, ny - halo, 0), halo, 1)
    yb = lax.dynamic_slice_in_dim(density, jnp.where(even, 0, ny - halo), halo, 1)
    ya = lax.ppermute(ya, "gy", pairs(count_y, 0))
    yb = lax.ppermute(yb, ("gx", "gy"), inner_pairs(count_x, count_y))
    rows = ny + 2 * halo
    packs = -(-nx * halo // nz)
    za, zb = pl.pallas_call(
        functools.partial(pack_kernel, halo),
        out_shape=[struct(packs, rows, nz)] * 2,
        in_specs=vmem(3), out_specs=vmem(2), compiler_params=params(4),
    )(density, ya, yb)
    za = lax.ppermute(za, "gz", pairs(count_z, 0))
    zb = lax.ppermute(zb, "gz", pairs(count_z, 1) + [(0, count_z - 1), (count_z - 1, 0)])
    own, near = nx // 2, nx // 2 + 2
    send, face = pl.pallas_call(
        functools.partial(pre_kernel, halo),
        out_shape=[struct(near // 2, ny // 2, nz), struct(halo + 1, rows, LANES)],
        in_specs=vmem(5), out_specs=vmem(2), compiler_params=params(10),
        scratch_shapes=[scratch(own, ny, nz)] * 2
        + [scratch(own, 2, rows, LANES)] * 2
        + [scratch(near, 2, rows + 2 * PAD, LANES)] * 2
        + [scratch(near, ny, nz)],
    )(density, ya, yb, za, zb)
    planes = nx + halo
    slots = (planes // 2, 2, rows, LANES)
    padded = (planes // 2, 2, rows + 2 * PAD, LANES)
    first = [send]
    first.append(lax.ppermute(send, "gy", flips(count_y, 2)))
    first.append(lax.ppermute(send, "gz", flips(count_z, 2)))
    swaps = flips(count_y * count_z, 2 * count_z + 2)
    first.append(lax.ppermute(send, ("gy", "gz"), swaps))
    face = lax.ppermute(face, "gx", flips(count_x, 1))
    block = pl.pallas_call(
        stack_kernel, out_shape=struct(4, *send.shape),
        in_specs=vmem(4), out_specs=pl.BlockSpec(memory_space=pltpu.VMEM), compiler_params=params(2),
    )(*first)
    second = [
        block,
        lax.ppermute(block, "gx", flips(count_x, 1)),
        lax.ppermute(block, "gy", flips(count_y, 1)),
        lax.ppermute(block, ("gx", "gy"), flips(count_x * count_y, count_y + 1)),
    ]
    gr, gb, black = pl.pallas_call(
        functools.partial(field_kernel, halo),
        out_shape=[struct(*slots)] * 3,
        in_specs=vmem(7), out_specs=vmem(3), compiler_params=params(8),
        scratch_shapes=[scratch(*padded)] * 2,
        cost_estimate=pl.CostEstimate(flops=20_000_000, bytes_accessed=2_000_000, transcendentals=0),
    )(density, ya, yb, za, zb, face, block)
    second[3], gr, gb, black = lax.optimization_barrier((second[3], gr, gb, black))
    third = [lax.ppermute(blocks, "gz", flips(count_z, 1)) for blocks in second]
    count1, rows1, rows2 = whole[0] // 4, whole[1] // 2, whole[1] // 4
    room = [scratch(count1, 2, rows1, LANES)] * 2
    room += [scratch(count1, 2, rows1 + 2 * PAD, LANES)] * 2
    room += [scratch(count1, rows1, LANES), scratch(planes // 2, rows // 2, 2 * LANES)]
    room += [scratch(*padded)] * 2 + [scratch(count1 // 2, 1, rows2 + 2 * PAD, LANES)]
    for count in small_shapes(whole):
        room += [scratch(count, rows2, LANES)] * 2
        room += [scratch(count, 1, rows2 + 2 * PAD, LANES)] * 2
        room += [scratch(count, rows2, LANES)] * 2
    return pl.pallas_call(
        functools.partial(solve_kernel, halo),
        out_shape=struct(nx, ny, nz),
        in_specs=vmem(12), out_specs=pl.BlockSpec(memory_space=pltpu.VMEM),
        compiler_params=params(16), scratch_shapes=room,
    )(*second, *third, gr, gb, black, cycle_matrix(whole))


def fits_block_cycle(shape):
    nx, ny, nz = shape
    count_x, count_y, count_z = (lax.axis_size(axis) for axis in ("gx", "gy", "gz"))
    whole = (nx * count_x, ny * count_y, nz * count_z)
    coarsest = [size >> (LEVELS - 1) for size in whole]
    exact = all(c << (LEVELS - 1) == size for c, size in zip(coarsest, whole))
    return (
        exact and coarsest[0] == coarsest[1] == 1 and nz == LANES and ny == 2 * HALO
        and count_x == 2 and count_y == 4 and count_z == 4
    )


def on_device(density):
    if fits_block_cycle(density.shape):
        return block_cycle(density)
    top = 4
    return shared_cycle(density, 0, top)


def solution(mesh):
    return jax.shard_map(
        on_device,
        mesh=mesh,
        in_specs=(P("gx", "gy", "gz"),),
        out_specs=P("gx", "gy", "gz"),
        check_vma=False,
    )
```
